32 devices in a mesh: ka: 8 (over z, y), ga: 4 (over x, core).
Axes of the slice: x: 2, y: 2, z: 4, core: 2. Of those that a mesh axis runs over, the one named last changes fastest.
Arguments:
- x_dens: bfloat16 [32, 64, 1500], P('ka', None, 'ga'), may hold values from -6 to 6
- y_dens: bfloat16 [32, 64, 1500], P('ka', None, 'ga'), may hold values from -0.15625 to 0.15625
- p_dens: bfloat16 [32, 64, 1500], P('ka', None, 'ga'), may hold values from -1 to 1
- coulomb: float32 [1500], P('ga'), may hold values from 0.1 to 2
- screened: bfloat16 [16, 1500, 1500], P('ka', 'ga'), may hold values from -0.15625 to 0.15625
- pairs: int32 [128, 3], P('ka'), may hold values from 0 to 31, as said below
- q_slot: int32 [16], replicated, may hold values from 0 to 15, as said below
Outputs:
- blocks: float32 [128, 4096], P('ka')
- mirrored: float32 [32, 4096], P('ka')
The draws below stay inside these ranges and needn't reach their ends.
Inputs may be any that keep to these rules, and one draw needn't show every extreme that they name: `pairs`: column 0 of the rows held by index d of ka lies in d * 4 to (d + 1) * 4 - 1; column 1 is any k-point; column 2 is a momentum transfer below 16. Among one index's 16 rows at most 2 have a second k-point held by one same index, and this is reached; at most 2 have q_slot[q] // 2 equal to one same value, and this is reached. `q_slot`: A permutation of the slots; slot s of screened is held by index s // 2 of ka.
All inputs are finite; a program needn't handle non-finite values.
Results may differ from the reference program's by a relative error of at most 0.0014.
Values may be sent and summed in bfloat16 or wider, within the bound.
A program may use at most 192 MiB of HBM per device.

```python
import math
import jax
import jax.numpy as jnp
from jax import lax

NT = 64
NG = 1500
K_DEV = 4
PAIR_DEV = 16
QS = 2
CAPQ = 2
CAPK = 2
K_ALL = 32
NQ = 16
PAIRS = 128
N_KA = 8


def shared_slots(key):
    return jax.random.permutation(jax.random.fold_in(key, 7), NQ).astype(jnp.int32)


def draw_q_slot(key, part):
    return shared_slots(key)


def draw_pairs(key, part):
    slot_of = shared_slots(key)
    inverse = jnp.zeros((NQ,), jnp.int32).at[slot_of].set(jnp.arange(NQ, dtype=jnp.int32))
    popular = jax.random.permutation(jax.random.fold_in(key, 9), N_KA) < max(1, N_KA // 8)

    def one_block(index):
        block_key = jax.random.fold_in(key, 100 + index)
        keys = jax.random.split(block_key, 7)
        firsts = index * K_DEV + jax.random.randint(keys[0], (PAIR_DEV,), 0, K_DEV)
        k_owners = jax.random.permutation(keys[1], N_KA)[jnp.arange(PAIR_DEV) // CAPK]
        k_owners = k_owners[jax.random.permutation(keys[2], PAIR_DEV)]
        seconds = k_owners * K_DEV + jax.random.randint(keys[3], (PAIR_DEV,), 0, K_DEV)
        scores = jax.random.randint(keys[4], (N_KA,), 0, 1000) + 800 * popular.astype(jnp.int32)
        scores = scores * N_KA + jnp.arange(N_KA, dtype=jnp.int32)
        ranking = jnp.argsort(-scores, stable=True).astype(jnp.int32)
        q_owners = ranking[jnp.arange(PAIR_DEV) // CAPQ]
        q_owners = q_owners[jax.random.permutation(keys[5], PAIR_DEV)]
        slots = q_owners * QS + jax.random.randint(keys[6], (PAIR_DEV,), 0, QS)
        transfers = inverse[slots]
        return jnp.stack([firsts, seconds, transfers], axis=1).astype(jnp.int32)
    return jax.vmap(one_block)(jnp.arange(N_KA, dtype=jnp.int32)).reshape(PAIRS, 3)


def block_levels(stream_key, dims, cuts, smallest, largest):
    level = 1.0
    for dim, shards_of in cuts:
        draws = jax.random.uniform(jax.random.fold_in(jax.random.fold_in(stream_key, 6), dim), (shards_of,), jnp.float32, smallest / len(cuts), largest / len(cuts))
        level = level * jnp.repeat(jnp.exp(draws), dims[dim] // shards_of).reshape((-1,) + (1,) * (len(dims) - 1 - dim))
    return level


def gaussian(own_key, shape, scale, reach, pieces=(), held_as=jnp.bfloat16):
    entries = jax.random.normal(own_key, shape, jnp.float32) * scale
    if len(pieces) > 0:
        entries = block_levels(own_key, shape, pieces, -0.22, 0.18) * entries
    return jnp.clip(entries, min=-reach, max=reach).astype(held_as)


def setup_inputs(seed: int = 0) -> dict:
    arg_keys = jax.random.split(jax.random.key(seed), 8)
    x_dens = gaussian(arg_keys[0], (K_ALL, NT, NG), 1.0, 6.0, ((0, 8), (2, 4)))
    y_dens = gaussian(arg_keys[1], (K_ALL, NT, NG), NG ** -0.5, 0.15625, ((0, 8), (2, 4)))
    p_dens = gaussian(arg_keys[2], (K_ALL, NT, NG), 0.16, 1.0, ((0, 8), (2, 4)))
    coulomb = jnp.clip(jnp.exp(math.log(2.0) - 2.9957323 * jax.random.uniform(arg_keys[3], (NG,), jnp.float32) ** block_levels(arg_keys[3], (NG,), ((0, 4),), -0.2, 0.2)), 0.1, 2.0)
    screened = gaussian(arg_keys[4], (NQ, NG, NG), NG ** -0.5, 0.15625, ((0, 8), (1, 4)))
    pairs = draw_pairs(jax.random.fold_in(arg_keys[7], 71), 0)
    q_slot = draw_q_slot(jax.random.fold_in(arg_keys[7], 71), 0)
    return {"x_dens": x_dens, "y_dens": y_dens, "p_dens": p_dens, "coulomb": coulomb, "screened": screened, "pairs": pairs, "q_slot": q_slot}


def reference(x_dens, y_dens, p_dens, coulomb, screened, pairs, q_slot):
    def one_pair(entry):
        k_index = entry[0]
        partner = entry[1]
        q_index = entry[2]
        w_matrix = screened[q_slot[q_index]]
        half_rows = jnp.dot(x_dens[k_index], w_matrix, preferred_element_type=jnp.float32).astype(jnp.bfloat16)
        direct = jnp.dot(half_rows, y_dens[partner].T, preferred_element_type=jnp.float32)
        weighted = p_dens[k_index].astype(jnp.float32) * coulomb[None, :]
        exchange_term = jnp.dot(weighted, p_dens[partner].astype(jnp.float32).T, precision=lax.Precision.HIGHEST)
        return 2.0 * exchange_term - direct

    kernel_blocks = lax.map(one_pair, pairs)
    flipped = jnp.transpose(kernel_blocks, (0, 2, 1)).reshape(PAIRS, NT * NT)
    mirrored = jax.ops.segment_sum(flipped, pairs[:, 1].astype(jnp.int32), num_segments=K_DEV * N_KA)
    return kernel_blocks.reshape(PAIRS, NT * NT), mirrored
```

```python
import functools
import jax
import jax.numpy as jnp
from jax import lax
from jax.experimental import pallas as pl
from jax.experimental.pallas import tpu as pltpu
from jax.sharding import PartitionSpec as P

CAPQ = 2
F32 = jnp.float32
BF16 = jnp.bfloat16
I32 = jnp.int32
VM = pl.BlockSpec(memory_space=pltpu.VMEM)
SM = pl.BlockSpec(memory_space=pltpu.SMEM)
HB = pl.BlockSpec(memory_space=pl.ANY)
LIMIT = 66000000
DIMS = (((1,), (1,)), ((), ()))


def start(c):
    c.start()


def sent(c):
    c.wait_send()


def remote(src, dst, ss, rs, to):
    return pltpu.make_async_remote_copy(
        src_ref=src,
        dst_ref=dst,
        send_sem=ss,
        recv_sem=rs,
        device_id=to,
        device_id_type=pl.DeviceIdType.MESH,
    )


def greet(n):
    barrier = pltpu.get_barrier_semaphore()
    me = lax.axis_index("ka")
    g = lax.axis_index("ga")
    n_ga = lax.axis_size("ga")

    def hello(to):
        pl.semaphore_signal(barrier, inc=1, device_id=to, device_id_type=pl.DeviceIdType.MESH)

    lax.fori_loop(1, n, lambda i, c: (hello({"ka": lax.rem(me + i, n)}), c)[1], 0)
    for i in range(1, n_ga):
        hello({"ga": lax.rem(g + i, n_ga)})
    pl.semaphore_wait(barrier, n - 1 + n_ga - 1)


class Gather:
    def __init__(self, n, src, out, send, recv, cut):
        self.n, self.nz = n, n // 2
        self.me = lax.axis_index("ka")
        self.z, self.y = self.me // 2, self.me % 2
        self.src, self.out, self.send, self.recv = src, out, send, recv
        self.size = src.shape[0]
        self.cut = cut

    def copy(self, zz, yy, k, way, own=False):
        at = (zz * 2 + yy) * self.size + k
        block = self.out.at[at]
        if way == 2:
            target = self.z * 2 + 1 - self.y
        else:
            target = (self.z + (1 if way == 0 else -1)) * 2 + self.y
        return remote(
            self.src.at[k] if own else block,
            block,
            self.send.at[way * self.n * self.size + at],
            self.recv.at[at],
            {"ka": target},
        )

    def chain(self, zz, yy, k, act, ways=(0, 1), own=False):
        for way in ways:
            free = self.z < self.nz - 1 if way == 0 else self.z > 0

            @pl.when(free)
            def _(way=way):
                act(self.copy(zz, yy, k, way, own))

    def early(self):
        return range(self.cut, self.size)

    def first(self):
        for k in self.early():
            self.copy(self.z, self.y, k, 2, True).start()
        for k in range(self.size):
            self.chain(self.z, self.y, k, start, own=True)
        for k in range(self.cut):
            self.copy(self.z, self.y, k, 2, True).start()
        self.out[pl.ds(self.me * self.size, self.size)] = self.src[...]

    def second(self):
        for k in self.early():
            self.copy(self.z, 1 - self.y, k, 2).wait_recv()
            self.chain(self.z, 1 - self.y, k, start)

    def sides(self, h, act):
        for way in (0, 1):
            zz = self.z - h if way == 0 else self.z + h
            there = zz >= 0 if way == 0 else zz < self.nz

            @pl.when(there)
            def _(zz=zz, way=way):
                act(zz, way)

    def hop(self, h):
        def one(k, yy, zz, way):
            self.copy(zz, yy, k, 2).wait_recv()
            self.chain(zz, yy, k, start, (way,))

        for k in range(self.size):

            def own(zz, way, k=k):
                one(k, self.y, zz, way)
                if k < self.cut:
                    self.copy(zz, self.y, k, 2).start()

            self.sides(h, own)
        for k in self.early():
            self.sides(h, lambda zz, way, k=k: one(k, 1 - self.y, zz, way))

    def finish(self):
        for k in range(self.size):
            self.chain(self.z, self.y, k, sent, own=True)
            self.copy(self.z, self.y, k, 2, True).wait_send()
        for k in self.early():
            self.chain(self.z, 1 - self.y, k, sent)
        for k in range(self.cut):
            self.copy(self.z, 1 - self.y, k, 2).wait_recv()

        def tail(h, carry):
            def side(zz, way):
                for k in range(self.size):
                    self.chain(zz, self.y, k, sent, (way,))
                for k in self.early():
                    self.chain(zz, 1 - self.y, k, sent, (way,))
                for k in range(self.cut):
                    self.copy(zz, self.y, k, 2).wait_send()
                    self.copy(zz, 1 - self.y, k, 2).wait_recv()

            self.sides(h, side)
            return carry

        lax.fori_loop(1, self.nz, tail, 0)


class Pick:
    def __init__(self, n, src, col, out, got, tab, send, recv, ps, pr):
        self.n, self.nz = n, n // 2
        self.me = lax.axis_index("ka")
        self.z, self.y = self.me // 2, self.me % 2
        self.src, self.col, self.out, self.got, self.tab = src, col, out, got, tab
        self.send, self.recv, self.ps, self.pr = send, recv, ps, pr
        self.size = src.shape[0]

    def copy(self, zz, k, way, own=False):
        at = zz * self.size + k
        target = (self.z + (1 if way == 0 else -1)) * 2 + self.y
        return remote(
            self.src.at[k] if own else self.col.at[at],
            self.col.at[at],
            self.send.at[way * self.nz * self.size + at],
            self.recv.at[at],
            {"ka": target},
        )

    def chain(self, zz, k, act, ways=(0, 1), own=False):
        for way in ways:
            free = self.z < self.nz - 1 if way == 0 else self.z > 0

            @pl.when(free)
            def _(way=way):
                act(self.copy(zz, k, way, own))

    def sides(self, h, act):
        for way in (0, 1):
            zz = self.z - h if way == 0 else self.z + h
            there = zz >= 0 if way == 0 else zz < self.nz

            @pl.when(there)
            def _(zz=zz, way=way):
                act(zz, way)

    def first(self):
        for k in range(self.size):
            self.chain(self.z, k, start, own=True)
        self.col[pl.ds(self.z * self.size, self.size)] = self.src[...]

    def hop(self, h):
        for k in range(self.size):

            def one(zz, way, k=k):
                self.copy(zz, k, way).wait_recv()
                self.chain(zz, k, start, (way,))

            self.sides(h, one)

    def chosen(self, zz, owner, r):
        which = self.tab[zz * 2 + self.y, owner * CAPQ + r]
        v = self.col[zz * self.size]
        for k in range(1, self.size):
            v = jnp.where(which == k, self.col[zz * self.size + k], v)
        return v

    def across(self, zz):
        rows = pl.ds(zz * CAPQ, CAPQ)
        return remote(
            self.out.at[rows],
            self.got.at[rows],
            self.ps.at[zz],
            self.pr.at[zz],
            {"ka": self.z * 2 + 1 - self.y},
        )

    def pass_on(self, zz):
        for r in range(CAPQ):
            self.out[zz * CAPQ + r] = self.chosen(zz, self.z * 2 + 1 - self.y, r)
        self.across(zz).start()

    def finish(self):
        for k in range(self.size):
            self.chain(self.z, k, sent, own=True)
        self.across(self.z).wait_send()

        def tail(h, carry):
            def side(zz, way):
                for k in range(self.size):
                    self.chain(zz, k, sent, (way,))
                self.across(zz).wait_send()

            self.sides(h, side)
            return carry

        lax.fori_loop(1, self.nz, tail, 0)


class Reduce:
    def __init__(self, part, out, recv1, tsend, recv2, s1, r1, s2, r2, per):
        self.g = lax.axis_index("ga")
        self.x, self.c = self.g // 2, self.g % 2
        self.part, self.out = part, out
        self.recv1, self.tsend, self.recv2 = recv1, tsend, recv2
        self.s1, self.r1, self.s2, self.r2, self.per = s1, r1, s2, r2, per

    def rows(self, i):
        return pl.ds(i * self.per, self.per)

    def one(self, t, i):
        xx = self.x if t else 1 - self.x
        return remote(
            self.part.at[xx * 2 + 1 - self.c, self.rows(i)],
            self.recv1.at[xx, self.rows(i)],
            self.s1.at[i * 2 + t],
            self.r1.at[i * 2 + t],
            {"ga": self.x * 2 + 1 - self.c},
        )

    def two(self, i):
        return remote(
            self.tsend.at[self.rows(i)],
            self.recv2.at[self.rows(i)],
            self.s2.at[i],
            self.r2.at[i],
            {"ga": (1 - self.x) * 2 + self.c},
        )

    def sum_one(self, xx, i):
        v = self.part[xx * 2 + self.c, self.rows(i)].astype(F32)
        return v + self.recv1[xx, self.rows(i)].astype(F32)

    def begin(self, i):
        self.one(0, i).start()
        self.one(1, i).start()

    def middle(self, i):
        self.one(0, i).wait_recv()
        self.tsend[self.rows(i)] = self.sum_one(1 - self.x, i).astype(self.tsend.dtype)
        self.two(i).start()

    def end(self, i):
        self.one(1, i).wait_recv()
        v = self.sum_one(self.x, i)
        self.two(i).wait_recv()
        v = v + self.recv2[self.rows(i)].astype(F32)
        self.out[self.rows(i)] = v.astype(self.out.dtype)
        self.one(0, i).wait_send()
        self.one(1, i).wait_send()
        self.two(i).wait_send()


def make_row(n, q_slots, per_dev, pairs_ref, qs_ref, tab, at_ref, kept):
    me = lax.axis_index("ka")
    rows = pairs_ref.shape[1]
    slots = n * CAPQ
    owners = []
    for j in range(rows):
        slot = qs_ref[pairs_ref[2, j]]
        owner = slot // q_slots
        rank = jnp.int32(0)
        for o in owners:
            rank = rank + jnp.where(o == owner, 1, 0)
        owners.append(owner)
        at_ref[j] = owner * CAPQ + rank
        kept[0, j] = pairs_ref[0, j] - me * per_dev
        kept[1, j] = slot - owner * q_slots
        kept[2, j] = pairs_ref[1, j]

    def one(s, carry):
        found = [jnp.int32(0), jnp.int32(0), jnp.int32(-1)]
        for j in range(rows):
            hit = at_ref[j] == s
            for i in range(3):
                found[i] = jnp.where(hit, kept[i, j], found[i])
        for i in range(3):
            tab[me, i * slots + s] = found[i]
        return carry

    lax.fori_loop(0, slots, one, 0)


def kernel(n, pairs_ref, qs_ref, x_ref, y_ref, p_ref, v_ref, w_hbm, blocks_ref, mirr_ref,
           tab, at_ref, kept, wt, w_ref, x_col, x_out, x_got, y_all, p_all, part, half,
           recv1, tsend, recv2, part2, own, q1, qt, q2, second, outbox, inbox, lines, turned, flat,
           ws, ts, tr, xs, xr, xps, xpr, ys, yr, ps, pr, s1, r1, s2, r2, t1, u1, t2, u2,
           as_, ar, gs, gr):
    per_dev, nt, width = x_ref.shape
    rows = pairs_ref.shape[1]
    q_slots = w_ref.shape[0]
    nz = n // 2
    slots = n * CAPQ
    n_ga = part.shape[0]
    me = lax.axis_index("ka")
    g = lax.axis_index("ga")
    z, y = me // 2, me % 2
    fetch = pltpu.make_async_copy(w_hbm, wt, ws)
    fetch.start()
    greet(n)
    xg = Pick(n, x_ref, x_col, x_out, x_got, tab, xs, xr, xps, xpr)
    yg = Gather(n, y_ref, y_all, ys, yr, per_dev - 1)
    pg = Gather(n, p_ref, p_all, ps, pr, per_dev - 1)
    xg.first()
    make_row(n, q_slots, per_dev, pairs_ref, qs_ref, tab, at_ref, kept)

    def row(i, whose):
        return remote(
            tab.at[whose], tab.at[whose], ts.at[i], tr.at[whose], {"ka": lax.rem(me + i, n)}
        )

    lax.fori_loop(1, n, lambda i, c: (row(i, me).start(), c)[1], 0)
    xg.pass_on(z)
    fetch.wait()
    for s in range(q_slots):
        w_ref[s] = wt[:, s, :]
    red = Reduce(part, half, recv1, tsend, recv2, s1, r1, s2, r2, 2 * CAPQ)

    def multiply(v, a, r):
        w = tab[a, slots + me * CAPQ + r]
        v = jnp.dot(v, w_ref[w], preferred_element_type=F32)
        for i in range(n_ga):
            part[i, a * CAPQ + r] = v[:, i * width : (i + 1) * width].astype(part.dtype)

    def piece(zz):
        for r in range(CAPQ):
            multiply(xg.chosen(zz, me, r), zz * 2 + y, r)
        xg.across(zz).wait_recv()
        for r in range(CAPQ):
            multiply(x_got[zz * CAPQ + r], zz * 2 + 1 - y, r)
        red.begin(zz)

    xg.hop(1)
    yg.first()
    lax.fori_loop(
        1, n, lambda i, c: (row(i, lax.rem(me + n - i, n)).wait_recv(), c)[1], 0
    )
    xg.sides(1, lambda zz, way: xg.pass_on(zz))
    piece(z)
    yg.second()

    def stage(h, carry):
        xg.hop(h)
        xg.sides(h, lambda zz, way: xg.pass_on(zz))

        @pl.when(h == 2)
        def _():
            pg.first()
            red.middle(z)

        xg.sides(h - 1, lambda zz, way: piece(zz))

        @pl.when(h > 2)
        def _():
            xg.sides(h - 2, lambda zz, way: red.middle(zz))

        return carry

    lax.fori_loop(2, nz, stage, 0)
    pg.second()
    xg.sides(nz - 1, lambda zz, way: piece(zz))
    xg.sides(nz - 2, lambda zz, way: red.middle(zz))
    yg.hop(1)
    pg.hop(1)
    xg.sides(nz - 1, lambda zz, way: red.middle(zz))

    def body(h, carry):
        yg.hop(h)
        pg.hop(h)
        return carry

    lax.fori_loop(2, nz, body, 0)
    xg.finish()
    lax.fori_loop(0, nz, lambda i, c: (red.end(i), c)[1], 0)
    yg.finish()
    pg.finish()
    lax.fori_loop(1, n, lambda i, c: (row(i, me).wait_send(), c)[1], 0)

    quarter = nt // n_ga
    weight = v_ref[...].reshape(1, width)

    def source(a, carry):
        both = []
        for r in range(CAPQ):
            k = tab[a, me * CAPQ + r] + a * per_dev
            k2 = jnp.maximum(tab[a, 2 * slots + me * CAPQ + r], 0)
            direct = lax.dot_general(half[a * CAPQ + r], y_all[k2], DIMS, preferred_element_type=F32)
            weighted = p_all[k].astype(F32) * weight
            high = weighted.astype(BF16)
            low = (weighted - high.astype(F32)).astype(BF16)
            other = p_all[k2]
            term = lax.dot_general(high, other, DIMS, preferred_element_type=F32)
            term += lax.dot_general(low, other, DIMS, preferred_element_type=F32)
            both.append(2.0 * term - direct)
        v = jnp.concatenate(both, axis=1)
        for i in range(n_ga):
            part2[i, a] = v[i * quarter : (i + 1) * quarter]
        return carry

    lax.fori_loop(0, n, source, 0)
    end = Reduce(part2, own, q1, qt, q2, t1, u1, t2, u2, n)
    end.begin(0)
    shape = own.shape[1:]
    left = lax.broadcasted_iota(I32, shape, 1) < nt

    def seconds(a, carry):
        at = 2 * slots + me * CAPQ
        second[a] = jnp.where(left, tab[a, at], tab[a, at + 1])
        return carry

    lax.fori_loop(0, n, seconds, 0)
    end.middle(0)
    end.end(0)
    doubles = per_dev // 2

    def fill(b, carry):
        outbox[b, 0] = own[b]

        def add(a, sums):
            out = []
            for i in range(per_dev):
                out.append(sums[i] + jnp.where(second[a] == b * per_dev + i, own[a], 0.0))
            return tuple(out)

        sums = lax.fori_loop(0, n, add, tuple(jnp.zeros(shape, F32) for _ in range(per_dev)))
        sums = [v[:, :nt] + v[:, nt:] for v in sums]
        for i in range(doubles):
            outbox[b, 1 + i] = jnp.concatenate([sums[i], sums[i + doubles]], axis=1)
        return carry

    lax.fori_loop(0, n, fill, 0)

    def cross(i, whose):
        to = lax.rem(me + i, n)
        return remote(outbox.at[to], inbox.at[whose], as_.at[i], ar.at[whose], {"ka": to})

    lax.fori_loop(1, n, lambda i, c: (cross(i, me).start(), c)[1], 0)
    inbox[me] = outbox[me]
    lax.fori_loop(1, n, lambda i, c: (cross(i, lax.rem(me + n - i, n)).wait_recv(), c)[1], 0)
    lax.fori_loop(1, n, lambda i, c: (cross(i, me).wait_send(), c)[1], 0)

    sub = quarter // 2
    for j in range(rows):
        at = at_ref[j]
        o, r = at // CAPQ, at % CAPQ
        even = inbox[o, 0, pl.ds(0, sub, stride=2)]
        odd = inbox[o, 0, pl.ds(1, sub, stride=2)]
        zero = jnp.concatenate([even[:, :nt], odd[:, :nt]], axis=1)
        one = jnp.concatenate([even[:, nt:], odd[:, nt:]], axis=1)
        lines[g, pl.ds(j * sub, sub)] = jnp.where(r == 0, zero, one)
    base = rows * sub
    for i in range(doubles):
        total = lax.fori_loop(
            1, n, lambda o, t, i=i: t + inbox[o, 1 + i], inbox[0, 1 + i]
        )
        lines[g, pl.ds(base + i * quarter, quarter)] = total
    x, c = g // 2, g % 2
    mate, far = x * 2 + 1 - c, (1 - x) * 2 + c

    def spread(i, whose, to):
        return remote(lines.at[whose], lines.at[whose], gs.at[i], gr.at[i], {"ga": to})

    spread(0, g, far).start()
    spread(1, g, mate).start()
    spread(0, far, far).wait_recv()
    spread(2, far, mate).start()
    spread(1, mate, mate).wait_recv()
    spread(2, (1 - x) * 2 + 1 - c, mate).wait_recv()
    spread(0, g, far).wait_send()
    spread(1, g, mate).wait_send()
    spread(2, far, mate).wait_send()

    lanes = 2 * nt
    for q in range(n_ga):
        for t in range(sub):
            blocks_ref[:, (q * sub + t) * lanes : (q * sub + t + 1) * lanes] = lines[
                q, pl.ds(t, rows, stride=sub)
            ]
    for i in range(doubles):
        whole = jnp.concatenate(
            [lines[q, pl.ds(base + i * quarter, quarter)] for q in range(n_ga)], axis=0
        )
        turned[...] = whole.T
        even = turned[pl.ds(0, nt, stride=2)]
        odd = turned[pl.ds(1, nt, stride=2)]
        both = jnp.concatenate([even, odd], axis=1)
        flat[pl.ds(i * nt // 2, nt // 2)] = both[: nt // 2]
        flat[pl.ds((i + doubles) * nt // 2, nt // 2)] = both[nt // 2 :]
    for t in range(nt // 2):
        mirr_ref[:, t * lanes : (t + 1) * lanes] = flat[pl.ds(t, per_dev, stride=nt // 2)]


def per_device(x_dens, y_dens, p_dens, coulomb, screened, pairs, q_slot):
    n = lax.axis_size("ka")
    n_ga = lax.axis_size("ga")
    per_dev, nt, g = x_dens.shape
    q_slots = screened.shape[0]
    rows = pairs.shape[0]
    slots = n * CAPQ
    nz = n // 2
    shape = jax.ShapeDtypeStruct
    wide = F32 if slots * nt <= 2048 else BF16
    quarter = nt // n_ga
    each = (quarter, CAPQ * nt)
    line = (n,) + each
    dma = lambda m: pltpu.SemaphoreType.DMA((m,))
    row_len = -(-3 * slots // 128) * 128
    k_all = n * per_dev
    blocks, mirrored = pl.pallas_call(
        functools.partial(kernel, n),
        out_shape=[shape((rows, nt * nt), F32), shape((per_dev, nt * nt), F32)],
        in_specs=[SM, SM, VM, VM, VM, VM, HB],
        out_specs=[VM, VM],
        scratch_shapes=[
            pltpu.SMEM((n, row_len), I32),
            pltpu.SMEM((rows,), I32),
            pltpu.SMEM((3, rows), I32),
            pltpu.VMEM((g, q_slots, screened.shape[2]), BF16),
            pltpu.VMEM((q_slots, g, screened.shape[2]), BF16),
            pltpu.VMEM((nz * per_dev, nt, g), BF16),
            pltpu.VMEM((nz * CAPQ, nt, g), BF16),
            pltpu.VMEM((nz * CAPQ, nt, g), BF16),
            pltpu.VMEM((k_all, nt, g), BF16),
            pltpu.VMEM((k_all, nt, g), BF16),
            pltpu.VMEM((n_ga, slots, nt, g), wide),
            pltpu.VMEM((slots, nt, g), BF16),
            pltpu.VMEM((2, slots, nt, g), wide),
            pltpu.VMEM((slots, nt, g), BF16),
            pltpu.VMEM((slots, nt, g), BF16),
            pltpu.VMEM((n_ga,) + line, F32),
            pltpu.VMEM(line, F32),
            pltpu.VMEM((2,) + line, F32),
            pltpu.VMEM(line, F32),
            pltpu.VMEM(line, F32),
            pltpu.VMEM(line, I32),
            pltpu.VMEM((n, 1 + per_dev // 2) + each, F32),
            pltpu.VMEM((n, 1 + per_dev // 2) + each, F32),
            pltpu.VMEM((n_ga, rows * quarter // 2 + per_dev // 2 * quarter, CAPQ * nt), F32),
            pltpu.VMEM((2 * nt, nt), F32),
            pltpu.VMEM((per_dev * nt // 2, 2 * nt), F32),
            pltpu.SemaphoreType.DMA,
            dma(n), dma(n),
            dma(2 * nz * per_dev), dma(nz * per_dev),
            dma(nz), dma(nz),
            dma(3 * k_all), dma(k_all),
            dma(3 * k_all), dma(k_all),
            dma(2 * nz), dma(2 * nz), dma(nz), dma(nz),
            dma(2), dma(2), dma(1), dma(1),
            dma(n), dma(n),
            dma(3), dma(3),
        ],
        compiler_params=pltpu.CompilerParams(
            collective_id=0, has_side_effects=True, vmem_limit_bytes=LIMIT
        ),
        name="window",
    )(pairs.T, q_slot, x_dens, y_dens, p_dens, coulomb, screened.transpose(1, 0, 2))
    return (blocks, mirrored)


def solution(mesh):
    in_specs = (
        P("ka", None, "ga"),
        P("ka", None, "ga"),
        P("ka", None, "ga"),
        P("ga"),
        P("ka", "ga", None),
        P("ka", None),
        P(),
    )
    out_specs = (P("ka", None), P("ka", None))
    return jax.shard_map(
        per_device, mesh=mesh, in_specs=in_specs, out_specs=out_specs, check_vma=False
    )
```

```python
import functools
import jax
import jax.numpy as jnp
from jax import lax
from jax.experimental import pallas as pl
from jax.experimental.pallas import tpu as pltpu
from jax.sharding import PartitionSpec as P

CAPQ = 2
F32 = jnp.float32
BF16 = jnp.bfloat16
I32 = jnp.int32
VM = pl.BlockSpec(memory_space=pltpu.VMEM)
SM = pl.BlockSpec(memory_space=pltpu.SMEM)
HB = pl.BlockSpec(memory_space=pl.ANY)
LIMIT = 66000000
DIMS = (((1,), (1,)), ((), ()))


def start(c):
    c.start()


def sent(c):
    c.wait_send()


def remote(src, dst, ss, rs, to):
    return pltpu.make_async_remote_copy(
        src_ref=src,
        dst_ref=dst,
        send_sem=ss,
        recv_sem=rs,
        device_id=to,
        device_id_type=pl.DeviceIdType.MESH,
    )


def greet(n):
    barrier = pltpu.get_barrier_semaphore()
    me = lax.axis_index("ka")
    g = lax.axis_index("ga")
    n_ga = lax.axis_size("ga")

    def hello(to):
        pl.semaphore_signal(barrier, inc=1, device_id=to, device_id_type=pl.DeviceIdType.MESH)

    lax.fori_loop(1, n, lambda i, c: (hello({"ka": lax.rem(me + i, n)}), c)[1], 0)
    for i in range(1, n_ga):
        hello({"ga": lax.rem(g + i, n_ga)})
    pl.semaphore_wait(barrier, n - 1 + n_ga - 1)


class Gather:
    def __init__(self, n, src, out, send, recv, cut):
        self.n, self.nz = n, n // 2
        self.me = lax.axis_index("ka")
        self.z, self.y = self.me // 2, self.me % 2
        self.src, self.out, self.send, self.recv = src, out, send, recv
        self.size = src.shape[0]
        self.cut = cut

    def copy(self, zz, yy, k, way, own=False):
        at = (zz * 2 + yy) * self.size + k
        block = self.out.at[at]
        if way == 2:
            target = self.z * 2 + 1 - self.y
        else:
            target = (self.z + (1 if way == 0 else -1)) * 2 + self.y
        return remote(
            self.src.at[k] if own else block,
            block,
            self.send.at[way * self.n * self.size + at],
            self.recv.at[at],
            {"ka": target},
        )

    def chain(self, zz, yy, k, act, ways=(0, 1), own=False):
        for way in ways:
            free = self.z < self.nz - 1 if way == 0 else self.z > 0

            @pl.when(free)
            def _(way=way):
                act(self.copy(zz, yy, k, way, own))

    def early(self):
        return range(self.cut, self.size)

    def first(self):
        for k in self.early():
            self.copy(self.z, self.y, k, 2, True).start()
        for k in range(self.size):
            self.chain(self.z, self.y, k, start, own=True)

    def late(self):
        for k in range(self.cut):
            self.copy(self.z, self.y, k, 2, True).start()
        self.out[pl.ds(self.me * self.size, self.size)] = self.src[...]

    def second(self):
        for k in self.early():
            self.copy(self.z, 1 - self.y, k, 2).wait_recv()
            self.chain(self.z, 1 - self.y, k, start)

    def sides(self, h, act):
        for way in (0, 1):
            zz = self.z - h if way == 0 else self.z + h
            there = zz >= 0 if way == 0 else zz < self.nz

            @pl.when(there)
            def _(zz=zz, way=way):
                act(zz, way)

    def hop(self, h):
        def one(k, yy, zz, way):
            self.copy(zz, yy, k, 2).wait_recv()
            self.chain(zz, yy, k, start, (way,))

        for k in range(self.size):

            def own(zz, way, k=k):
                one(k, self.y, zz, way)
                if k < self.cut:
                    self.copy(zz, self.y, k, 2).start()

            self.sides(h, own)
        for k in self.early():
            self.sides(h, lambda zz, way, k=k: one(k, 1 - self.y, zz, way))

    def finish(self):
        for k in range(self.size):
            self.chain(self.z, self.y, k, sent, own=True)
            self.copy(self.z, self.y, k, 2, True).wait_send()
        for k in self.early():
            self.chain(self.z, 1 - self.y, k, sent)
        for k in range(self.cut):
            self.copy(self.z, 1 - self.y, k, 2).wait_recv()

        def tail(h, carry):
            def side(zz, way):
                for k in range(self.size):
                    self.chain(zz, self.y, k, sent, (way,))
                for k in self.early():
                    self.chain(zz, 1 - self.y, k, sent, (way,))
                for k in range(self.cut):
                    self.copy(zz, self.y, k, 2).wait_send()
                    self.copy(zz, 1 - self.y, k, 2).wait_recv()

            self.sides(h, side)
            return carry

        lax.fori_loop(1, self.nz, tail, 0)


class Hub(Gather):
    def __init__(self, n, src, out, send, recv):
        super().__init__(n, src, out, send, recv, src.shape[0])
        self.inner = jnp.logical_and(self.z >= 1, self.z <= self.nz - 2)
        self.edged = jnp.logical_or(self.z == 1, self.z == self.nz - 2)
        self.edge = jnp.where(self.z == 1, 0, self.nz - 1)

    def chain(self, zz, yy, k, act, ways=(0, 1), own=False):
        for way in ways:
            free = self.z <= self.nz - 3 if way == 0 else self.z >= 2

            @pl.when(free)
            def _(way=way):
                act(self.copy(zz, yy, k, way, own))

    def first(self):
        for k in range(self.size):
            self.chain(self.z, self.y, k, start, own=True)

        @pl.when(self.inner)
        def _():
            for k in range(self.size):
                self.copy(self.z, self.y, k, 2, True).start()

        self.out[pl.ds(self.me * self.size, self.size)] = self.src[...]

    def hop(self, h):
        def own(zz, way):
            last = jnp.logical_and(self.edged, zz == self.edge)
            for k in range(self.size):
                self.copy(zz, self.y, k, 2).wait_recv()
                self.chain(zz, self.y, k, start, (way,))

                @pl.when(last)
                def _(k=k):
                    self.copy(zz, self.y, k, 2).start()

        @pl.when(self.inner)
        def _():
            self.sides(h, own)

    def finish(self):
        for k in range(self.size):
            self.chain(self.z, self.y, k, sent, own=True)

        @pl.when(self.inner)
        def _():
            for k in range(self.size):
                self.copy(self.z, self.y, k, 2, True).wait_send()
                self.copy(self.z, 1 - self.y, k, 2).wait_recv()

            @pl.when(self.edged)
            def _():
                for k in range(self.size):
                    self.copy(self.edge, self.y, k, 2).wait_send()
                    self.copy(self.edge, 1 - self.y, k, 2).wait_recv()

            def tail(h, carry):
                def side(zz, way):
                    for k in range(self.size):
                        self.chain(zz, self.y, k, sent, (way,))

                self.sides(h, side)
                return carry

            lax.fori_loop(1, self.nz, tail, 0)


class Pick:
    def __init__(self, n, src, col, out, got, tab, send, recv, ps, pr):
        self.n, self.nz = n, n // 2
        self.me = lax.axis_index("ka")
        self.z, self.y = self.me // 2, self.me % 2
        self.src, self.col, self.out, self.got, self.tab = src, col, out, got, tab
        self.send, self.recv, self.ps, self.pr = send, recv, ps, pr
        self.size = src.shape[0]

    def copy(self, zz, k, way, own=False):
        at = zz * self.size + k
        target = (self.z + (1 if way == 0 else -1)) * 2 + self.y
        return remote(
            self.src.at[k] if own else self.col.at[at],
            self.col.at[at],
            self.send.at[way * self.nz * self.size + at],
            self.recv.at[at],
            {"ka": target},
        )

    def chain(self, zz, k, act, ways=(0, 1), own=False):
        for way in ways:
            free = self.z < self.nz - 1 if way == 0 else self.z > 0

            @pl.when(free)
            def _(way=way):
                act(self.copy(zz, k, way, own))

    def sides(self, h, act):
        for way in (0, 1):
            zz = self.z - h if way == 0 else self.z + h
            there = zz >= 0 if way == 0 else zz < self.nz

            @pl.when(there)
            def _(zz=zz, way=way):
                act(zz, way)

    def first(self):
        for k in range(self.size):
            self.chain(self.z, k, start, own=True)
        self.col[pl.ds(self.z * self.size, self.size)] = self.src[...]

    def hop(self, h):
        for k in range(self.size):

            def one(zz, way, k=k):
                self.copy(zz, k, way).wait_recv()
                self.chain(zz, k, start, (way,))

            self.sides(h, one)

    def chosen(self, zz, owner, r):
        which = self.tab[zz * 2 + self.y, owner * CAPQ + r]
        v = self.col[zz * self.size]
        for k in range(1, self.size):
            v = jnp.where(which == k, self.col[zz * self.size + k], v)
        return v

    def across(self, zz):
        rows = pl.ds(zz * CAPQ, CAPQ)
        return remote(
            self.out.at[rows],
            self.got.at[rows],
            self.ps.at[zz],
            self.pr.at[zz],
            {"ka": self.z * 2 + 1 - self.y},
        )

    def pass_on(self, zz):
        for r in range(CAPQ):
            self.out[zz * CAPQ + r] = self.chosen(zz, self.z * 2 + 1 - self.y, r)
        self.across(zz).start()

    def finish(self):
        for k in range(self.size):
            self.chain(self.z, k, sent, own=True)
        self.across(self.z).wait_send()

        def tail(h, carry):
            def side(zz, way):
                for k in range(self.size):
                    self.chain(zz, k, sent, (way,))
                self.across(zz).wait_send()

            self.sides(h, side)
            return carry

        lax.fori_loop(1, self.nz, tail, 0)


class Reduce:
    def __init__(self, part, out, recv1, tsend, recv2, s1, r1, s2, r2, per):
        self.g = lax.axis_index("ga")
        self.x, self.c = self.g // 2, self.g % 2
        self.part, self.out = part, out
        self.recv1, self.tsend, self.recv2 = recv1, tsend, recv2
        self.s1, self.r1, self.s2, self.r2, self.per = s1, r1, s2, r2, per

    def rows(self, i):
        return pl.ds(i * self.per, self.per)

    def one(self, t, i):
        xx = self.x if t else 1 - self.x
        return remote(
            self.part.at[xx * 2 + 1 - self.c, self.rows(i)],
            self.recv1.at[xx, self.rows(i)],
            self.s1.at[i * 2 + t],
            self.r1.at[i * 2 + t],
            {"ga": self.x * 2 + 1 - self.c},
        )

    def two(self, i):
        return remote(
            self.tsend.at[self.rows(i)],
            self.recv2.at[self.rows(i)],
            self.s2.at[i],
            self.r2.at[i],
            {"ga": (1 - self.x) * 2 + self.c},
        )

    def sum_one(self, xx, i):
        v = self.part[xx * 2 + self.c, self.rows(i)].astype(F32)
        return v + self.recv1[xx, self.rows(i)].astype(F32)

    def begin(self, i):
        self.one(0, i).start()
        self.one(1, i).start()

    def middle(self, i):
        self.one(0, i).wait_recv()
        self.tsend[self.rows(i)] = self.sum_one(1 - self.x, i).astype(self.tsend.dtype)
        self.two(i).start()

    def end(self, i):
        self.one(1, i).wait_recv()
        v = self.sum_one(self.x, i)
        self.two(i).wait_recv()
        v = v + self.recv2[self.rows(i)].astype(F32)
        self.out[self.rows(i)] = v.astype(self.out.dtype)
        self.one(0, i).wait_send()
        self.one(1, i).wait_send()
        self.two(i).wait_send()


def make_row(n, q_slots, per_dev, pairs_ref, qs_ref, tab, at_ref, kept):
    me = lax.axis_index("ka")
    rows = pairs_ref.shape[1]
    slots = n * CAPQ
    holders = ([], [])
    for j in range(rows):
        slot = qs_ref[pairs_ref[2, j]]
        owner = slot // q_slots
        kept[0, j] = pairs_ref[0, j] % per_dev
        kept[1, j] = slot - owner * q_slots
        kept[2, j] = pairs_ref[1, j]
        for i, o in enumerate((owner, pairs_ref[1, j] // per_dev)):
            rank = jnp.int32(0)
            for other in holders[i]:
                rank = rank + jnp.where(other == o, 1, 0)
            holders[i].append(o)
            at_ref[i, j] = o * CAPQ + rank

    def one(s, carry):
        for i, which in ((0, (0, 1, 2)), (1, (0, 2))):
            found = [jnp.int32(-1 if w == 2 else 0) for w in which]
            for j in range(rows):
                hit = at_ref[i, j] == s
                found = [jnp.where(hit, kept[w, j], f) for w, f in zip(which, found)]
            for w, f in enumerate(found):
                tab[me, (3 * i + w) * slots + s] = f
        return carry

    lax.fori_loop(0, slots, one, 0)


def kernel(n, pairs_ref, qs_ref, x_ref, y_ref, p_ref, v_ref, w_hbm, blocks_ref, mirr_ref,
           tab, at_ref, kept, wt, w_ref, x_col, x_out, x_got, y_all, p_all, part, half,
           recv1, tsend, recv2, part2, own, q1, qt, q2, second, outbox, inbox, lines, turned, flat,
           split, part3, eown, e1, et, e2, ebox, ein, emir,
           ws, ts, tr, xs, xr, xps, xpr, ys, yr, ps, pr, s1, r1, s2, r2, t1, u1, t2, u2,
           v1, w1, v2, w2, es, er, fs, fr, as_, ar, gs, gr):
    per_dev, nt, width = x_ref.shape
    rows = pairs_ref.shape[1]
    q_slots = w_ref.shape[0]
    nz = n // 2
    slots = n * CAPQ
    n_ga = part.shape[0]
    me = lax.axis_index("ka")
    g = lax.axis_index("ga")
    z, y = me // 2, me % 2
    fetch = pltpu.make_async_copy(w_hbm, wt, ws)
    fetch.start()
    greet(n)
    xg = Pick(n, x_ref, x_col, x_out, x_got, tab, xs, xr, xps, xpr)
    yg = Gather(n, y_ref, y_all, ys, yr, per_dev - 1)
    pg = Hub(n, p_ref, p_all, ps, pr)
    xg.first()
    yg.first()
    make_row(n, q_slots, per_dev, pairs_ref, qs_ref, tab, at_ref, kept)

    def row(i, whose):
        return remote(
            tab.at[whose], tab.at[whose], ts.at[i], tr.at[whose], {"ka": lax.rem(me + i, n)}
        )

    lax.fori_loop(1, n, lambda i, c: (row(i, me).start(), c)[1], 0)
    xg.pass_on(z)
    yg.late()
    fetch.wait()
    for s in range(q_slots):
        w_ref[s] = wt[:, s, :]
    red = Reduce(part, half, recv1, tsend, recv2, s1, r1, s2, r2, 2 * CAPQ)

    def multiply(v, a, r):
        w = tab[a, slots + me * CAPQ + r]
        v = jnp.dot(v, w_ref[w], preferred_element_type=F32)
        for i in range(n_ga):
            part[i, a * CAPQ + r] = v[:, i * width : (i + 1) * width].astype(part.dtype)

    def piece(zz):
        for r in range(CAPQ):
            multiply(xg.chosen(zz, me, r), zz * 2 + y, r)
        xg.across(zz).wait_recv()
        for r in range(CAPQ):
            multiply(x_got[zz * CAPQ + r], zz * 2 + 1 - y, r)
        red.begin(zz)

    xg.hop(1)
    pg.first()
    lax.fori_loop(
        1, n, lambda i, c: (row(i, lax.rem(me + n - i, n)).wait_recv(), c)[1], 0
    )
    xg.sides(1, lambda zz, way: xg.pass_on(zz))
    yg.second()
    piece(z)

    def stage(h, carry):
        @pl.when(h < nz)
        def _():
            xg.hop(h)
            xg.sides(h, lambda zz, way: xg.pass_on(zz))

        yg.hop(h - 1)
        pg.hop(h - 1)
        xg.sides(h - 1, lambda zz, way: piece(zz))

        @pl.when(h == 2)
        def _():
            red.middle(z)

        @pl.when(h > 2)
        def _():
            xg.sides(h - 2, lambda zz, way: red.middle(zz))

        return carry

    lax.fori_loop(2, nz + 1, stage, 0)
    xg.finish()
    pg.finish()
    xg.sides(nz - 1, lambda zz, way: red.middle(zz))

    quarter = nt // n_ga
    weight = v_ref[...].reshape(1, width)
    sets = jnp.where(pg.edged, 4, 2)
    ered = Reduce(part3, eown, e1, et, e2, v1, w1, v2, w2, 4 * nz)

    def of(q):
        return jnp.where(q // 2 == 0, z, pg.edge) * 2 + q % 2

    def joined(both, out, at):
        v = jnp.concatenate(both, axis=1)
        for i in range(n_ga):
            out[i, at] = v[i * quarter : (i + 1) * quarter]

    @pl.when(pg.inner)
    def _():
        def exchange(q, carry):
            a = of(q)
            for k in range(per_dev):
                weighted = p_all[a * per_dev + k].astype(F32) * weight
                high = weighted.astype(BF16)
                split[k, :nt] = high
                split[k, nt:] = (weighted - high.astype(F32)).astype(BF16)

            def level(zz, carry):
                both = []
                for r in range(CAPQ):
                    at = 3 * slots + (zz * 2 + y) * CAPQ + r
                    k2 = jnp.maximum(tab[a, at + slots], 0)
                    v = lax.dot_general(
                        split[tab[a, at]], p_all[k2], DIMS, preferred_element_type=F32
                    )
                    both.append(v[:nt] + v[nt:])
                joined(both, part3, q * nz + zz)
                return carry

            lax.fori_loop(0, nz, level, 0)
            return carry

        lax.fori_loop(0, sets, exchange, 0)
        ered.begin(0)

    lax.fori_loop(0, nz, lambda i, c: (red.end(i), c)[1], 0)
    yg.finish()

    @pl.when(pg.inner)
    def _():
        ered.middle(0)

    lax.fori_loop(1, n, lambda i, c: (row(i, me).wait_send(), c)[1], 0)

    def source(a, carry):
        both = []
        for r in range(CAPQ):
            k2 = jnp.maximum(tab[a, 2 * slots + me * CAPQ + r], 0)
            both.append(
                lax.dot_general(half[a * CAPQ + r], y_all[k2], DIMS, preferred_element_type=F32)
            )
        joined(both, part2, a)
        return carry

    lax.fori_loop(0, n, source, 0)
    end = Reduce(part2, own, q1, qt, q2, t1, u1, t2, u2, n)
    end.begin(0)
    shape = own.shape[1:]
    left = lax.broadcasted_iota(I32, shape, 1) < nt
    doubles = per_dev // 2

    def paired(sums):
        sums = [v[:, :nt] + v[:, nt:] for v in sums]
        return [
            jnp.concatenate([sums[i], sums[i + doubles]], axis=1) for i in range(doubles)
        ]

    def seconds(a, carry):
        at = 2 * slots + me * CAPQ
        second[a] = jnp.where(left, tab[a, at], tab[a, at + 1])
        return carry

    lax.fori_loop(0, n, seconds, 0)

    def to_first(q):
        return remote(
            eown.at[pl.ds(q * nz, nz)], ein.at[y], es.at[q], er.at[y], {"ka": of(q)}
        )

    def to_second(zz):
        return remote(ebox.at[zz], emir.at[z], fs.at[zz], fr.at[z], {"ka": zz * 2 + y})

    def others(act):
        def one(q, carry):
            @pl.when(q != y)
            def _():
                act(to_first(q))

            return carry

        lax.fori_loop(0, sets, one, 0)

    def levels(act):
        def one(zz, carry):
            @pl.when(zz != z)
            def _():
                act(to_second(zz))

            return carry

        lax.fori_loop(0, nz, one, 0)

    @pl.when(pg.inner)
    def _():
        ered.end(0)
        others(start)
        ein[y] = eown[pl.ds(y * nz, nz)]

        def level(zz, carry):
            def add(q, sums):
                at = 4 * slots + (zz * 2 + y) * CAPQ
                k2 = jnp.where(left, tab[of(q), at], tab[of(q), at + 1])
                v = eown[q * nz + zz]
                base = (zz * 2 + y) * per_dev
                return tuple(
                    t + jnp.where(k2 == base + i, v, 0.0) for i, t in enumerate(sums)
                )

            sums = lax.fori_loop(
                0, sets, add, tuple(jnp.zeros(shape, F32) for _ in range(per_dev))
            )
            for i, v in enumerate(paired(sums)):
                ebox[zz, i] = v
            return carry

        lax.fori_loop(0, nz, level, 0)
        levels(start)
        emir[z] = ebox[z]

    end.middle(0)
    end.end(0)

    def fill(b, carry):
        outbox[b, 0] = own[b]

        def add(a, sums):
            out = []
            for i in range(per_dev):
                out.append(sums[i] + jnp.where(second[a] == b * per_dev + i, own[a], 0.0))
            return tuple(out)

        sums = lax.fori_loop(0, n, add, tuple(jnp.zeros(shape, F32) for _ in range(per_dev)))
        for i, v in enumerate(paired(sums)):
            outbox[b, 1 + i] = v
        return carry

    lax.fori_loop(0, n, fill, 0)

    def cross(i, whose):
        to = lax.rem(me + i, n)
        return remote(outbox.at[to], inbox.at[whose], as_.at[i], ar.at[whose], {"ka": to})

    lax.fori_loop(1, n, lambda i, c: (cross(i, me).start(), c)[1], 0)
    inbox[me] = outbox[me]
    for yy in range(2):

        @pl.when(jnp.logical_or(jnp.logical_not(pg.inner), yy != y))
        def _(yy=yy):
            remote(ein.at[yy], ein.at[yy], es.at[0], er.at[yy], {"ka": z * 2 + 1 - y}).wait_recv()

    def inner_level(zz, carry):
        @pl.when(zz != z)
        def _():
            remote(
                emir.at[zz], emir.at[zz], fs.at[0], fr.at[zz], {"ka": z * 2 + 1 - y}
            ).wait_recv()

        return carry

    lax.fori_loop(1, nz - 1, inner_level, 0)
    lax.fori_loop(1, n, lambda i, c: (cross(i, lax.rem(me + n - i, n)).wait_recv(), c)[1], 0)
    lax.fori_loop(1, n, lambda i, c: (cross(i, me).wait_send(), c)[1], 0)

    @pl.when(pg.inner)
    def _():
        others(sent)
        levels(sent)

    sub = quarter // 2

    def picked(ref, at, r):
        even = ref[at + (pl.ds(0, sub, stride=2),)]
        odd = ref[at + (pl.ds(1, sub, stride=2),)]
        zero = jnp.concatenate([even[:, :nt], odd[:, :nt]], axis=1)
        one = jnp.concatenate([even[:, nt:], odd[:, nt:]], axis=1)
        return jnp.where(r == 0, zero, one)

    for j in range(rows):
        at, et_ = at_ref[0, j], at_ref[1, j]
        b = et_ // CAPQ
        direct = picked(inbox, (at // CAPQ, 0), at % CAPQ)
        term = picked(ein, (b % 2, b // 2), et_ % CAPQ)
        lines[g, pl.ds(j * sub, sub)] = 2.0 * term - direct
    base = rows * sub
    for i in range(doubles):
        total = lax.fori_loop(
            1, n, lambda o, t, i=i: t + inbox[o, 1 + i], inbox[0, 1 + i]
        )
        term = lax.fori_loop(
            2, nz - 1, lambda zz, t, i=i: t + emir[zz, i], emir[1, i]
        )
        lines[g, pl.ds(base + i * quarter, quarter)] = 2.0 * term - total
    x, c = g // 2, g % 2
    mate, far = x * 2 + 1 - c, (1 - x) * 2 + c

    def spread(i, whose, to):
        return remote(lines.at[whose], lines.at[whose], gs.at[i], gr.at[i], {"ga": to})

    spread(0, g, far).start()
    spread(1, g, mate).start()
    spread(0, far, far).wait_recv()
    spread(2, far, mate).start()
    spread(1, mate, mate).wait_recv()
    spread(2, (1 - x) * 2 + 1 - c, mate).wait_recv()
    spread(0, g, far).wait_send()
    spread(1, g, mate).wait_send()
    spread(2, far, mate).wait_send()

    lanes = 2 * nt
    for q in range(n_ga):
        for t in range(sub):
            blocks_ref[:, (q * sub + t) * lanes : (q * sub + t + 1) * lanes] = lines[
                q, pl.ds(t, rows, stride=sub)
            ]
    for i in range(doubles):
        whole = jnp.concatenate(
            [lines[q, pl.ds(base + i * quarter, quarter)] for q in range(n_ga)], axis=0
        )
        turned[...] = whole.T
        even = turned[pl.ds(0, nt, stride=2)]
        odd = turned[pl.ds(1, nt, stride=2)]
        both = jnp.concatenate([even, odd], axis=1)
        flat[pl.ds(i * nt // 2, nt // 2)] = both[: nt // 2]
        flat[pl.ds((i + doubles) * nt // 2, nt // 2)] = both[nt // 2 :]
    for t in range(nt // 2):
        mirr_ref[:, t * lanes : (t + 1) * lanes] = flat[pl.ds(t, per_dev, stride=nt // 2)]


def per_device(x_dens, y_dens, p_dens, coulomb, screened, pairs, q_slot):
    n = lax.axis_size("ka")
    n_ga = lax.axis_size("ga")
    per_dev, nt, g = x_dens.shape
    q_slots = screened.shape[0]
    rows = pairs.shape[0]
    slots = n * CAPQ
    nz = n // 2
    shape = jax.ShapeDtypeStruct
    wide = F32 if slots * nt <= 2048 else BF16
    quarter = nt // n_ga
    each = (quarter, CAPQ * nt)
    line = (n,) + each
    dma = lambda m: pltpu.SemaphoreType.DMA((m,))
    row_len = -(-5 * slots // 128) * 128
    k_all = n * per_dev
    blocks, mirrored = pl.pallas_call(
        functools.partial(kernel, n),
        out_shape=[shape((rows, nt * nt), F32), shape((per_dev, nt * nt), F32)],
        in_specs=[SM, SM, VM, VM, VM, VM, HB],
        out_specs=[VM, VM],
        scratch_shapes=[
            pltpu.SMEM((n, row_len), I32),
            pltpu.SMEM((2, rows), I32),
            pltpu.SMEM((3, rows), I32),
            pltpu.VMEM((g, q_slots, screened.shape[2]), BF16),
            pltpu.VMEM((q_slots, g, screened.shape[2]), BF16),
            pltpu.VMEM((nz * per_dev, nt, g), BF16),
            pltpu.VMEM((nz * CAPQ, nt, g), BF16),
            pltpu.VMEM((nz * CAPQ, nt, g), BF16),
            pltpu.VMEM((k_all, nt, g), BF16),
            pltpu.VMEM((k_all, nt, g), BF16),
            pltpu.VMEM((n_ga, slots, nt, g), wide),
            pltpu.VMEM((slots, nt, g), BF16),
            pltpu.VMEM((2, slots, nt, g), wide),
            pltpu.VMEM((slots, nt, g), BF16),
            pltpu.VMEM((slots, nt, g), BF16),
            pltpu.VMEM((n_ga,) + line, F32),
            pltpu.VMEM(line, F32),
            pltpu.VMEM((2,) + line, F32),
            pltpu.VMEM(line, F32),
            pltpu.VMEM(line, F32),
            pltpu.VMEM(line, I32),
            pltpu.VMEM((n, 1 + per_dev // 2) + each, F32),
            pltpu.VMEM((n, 1 + per_dev // 2) + each, F32),
            pltpu.VMEM((n_ga, rows * quarter // 2 + per_dev // 2 * quarter, CAPQ * nt), F32),
            pltpu.VMEM((2 * nt, nt), F32),
            pltpu.VMEM((per_dev * nt // 2, 2 * nt), F32),
            pltpu.VMEM((per_dev, 2 * nt, g), BF16),
            pltpu.VMEM((n_ga, 4 * nz) + each, F32),
            pltpu.VMEM((4 * nz,) + each, F32),
            pltpu.VMEM((2, 4 * nz) + each, F32),
            pltpu.VMEM((4 * nz,) + each, F32),
            pltpu.VMEM((4 * nz,) + each, F32),
            pltpu.VMEM((nz, per_dev // 2) + each, F32),
            pltpu.VMEM((2, nz) + each, F32),
            pltpu.VMEM((nz, per_dev // 2) + each, F32),
            pltpu.SemaphoreType.DMA,
            dma(n), dma(n),
            dma(2 * nz * per_dev), dma(nz * per_dev),
            dma(nz), dma(nz),
            dma(3 * k_all), dma(k_all),
            dma(3 * k_all), dma(k_all),
            dma(2 * nz), dma(2 * nz), dma(nz), dma(nz),
            dma(2), dma(2), dma(1), dma(1),
            dma(2), dma(2), dma(1), dma(1),
            dma(4), dma(2), dma(nz), dma(nz),
            dma(n), dma(n),
            dma(3), dma(3),
        ],
        compiler_params=pltpu.CompilerParams(
            collective_id=0, has_side_effects=True, vmem_limit_bytes=LIMIT
        ),
        name="window",
    )(pairs.T, q_slot, x_dens, y_dens, p_dens, coulomb, screened.transpose(1, 0, 2))
    return (blocks, mirrored)


def solution(mesh):
    in_specs = (
        P("ka", None, "ga"),
        P("ka", None, "ga"),
        P("ka", None, "ga"),
        P("ga"),
        P("ka", "ga", None),
        P("ka", None),
        P(),
    )
    out_specs = (P("ka", None), P("ka", None))
    return jax.shard_map(
        per_device, mesh=mesh, in_specs=in_specs, out_specs=out_specs, check_vma=False
    )
```

```python
import functools
import jax
import jax.numpy as jnp
from jax import lax
from jax.experimental import pallas as pl
from jax.experimental.pallas import tpu as pltpu
from jax.sharding import PartitionSpec as P

CAPQ = 2
F32 = jnp.float32
BF16 = jnp.bfloat16
I32 = jnp.int32
VM = pl.BlockSpec(memory_space=pltpu.VMEM)
SM = pl.BlockSpec(memory_space=pltpu.SMEM)
HB = pl.BlockSpec(memory_space=pl.ANY)
LIMIT = 66000000
DIMS = (((1,), (1,)), ((), ()))


def start(c):
    c.start()


def sent(c):
    c.wait_send()


def remote(src, dst, ss, rs, to):
    return pltpu.make_async_remote_copy(
        src_ref=src,
        dst_ref=dst,
        send_sem=ss,
        recv_sem=rs,
        device_id=to,
        device_id_type=pl.DeviceIdType.MESH,
    )


def greet(n):
    barrier = pltpu.get_barrier_semaphore()
    me = lax.axis_index("ka")
    g = lax.axis_index("ga")
    n_ga = lax.axis_size("ga")

    def hello(to):
        pl.semaphore_signal(barrier, inc=1, device_id=to, device_id_type=pl.DeviceIdType.MESH)

    lax.fori_loop(1, n, lambda i, c: (hello({"ka": lax.rem(me + i, n)}), c)[1], 0)
    for i in range(1, n_ga):
        hello({"ga": lax.rem(g + i, n_ga)})
    pl.semaphore_wait(barrier, n - 1 + n_ga - 1)


class Gather:
    def __init__(self, n, src, out, send, recv, cut):
        self.n, self.nz = n, n // 2
        self.me = lax.axis_index("ka")
        self.z, self.y = self.me // 2, self.me % 2
        self.src, self.out, self.send, self.recv = src, out, send, recv
        self.size = src.shape[0]
        self.cut = cut

    def copy(self, zz, yy, k, way, own=False):
        at = (zz * 2 + yy) * self.size + k
        block = self.out.at[at]
        if way == 2:
            target = self.z * 2 + 1 - self.y
        else:
            target = (self.z + (1 if way == 0 else -1)) * 2 + self.y
        return remote(
            self.src.at[k] if own else block,
            block,
            self.send.at[way * self.n * self.size + at],
            self.recv.at[at],
            {"ka": target},
        )

    def chain(self, zz, yy, k, act, ways=(0, 1), own=False):
        for way in ways:
            free = self.z < self.nz - 1 if way == 0 else self.z > 0

            @pl.when(free)
            def _(way=way):
                act(self.copy(zz, yy, k, way, own))

    def early(self):
        return range(self.cut, self.size)

    def across(self):
        for k in reversed(range(self.size)):
            self.copy(self.z, self.y, k, 2, True).start()
        self.out[pl.ds(self.me * self.size, self.size)] = self.src[...]

    def first(self):
        for k in range(self.size):
            self.chain(self.z, self.y, k, start, own=True)

    def second(self):
        for k in self.early():
            self.copy(self.z, 1 - self.y, k, 2).wait_recv()
            self.chain(self.z, 1 - self.y, k, start)

    def sides(self, h, act):
        for way in (0, 1):
            zz = self.z - h if way == 0 else self.z + h
            there = zz >= 0 if way == 0 else zz < self.nz

            @pl.when(there)
            def _(zz=zz, way=way):
                act(zz, way)

    def hop(self, h):
        def one(k, yy, zz, way):
            self.copy(zz, yy, k, 2).wait_recv()
            self.chain(zz, yy, k, start, (way,))

        for k in range(self.size):

            def own(zz, way, k=k):
                one(k, self.y, zz, way)
                if k < self.cut:
                    self.copy(zz, self.y, k, 2).start()

            self.sides(h, own)
        for k in self.early():
            self.sides(h, lambda zz, way, k=k: one(k, 1 - self.y, zz, way))

    def finish(self):
        for k in range(self.size):
            self.chain(self.z, self.y, k, sent, own=True)
            self.copy(self.z, self.y, k, 2, True).wait_send()
        for k in self.early():
            self.chain(self.z, 1 - self.y, k, sent)
        for k in range(self.cut):
            self.copy(self.z, 1 - self.y, k, 2).wait_recv()

        def tail(h, carry):
            def side(zz, way):
                for k in range(self.size):
                    self.chain(zz, self.y, k, sent, (way,))
                for k in self.early():
                    self.chain(zz, 1 - self.y, k, sent, (way,))
                for k in range(self.cut):
                    self.copy(zz, self.y, k, 2).wait_send()
                    self.copy(zz, 1 - self.y, k, 2).wait_recv()

            self.sides(h, side)
            return carry

        lax.fori_loop(1, self.nz, tail, 0)


class Hub(Gather):
    def __init__(self, n, src, out, send, recv):
        super().__init__(n, src, out, send, recv, src.shape[0])
        self.inner = jnp.logical_and(self.z >= 1, self.z <= self.nz - 2)
        self.edged = jnp.logical_or(self.z == 1, self.z == self.nz - 2)
        self.edge = jnp.where(self.z == 1, 0, self.nz - 1)

    def chain(self, zz, yy, k, act, ways=(0, 1), own=False):
        for way in ways:
            free = self.z <= self.nz - 3 if way == 0 else self.z >= 2

            @pl.when(free)
            def _(way=way):
                act(self.copy(zz, yy, k, way, own))

    def first(self):
        for k in range(self.size):
            self.chain(self.z, self.y, k, start, own=True)

        @pl.when(self.inner)
        def _():
            for k in range(self.size):
                self.copy(self.z, self.y, k, 2, True).start()

        self.out[pl.ds(self.me * self.size, self.size)] = self.src[...]

    def hop(self, h):
        def own(zz, way):
            last = jnp.logical_and(self.edged, zz == self.edge)
            for k in range(self.size):
                self.copy(zz, self.y, k, 2).wait_recv()
                self.chain(zz, self.y, k, start, (way,))

                @pl.when(last)
                def _(k=k):
                    self.copy(zz, self.y, k, 2).start()

        @pl.when(self.inner)
        def _():
            self.sides(h, own)

    def finish(self):
        for k in range(self.size):
            self.chain(self.z, self.y, k, sent, own=True)

        @pl.when(self.inner)
        def _():
            for k in range(self.size):
                self.copy(self.z, self.y, k, 2, True).wait_send()
                self.copy(self.z, 1 - self.y, k, 2).wait_recv()

            @pl.when(self.edged)
            def _():
                for k in range(self.size):
                    self.copy(self.edge, self.y, k, 2).wait_send()
                    self.copy(self.edge, 1 - self.y, k, 2).wait_recv()

            def tail(h, carry):
                def side(zz, way):
                    for k in range(self.size):
                        self.chain(zz, self.y, k, sent, (way,))

                self.sides(h, side)
                return carry

            lax.fori_loop(1, self.nz, tail, 0)


class Pick:
    def __init__(self, n, src, col, out, got, tab, send, recv, ps, pr):
        self.n, self.nz = n, n // 2
        self.me = lax.axis_index("ka")
        self.z, self.y = self.me // 2, self.me % 2
        self.src, self.col, self.out, self.got, self.tab = src, col, out, got, tab
        self.send, self.recv, self.ps, self.pr = send, recv, ps, pr
        self.size = src.shape[0]

    def copy(self, zz, k, way, own=False):
        at = zz * self.size + k
        target = (self.z + (1 if way == 0 else -1)) * 2 + self.y
        return remote(
            self.src.at[k] if own else self.col.at[at],
            self.col.at[at],
            self.send.at[way * self.nz * self.size + at],
            self.recv.at[at],
            {"ka": target},
        )

    def chain(self, zz, k, act, ways=(0, 1), own=False):
        for way in ways:
            free = self.z < self.nz - 1 if way == 0 else self.z > 0

            @pl.when(free)
            def _(way=way):
                act(self.copy(zz, k, way, own))

    def sides(self, h, act):
        for way in (0, 1):
            zz = self.z - h if way == 0 else self.z + h
            there = zz >= 0 if way == 0 else zz < self.nz

            @pl.when(there)
            def _(zz=zz, way=way):
                act(zz, way)

    def first(self):
        for k in range(self.size):
            self.chain(self.z, k, start, own=True)
        self.col[pl.ds(self.z * self.size, self.size)] = self.src[...]

    def hop(self, h):
        for k in range(self.size):

            def one(zz, way, k=k):
                self.copy(zz, k, way).wait_recv()
                self.chain(zz, k, start, (way,))

            self.sides(h, one)

    def chosen(self, zz, owner, r):
        which = self.tab[zz * 2 + self.y, owner * CAPQ + r]
        v = self.col[zz * self.size]
        for k in range(1, self.size):
            v = jnp.where(which == k, self.col[zz * self.size + k], v)
        return v

    def across(self, zz):
        rows = pl.ds(zz * CAPQ, CAPQ)
        return remote(
            self.out.at[rows],
            self.got.at[rows],
            self.ps.at[zz],
            self.pr.at[zz],
            {"ka": self.z * 2 + 1 - self.y},
        )

    def pass_on(self, zz):
        for r in range(CAPQ):
            self.out[zz * CAPQ + r] = self.chosen(zz, self.z * 2 + 1 - self.y, r)
        self.across(zz).start()

    def finish(self):
        for k in range(self.size):
            self.chain(self.z, k, sent, own=True)
        self.across(self.z).wait_send()

        def tail(h, carry):
            def side(zz, way):
                for k in range(self.size):
                    self.chain(zz, k, sent, (way,))
                self.across(zz).wait_send()

            self.sides(h, side)
            return carry

        lax.fori_loop(1, self.nz, tail, 0)


class Reduce:
    def __init__(self, part, out, recv1, tsend, recv2, s1, r1, s2, r2, per):
        self.g = lax.axis_index("ga")
        self.x, self.c = self.g // 2, self.g % 2
        self.part, self.out = part, out
        self.recv1, self.tsend, self.recv2 = recv1, tsend, recv2
        self.s1, self.r1, self.s2, self.r2, self.per = s1, r1, s2, r2, per

    def rows(self, i):
        return pl.ds(i * self.per, self.per)

    def one(self, t, i):
        xx = self.x if t else 1 - self.x
        return remote(
            self.part.at[xx * 2 + 1 - self.c, self.rows(i)],
            self.recv1.at[xx, self.rows(i)],
            self.s1.at[i * 2 + t],
            self.r1.at[i * 2 + t],
            {"ga": self.x * 2 + 1 - self.c},
        )

    def two(self, i):
        return remote(
            self.tsend.at[self.rows(i)],
            self.recv2.at[self.rows(i)],
            self.s2.at[i],
            self.r2.at[i],
            {"ga": (1 - self.x) * 2 + self.c},
        )

    def sum_one(self, xx, i):
        v = self.part[xx * 2 + self.c, self.rows(i)].astype(F32)
        return v + self.recv1[xx, self.rows(i)].astype(F32)

    def begin(self, i):
        self.one(0, i).start()
        self.one(1, i).start()

    def middle(self, i):
        self.one(0, i).wait_recv()
        self.tsend[self.rows(i)] = self.sum_one(1 - self.x, i).astype(self.tsend.dtype)
        self.two(i).start()

    def end(self, i):
        self.one(1, i).wait_recv()
        v = self.sum_one(self.x, i)
        self.two(i).wait_recv()
        v = v + self.recv2[self.rows(i)].astype(F32)
        self.out[self.rows(i)] = v.astype(self.out.dtype)
        self.one(0, i).wait_send()
        self.one(1, i).wait_send()
        self.two(i).wait_send()


def make_row(n, q_slots, per_dev, pairs_ref, qs_ref, row_ref, at_ref):
    rows = pairs_ref.shape[1]
    slots = n * CAPQ
    lane = lax.broadcasted_iota(I32, row_ref.shape, 1)
    section = lane // slots
    spot = lane % slots
    row = jnp.where(jnp.logical_or(section == 2, section == 4), -1, 0)
    holders = ([], [])
    for j in range(rows):
        slot = qs_ref[pairs_ref[2, j]]
        owner = slot // q_slots
        first, second = pairs_ref[0, j] % per_dev, pairs_ref[1, j]
        at = []
        for i, o in enumerate((owner, second // per_dev)):
            rank = jnp.int32(0)
            for other in holders[i]:
                rank = rank + jnp.where(other == o, 1, 0)
            holders[i].append(o)
            at.append(o * CAPQ + rank)
            at_ref[i, j] = at[i]
        value = jnp.where(section == 1, slot - owner * q_slots, second)
        value = jnp.where(jnp.logical_or(section == 0, section == 3), first, value)
        hit = spot == jnp.where(section < 3, at[0], at[1])
        row = jnp.where(hit, value, row)
    row_ref[...] = row


def kernel(n, pairs_ref, qs_ref, x_ref, y_ref, p_ref, v_ref, w_hbm, lines,
           tab, at_ref, row_ref, wt, w_ref, x_col, x_out, x_got, y_all, p_all, part, half,
           recv1, tsend, recv2, part2, own, q1, qt, q2, second, outbox, inbox,
           split, part3, eown, e1, et, e2, ebox, ein, emir,
           ws, ls, ts, tr, xs, xr, xps, xpr, ys, yr, ps, pr, s1, r1, s2, r2, t1, u1, t2, u2,
           v1, w1, v2, w2, es, er, fs, fr, as_, ar, gs, gr):
    per_dev, nt, width = x_ref.shape
    rows = pairs_ref.shape[1]
    q_slots = w_ref.shape[0]
    nz = n // 2
    slots = n * CAPQ
    n_ga = part.shape[0]
    me = lax.axis_index("ka")
    g = lax.axis_index("ga")
    z, y = me // 2, me % 2
    fetch = pltpu.make_async_copy(w_hbm, wt, ws)
    fetch.start()
    greet(n)
    xg = Pick(n, x_ref, x_col, x_out, x_got, tab, xs, xr, xps, xpr)
    yg = Gather(n, y_ref, y_all, ys, yr, per_dev - 1)
    pg = Hub(n, p_ref, p_all, ps, pr)
    xg.first()
    make_row(n, q_slots, per_dev, pairs_ref, qs_ref, row_ref, at_ref)
    keep = pltpu.make_async_copy(row_ref.at[0], tab.at[me], ls)
    keep.start()

    def row(i, whose):
        return remote(
            row_ref.at[0], tab.at[whose], ts.at[i], tr.at[whose], {"ka": lax.rem(me + i, n)}
        )

    lax.fori_loop(1, n, lambda i, c: (row(i, me).start(), c)[1], 0)
    keep.wait()
    xg.pass_on(z)
    yg.across()
    fetch.wait()
    turn = 16
    whole = width // turn * turn

    def relay(i, carry):
        at = pl.ds(pl.multiple_of(i * turn, turn), turn)
        w_ref[:, at] = jnp.swapaxes(wt[at], 0, 1)
        return carry

    lax.fori_loop(0, width // turn, relay, 0)
    if whole < width:
        w_ref[:, whole:] = jnp.swapaxes(wt[whole:], 0, 1)
    red = Reduce(part, half, recv1, tsend, recv2, s1, r1, s2, r2, 2 * CAPQ)

    def multiply(v, a, r):
        w = tab[a, slots + me * CAPQ + r]
        v = jnp.dot(v, w_ref[w], preferred_element_type=F32)
        for i in range(n_ga):
            part[i, a * CAPQ + r] = v[:, i * width : (i + 1) * width].astype(part.dtype)

    def piece(zz):
        for r in range(CAPQ):
            multiply(xg.chosen(zz, me, r), zz * 2 + y, r)
        xg.across(zz).wait_recv()
        for r in range(CAPQ):
            multiply(x_got[zz * CAPQ + r], zz * 2 + 1 - y, r)
        red.begin(zz)

    xg.hop(1)
    lax.fori_loop(
        1, n, lambda i, c: (row(i, lax.rem(me + n - i, n)).wait_recv(), c)[1], 0
    )
    xg.sides(1, lambda zz, way: xg.pass_on(zz))
    piece(z)

    def stage(h, carry):
        @pl.when(h < nz)
        def _():
            xg.hop(h)

        @pl.when(h == 2)
        def _():
            yg.first()
            pg.first()

        @pl.when(h < nz)
        def _():
            xg.sides(h, lambda zz, way: xg.pass_on(zz))

        @pl.when(h == 2)
        def _():
            yg.second()

        xg.sides(h - 1, lambda zz, way: piece(zz))

        @pl.when(h == 2)
        def _():
            red.middle(z)

        @pl.when(h > 2)
        def _():
            xg.sides(h - 2, lambda zz, way: red.middle(zz))
            yg.hop(h - 2)
            pg.hop(h - 2)

        return carry

    lax.fori_loop(2, nz + 1, stage, 0)
    xg.sides(nz - 1, lambda zz, way: red.middle(zz))
    yg.hop(nz - 1)
    pg.hop(nz - 1)
    xg.finish()
    pg.finish()

    quarter = nt // n_ga
    weight = v_ref[...].reshape(1, width)
    sets = jnp.where(pg.edged, 4, 2)
    ered = Reduce(part3, eown, e1, et, e2, v1, w1, v2, w2, 4 * nz)

    def of(q):
        return jnp.where(q // 2 == 0, z, pg.edge) * 2 + q % 2

    def joined(both, out, at):
        v = jnp.concatenate(both, axis=1)
        for i in range(n_ga):
            out[i, at] = v[i * quarter : (i + 1) * quarter]

    @pl.when(pg.inner)
    def _():
        def exchange(q, carry):
            a = of(q)
            for k in range(per_dev):
                weighted = p_all[a * per_dev + k].astype(F32) * weight
                high = weighted.astype(BF16)
                split[k, :nt] = high
                split[k, nt:] = (weighted - high.astype(F32)).astype(BF16)

            def level(zz, carry):
                both = []
                for r in range(CAPQ):
                    at = 3 * slots + (zz * 2 + y) * CAPQ + r
                    k2 = jnp.maximum(tab[a, at + slots], 0)
                    v = lax.dot_general(
                        split[tab[a, at]], p_all[k2], DIMS, preferred_element_type=F32
                    )
                    both.append(v[:nt] + v[nt:])
                joined(both, part3, q * nz + zz)
                return carry

            lax.fori_loop(0, nz, level, 0)
            return carry

        lax.fori_loop(0, sets, exchange, 0)
        ered.begin(0)

    lax.fori_loop(0, nz, lambda i, c: (red.end(i), c)[1], 0)
    yg.finish()

    @pl.when(pg.inner)
    def _():
        ered.middle(0)

    lax.fori_loop(1, n, lambda i, c: (row(i, me).wait_send(), c)[1], 0)

    def source(a, carry):
        both = []
        for r in range(CAPQ):
            k2 = jnp.maximum(tab[a, 2 * slots + me * CAPQ + r], 0)
            both.append(
                lax.dot_general(half[a * CAPQ + r], y_all[k2], DIMS, preferred_element_type=F32)
            )
        joined(both, part2, a)
        return carry

    lax.fori_loop(0, n, source, 0, unroll=2)
    end = Reduce(part2, own, q1, qt, q2, t1, u1, t2, u2, n)
    end.begin(0)
    shape = own.shape[1:]
    left = lax.broadcasted_iota(I32, shape, 1) < nt
    doubles = per_dev // 2

    def paired(sums):
        sums = [v[:, :nt] + v[:, nt:] for v in sums]
        return [
            jnp.concatenate([sums[i], sums[i + doubles]], axis=1) for i in range(doubles)
        ]

    def seconds(a, carry):
        at = 2 * slots + me * CAPQ
        second[a] = jnp.where(left, tab[a, at], tab[a, at + 1])
        return carry

    lax.fori_loop(0, n, seconds, 0)

    def to_first(q):
        return remote(
            eown.at[pl.ds(q * nz, nz)], ein.at[y], es.at[q], er.at[y], {"ka": of(q)}
        )

    def to_second(zz):
        return remote(ebox.at[zz], emir.at[z], fs.at[zz], fr.at[z], {"ka": zz * 2 + y})

    def others(act):
        def one(q, carry):
            @pl.when(q != y)
            def _():
                act(to_first(q))

            return carry

        lax.fori_loop(0, sets, one, 0)

    def levels(act):
        def one(zz, carry):
            @pl.when(zz != z)
            def _():
                act(to_second(zz))

            return carry

        lax.fori_loop(0, nz, one, 0)

    @pl.when(pg.inner)
    def _():
        ered.end(0)
        others(start)
        ein[y] = eown[pl.ds(y * nz, nz)]

        def level(zz, carry):
            def add(q, sums):
                at = 4 * slots + (zz * 2 + y) * CAPQ
                k2 = jnp.where(left, tab[of(q), at], tab[of(q), at + 1])
                v = eown[q * nz + zz]
                base = (zz * 2 + y) * per_dev
                return tuple(
                    t + jnp.where(k2 == base + i, v, 0.0) for i, t in enumerate(sums)
                )

            sums = lax.fori_loop(
                0, sets, add, tuple(jnp.zeros(shape, F32) for _ in range(per_dev))
            )
            for i, v in enumerate(paired(sums)):
                ebox[zz, i] = v
            return carry

        lax.fori_loop(0, nz, level, 0)
        levels(start)
        emir[z] = ebox[z]

    end.middle(0)
    end.end(0)

    def fill(b, carry):
        outbox[b, 0] = own[b]

        def add(a, sums):
            out = []
            for i in range(per_dev):
                out.append(sums[i] + jnp.where(second[a] == b * per_dev + i, own[a], 0.0))
            return tuple(out)

        sums = tuple(jnp.zeros(shape, F32) for _ in range(per_dev))
        sums = lax.fori_loop(0, n, add, sums, unroll=min(n, 8))
        for i, v in enumerate(paired(sums)):
            outbox[b, 1 + i] = v
        return carry

    lax.fori_loop(0, n, fill, 0)

    def cross(i, whose):
        to = lax.rem(me + i, n)
        return remote(outbox.at[to], inbox.at[whose], as_.at[i], ar.at[whose], {"ka": to})

    lax.fori_loop(1, n, lambda i, c: (cross(i, me).start(), c)[1], 0)
    inbox[me] = outbox[me]
    for yy in range(2):

        @pl.when(jnp.logical_or(jnp.logical_not(pg.inner), yy != y))
        def _(yy=yy):
            remote(ein.at[yy], ein.at[yy], es.at[0], er.at[yy], {"ka": z * 2 + 1 - y}).wait_recv()

    def inner_level(zz, carry):
        @pl.when(zz != z)
        def _():
            remote(
                emir.at[zz], emir.at[zz], fs.at[0], fr.at[zz], {"ka": z * 2 + 1 - y}
            ).wait_recv()

        return carry

    lax.fori_loop(1, nz - 1, inner_level, 0)
    lax.fori_loop(1, n, lambda i, c: (cross(i, lax.rem(me + n - i, n)).wait_recv(), c)[1], 0)
    lax.fori_loop(1, n, lambda i, c: (cross(i, me).wait_send(), c)[1], 0)

    @pl.when(pg.inner)
    def _():
        others(sent)
        levels(sent)

    sub = quarter // 2

    def picked(ref, at, r):
        even = ref[at + (pl.ds(0, sub, stride=2),)]
        odd = ref[at + (pl.ds(1, sub, stride=2),)]
        zero = jnp.concatenate([even[:, :nt], odd[:, :nt]], axis=1)
        one = jnp.concatenate([even[:, nt:], odd[:, nt:]], axis=1)
        return jnp.where(r == 0, zero, one)

    for j in range(rows):
        at, et_ = at_ref[0, j], at_ref[1, j]
        b = et_ // CAPQ
        direct = picked(inbox, (at // CAPQ, 0), at % CAPQ)
        term = picked(ein, (b % 2, b // 2), et_ % CAPQ)
        lines[g, pl.ds(j * sub, sub)] = 2.0 * term - direct
    base = rows * sub
    for i in range(doubles):
        total = lax.fori_loop(
            1, n, lambda o, t, i=i: t + inbox[o, 1 + i], inbox[0, 1 + i]
        )
        term = lax.fori_loop(
            2, nz - 1, lambda zz, t, i=i: t + emir[zz, i], emir[1, i]
        )
        lines[g, pl.ds(base + i * quarter, quarter)] = 2.0 * term - total
    x, c = g // 2, g % 2
    mate, far = x * 2 + 1 - c, (1 - x) * 2 + c

    def spread(i, whose, to):
        return remote(lines.at[whose], lines.at[whose], gs.at[i], gr.at[i], {"ga": to})

    spread(0, g, far).start()
    spread(1, g, mate).start()
    spread(0, far, far).wait_recv()
    spread(2, far, mate).start()
    spread(1, mate, mate).wait_recv()
    spread(2, (1 - x) * 2 + 1 - c, mate).wait_recv()
    spread(0, g, far).wait_send()
    spread(1, g, mate).wait_send()
    spread(2, far, mate).wait_send()


def layout(lines, blocks_ref, mirr_ref, turned, flat):
    n_ga = lines.shape[0]
    rows, per_dev = blocks_ref.shape[0], mirr_ref.shape[0]
    nt = turned.shape[1]
    quarter, sub, doubles = nt // n_ga, nt // n_ga // 2, per_dev // 2
    base = rows * sub
    lanes = 2 * nt
    for q in range(n_ga):
        for t in range(sub):
            blocks_ref[:, (q * sub + t) * lanes : (q * sub + t + 1) * lanes] = lines[
                q, pl.ds(t, rows, stride=sub)
            ]
    for i in range(doubles):
        whole = jnp.concatenate(
            [lines[q, pl.ds(base + i * quarter, quarter)] for q in range(n_ga)], axis=0
        )
        turned[...] = whole.T
        even = turned[pl.ds(0, nt, stride=2)]
        odd = turned[pl.ds(1, nt, stride=2)]
        both = jnp.concatenate([even, odd], axis=1)
        flat[pl.ds(i * nt // 2, nt // 2)] = both[: nt // 2]
        flat[pl.ds((i + doubles) * nt // 2, nt // 2)] = both[nt // 2 :]
    for t in range(nt // 2):
        mirr_ref[:, t * lanes : (t + 1) * lanes] = flat[pl.ds(t, per_dev, stride=nt // 2)]


def per_device(x_dens, y_dens, p_dens, coulomb, screened, pairs, q_slot):
    n = lax.axis_size("ka")
    n_ga = lax.axis_size("ga")
    per_dev, nt, g = x_dens.shape
    q_slots = screened.shape[0]
    rows = pairs.shape[0]
    slots = n * CAPQ
    nz = n // 2
    shape = jax.ShapeDtypeStruct
    wide = F32 if slots * nt <= 2048 else BF16
    quarter = nt // n_ga
    each = (quarter, CAPQ * nt)
    line = (n,) + each
    dma = lambda m: pltpu.SemaphoreType.DMA((m,))
    row_len = -(-5 * slots // 128) * 128
    k_all = n * per_dev
    lines = pl.pallas_call(
        functools.partial(kernel, n),
        out_shape=shape((n_ga, rows * quarter // 2 + per_dev // 2 * quarter, CAPQ * nt), F32),
        in_specs=[SM, SM, VM, VM, VM, VM, HB],
        out_specs=VM,
        scratch_shapes=[
            pltpu.SMEM((n, row_len), I32),
            pltpu.SMEM((2, rows), I32),
            pltpu.VMEM((1, row_len), I32),
            pltpu.VMEM((g, q_slots, screened.shape[2]), BF16),
            pltpu.VMEM((q_slots, g, screened.shape[2]), BF16),
            pltpu.VMEM((nz * per_dev, nt, g), BF16),
            pltpu.VMEM((nz * CAPQ, nt, g), BF16),
            pltpu.VMEM((nz * CAPQ, nt, g), BF16),
            pltpu.VMEM((k_all, nt, g), BF16),
            pltpu.VMEM((k_all, nt, g), BF16),
            pltpu.VMEM((n_ga, slots, nt, g), wide),
            pltpu.VMEM((slots, nt, g), BF16),
            pltpu.VMEM((2, slots, nt, g), wide),
            pltpu.VMEM((slots, nt, g), BF16),
            pltpu.VMEM((slots, nt, g), BF16),
            pltpu.VMEM((n_ga,) + line, F32),
            pltpu.VMEM(line, F32),
            pltpu.VMEM((2,) + line, F32),
            pltpu.VMEM(line, F32),
            pltpu.VMEM(line, F32),
            pltpu.VMEM(line, I32),
            pltpu.VMEM((n, 1 + per_dev // 2) + each, F32),
            pltpu.VMEM((n, 1 + per_dev // 2) + each, F32),
            pltpu.VMEM((per_dev, 2 * nt, g), BF16),
            pltpu.VMEM((n_ga, 4 * nz) + each, F32),
            pltpu.VMEM((4 * nz,) + each, F32),
            pltpu.VMEM((2, 4 * nz) + each, F32),
            pltpu.VMEM((4 * nz,) + each, F32),
            pltpu.VMEM((4 * nz,) + each, F32),
            pltpu.VMEM((nz, per_dev // 2) + each, F32),
            pltpu.VMEM((2, nz) + each, F32),
            pltpu.VMEM((nz, per_dev // 2) + each, F32),
            pltpu.SemaphoreType.DMA,
            pltpu.SemaphoreType.DMA,
            dma(n), dma(n),
            dma(2 * nz * per_dev), dma(nz * per_dev),
            dma(nz), dma(nz),
            dma(3 * k_all), dma(k_all),
            dma(3 * k_all), dma(k_all),
            dma(2 * nz), dma(2 * nz), dma(nz), dma(nz),
            dma(2), dma(2), dma(1), dma(1),
            dma(2), dma(2), dma(1), dma(1),
            dma(4), dma(2), dma(nz), dma(nz),
            dma(n), dma(n),
            dma(3), dma(3),
        ],
        compiler_params=pltpu.CompilerParams(
            collective_id=0, has_side_effects=True, vmem_limit_bytes=LIMIT
        ),
        name="window",
    )(pairs.T, q_slot, x_dens, y_dens, p_dens, coulomb, screened.transpose(1, 0, 2))
    blocks, mirrored = pl.pallas_call(
        layout,
        out_shape=[shape((rows, nt * nt), F32), shape((per_dev, nt * nt), F32)],
        in_specs=[VM],
        out_specs=[VM, VM],
        scratch_shapes=[
            pltpu.VMEM((2 * nt, nt), F32),
            pltpu.VMEM((per_dev * nt // 2, 2 * nt), F32),
        ],
        name="layout",
    )(lines)
    return (blocks, mirrored)


def solution(mesh):
    in_specs = (
        P("ka", None, "ga"),
        P("ka", None, "ga"),
        P("ka", None, "ga"),
        P("ga"),
        P("ka", "ga", None),
        P("ka", None),
        P(),
    )
    out_specs = (P("ka", None), P("ka", None))
    return jax.shard_map(
        per_device, mesh=mesh, in_specs=in_specs, out_specs=out_specs, check_vma=False
    )
```

```python
import functools
import jax
import jax.numpy as jnp
from jax import lax
from jax.experimental import pallas as pl
from jax.experimental.pallas import tpu as pltpu
from jax.sharding import PartitionSpec as P

CAPQ = 2
F32 = jnp.float32
BF16 = jnp.bfloat16
I32 = jnp.int32
VM = pl.BlockSpec(memory_space=pltpu.VMEM)
SM = pl.BlockSpec(memory_space=pltpu.SMEM)
HB = pl.BlockSpec(memory_space=pl.ANY)
LIMIT = 66000000
DIMS = (((1,), (1,)), ((), ()))


def start(c):
    c.start()


def sent(c):
    c.wait_send()


def remote(src, dst, ss, rs, to):
    return pltpu.make_async_remote_copy(
        src_ref=src,
        dst_ref=dst,
        send_sem=ss,
        recv_sem=rs,
        device_id=to,
        device_id_type=pl.DeviceIdType.MESH,
    )


def greet(n):
    barrier = pltpu.get_barrier_semaphore()
    me = lax.axis_index("ka")
    g = lax.axis_index("ga")
    n_ga = lax.axis_size("ga")

    def hello(to):
        pl.semaphore_signal(barrier, inc=1, device_id=to, device_id_type=pl.DeviceIdType.MESH)

    lax.fori_loop(1, n, lambda i, c: (hello({"ka": lax.rem(me + i, n)}), c)[1], 0)
    for i in range(1, n_ga):
        hello({"ga": lax.rem(g + i, n_ga)})
    pl.semaphore_wait(barrier, n - 1 + n_ga - 1)


class Gather:
    def __init__(self, n, src, out, send, recv, cut):
        self.n, self.nz = n, n // 2
        self.me = lax.axis_index("ka")
        self.z, self.y = self.me // 2, self.me % 2
        self.src, self.out, self.send, self.recv = src, out, send, recv
        self.size = src.shape[0]
        self.cut = cut

    def copy(self, zz, yy, k, way, own=False):
        at = (zz * 2 + yy) * self.size + k
        block = self.out.at[at]
        if way == 2:
            target = self.z * 2 + 1 - self.y
        else:
            target = (self.z + (1 if way == 0 else -1)) * 2 + self.y
        return remote(
            self.src.at[k] if own else block,
            block,
            self.send.at[way * self.n * self.size + at],
            self.recv.at[at],
            {"ka": target},
        )

    def chain(self, zz, yy, k, act, ways=(0, 1), own=False):
        for way in ways:
            free = self.z < self.nz - 1 if way == 0 else self.z > 0

            @pl.when(free)
            def _(way=way):
                act(self.copy(zz, yy, k, way, own))

    def early(self):
        return range(self.cut, self.size)

    def across_early(self):
        for k in self.early():
            self.copy(self.z, self.y, k, 2, True).start()

    def across_late(self):
        for k in range(self.cut):
            self.copy(self.z, self.y, k, 2, True).start()
        self.out[pl.ds(self.me * self.size, self.size)] = self.src[...]

    def first(self):
        for k in range(self.size):
            self.chain(self.z, self.y, k, start, own=True)

    def second(self):
        for k in self.early():
            self.copy(self.z, 1 - self.y, k, 2).wait_recv()
            self.chain(self.z, 1 - self.y, k, start)

    def sides(self, h, act):
        for way in (0, 1):
            zz = self.z - h if way == 0 else self.z + h
            there = zz >= 0 if way == 0 else zz < self.nz

            @pl.when(there)
            def _(zz=zz, way=way):
                act(zz, way)

    def hop(self, h):
        def one(k, yy, zz, way):
            self.copy(zz, yy, k, 2).wait_recv()
            self.chain(zz, yy, k, start, (way,))

        for k in range(self.size):

            def own(zz, way, k=k):
                one(k, self.y, zz, way)
                if k < self.cut:
                    self.copy(zz, self.y, k, 2).start()

            self.sides(h, own)
        for k in self.early():
            self.sides(h, lambda zz, way, k=k: one(k, 1 - self.y, zz, way))

    def finish(self):
        for k in range(self.size):
            self.chain(self.z, self.y, k, sent, own=True)
            self.copy(self.z, self.y, k, 2, True).wait_send()
        for k in self.early():
            self.chain(self.z, 1 - self.y, k, sent)
        for k in range(self.cut):
            self.copy(self.z, 1 - self.y, k, 2).wait_recv()

        def tail(h, carry):
            def side(zz, way):
                for k in range(self.size):
                    self.chain(zz, self.y, k, sent, (way,))
                for k in self.early():
                    self.chain(zz, 1 - self.y, k, sent, (way,))
                for k in range(self.cut):
                    self.copy(zz, self.y, k, 2).wait_send()
                    self.copy(zz, 1 - self.y, k, 2).wait_recv()

            self.sides(h, side)
            return carry

        lax.fori_loop(1, self.nz, tail, 0)


class Hub(Gather):
    def __init__(self, n, src, out, send, recv):
        super().__init__(n, src, out, send, recv, src.shape[0])
        self.inner = jnp.logical_and(self.z >= 1, self.z <= self.nz - 2)
        self.edged = jnp.logical_or(self.z == 1, self.z == self.nz - 2)
        self.edge = jnp.where(self.z == 1, 0, self.nz - 1)

    def chain(self, zz, yy, k, act, ways=(0, 1), own=False):
        for way in ways:
            free = self.z <= self.nz - 3 if way == 0 else self.z >= 2

            @pl.when(free)
            def _(way=way):
                act(self.copy(zz, yy, k, way, own))

    def first(self):
        for k in range(self.size):
            self.chain(self.z, self.y, k, start, own=True)
        self.out[pl.ds(self.me * self.size, self.size)] = self.src[...]

    def across(self):
        for k in range(self.size):
            self.copy(self.z, self.y, k, 2, True).start()

    def onward(self, zz, way):
        last = jnp.logical_and(self.edged, zz == self.edge)
        free = self.z <= self.nz - 3 if way == 0 else self.z >= 2
        return jnp.logical_or(last, free)

    def hop(self, h):
        def own(zz, way):
            on = self.onward(zz, way)

            @pl.when(on)
            def _():
                for k in range(self.size):
                    self.copy(zz, self.y, k, 2).wait_recv()
                    self.chain(zz, self.y, k, start, (way,))

        self.sides(h, own)

    def across_edge(self):
        @pl.when(self.edged)
        def _():
            for k in range(self.size):
                self.copy(self.edge, self.y, k, 2).start()

    def finish(self):
        for k in range(self.size):
            self.chain(self.z, self.y, k, sent, own=True)

        @pl.when(self.inner)
        def _():
            for k in range(self.size):
                self.copy(self.z, self.y, k, 2, True).wait_send()
                self.copy(self.z, 1 - self.y, k, 2).wait_recv()

            @pl.when(self.edged)
            def _():
                for k in range(self.size):
                    self.copy(self.edge, self.y, k, 2).wait_send()
                    self.copy(self.edge, 1 - self.y, k, 2).wait_recv()

            def tail(h, carry):
                def side(zz, way):
                    on = self.onward(zz, way)
                    for k in range(self.size):
                        self.chain(zz, self.y, k, sent, (way,))

                        @pl.when(jnp.logical_not(on))
                        def _(k=k):
                            self.copy(zz, self.y, k, 2).wait_recv()

                self.sides(h, side)
                return carry

            lax.fori_loop(1, self.nz, tail, 0)


class Pick:
    def __init__(self, n, src, col, out, got, tab, send, recv, ps, pr):
        self.n, self.nz = n, n // 2
        self.me = lax.axis_index("ka")
        self.z, self.y = self.me // 2, self.me % 2
        self.src, self.col, self.out, self.got, self.tab = src, col, out, got, tab
        self.send, self.recv, self.ps, self.pr = send, recv, ps, pr
        self.size = src.shape[0]

    def copy(self, zz, k, way, own=False):
        at = zz * self.size + k
        target = (self.z + (1 if way == 0 else -1)) * 2 + self.y
        return remote(
            self.src.at[k] if own else self.col.at[at],
            self.col.at[at],
            self.send.at[way * self.nz * self.size + at],
            self.recv.at[at],
            {"ka": target},
        )

    def chain(self, zz, k, act, ways=(0, 1), own=False):
        for way in ways:
            free = self.z < self.nz - 1 if way == 0 else self.z > 0

            @pl.when(free)
            def _(way=way):
                act(self.copy(zz, k, way, own))

    def sides(self, h, act):
        for way in (0, 1):
            zz = self.z - h if way == 0 else self.z + h
            there = zz >= 0 if way == 0 else zz < self.nz

            @pl.when(there)
            def _(zz=zz, way=way):
                act(zz, way)

    def first(self):
        for k in range(self.size):
            self.chain(self.z, k, start, own=True)
        self.col[pl.ds(self.z * self.size, self.size)] = self.src[...]

    def hop(self, h):
        for k in range(self.size):

            def one(zz, way, k=k):
                self.copy(zz, k, way).wait_recv()
                self.chain(zz, k, start, (way,))

            self.sides(h, one)

    def chosen(self, zz, owner, r):
        which = self.tab[zz * 2 + self.y, owner * CAPQ + r]
        v = self.col[zz * self.size]
        for k in range(1, self.size):
            v = jnp.where(which == k, self.col[zz * self.size + k], v)
        return v

    def across(self, zz):
        rows = pl.ds(zz * CAPQ, CAPQ)
        return remote(
            self.out.at[rows],
            self.got.at[rows],
            self.ps.at[zz],
            self.pr.at[zz],
            {"ka": self.z * 2 + 1 - self.y},
        )

    def pass_on(self, zz):
        for r in range(CAPQ):
            self.out[zz * CAPQ + r] = self.chosen(zz, self.z * 2 + 1 - self.y, r)
        self.across(zz).start()

    def finish(self):
        for k in range(self.size):
            self.chain(self.z, k, sent, own=True)
        self.across(self.z).wait_send()

        def tail(h, carry):
            def side(zz, way):
                for k in range(self.size):
                    self.chain(zz, k, sent, (way,))
                self.across(zz).wait_send()

            self.sides(h, side)
            return carry

        lax.fori_loop(1, self.nz, tail, 0)


class Reduce:
    def __init__(self, part, out, recv1, tsend, recv2, s1, r1, s2, r2, per):
        self.g = lax.axis_index("ga")
        self.x, self.c = self.g // 2, self.g % 2
        self.part, self.out = part, out
        self.recv1, self.tsend, self.recv2 = recv1, tsend, recv2
        self.s1, self.r1, self.s2, self.r2, self.per = s1, r1, s2, r2, per

    def rows(self, i):
        return pl.ds(i * self.per, self.per)

    def one(self, t, i):
        xx = self.x if t else 1 - self.x
        return remote(
            self.part.at[xx * 2 + 1 - self.c, self.rows(i)],
            self.recv1.at[xx, self.rows(i)],
            self.s1.at[i * 2 + t],
            self.r1.at[i * 2 + t],
            {"ga": self.x * 2 + 1 - self.c},
        )

    def two(self, i):
        return remote(
            self.tsend.at[self.rows(i)],
            self.recv2.at[self.rows(i)],
            self.s2.at[i],
            self.r2.at[i],
            {"ga": (1 - self.x) * 2 + self.c},
        )

    def sum_one(self, xx, i):
        v = self.part[xx * 2 + self.c, self.rows(i)].astype(F32)
        return v + self.recv1[xx, self.rows(i)].astype(F32)

    def begin(self, i):
        self.one(0, i).start()
        self.one(1, i).start()

    def middle(self, i):
        self.one(0, i).wait_recv()
        self.tsend[self.rows(i)] = self.sum_one(1 - self.x, i).astype(self.tsend.dtype)
        self.two(i).start()

    def end(self, i):
        self.one(1, i).wait_recv()
        v = self.sum_one(self.x, i)
        self.two(i).wait_recv()
        v = v + self.recv2[self.rows(i)].astype(F32)
        self.out[self.rows(i)] = v.astype(self.out.dtype)
        self.one(0, i).wait_send()
        self.one(1, i).wait_send()
        self.two(i).wait_send()


def make_row(n, q_slots, per_dev, pairs_ref, qs_ref, row_ref, at_ref):
    rows = pairs_ref.shape[1]
    slots = n * CAPQ
    lane = lax.broadcasted_iota(I32, row_ref.shape, 1)
    section = lane // slots
    spot = lane % slots
    row = jnp.where(jnp.logical_or(section == 2, section == 4), -1, 0)
    holders = ([], [])
    for j in range(rows):
        slot = qs_ref[pairs_ref[2, j]]
        owner = slot // q_slots
        first, second = pairs_ref[0, j] % per_dev, pairs_ref[1, j]
        at = []
        for i, o in enumerate((owner, second // per_dev)):
            rank = jnp.int32(0)
            for other in holders[i]:
                rank = rank + jnp.where(other == o, 1, 0)
            holders[i].append(o)
            at.append(o * CAPQ + rank)
            at_ref[i, j] = at[i]
        value = jnp.where(section == 1, slot - owner * q_slots, second)
        value = jnp.where(jnp.logical_or(section == 0, section == 3), first, value)
        hit = spot == jnp.where(section < 3, at[0], at[1])
        row = jnp.where(hit, value, row)
    row_ref[...] = row


def kernel(n, pairs_ref, qs_ref, x_ref, y_ref, p_ref, v_ref, w_hbm, lines,
           tab, at_ref, row_ref, wt, w_ref, x_col, x_out, x_got, y_all, p_all, part, half,
           recv1, tsend, recv2, part2, own, q1, qt, q2, second, outbox, inbox,
           split, part3, eown, e1, et, e2, ebox, ein, emir,
           ws, ls, ts, tr, xs, xr, xps, xpr, ys, yr, ps, pr, s1, r1, s2, r2, t1, u1, t2, u2,
           v1, w1, v2, w2, es, er, fs, fr, as_, ar, gs, gr):
    per_dev, nt, width = x_ref.shape
    rows = pairs_ref.shape[1]
    q_slots = w_ref.shape[0]
    nz = n // 2
    slots = n * CAPQ
    n_ga = part.shape[0]
    me = lax.axis_index("ka")
    g = lax.axis_index("ga")
    z, y = me // 2, me % 2
    fetch = pltpu.make_async_copy(w_hbm, wt, ws)
    fetch.start()
    greet(n)
    xg = Pick(n, x_ref, x_col, x_out, x_got, tab, xs, xr, xps, xpr)
    yg = Gather(n, y_ref, y_all, ys, yr, per_dev - 1)
    pg = Hub(n, p_ref, p_all, ps, pr)
    outer = jnp.logical_not(pg.inner)
    xg.first()
    make_row(n, q_slots, per_dev, pairs_ref, qs_ref, row_ref, at_ref)
    keep = pltpu.make_async_copy(row_ref.at[0], tab.at[me], ls)
    keep.start()

    def row(i, whose):
        return remote(
            row_ref.at[0], tab.at[whose], ts.at[i], tr.at[whose], {"ka": lax.rem(me + i, n)}
        )

    lax.fori_loop(1, n, lambda i, c: (row(i, me).start(), c)[1], 0)
    keep.wait()
    xg.pass_on(z)

    yg.across_early()

    @pl.when(outer)
    def _():
        pg.first()
        yg.first()
        yg.across_late()

    @pl.when(pg.inner)
    def _():
        pg.across()

    fetch.wait()
    turn = 16
    whole = width // turn * turn

    def relay(i, carry):
        at = pl.ds(pl.multiple_of(i * turn, turn), turn)
        w_ref[:, at] = jnp.swapaxes(wt[at], 0, 1)
        return carry

    lax.fori_loop(0, width // turn, relay, 0)
    if whole < width:
        w_ref[:, whole:] = jnp.swapaxes(wt[whole:], 0, 1)
    red = Reduce(part, half, recv1, tsend, recv2, s1, r1, s2, r2, 2 * CAPQ)

    def multiply(v, a, r):
        w = tab[a, slots + me * CAPQ + r]
        v = jnp.dot(v, w_ref[w], preferred_element_type=F32)
        for i in range(n_ga):
            part[i, a * CAPQ + r] = v[:, i * width : (i + 1) * width].astype(part.dtype)

    def piece(zz):
        for r in range(CAPQ):
            multiply(xg.chosen(zz, me, r), zz * 2 + y, r)
        xg.across(zz).wait_recv()
        for r in range(CAPQ):
            multiply(x_got[zz * CAPQ + r], zz * 2 + 1 - y, r)
        red.begin(zz)

    quarter = nt // n_ga
    weight = v_ref[...].reshape(1, width)
    sets = jnp.where(pg.edged, 4, 2)
    ered = Reduce(part3, eown, e1, et, e2, v1, w1, v2, w2, 4 * nz)

    def of(q):
        return jnp.where(q // 2 == 0, z, pg.edge) * 2 + q % 2

    def joined(both, out, at):
        v = jnp.concatenate(both, axis=1)
        for i in range(n_ga):
            out[i, at] = v[i * quarter : (i + 1) * quarter]

    def exchange(q, carry):
        a = of(q)
        for k in range(per_dev):
            weighted = p_all[a * per_dev + k].astype(F32) * weight
            high = weighted.astype(BF16)
            split[k, :nt] = high
            split[k, nt:] = (weighted - high.astype(F32)).astype(BF16)

        def level(zz, carry):
            both = []
            for r in range(CAPQ):
                at = 3 * slots + (zz * 2 + y) * CAPQ + r
                k2 = jnp.maximum(tab[a, at + slots], 0)
                v = lax.dot_general(
                    split[tab[a, at]], p_all[k2], DIMS, preferred_element_type=F32
                )
                both.append(v[:nt] + v[nt:])
            joined(both, part3, q * nz + zz)
            return carry

        lax.fori_loop(0, nz, level, 0, unroll=2)
        return carry

    xg.hop(1)

    @pl.when(pg.inner)
    def _():
        pg.first()

    lax.fori_loop(
        1, n, lambda i, c: (row(i, lax.rem(me + n - i, n)).wait_recv(), c)[1], 0
    )
    xg.sides(1, lambda zz, way: xg.pass_on(zz))
    piece(z)

    def stage(h, carry):
        @pl.when(h < nz)
        def _():
            xg.hop(h)

        @pl.when(h == 2)
        def _():
            @pl.when(pg.inner)
            def _():
                lax.fori_loop(1, nz, lambda i, c: (pg.hop(i), c)[1], 0)
                yg.first()

            yg.second()

        @pl.when(h < nz)
        def _():
            xg.sides(h, lambda zz, way: xg.pass_on(zz))

        @pl.when(h == 2)
        def _():
            @pl.when(pg.inner)
            def _():
                pg.across_edge()
                yg.across_late()

            red.middle(z)

        @pl.when(h > 2)
        def _():
            xg.sides(h - 2, lambda zz, way: red.middle(zz))

        xg.sides(h - 1, lambda zz, way: piece(zz))

        @pl.when(h == 3)
        def _():
            pg.finish()

        @pl.when(h > 3)
        def _():
            yg.hop(h - 3)

        @pl.when(jnp.logical_and(jnp.logical_and(h >= 3, h <= 4), pg.inner))
        def _():
            low = (h - 3) * 2
            lax.fori_loop(low, jnp.minimum(low + 2, sets), exchange, 0)

            @pl.when(h == 4)
            def _():
                ered.begin(0)

        return carry

    lax.fori_loop(2, nz + 1, stage, 0)
    xg.sides(nz - 1, lambda zz, way: red.middle(zz))
    yg.hop(nz - 2)

    @pl.when(pg.inner)
    def _():
        ered.middle(0)

    yg.hop(nz - 1)
    xg.finish()
    lax.fori_loop(0, nz, lambda i, c: (red.end(i), c)[1], 0)
    yg.finish()
    lax.fori_loop(1, n, lambda i, c: (row(i, me).wait_send(), c)[1], 0)

    def source(a, carry):
        both = []
        for r in range(CAPQ):
            k2 = jnp.maximum(tab[a, 2 * slots + me * CAPQ + r], 0)
            both.append(
                lax.dot_general(half[a * CAPQ + r], y_all[k2], DIMS, preferred_element_type=F32)
            )
        joined(both, part2, a)
        return carry

    lax.fori_loop(0, n, source, 0, unroll=2)
    end = Reduce(part2, own, q1, qt, q2, t1, u1, t2, u2, n)
    end.begin(0)
    shape = own.shape[1:]
    left = lax.broadcasted_iota(I32, shape, 1) < nt
    doubles = per_dev // 2

    def paired(sums):
        sums = [v[:, :nt] + v[:, nt:] for v in sums]
        return [
            jnp.concatenate([sums[i], sums[i + doubles]], axis=1) for i in range(doubles)
        ]

    def seconds(a, carry):
        at = 2 * slots + me * CAPQ
        second[a] = jnp.where(left, tab[a, at], tab[a, at + 1])
        return carry

    lax.fori_loop(0, n, seconds, 0)

    def to_first(q):
        return remote(
            eown.at[pl.ds(q * nz, nz)], ein.at[y], es.at[q], er.at[y], {"ka": of(q)}
        )

    def to_second(zz):
        return remote(ebox.at[zz], emir.at[z], fs.at[zz], fr.at[z], {"ka": zz * 2 + y})

    def others(act):
        def one(q, carry):
            @pl.when(q != y)
            def _():
                act(to_first(q))

            return carry

        lax.fori_loop(0, sets, one, 0)

    def levels(act):
        def one(zz, carry):
            @pl.when(zz != z)
            def _():
                act(to_second(zz))

            return carry

        lax.fori_loop(0, nz, one, 0)

    @pl.when(pg.inner)
    def _():
        ered.end(0)
        others(start)
        ein[y] = eown[pl.ds(y * nz, nz)]

        def level(zz, carry):
            def add(q, sums):
                at = 4 * slots + (zz * 2 + y) * CAPQ
                k2 = jnp.where(left, tab[of(q), at], tab[of(q), at + 1])
                v = eown[q * nz + zz]
                base = (zz * 2 + y) * per_dev
                return tuple(
                    t + jnp.where(k2 == base + i, v, 0.0) for i, t in enumerate(sums)
                )

            sums = lax.fori_loop(
                0, sets, add, tuple(jnp.zeros(shape, F32) for _ in range(per_dev))
            )
            for i, v in enumerate(paired(sums)):
                ebox[zz, i] = v
            return carry

        lax.fori_loop(0, nz, level, 0)
        levels(start)
        emir[z] = ebox[z]

    end.middle(0)
    end.end(0)

    def fill(b, carry):
        outbox[b, 0] = own[b]

        def add(a, sums):
            out = []
            for i in range(per_dev):
                out.append(sums[i] + jnp.where(second[a] == b * per_dev + i, own[a], 0.0))
            return tuple(out)

        sums = tuple(jnp.zeros(shape, F32) for _ in range(per_dev))
        sums = lax.fori_loop(0, n, add, sums, unroll=min(n, 8))
        for i, v in enumerate(paired(sums)):
            outbox[b, 1 + i] = v
        return carry

    lax.fori_loop(0, n, fill, 0)

    def cross(i, whose):
        to = lax.rem(me + i, n)
        return remote(outbox.at[to], inbox.at[whose], as_.at[i], ar.at[whose], {"ka": to})

    lax.fori_loop(1, n, lambda i, c: (cross(i, me).start(), c)[1], 0)
    inbox[me] = outbox[me]
    for yy in range(2):

        @pl.when(jnp.logical_or(jnp.logical_not(pg.inner), yy != y))
        def _(yy=yy):
            remote(ein.at[yy], ein.at[yy], es.at[0], er.at[yy], {"ka": z * 2 + 1 - y}).wait_recv()

    def inner_level(zz, carry):
        @pl.when(zz != z)
        def _():
            remote(
                emir.at[zz], emir.at[zz], fs.at[0], fr.at[zz], {"ka": z * 2 + 1 - y}
            ).wait_recv()

        return carry

    lax.fori_loop(1, nz - 1, inner_level, 0)
    lax.fori_loop(1, n, lambda i, c: (cross(i, lax.rem(me + n - i, n)).wait_recv(), c)[1], 0)
    lax.fori_loop(1, n, lambda i, c: (cross(i, me).wait_send(), c)[1], 0)

    @pl.when(pg.inner)
    def _():
        others(sent)
        levels(sent)

    sub = quarter // 2

    def picked(ref, at, r):
        even = ref[at + (pl.ds(0, sub, stride=2),)]
        odd = ref[at + (pl.ds(1, sub, stride=2),)]
        zero = jnp.concatenate([even[:, :nt], odd[:, :nt]], axis=1)
        one = jnp.concatenate([even[:, nt:], odd[:, nt:]], axis=1)
        return jnp.where(r == 0, zero, one)

    for j in range(rows):
        at, et_ = at_ref[0, j], at_ref[1, j]
        b = et_ // CAPQ
        direct = picked(inbox, (at // CAPQ, 0), at % CAPQ)
        term = picked(ein, (b % 2, b // 2), et_ % CAPQ)
        lines[g, pl.ds(j * sub, sub)] = 2.0 * term - direct
    base = rows * sub
    for i in range(doubles):
        total = lax.fori_loop(
            1, n, lambda o, t, i=i: t + inbox[o, 1 + i], inbox[0, 1 + i]
        )
        term = lax.fori_loop(
            2, nz - 1, lambda zz, t, i=i: t + emir[zz, i], emir[1, i]
        )
        lines[g, pl.ds(base + i * quarter, quarter)] = 2.0 * term - total
    x, c = g // 2, g % 2
    mate, far = x * 2 + 1 - c, (1 - x) * 2 + c

    def spread(i, whose, to):
        return remote(lines.at[whose], lines.at[whose], gs.at[i], gr.at[i], {"ga": to})

    spread(0, g, far).start()
    spread(1, g, mate).start()
    spread(0, far, far).wait_recv()
    spread(2, far, mate).start()
    spread(1, mate, mate).wait_recv()
    spread(2, (1 - x) * 2 + 1 - c, mate).wait_recv()
    spread(0, g, far).wait_send()
    spread(1, g, mate).wait_send()
    spread(2, far, mate).wait_send()


def layout(lines, blocks_ref, mirr_ref, turned, flat):
    n_ga = lines.shape[0]
    rows, per_dev = blocks_ref.shape[0], mirr_ref.shape[0]
    nt = turned.shape[1]
    quarter, sub, doubles = nt // n_ga, nt // n_ga // 2, per_dev // 2
    base = rows * sub
    lanes = 2 * nt
    for q in range(n_ga):
        for t in range(sub):
            blocks_ref[:, (q * sub + t) * lanes : (q * sub + t + 1) * lanes] = lines[
                q, pl.ds(t, rows, stride=sub)
            ]
    for i in range(doubles):
        whole = jnp.concatenate(
            [lines[q, pl.ds(base + i * quarter, quarter)] for q in range(n_ga)], axis=0
        )
        turned[...] = whole.T
        even = turned[pl.ds(0, nt, stride=2)]
        odd = turned[pl.ds(1, nt, stride=2)]
        both = jnp.concatenate([even, odd], axis=1)
        flat[pl.ds(i * nt // 2, nt // 2)] = both[: nt // 2]
        flat[pl.ds((i + doubles) * nt // 2, nt // 2)] = both[nt // 2 :]
    for t in range(nt // 2):
        mirr_ref[:, t * lanes : (t + 1) * lanes] = flat[pl.ds(t, per_dev, stride=nt // 2)]


def per_device(x_dens, y_dens, p_dens, coulomb, screened, pairs, q_slot):
    n = lax.axis_size("ka")
    n_ga = lax.axis_size("ga")
    per_dev, nt, g = x_dens.shape
    q_slots = screened.shape[0]
    rows = pairs.shape[0]
    slots = n * CAPQ
    nz = n // 2
    shape = jax.ShapeDtypeStruct
    wide = F32 if slots * nt <= 2048 else BF16
    quarter = nt // n_ga
    each = (quarter, CAPQ * nt)
    line = (n,) + each
    dma = lambda m: pltpu.SemaphoreType.DMA((m,))
    row_len = -(-5 * slots // 128) * 128
    k_all = n * per_dev
    lines = pl.pallas_call(
        functools.partial(kernel, n),
        out_shape=shape((n_ga, rows * quarter // 2 + per_dev // 2 * quarter, CAPQ * nt), F32),
        in_specs=[SM, SM, VM, VM, VM, VM, HB],
        out_specs=VM,
        scratch_shapes=[
            pltpu.SMEM((n, row_len), I32),
            pltpu.SMEM((2, rows), I32),
            pltpu.VMEM((1, row_len), I32),
            pltpu.VMEM((g, q_slots, screened.shape[2]), BF16),
            pltpu.VMEM((q_slots, g, screened.shape[2]), BF16),
            pltpu.VMEM((nz * per_dev, nt, g), BF16),
            pltpu.VMEM((nz * CAPQ, nt, g), BF16),
            pltpu.VMEM((nz * CAPQ, nt, g), BF16),
            pltpu.VMEM((k_all, nt, g), BF16),
            pltpu.VMEM((k_all, nt, g), BF16),
            pltpu.VMEM((n_ga, slots, nt, g), wide),
            pltpu.VMEM((slots, nt, g), BF16),
            pltpu.VMEM((2, slots, nt, g), wide),
            pltpu.VMEM((slots, nt, g), BF16),
            pltpu.VMEM((slots, nt, g), BF16),
            pltpu.VMEM((n_ga,) + line, F32),
            pltpu.VMEM(line, F32),
            pltpu.VMEM((2,) + line, F32),
            pltpu.VMEM(line, F32),
            pltpu.VMEM(line, F32),
            pltpu.VMEM(line, I32),
            pltpu.VMEM((n, 1 + per_dev // 2) + each, F32),
            pltpu.VMEM((n, 1 + per_dev // 2) + each, F32),
            pltpu.VMEM((per_dev, 2 * nt, g), BF16),
            pltpu.VMEM((n_ga, 4 * nz) + each, F32),
            pltpu.VMEM((4 * nz,) + each, F32),
            pltpu.VMEM((2, 4 * nz) + each, F32),
            pltpu.VMEM((4 * nz,) + each, F32),
            pltpu.VMEM((4 * nz,) + each, F32),
            pltpu.VMEM((nz, per_dev // 2) + each, F32),
            pltpu.VMEM((2, nz) + each, F32),
            pltpu.VMEM((nz, per_dev // 2) + each, F32),
            pltpu.SemaphoreType.DMA,
            pltpu.SemaphoreType.DMA,
            dma(n), dma(n),
            dma(2 * nz * per_dev), dma(nz * per_dev),
            dma(nz), dma(nz),
            dma(3 * k_all), dma(k_all),
            dma(3 * k_all), dma(k_all),
            dma(2 * nz), dma(2 * nz), dma(nz), dma(nz),
            dma(2), dma(2), dma(1), dma(1),
            dma(2), dma(2), dma(1), dma(1),
            dma(4), dma(2), dma(nz), dma(nz),
            dma(n), dma(n),
            dma(3), dma(3),
        ],
        compiler_params=pltpu.CompilerParams(
            collective_id=0, has_side_effects=True, vmem_limit_bytes=LIMIT
        ),
        name="window",
    )(pairs.T, q_slot, x_dens, y_dens, p_dens, coulomb, screened.transpose(1, 0, 2))
    blocks, mirrored = pl.pallas_call(
        layout,
        out_shape=[shape((rows, nt * nt), F32), shape((per_dev, nt * nt), F32)],
        in_specs=[VM],
        out_specs=[VM, VM],
        scratch_shapes=[
            pltpu.VMEM((2 * nt, nt), F32),
            pltpu.VMEM((per_dev * nt // 2, 2 * nt), F32),
        ],
        name="layout",
    )(lines)
    return (blocks, mirrored)


def solution(mesh):
    in_specs = (
        P("ka", None, "ga"),
        P("ka", None, "ga"),
        P("ka", None, "ga"),
        P("ga"),
        P("ka", "ga", None),
        P("ka", None),
        P(),
    )
    out_specs = (P("ka", None), P("ka", None))
    return jax.shard_map(
        per_device, mesh=mesh, in_specs=in_specs, out_specs=out_specs, check_vma=False
    )
```

```python
import functools
import jax
import jax.numpy as jnp
from jax import lax
from jax.experimental import pallas as pl
from jax.experimental.pallas import tpu as pltpu
from jax.sharding import PartitionSpec as P

CAPQ = 2
F32 = jnp.float32
BF16 = jnp.bfloat16
I32 = jnp.int32
VM = pl.BlockSpec(memory_space=pltpu.VMEM)
SM = pl.BlockSpec(memory_space=pltpu.SMEM)
HB = pl.BlockSpec(memory_space=pl.ANY)
LIMIT = 66000000
DIMS = (((1,), (1,)), ((), ()))


def start(c):
    c.start()


def sent(c):
    c.wait_send()


def remote(src, dst, ss, rs, to):
    return pltpu.make_async_remote_copy(
        src_ref=src,
        dst_ref=dst,
        send_sem=ss,
        recv_sem=rs,
        device_id=to,
        device_id_type=pl.DeviceIdType.MESH,
    )


def greet(n):
    barrier = pltpu.get_barrier_semaphore()
    me = lax.axis_index("ka")
    g = lax.axis_index("ga")
    n_ga = lax.axis_size("ga")

    def hello(to):
        pl.semaphore_signal(barrier, inc=1, device_id=to, device_id_type=pl.DeviceIdType.MESH)

    lax.fori_loop(1, n, lambda i, c: (hello({"ka": lax.rem(me + i, n)}), c)[1], 0)
    for i in range(1, n_ga):
        hello({"ga": lax.rem(g + i, n_ga)})
    pl.semaphore_wait(barrier, n - 1 + n_ga - 1)


class Gather:
    def __init__(self, n, src, out, send, recv, cut):
        self.n, self.nz = n, n // 2
        self.me = lax.axis_index("ka")
        self.z, self.y = self.me // 2, self.me % 2
        self.src, self.out, self.send, self.recv = src, out, send, recv
        self.size = src.shape[0]
        self.cut = cut

    def copy(self, zz, yy, k, way, own=False):
        at = (zz * 2 + yy) * self.size + k
        block = self.out.at[at]
        if way == 2:
            target = self.z * 2 + 1 - self.y
        else:
            target = (self.z + (1 if way == 0 else -1)) * 2 + self.y
        return remote(
            self.src.at[k] if own else block,
            block,
            self.send.at[way * self.n + zz * 2 + yy],
            self.recv.at[at],
            {"ka": target},
        )

    def all_sent(self, zz, yy, way, count):
        block = self.out.at[pl.ds((zz * 2 + yy) * self.size, count)]
        done = self.send.at[way * self.n + zz * 2 + yy]
        remote(block, block, done, done, {"ka": self.z * 2 + 1 - self.y}).wait_send()

    def chained(self, zz, yy, count, ways=(0, 1)):
        for way in ways:
            free = self.z < self.nz - 1 if way == 0 else self.z > 0

            @pl.when(free)
            def _(way=way):
                self.all_sent(zz, yy, way, count)

    def chain(self, zz, yy, k, act, ways=(0, 1), own=False):
        for way in ways:
            free = self.z < self.nz - 1 if way == 0 else self.z > 0

            @pl.when(free)
            def _(way=way):
                act(self.copy(zz, yy, k, way, own))

    def early(self):
        return range(self.cut, self.size)

    def across_early(self):
        for k in self.early():
            self.copy(self.z, self.y, k, 2, True).start()

    def across_late(self):
        for k in range(self.cut):
            self.copy(self.z, self.y, k, 2, True).start()
        self.out[pl.ds(self.me * self.size, self.size)] = self.src[...]

    def first(self):
        for k in range(self.size):
            self.chain(self.z, self.y, k, start, own=True)

    def second(self):
        for k in self.early():
            self.copy(self.z, 1 - self.y, k, 2).wait_recv()
            self.chain(self.z, 1 - self.y, k, start)

    def sides(self, h, act):
        for way in (0, 1):
            zz = self.z - h if way == 0 else self.z + h
            there = zz >= 0 if way == 0 else zz < self.nz

            @pl.when(there)
            def _(zz=zz, way=way):
                act(zz, way)

    def hop(self, h):
        def one(k, yy, zz, way):
            self.copy(zz, yy, k, 2).wait_recv()
            self.chain(zz, yy, k, start, (way,))

        for k in range(self.size):

            def own(zz, way, k=k):
                one(k, self.y, zz, way)
                if k < self.cut:
                    self.copy(zz, self.y, k, 2).start()

            self.sides(h, own)
        for k in self.early():
            self.sides(h, lambda zz, way, k=k: one(k, 1 - self.y, zz, way))

    def finish(self):
        few = len(self.early())
        self.chained(self.z, self.y, self.size)
        self.all_sent(self.z, self.y, 2, self.size)
        self.chained(self.z, 1 - self.y, few)
        for k in range(self.cut):
            self.copy(self.z, 1 - self.y, k, 2).wait_recv()

        def tail(h, carry):
            def side(zz, way):
                self.chained(zz, self.y, self.size, (way,))
                self.chained(zz, 1 - self.y, few, (way,))
                self.all_sent(zz, self.y, 2, self.cut)
                for k in range(self.cut):
                    self.copy(zz, 1 - self.y, k, 2).wait_recv()

            self.sides(h, side)
            return carry

        lax.fori_loop(1, self.nz, tail, 0)


class Hub(Gather):
    def __init__(self, n, src, out, send, recv):
        super().__init__(n, src, out, send, recv, src.shape[0])
        self.inner = jnp.logical_and(self.z >= 1, self.z <= self.nz - 2)
        self.edged = jnp.logical_or(self.z == 1, self.z == self.nz - 2)
        self.edge = jnp.where(self.z == 1, 0, self.nz - 1)

    def copy(self, zz, yy, k, way, own=False):
        base = (zz * 2 + yy) * self.size
        target = (self.z + (1 if way == 0 else -1)) * 2 + self.y
        return remote(
            self.src.at[k] if own else self.out.at[base + k],
            self.out.at[base + k],
            self.send.at[way * self.nz + zz],
            self.recv.at[zz * self.size + k],
            {"ka": target},
        )

    def cross(self, zz, yy, i):
        block = self.out.at[pl.ds((zz * 2 + yy) * self.size, self.size)]
        return remote(
            self.src if i == 0 and yy is self.y else block,
            block,
            self.send.at[2 * self.nz + i],
            self.recv.at[self.nz * self.size + i],
            {"ka": self.z * 2 + 1 - self.y},
        )

    def all_sent(self, zz, yy, way, count):
        block = self.out.at[pl.ds((zz * 2 + yy) * self.size, count)]
        done = self.send.at[way * self.nz + zz]
        remote(block, block, done, done, {"ka": self.z * 2 + 1 - self.y}).wait_send()

    def chained(self, zz, yy, count, ways=(0, 1)):
        for way in ways:
            free = self.z <= self.nz - 3 if way == 0 else self.z >= 2

            @pl.when(free)
            def _(way=way):
                self.all_sent(zz, yy, way, count)

    def chain(self, zz, yy, k, act, ways=(0, 1), own=False):
        for way in ways:
            free = self.z <= self.nz - 3 if way == 0 else self.z >= 2

            @pl.when(free)
            def _(way=way):
                act(self.copy(zz, yy, k, way, own))

    def first(self):
        for k in range(self.size):
            self.chain(self.z, self.y, k, start, own=True)
        self.out[pl.ds(self.me * self.size, self.size)] = self.src[...]

    def across(self):
        self.cross(self.z, self.y, 0).start()

    def onward(self, zz, way):
        last = jnp.logical_and(self.edged, zz == self.edge)
        free = self.z <= self.nz - 3 if way == 0 else self.z >= 2
        return jnp.logical_or(last, free)

    def hop(self, h):
        def own(zz, way):
            on = self.onward(zz, way)

            @pl.when(on)
            def _():
                for k in range(self.size):
                    self.copy(zz, self.y, k, way).wait_recv()
                    self.chain(zz, self.y, k, start, (way,))

        self.sides(h, own)

    def across_edge(self):
        @pl.when(self.edged)
        def _():
            self.cross(self.edge, self.y, 1).start()

    def finish(self):
        self.chained(self.z, self.y, self.size)

        @pl.when(self.inner)
        def _():
            self.cross(self.z, self.y, 0).wait_send()
            self.cross(self.z, 1 - self.y, 0).wait_recv()

            @pl.when(self.edged)
            def _():
                self.cross(self.edge, self.y, 1).wait_send()
                self.cross(self.edge, 1 - self.y, 1).wait_recv()

            def tail(h, carry):
                def side(zz, way):
                    self.chained(zz, self.y, self.size, (way,))

                    @pl.when(jnp.logical_not(self.onward(zz, way)))
                    def _():
                        for k in range(self.size):
                            self.copy(zz, self.y, k, way).wait_recv()

                self.sides(h, side)
                return carry

            lax.fori_loop(1, self.nz, tail, 0)


class Pick:
    def __init__(self, n, src, col, out, got, tab, send, recv, ps, pr):
        self.n, self.nz = n, n // 2
        self.me = lax.axis_index("ka")
        self.z, self.y = self.me // 2, self.me % 2
        self.src, self.col, self.out, self.got, self.tab = src, col, out, got, tab
        self.send, self.recv, self.ps, self.pr = send, recv, ps, pr
        self.size = src.shape[0]

    def copy(self, zz, k, way, own=False):
        at = zz * self.size + k
        target = (self.z + (1 if way == 0 else -1)) * 2 + self.y
        return remote(
            self.src.at[k] if own else self.col.at[at],
            self.col.at[at],
            self.send.at[way * self.nz + zz],
            self.recv.at[at],
            {"ka": target},
        )

    def chain(self, zz, k, act, ways=(0, 1), own=False):
        for way in ways:
            free = self.z < self.nz - 1 if way == 0 else self.z > 0

            @pl.when(free)
            def _(way=way):
                act(self.copy(zz, k, way, own))

    def sides(self, h, act):
        for way in (0, 1):
            zz = self.z - h if way == 0 else self.z + h
            there = zz >= 0 if way == 0 else zz < self.nz

            @pl.when(there)
            def _(zz=zz, way=way):
                act(zz, way)

    def first(self):
        for k in range(self.size):
            self.chain(self.z, k, start, own=True)
        self.col[pl.ds(self.z * self.size, self.size)] = self.src[...]

    def hop(self, h):
        for k in range(self.size):

            def one(zz, way, k=k):
                self.copy(zz, k, way).wait_recv()
                self.chain(zz, k, start, (way,))

            self.sides(h, one)

    def chosen(self, zz, owner, r):
        which = self.tab[zz * 2 + self.y, owner * CAPQ + r]
        v = self.col[zz * self.size]
        for k in range(1, self.size):
            v = jnp.where(which == k, self.col[zz * self.size + k], v)
        return v

    def across(self, zz):
        rows = pl.ds(zz * CAPQ, CAPQ)
        return remote(
            self.out.at[rows],
            self.got.at[rows],
            self.ps.at[zz],
            self.pr.at[zz],
            {"ka": self.z * 2 + 1 - self.y},
        )

    def pass_on(self, zz):
        for r in range(CAPQ):
            self.out[zz * CAPQ + r] = self.chosen(zz, self.z * 2 + 1 - self.y, r)
        self.across(zz).start()

    def chained(self, zz, ways=(0, 1)):
        block = self.col.at[pl.ds(zz * self.size, self.size)]
        for way in ways:
            free = self.z < self.nz - 1 if way == 0 else self.z > 0
            done = self.send.at[way * self.nz + zz]

            @pl.when(free)
            def _(done=done):
                remote(block, block, done, done, {"ka": self.z * 2 + 1 - self.y}).wait_send()

    def finish(self):
        self.chained(self.z)
        self.across(self.z).wait_send()

        def tail(h, carry):
            def side(zz, way):
                self.chained(zz, (way,))
                self.across(zz).wait_send()

            self.sides(h, side)
            return carry

        lax.fori_loop(1, self.nz, tail, 0)


class Reduce:
    def __init__(self, part, out, recv1, tsend, recv2, s1, r1, s2, r2, per):
        self.g = lax.axis_index("ga")
        self.x, self.c = self.g // 2, self.g % 2
        self.part, self.out = part, out
        self.recv1, self.tsend, self.recv2 = recv1, tsend, recv2
        self.s1, self.r1, self.s2, self.r2, self.per = s1, r1, s2, r2, per

    def rows(self, i):
        return pl.ds(i * self.per, self.per)

    def one(self, t, i):
        xx = self.x if t else 1 - self.x
        return remote(
            self.part.at[xx * 2 + 1 - self.c, self.rows(i)],
            self.recv1.at[xx, self.rows(i)],
            self.s1,
            self.r1.at[i * 2 + t],
            {"ga": self.x * 2 + 1 - self.c},
        )

    def two(self, i):
        return remote(
            self.tsend.at[self.rows(i)],
            self.recv2.at[self.rows(i)],
            self.s2,
            self.r2.at[i],
            {"ga": (1 - self.x) * 2 + self.c},
        )

    def sum_one(self, xx, i):
        v = self.part[xx * 2 + self.c, self.rows(i)].astype(F32)
        return v + self.recv1[xx, self.rows(i)].astype(F32)

    def begin(self, i):
        self.one(0, i).start()
        self.one(1, i).start()

    def middle(self, i):
        self.one(0, i).wait_recv()
        self.tsend[self.rows(i)] = self.sum_one(1 - self.x, i).astype(self.tsend.dtype)
        self.two(i).start()

    def end(self, i):
        self.one(1, i).wait_recv()
        v = self.sum_one(self.x, i)
        self.two(i).wait_recv()
        v = v + self.recv2[self.rows(i)].astype(F32)
        self.out[self.rows(i)] = v.astype(self.out.dtype)

    def finish(self):
        to = {"ga": self.x * 2 + 1 - self.c}
        both = self.part.at[pl.ds(0, 2)]
        remote(both, both, self.s1, self.s1, to).wait_send()
        remote(self.tsend, self.tsend, self.s2, self.s2, to).wait_send()


def make_row(n, q_slots, per_dev, pairs_ref, qs_ref, row_ref, at_ref):
    rows = pairs_ref.shape[1]
    slots = n * CAPQ
    lane = lax.broadcasted_iota(I32, row_ref.shape, 1)
    section = lane // slots
    spot = lane % slots
    row = jnp.where(jnp.logical_or(section == 2, section == 4), -1, 0)
    holders = ([], [])
    for j in range(rows):
        slot = qs_ref[pairs_ref[2, j]]
        owner = slot // q_slots
        first, second = pairs_ref[0, j] % per_dev, pairs_ref[1, j]
        at = []
        for i, o in enumerate((owner, second // per_dev)):
            rank = jnp.int32(0)
            for other in holders[i]:
                rank = rank + jnp.where(other == o, 1, 0)
            holders[i].append(o)
            at.append(o * CAPQ + rank)
            at_ref[i, j] = at[i]
        value = jnp.where(section == 1, slot - owner * q_slots, second)
        value = jnp.where(jnp.logical_or(section == 0, section == 3), first, value)
        hit = spot == jnp.where(section < 3, at[0], at[1])
        row = jnp.where(hit, value, row)
    row_ref[...] = row


def kernel(n, pairs_ref, qs_ref, x_ref, y_ref, p_ref, v_ref, w_hbm, lines,
           tab, at_ref, row_ref, wt, w_ref, x_col, x_out, x_got, y_all, p_all, part, half,
           recv1, tsend, recv2, part2, own, q1, qt, q2, second, outbox, sumbox, inbox,
           split, part3, eown, e1, et, e2, ebox, ein, emir,
           ws, ls, ts, tr, xs, xr, xps, xpr, ys, yr, ps, pr, s1, r1, s2, r2, t1, u1, t2, u2,
           v1, w1, v2, w2, es, er, fs, fr, as_, ar, bs, br, gs, gr):
    per_dev, nt, width = x_ref.shape
    rows = pairs_ref.shape[1]
    q_slots = w_ref.shape[0]
    nz = n // 2
    slots = n * CAPQ
    n_ga = part.shape[0]
    me = lax.axis_index("ka")
    g = lax.axis_index("ga")
    z, y = me // 2, me % 2
    fetch = pltpu.make_async_copy(w_hbm, wt, ws)
    fetch.start()
    greet(n)
    xg = Pick(n, x_ref, x_col, x_out, x_got, tab, xs, xr, xps, xpr)
    yg = Gather(n, y_ref, y_all, ys, yr, per_dev - 1)
    pg = Hub(n, p_ref, p_all, ps, pr)
    outer = jnp.logical_not(pg.inner)
    xg.first()
    make_row(n, q_slots, per_dev, pairs_ref, qs_ref, row_ref, at_ref)
    keep = pltpu.make_async_copy(row_ref.at[0], tab.at[me], ls)
    keep.start()

    def row(i, whose):
        return remote(
            row_ref.at[0], tab.at[whose], ts.at[i], tr.at[whose], {"ka": lax.rem(me + i, n)}
        )

    lax.fori_loop(1, n, lambda i, c: (row(i, me).start(), c)[1], 0)
    keep.wait()
    xg.pass_on(z)

    yg.across_early()

    @pl.when(outer)
    def _():
        pg.first()
        yg.first()
        yg.across_late()

    @pl.when(pg.inner)
    def _():
        pg.across()

    fetch.wait()
    turn = 16
    whole = width // turn * turn

    def relay(i, carry):
        at = pl.ds(pl.multiple_of(i * turn, turn), turn)
        w_ref[:, at] = jnp.swapaxes(wt[at], 0, 1)
        return carry

    lax.fori_loop(0, width // turn, relay, 0)
    if whole < width:
        w_ref[:, whole:] = jnp.swapaxes(wt[whole:], 0, 1)
    red = Reduce(part, half, recv1, tsend, recv2, s1, r1, s2, r2, 2 * CAPQ)

    def multiply(v, a, r):
        w = tab[a, slots + me * CAPQ + r]
        v = jnp.dot(v, w_ref[w], preferred_element_type=F32)
        for i in range(n_ga):
            part[i, a * CAPQ + r] = v[:, i * width : (i + 1) * width].astype(part.dtype)

    def piece(zz):
        for r in range(CAPQ):
            multiply(xg.chosen(zz, me, r), zz * 2 + y, r)
        xg.across(zz).wait_recv()
        for r in range(CAPQ):
            multiply(x_got[zz * CAPQ + r], zz * 2 + 1 - y, r)
        red.begin(zz)

    quarter = nt // n_ga
    weight = v_ref[...].reshape(1, width)
    sets = jnp.where(pg.edged, 4, 2)
    ered = Reduce(part3, eown, e1, et, e2, v1, w1, v2, w2, 4 * nz)

    def of(q):
        return jnp.where(q // 2 == 0, z, pg.edge) * 2 + q % 2

    def joined(both, out, at):
        v = jnp.concatenate(both, axis=1)
        for i in range(n_ga):
            out[i, at] = v[i * quarter : (i + 1) * quarter]

    def exchange(q, carry):
        a = of(q)
        for k in range(per_dev):
            weighted = p_all[a * per_dev + k].astype(F32) * weight
            high = weighted.astype(BF16)
            split[k, :nt] = high
            split[k, nt:] = (weighted - high.astype(F32)).astype(BF16)

        def level(zz, carry):
            both = []
            for r in range(CAPQ):
                at = 3 * slots + (zz * 2 + y) * CAPQ + r
                k2 = jnp.maximum(tab[a, at + slots], 0)
                v = lax.dot_general(
                    split[tab[a, at]], p_all[k2], DIMS, preferred_element_type=F32
                )
                both.append(v[:nt] + v[nt:])
            joined(both, part3, q * nz + zz)
            return carry

        lax.fori_loop(0, nz, level, 0, unroll=2)
        return carry

    xg.hop(1)

    @pl.when(pg.inner)
    def _():
        pg.first()

    lax.fori_loop(
        1, n, lambda i, c: (row(i, lax.rem(me + n - i, n)).wait_recv(), c)[1], 0
    )
    xg.sides(1, lambda zz, way: xg.pass_on(zz))
    piece(z)

    def stage(h, carry):
        @pl.when(h < nz)
        def _():
            xg.hop(h)

        @pl.when(h == 2)
        def _():
            @pl.when(pg.inner)
            def _():
                lax.fori_loop(1, nz, lambda i, c: (pg.hop(i), c)[1], 0)
                yg.first()

            yg.second()

        @pl.when(h < nz)
        def _():
            xg.sides(h, lambda zz, way: xg.pass_on(zz))

        @pl.when(h == 2)
        def _():
            @pl.when(pg.inner)
            def _():
                pg.across_edge()
                yg.across_late()

            red.middle(z)

        @pl.when(h > 2)
        def _():
            xg.sides(h - 2, lambda zz, way: red.middle(zz))

        xg.sides(h - 1, lambda zz, way: piece(zz))

        @pl.when(jnp.logical_and(h >= 3, h < nz))
        def _():
            yg.hop(h - 2)

        return carry

    lax.fori_loop(2, nz + 1, stage, 0)
    pg.finish()

    @pl.when(pg.inner)
    def _():
        lax.fori_loop(0, 2, exchange, 0)

    xg.sides(nz - 1, lambda zz, way: red.middle(zz))
    yg.hop(nz - 2)

    @pl.when(pg.inner)
    def _():
        lax.fori_loop(2, sets, exchange, 0)
        ered.begin(0)

    yg.hop(nz - 1)

    @pl.when(pg.inner)
    def _():
        ered.middle(0)

    xg.finish()
    lax.fori_loop(0, nz, lambda i, c: (red.end(i), c)[1], 0)
    yg.finish()
    lax.fori_loop(1, n, lambda i, c: (row(i, me).wait_send(), c)[1], 0)
    red.finish()

    def source(a, carry):
        both = []
        for r in range(CAPQ):
            k2 = jnp.maximum(tab[a, 2 * slots + me * CAPQ + r], 0)
            both.append(
                lax.dot_general(half[a * CAPQ + r], y_all[k2], DIMS, preferred_element_type=F32)
            )
        joined(both, part2, a)
        return carry

    end = Reduce(part2, own, q1, qt, q2, t1, u1, t2, u2, n // 2)
    for i in range(2):
        lax.fori_loop(i * n // 2, (i + 1) * n // 2, source, 0, unroll=2)
        end.begin(i)
    shape = own.shape[1:]
    left = lax.broadcasted_iota(I32, shape, 1) < nt
    doubles = per_dev // 2

    def paired(sums):
        sums = [v[:, :nt] + v[:, nt:] for v in sums]
        return [
            jnp.concatenate([sums[i], sums[i + doubles]], axis=1) for i in range(doubles)
        ]

    def seconds(a, carry):
        at = 2 * slots + me * CAPQ
        second[a] = jnp.where(left, tab[a, at], tab[a, at + 1])
        return carry

    lax.fori_loop(0, n, seconds, 0)

    def to_first(q):
        return remote(
            eown.at[pl.ds(q * nz, nz)], ein.at[y], es.at[q], er.at[y], {"ka": of(q)}
        )

    def to_second(zz):
        return remote(ebox.at[zz], emir.at[z], fs, fr.at[z], {"ka": zz * 2 + y})

    def others(act):
        def one(q, carry):
            @pl.when(q != y)
            def _():
                act(to_first(q))

            return carry

        lax.fori_loop(0, sets, one, 0)

    def levels(act):
        def one(zz, carry):
            @pl.when(zz != z)
            def _():
                act(to_second(zz))

            return carry

        lax.fori_loop(0, nz, one, 0)

    @pl.when(pg.inner)
    def _():
        ered.end(0)
        ered.finish()
        others(start)
        ein[y] = eown[pl.ds(y * nz, nz)]

        def level(zz, carry):
            def add(q, sums):
                at = 4 * slots + (zz * 2 + y) * CAPQ
                k2 = jnp.where(left, tab[of(q), at], tab[of(q), at + 1])
                v = eown[q * nz + zz]
                base = (zz * 2 + y) * per_dev
                return tuple(
                    t + jnp.where(k2 == base + i, v, 0.0) for i, t in enumerate(sums)
                )

            sums = lax.fori_loop(
                0, sets, add, tuple(jnp.zeros(shape, F32) for _ in range(per_dev))
            )
            for i, v in enumerate(paired(sums)):
                ebox[zz, i] = v
            return carry

        lax.fori_loop(0, nz, level, 0)
        levels(start)
        emir[z] = ebox[z]

    end.middle(0)
    end.middle(1)

    def cross(src, box, i, whose, ss, rs):
        to = lax.rem(me + i, n)
        return remote(src.at[to], box.at[whose], ss, rs.at[whose], {"ka": to})

    end.end(0)
    end.end(1)
    end.finish()
    lax.fori_loop(1, n, lambda i, c: (cross(own, inbox, i, me, as_, ar).start(), c)[1], 0)
    inbox[me] = own[me]

    def fill(i, carry):
        b = lax.rem(me + i, n)

        def add(a, sums):
            out = []
            for i in range(per_dev):
                out.append(sums[i] + jnp.where(second[a] == b * per_dev + i, own[a], 0.0))
            return tuple(out)

        sums = tuple(jnp.zeros(shape, F32) for _ in range(per_dev))
        sums = lax.fori_loop(0, n, add, sums, unroll=min(n, 8))
        for i_, v in enumerate(paired(sums)):
            outbox[b, i_] = v

        @pl.when(i > 0)
        def _():
            cross(outbox, sumbox, i, me, bs, br).start()

        return carry

    lax.fori_loop(1, n, fill, 0)
    fill(jnp.int32(0), 0)
    sumbox[me] = outbox[me]
    for yy in range(2):

        @pl.when(jnp.logical_or(jnp.logical_not(pg.inner), yy != y))
        def _(yy=yy):
            remote(ein.at[yy], ein.at[yy], es.at[0], er.at[yy], {"ka": z * 2 + 1 - y}).wait_recv()

    def inner_level(zz, carry):
        @pl.when(zz != z)
        def _():
            remote(
                emir.at[zz], emir.at[zz], fs, fr.at[zz], {"ka": z * 2 + 1 - y}
            ).wait_recv()

        return carry

    lax.fori_loop(1, nz - 1, inner_level, 0)
    for box, src, ss, rs in ((inbox, own, as_, ar), (sumbox, outbox, bs, br)):

        def arrived(i, carry, box=box, src=src, ss=ss, rs=rs):
            cross(src, box, i, lax.rem(me + n - i, n), ss, rs).wait_recv()
            return carry

        lax.fori_loop(1, n, arrived, 0)
        rest = src.at[pl.ds(0, n - 1)]
        remote(rest, rest, ss, ss, {"ka": z * 2 + 1 - y}).wait_send()

    @pl.when(pg.inner)
    def _():
        others(sent)
        rest = ebox.at[pl.ds(0, nz - 1)]
        remote(rest, rest, fs, fs, {"ka": z * 2 + 1 - y}).wait_send()

    sub = quarter // 2

    def picked(ref, at, r):
        even = ref[at + (pl.ds(0, sub, stride=2),)]
        odd = ref[at + (pl.ds(1, sub, stride=2),)]
        zero = jnp.concatenate([even[:, :nt], odd[:, :nt]], axis=1)
        one = jnp.concatenate([even[:, nt:], odd[:, nt:]], axis=1)
        return jnp.where(r == 0, zero, one)

    for j in range(rows):
        at, et_ = at_ref[0, j], at_ref[1, j]
        b = et_ // CAPQ
        direct = picked(inbox, (at // CAPQ,), at % CAPQ)
        term = picked(ein, (b % 2, b // 2), et_ % CAPQ)
        lines[g, pl.ds(j * sub, sub)] = 2.0 * term - direct
    base = rows * sub
    for i in range(doubles):
        total = lax.fori_loop(
            1, n, lambda o, t, i=i: t + sumbox[o, i], sumbox[0, i]
        )
        term = lax.fori_loop(
            2, nz - 1, lambda zz, t, i=i: t + emir[zz, i], emir[1, i]
        )
        lines[g, pl.ds(base + i * quarter, quarter)] = 2.0 * term - total
    x, c = g // 2, g % 2
    mate, far = x * 2 + 1 - c, (1 - x) * 2 + c

    def spread(i, whose, to):
        return remote(lines.at[whose], lines.at[whose], gs.at[i], gr.at[i], {"ga": to})

    spread(0, g, far).start()
    spread(1, g, mate).start()
    spread(0, far, far).wait_recv()
    spread(2, far, mate).start()
    spread(1, mate, mate).wait_recv()
    spread(2, (1 - x) * 2 + 1 - c, mate).wait_recv()
    spread(0, g, far).wait_send()
    spread(1, g, mate).wait_send()
    spread(2, far, mate).wait_send()


def layout(lines, blocks_ref, mirr_ref, turned, flat):
    n_ga = lines.shape[0]
    rows, per_dev = blocks_ref.shape[0], mirr_ref.shape[0]
    nt = turned.shape[1]
    quarter, sub, doubles = nt // n_ga, nt // n_ga // 2, per_dev // 2
    base = rows * sub
    lanes = 2 * nt
    for q in range(n_ga):
        for t in range(sub):
            blocks_ref[:, (q * sub + t) * lanes : (q * sub + t + 1) * lanes] = lines[
                q, pl.ds(t, rows, stride=sub)
            ]
    for i in range(doubles):
        whole = jnp.concatenate(
            [lines[q, pl.ds(base + i * quarter, quarter)] for q in range(n_ga)], axis=0
        )
        turned[...] = whole.T
        even = turned[pl.ds(0, nt, stride=2)]
        odd = turned[pl.ds(1, nt, stride=2)]
        both = jnp.concatenate([even, odd], axis=1)
        flat[pl.ds(i * nt // 2, nt // 2)] = both[: nt // 2]
        flat[pl.ds((i + doubles) * nt // 2, nt // 2)] = both[nt // 2 :]
    for t in range(nt // 2):
        mirr_ref[:, t * lanes : (t + 1) * lanes] = flat[pl.ds(t, per_dev, stride=nt // 2)]


def per_device(x_dens, y_dens, p_dens, coulomb, screened, pairs, q_slot):
    n = lax.axis_size("ka")
    n_ga = lax.axis_size("ga")
    per_dev, nt, g = x_dens.shape
    q_slots = screened.shape[0]
    rows = pairs.shape[0]
    slots = n * CAPQ
    nz = n // 2
    shape = jax.ShapeDtypeStruct
    wide = F32 if slots * nt <= 2048 else BF16
    quarter = nt // n_ga
    each = (quarter, CAPQ * nt)
    line = (n,) + each
    dma = lambda m: pltpu.SemaphoreType.DMA((m,))
    one = pltpu.SemaphoreType.DMA
    row_len = -(-5 * slots // 128) * 128
    k_all = n * per_dev
    lines = pl.pallas_call(
        functools.partial(kernel, n),
        out_shape=shape((n_ga, rows * quarter // 2 + per_dev // 2 * quarter, CAPQ * nt), F32),
        in_specs=[SM, SM, VM, VM, VM, VM, HB],
        out_specs=VM,
        scratch_shapes=[
            pltpu.SMEM((n, row_len), I32),
            pltpu.SMEM((2, rows), I32),
            pltpu.VMEM((1, row_len), I32),
            pltpu.VMEM((g, q_slots, screened.shape[2]), BF16),
            pltpu.VMEM((q_slots, g, screened.shape[2]), BF16),
            pltpu.VMEM((nz * per_dev, nt, g), BF16),
            pltpu.VMEM((nz * CAPQ, nt, g), BF16),
            pltpu.VMEM((nz * CAPQ, nt, g), BF16),
            pltpu.VMEM((k_all, nt, g), BF16),
            pltpu.VMEM((k_all, nt, g), BF16),
            pltpu.VMEM((n_ga, slots, nt, g), wide),
            pltpu.VMEM((slots, nt, g), BF16),
            pltpu.VMEM((2, slots, nt, g), wide),
            pltpu.VMEM((slots, nt, g), BF16),
            pltpu.VMEM((slots, nt, g), BF16),
            pltpu.VMEM((n_ga,) + line, F32),
            pltpu.VMEM(line, F32),
            pltpu.VMEM((2,) + line, F32),
            pltpu.VMEM(line, F32),
            pltpu.VMEM(line, F32),
            pltpu.VMEM(line, I32),
            pltpu.VMEM((n, per_dev // 2) + each, F32),
            pltpu.VMEM((n, per_dev // 2) + each, F32),
            pltpu.VMEM(line, F32),
            pltpu.VMEM((per_dev, 2 * nt, g), BF16),
            pltpu.VMEM((n_ga, 4 * nz) + each, F32),
            pltpu.VMEM((4 * nz,) + each, F32),
            pltpu.VMEM((2, 4 * nz) + each, F32),
            pltpu.VMEM((4 * nz,) + each, F32),
            pltpu.VMEM((4 * nz,) + each, F32),
            pltpu.VMEM((nz, per_dev // 2) + each, F32),
            pltpu.VMEM((2, nz) + each, F32),
            pltpu.VMEM((nz, per_dev // 2) + each, F32),
            one, one,
            dma(n), dma(n),
            dma(2 * nz), dma(nz * per_dev),
            dma(nz), dma(nz),
            dma(3 * n), dma(k_all),
            dma(2 * nz + 2), dma(nz * per_dev + 2),
            one, dma(2 * nz), one, dma(nz),
            one, dma(4), one, dma(2),
            one, dma(2), one, dma(1),
            dma(4), dma(2), one, dma(nz),
            one, dma(n), one, dma(n),
            dma(3), dma(3),
        ],
        compiler_params=pltpu.CompilerParams(
            collective_id=0, has_side_effects=True, vmem_limit_bytes=LIMIT
        ),
        name="window",
    )(pairs.T, q_slot, x_dens, y_dens, p_dens, coulomb, screened.transpose(1, 0, 2))
    blocks, mirrored = pl.pallas_call(
        layout,
        out_shape=[shape((rows, nt * nt), F32), shape((per_dev, nt * nt), F32)],
        in_specs=[VM],
        out_specs=[VM, VM],
        scratch_shapes=[
            pltpu.VMEM((2 * nt, nt), F32),
            pltpu.VMEM((per_dev * nt // 2, 2 * nt), F32),
        ],
        name="layout",
    )(lines)
    return (blocks, mirrored)


def solution(mesh):
    in_specs = (
        P("ka", None, "ga"),
        P("ka", None, "ga"),
        P("ka", None, "ga"),
        P("ga"),
        P("ka", "ga", None),
        P("ka", None),
        P(),
    )
    out_specs = (P("ka", None), P("ka", None))
    return jax.shard_map(
        per_device, mesh=mesh, in_specs=in_specs, out_specs=out_specs, check_vma=False
    )
```

```python
import functools
import jax
import jax.numpy as jnp
from jax import lax
from jax.experimental import pallas as pl
from jax.experimental.pallas import tpu as pltpu
from jax.sharding import PartitionSpec as P

CAPQ = 2
F32 = jnp.float32
BF16 = jnp.bfloat16
I32 = jnp.int32
VM = pl.BlockSpec(memory_space=pltpu.VMEM)
SM = pl.BlockSpec(memory_space=pltpu.SMEM)
HB = pl.BlockSpec(memory_space=pl.ANY)
LIMIT = 66000000
DIMS = (((1,), (1,)), ((), ()))


def start(c):
    c.start()


def sent(c):
    c.wait_send()


def remote(src, dst, ss, rs, to):
    return pltpu.make_async_remote_copy(
        src_ref=src,
        dst_ref=dst,
        send_sem=ss,
        recv_sem=rs,
        device_id=to,
        device_id_type=pl.DeviceIdType.MESH,
    )


def greet(n):
    barrier = pltpu.get_barrier_semaphore()
    me = lax.axis_index("ka")
    g = lax.axis_index("ga")
    n_ga = lax.axis_size("ga")

    def hello(to):
        pl.semaphore_signal(barrier, inc=1, device_id=to, device_id_type=pl.DeviceIdType.MESH)

    lax.fori_loop(1, n, lambda i, c: (hello({"ka": lax.rem(me + i, n)}), c)[1], 0)
    for i in range(1, n_ga):
        hello({"ga": lax.rem(g + i, n_ga)})
    pl.semaphore_wait(barrier, n - 1 + n_ga - 1)


class Gather:
    def __init__(self, n, src, out, send, recv, cut):
        self.n, self.nz = n, n // 2
        self.me = lax.axis_index("ka")
        self.z, self.y = self.me // 2, self.me % 2
        self.src, self.out, self.send, self.recv = src, out, send, recv
        self.size = src.shape[0]
        self.cut = cut

    def copy(self, zz, yy, k, way, own=False):
        at = (zz * 2 + yy) * self.size + k
        block = self.out.at[at]
        if way == 2:
            target = self.z * 2 + 1 - self.y
        else:
            target = (self.z + (1 if way == 0 else -1)) * 2 + self.y
        return remote(
            self.src.at[k] if own else block,
            block,
            self.send.at[way * self.n + zz * 2 + yy],
            self.recv.at[at],
            {"ka": target},
        )

    def all_sent(self, zz, yy, way, count):
        block = self.out.at[pl.ds((zz * 2 + yy) * self.size, count)]
        done = self.send.at[way * self.n + zz * 2 + yy]
        remote(block, block, done, done, {"ka": self.z * 2 + 1 - self.y}).wait_send()

    def chained(self, zz, yy, count, ways=(0, 1)):
        for way in ways:
            free = self.z < self.nz - 1 if way == 0 else self.z > 0

            @pl.when(free)
            def _(way=way):
                self.all_sent(zz, yy, way, count)

    def chain(self, zz, yy, k, act, ways=(0, 1), own=False):
        for way in ways:
            free = self.z < self.nz - 1 if way == 0 else self.z > 0

            @pl.when(free)
            def _(way=way):
                act(self.copy(zz, yy, k, way, own))

    def early(self):
        return range(self.cut, self.size)

    def across_early(self):
        for k in self.early():
            self.copy(self.z, self.y, k, 2, True).start()

    def across_late(self):
        for k in range(self.cut):
            self.copy(self.z, self.y, k, 2, True).start()
        self.out[pl.ds(self.me * self.size, self.size)] = self.src[...]

    def first(self):
        for k in range(self.size):
            self.chain(self.z, self.y, k, start, own=True)

    def second(self):
        for k in self.early():
            self.copy(self.z, 1 - self.y, k, 2).wait_recv()
            self.chain(self.z, 1 - self.y, k, start)

    def sides(self, h, act):
        for way in (0, 1):
            zz = self.z - h if way == 0 else self.z + h
            there = zz >= 0 if way == 0 else zz < self.nz

            @pl.when(there)
            def _(zz=zz, way=way):
                act(zz, way)

    def hop(self, h, low=0, high=None):
        def one(k, yy, zz, way):
            self.copy(zz, yy, k, 2).wait_recv()
            self.chain(zz, yy, k, start, (way,))

        for k in range(self.size)[low:high]:

            def own(zz, way, k=k):
                one(k, self.y, zz, way)
                if k < self.cut:
                    self.copy(zz, self.y, k, 2).start()

            self.sides(h, own)
        for k in self.early() if high is None else ():
            self.sides(h, lambda zz, way, k=k: one(k, 1 - self.y, zz, way))

    def finish(self):
        few = len(self.early())
        self.chained(self.z, self.y, self.size)
        self.all_sent(self.z, self.y, 2, self.size)
        self.chained(self.z, 1 - self.y, few)
        for k in range(self.cut):
            self.copy(self.z, 1 - self.y, k, 2).wait_recv()

        def tail(h, carry):
            def side(zz, way):
                self.chained(zz, self.y, self.size, (way,))
                self.chained(zz, 1 - self.y, few, (way,))
                self.all_sent(zz, self.y, 2, self.cut)
                for k in range(self.cut):
                    self.copy(zz, 1 - self.y, k, 2).wait_recv()

            self.sides(h, side)
            return carry

        lax.fori_loop(1, self.nz, tail, 0)


class Hub(Gather):
    def __init__(self, n, src, out, send, recv):
        super().__init__(n, src, out, send, recv, src.shape[0])
        self.inner = jnp.logical_and(self.z >= 1, self.z <= self.nz - 2)
        self.edged = jnp.logical_or(self.z == 1, self.z == self.nz - 2)
        self.edge = jnp.where(self.z == 1, 0, self.nz - 1)

    def copy(self, zz, yy, k, way, own=False):
        base = (zz * 2 + yy) * self.size
        target = (self.z + (1 if way == 0 else -1)) * 2 + self.y
        return remote(
            self.src.at[k] if own else self.out.at[base + k],
            self.out.at[base + k],
            self.send.at[way * self.nz + zz],
            self.recv.at[zz * self.size + k],
            {"ka": target},
        )

    def cross(self, zz, yy, i):
        block = self.out.at[pl.ds((zz * 2 + yy) * self.size, self.size)]
        return remote(
            self.src if i == 0 and yy is self.y else block,
            block,
            self.send.at[2 * self.nz + i],
            self.recv.at[self.nz * self.size + i],
            {"ka": self.z * 2 + 1 - self.y},
        )

    def all_sent(self, zz, yy, way, count):
        block = self.out.at[pl.ds((zz * 2 + yy) * self.size, count)]
        done = self.send.at[way * self.nz + zz]
        remote(block, block, done, done, {"ka": self.z * 2 + 1 - self.y}).wait_send()

    def chained(self, zz, yy, count, ways=(0, 1)):
        for way in ways:
            free = self.z <= self.nz - 3 if way == 0 else self.z >= 2

            @pl.when(free)
            def _(way=way):
                self.all_sent(zz, yy, way, count)

    def chain(self, zz, yy, k, act, ways=(0, 1), own=False):
        for way in ways:
            free = self.z <= self.nz - 3 if way == 0 else self.z >= 2

            @pl.when(free)
            def _(way=way):
                act(self.copy(zz, yy, k, way, own))

    def first(self):
        for k in range(self.size):
            self.chain(self.z, self.y, k, start, own=True)
        self.out[pl.ds(self.me * self.size, self.size)] = self.src[...]

    def across(self):
        self.cross(self.z, self.y, 0).start()

    def hop(self, h):
        def own(zz, way):
            end = jnp.logical_and(self.edged, zz == self.edge)
            for k in range(self.size):

                @pl.when(jnp.logical_not(end))
                def _(k=k):
                    self.copy(zz, self.y, k, way).wait_recv()

                self.chain(zz, self.y, k, start, (way,))

        self.sides(h, own)

    def crossed(self):
        self.cross(self.z, 1 - self.y, 0).wait_recv()

        @pl.when(self.edged)
        def _():
            self.cross(self.edge, 1 - self.y, 1).wait_recv()

    def across_edge(self):
        @pl.when(self.edged)
        def _():
            self.cross(self.edge, self.y, 1).start()

    def edge_in(self):
        @pl.when(self.edged)
        def _():
            for k in range(self.size):
                self.copy(self.edge, self.y, k, 2).wait_recv()

    def finish(self):
        self.chained(self.z, self.y, self.size)

        @pl.when(self.inner)
        def _():
            self.cross(self.z, self.y, 0).wait_send()

            @pl.when(self.edged)
            def _():
                self.cross(self.edge, self.y, 1).wait_send()

            def tail(h, carry):
                self.sides(h, lambda zz, way: self.chained(zz, self.y, self.size, (way,)))
                return carry

            lax.fori_loop(1, self.nz, tail, 0)


class Pick:
    def __init__(self, n, src, col, out, got, tab, send, recv, ps, pr):
        self.n, self.nz = n, n // 2
        self.me = lax.axis_index("ka")
        self.z, self.y = self.me // 2, self.me % 2
        self.src, self.col, self.out, self.got, self.tab = src, col, out, got, tab
        self.send, self.recv, self.ps, self.pr = send, recv, ps, pr
        self.size = src.shape[0]

    def copy(self, zz, k, way, own=False):
        at = zz * self.size + k
        target = (self.z + (1 if way == 0 else -1)) * 2 + self.y
        return remote(
            self.src.at[k] if own else self.col.at[at],
            self.col.at[at],
            self.send.at[way * self.nz + zz],
            self.recv.at[at],
            {"ka": target},
        )

    def chain(self, zz, k, act, ways=(0, 1), own=False):
        for way in ways:
            free = self.z < self.nz - 1 if way == 0 else self.z > 0

            @pl.when(free)
            def _(way=way):
                act(self.copy(zz, k, way, own))

    def sides(self, h, act):
        for way in (0, 1):
            zz = self.z - h if way == 0 else self.z + h
            there = zz >= 0 if way == 0 else zz < self.nz

            @pl.when(there)
            def _(zz=zz, way=way):
                act(zz, way)

    def first(self):
        for k in range(self.size):
            self.chain(self.z, k, start, own=True)
        self.col[pl.ds(self.z * self.size, self.size)] = self.src[...]

    def hop(self, h):
        for k in range(self.size):

            def one(zz, way, k=k):
                self.copy(zz, k, way).wait_recv()
                self.chain(zz, k, start, (way,))

            self.sides(h, one)

    def chosen(self, zz, owner, r):
        which = self.tab[zz * 2 + self.y, owner * CAPQ + r]
        v = self.col[zz * self.size]
        for k in range(1, self.size):
            v = jnp.where(which == k, self.col[zz * self.size + k], v)
        return v

    def across(self, zz):
        rows = pl.ds(zz * CAPQ, CAPQ)
        return remote(
            self.out.at[rows],
            self.got.at[rows],
            self.ps.at[zz],
            self.pr.at[zz],
            {"ka": self.z * 2 + 1 - self.y},
        )

    def pass_on(self, zz):
        for r in range(CAPQ):
            self.out[zz * CAPQ + r] = self.chosen(zz, self.z * 2 + 1 - self.y, r)
        self.across(zz).start()

    def chained(self, zz, ways=(0, 1)):
        block = self.col.at[pl.ds(zz * self.size, self.size)]
        for way in ways:
            free = self.z < self.nz - 1 if way == 0 else self.z > 0
            done = self.send.at[way * self.nz + zz]

            @pl.when(free)
            def _(done=done):
                remote(block, block, done, done, {"ka": self.z * 2 + 1 - self.y}).wait_send()

    def finish(self):
        self.chained(self.z)
        self.across(self.z).wait_send()

        def tail(h, carry):
            def side(zz, way):
                self.chained(zz, (way,))
                self.across(zz).wait_send()

            self.sides(h, side)
            return carry

        lax.fori_loop(1, self.nz, tail, 0)


class Reduce:
    def __init__(self, part, out, recv1, tsend, recv2, s1, r1, s2, r2, per):
        self.g = lax.axis_index("ga")
        self.x, self.c = self.g // 2, self.g % 2
        self.part, self.out = part, out
        self.recv1, self.tsend, self.recv2 = recv1, tsend, recv2
        self.s1, self.r1, self.s2, self.r2, self.per = s1, r1, s2, r2, per

    def rows(self, i):
        return pl.ds(i * self.per, self.per)

    def one(self, t, i):
        xx = self.x if t else 1 - self.x
        return remote(
            self.part.at[xx * 2 + 1 - self.c, self.rows(i)],
            self.recv1.at[xx, self.rows(i)],
            self.s1,
            self.r1.at[i * 2 + t],
            {"ga": self.x * 2 + 1 - self.c},
        )

    def two(self, i):
        return remote(
            self.tsend.at[self.rows(i)],
            self.recv2.at[self.rows(i)],
            self.s2,
            self.r2.at[i],
            {"ga": (1 - self.x) * 2 + self.c},
        )

    def sum_one(self, xx, i):
        v = self.part[xx * 2 + self.c, self.rows(i)].astype(F32)
        return v + self.recv1[xx, self.rows(i)].astype(F32)

    def begin(self, i):
        self.one(0, i).start()
        self.one(1, i).start()

    def middle(self, i):
        self.one(0, i).wait_recv()
        self.tsend[self.rows(i)] = self.sum_one(1 - self.x, i).astype(self.tsend.dtype)
        self.two(i).start()

    def end(self, i):
        self.one(1, i).wait_recv()
        v = self.sum_one(self.x, i)
        self.two(i).wait_recv()
        v = (v + self.recv2[self.rows(i)].astype(F32)).astype(self.out.dtype)
        if len(self.out.shape) == len(self.tsend.shape):
            self.out[self.rows(i)] = v
        else:
            self.out[i] = v

    def finish(self):
        to = {"ga": self.x * 2 + 1 - self.c}
        both = self.part.at[pl.ds(0, 2)]
        remote(both, both, self.s1, self.s1, to).wait_send()
        remote(self.tsend, self.tsend, self.s2, self.s2, to).wait_send()


def make_row(n, q_slots, per_dev, pairs_ref, qs_ref, row_ref, at_ref):
    rows = pairs_ref.shape[1]
    slots = n * CAPQ
    lane = lax.broadcasted_iota(I32, row_ref.shape, 1)
    section = lane // slots
    spot = lane % slots
    row = jnp.where(jnp.logical_or(section == 2, section == 4), -1, 0)
    holders = ([], [])
    for j in range(rows):
        slot = qs_ref[pairs_ref[2, j]]
        owner = slot // q_slots
        first, second = pairs_ref[0, j] % per_dev, pairs_ref[1, j]
        at = []
        for i, o in enumerate((owner, second // per_dev)):
            rank = jnp.int32(0)
            for other in holders[i]:
                rank = rank + jnp.where(other == o, 1, 0)
            holders[i].append(o)
            at.append(o * CAPQ + rank)
            at_ref[i, j] = at[i]
        value = jnp.where(section == 1, slot - owner * q_slots, second)
        value = jnp.where(jnp.logical_or(section == 0, section == 3), first, value)
        hit = spot == jnp.where(section < 3, at[0], at[1])
        row = jnp.where(hit, value, row)
    row_ref[...] = row


def kernel(n, pairs_ref, qs_ref, x_ref, y_ref, p_ref, v_ref, w_hbm, lines,
           tab, at_ref, row_ref, wt, w_ref, x_col, x_out, x_got, y_all, p_all, part, half,
           recv1, tsend, recv2, part2, own, q1, qt, q2, second, outbox, sumbox, inbox,
           split, part3, eown, e1, et, e2, ebox, ein, emir,
           ws, ls, ts, tr, xs, xr, xps, xpr, ys, yr, ps, pr, s1, r1, s2, r2, t1, u1, t2, u2,
           v1, w1, v2, w2, es, er, fs, fr, as_, ar, bs, br, gs, gr):
    per_dev, nt, width = x_ref.shape
    rows = pairs_ref.shape[1]
    q_slots = w_ref.shape[0]
    nz = n // 2
    slots = n * CAPQ
    n_ga = part.shape[0]
    me = lax.axis_index("ka")
    g = lax.axis_index("ga")
    z, y = me // 2, me % 2
    fetch = pltpu.make_async_copy(w_hbm, wt, ws)
    fetch.start()
    greet(n)
    xg = Pick(n, x_ref, x_col, x_out, x_got, tab, xs, xr, xps, xpr)
    yg = Gather(n, y_ref, y_all, ys, yr, per_dev - 1)
    pg = Hub(n, p_ref, p_all, ps, pr)
    outer = jnp.logical_not(pg.inner)
    xg.first()
    make_row(n, q_slots, per_dev, pairs_ref, qs_ref, row_ref, at_ref)
    keep = pltpu.make_async_copy(row_ref.at[0], tab.at[me], ls)
    keep.start()

    def row(i, whose):
        return remote(
            row_ref.at[0], tab.at[whose], ts.at[i], tr.at[whose], {"ka": lax.rem(me + i, n)}
        )

    lax.fori_loop(1, n, lambda i, c: (row(i, me).start(), c)[1], 0)
    keep.wait()
    xg.pass_on(z)

    yg.across_early()

    @pl.when(outer)
    def _():
        pg.first()
        yg.first()
        yg.across_late()

    @pl.when(pg.inner)
    def _():
        pg.across()

    fetch.wait()
    turn = 16
    whole = width // turn * turn

    def relay(i, carry):
        at = pl.ds(pl.multiple_of(i * turn, turn), turn)
        w_ref[:, at] = jnp.swapaxes(wt[at], 0, 1)
        return carry

    lax.fori_loop(0, width // turn, relay, 0)
    if whole < width:
        w_ref[:, whole:] = jnp.swapaxes(wt[whole:], 0, 1)
    red = Reduce(part, half, recv1, tsend, recv2, s1, r1, s2, r2, 2 * CAPQ)

    def multiply(v, a, r):
        w = tab[a, slots + me * CAPQ + r]
        v = jnp.dot(v, w_ref[w], preferred_element_type=F32)
        for i in range(n_ga):
            part[i, a * CAPQ + r] = v[:, i * width : (i + 1) * width].astype(part.dtype)

    def piece(zz):
        for r in range(CAPQ):
            multiply(xg.chosen(zz, me, r), zz * 2 + y, r)
        xg.across(zz).wait_recv()
        for r in range(CAPQ):
            multiply(x_got[zz * CAPQ + r], zz * 2 + 1 - y, r)
        red.begin(zz)

    quarter = nt // n_ga
    weight = v_ref[...].reshape(1, width)
    sets = jnp.where(pg.edged, 4, 2)
    ered = Reduce(part3, eown, e1, et, e2, v1, w1, v2, w2, 4)

    def of(q):
        return jnp.where(q // 2 == 0, z, pg.edge) * 2 + q % 2

    def joined(both, out, at):
        v = jnp.concatenate(both, axis=1)
        for i in range(n_ga):
            out[i, at] = v[i * quarter : (i + 1) * quarter]

    def weigh(q, carry):
        for k in range(per_dev):
            weighted = p_all[of(q) * per_dev + k].astype(F32) * weight
            high = weighted.astype(BF16)
            split[q * per_dev + k, :nt] = high
            split[q * per_dev + k, nt:] = (weighted - high.astype(F32)).astype(BF16)
        return carry

    def exchange(zz):
        base = (zz * 2 + y) * per_dev

        def one(q, carry):
            a = of(q)
            both = []
            for r in range(CAPQ):
                at = 3 * slots + (zz * 2 + y) * CAPQ + r
                which = tab[a, at + slots] - base
                other = p_all[base]
                for k in range(1, per_dev):
                    other = jnp.where(which == k, p_all[base + k], other)
                v = lax.dot_general(
                    split[q * per_dev + tab[a, at]], other, DIMS, preferred_element_type=F32
                )
                both.append(v[:nt] + v[nt:])
            joined(both, part3, zz * 4 + q)
            return carry

        lax.fori_loop(0, sets, one, 0)
        ered.begin(zz)

    xg.hop(1)

    @pl.when(pg.inner)
    def _():
        pg.first()

    lax.fori_loop(
        1, n, lambda i, c: (row(i, lax.rem(me + n - i, n)).wait_recv(), c)[1], 0
    )
    xg.sides(1, lambda zz, way: xg.pass_on(zz))
    piece(z)

    def stage(h, carry):
        @pl.when(h < nz)
        def _():
            xg.hop(h)

        @pl.when(h == 2)
        def _():
            @pl.when(pg.inner)
            def _():
                yg.first()

            yg.second()

        @pl.when(h < nz)
        def _():
            xg.sides(h, lambda zz, way: xg.pass_on(zz))

        @pl.when(h == 2)
        def _():
            @pl.when(pg.inner)
            def _():
                pg.edge_in()
                pg.across_edge()
                yg.across_late()

            red.middle(z)

        @pl.when(h > 2)
        def _():
            xg.sides(h - 2, lambda zz, way: red.middle(zz))

        xg.sides(h - 1, lambda zz, way: piece(zz))

        @pl.when(jnp.logical_and(h >= 3, h < nz))
        def _():
            yg.hop(h - 2)

        return carry

    lax.fori_loop(2, nz + 1, stage, 0)

    @pl.when(pg.inner)
    def _():
        pg.hop(1)
        pg.crossed()
        lax.fori_loop(0, sets, weigh, 0)
        exchange(z)

    xg.sides(nz - 1, lambda zz, way: red.middle(zz))
    half_way = per_dev // 2
    yg.hop(nz - 2, 0, half_way)

    @pl.when(pg.inner)
    def _():
        pg.sides(1, lambda zz, way: exchange(zz))

    yg.hop(nz - 2, half_way)

    @pl.when(pg.inner)
    def _():
        ered.middle(z)
        pg.sides(1, lambda zz, way: ered.middle(zz))

    @pl.when(pg.inner)
    def _():
        def level(h, carry):
            pg.hop(h)
            pg.sides(h, lambda zz, way: exchange(zz))
            return carry

        lax.fori_loop(2, nz, level, 0)

    pg.finish()
    yg.hop(nz - 1)

    @pl.when(pg.inner)
    def _():
        def level(h, carry):
            pg.sides(h, lambda zz, way: ered.middle(zz))
            return carry

        lax.fori_loop(2, nz, level, 0)

    xg.finish()
    lax.fori_loop(0, nz, lambda i, c: (red.end(i), c)[1], 0)
    yg.finish()
    lax.fori_loop(1, n, lambda i, c: (row(i, me).wait_send(), c)[1], 0)
    red.finish()

    def source(a, carry):
        both = []
        for r in range(CAPQ):
            k2 = jnp.maximum(tab[a, 2 * slots + me * CAPQ + r], 0)
            both.append(
                lax.dot_general(half[a * CAPQ + r], y_all[k2], DIMS, preferred_element_type=F32)
            )
        joined(both, part2, a)
        return carry

    end = Reduce(part2, own, q1, qt, q2, t1, u1, t2, u2, n // 2)
    for i in range(2):
        lax.fori_loop(i * n // 2, (i + 1) * n // 2, source, 0, unroll=2)
        end.begin(i)
    shape = own.shape[1:]
    left = lax.broadcasted_iota(I32, shape, 1) < nt
    doubles = per_dev // 2

    def paired(sums):
        sums = [v[:, :nt] + v[:, nt:] for v in sums]
        return [
            jnp.concatenate([sums[i], sums[i + doubles]], axis=1) for i in range(doubles)
        ]

    def seconds(a, carry):
        at = 2 * slots + me * CAPQ
        second[a] = jnp.where(left, tab[a, at], tab[a, at + 1])
        return carry

    lax.fori_loop(0, n, seconds, 0)

    def to_first(q):
        return remote(
            eown.at[:, q], ein.at[y], es.at[q], er.at[y], {"ka": of(q)}
        )

    def to_second(zz):
        return remote(ebox.at[zz], emir.at[z], fs, fr.at[z], {"ka": zz * 2 + y})

    def others(act):
        def one(q, carry):
            @pl.when(q != y)
            def _():
                act(to_first(q))

            return carry

        lax.fori_loop(0, sets, one, 0)

    def levels(act):
        def one(zz, carry):
            @pl.when(zz != z)
            def _():
                act(to_second(zz))

            return carry

        lax.fori_loop(0, nz, one, 0)

    end.middle(0)
    end.middle(1)

    @pl.when(pg.inner)
    def _():
        lax.fori_loop(0, nz, lambda i, c: (ered.end(i), c)[1], 0)
        ered.finish()
        others(start)
        ein[y] = eown[:, y]

        def level(zz, carry):
            def add(q, sums):
                at = 4 * slots + (zz * 2 + y) * CAPQ
                k2 = jnp.where(left, tab[of(q), at], tab[of(q), at + 1])
                v = eown[zz, q]
                base = (zz * 2 + y) * per_dev
                return tuple(
                    t + jnp.where(k2 == base + i, v, 0.0) for i, t in enumerate(sums)
                )

            sums = lax.fori_loop(
                0, sets, add, tuple(jnp.zeros(shape, F32) for _ in range(per_dev))
            )
            for i, v in enumerate(paired(sums)):
                ebox[zz, i] = v
            return carry

        lax.fori_loop(0, nz, level, 0)
        levels(start)
        emir[z] = ebox[z]

    def cross(src, box, i, whose, ss, rs):
        to = lax.rem(me + i, n)
        return remote(src.at[to], box.at[whose], ss, rs.at[whose], {"ka": to})

    end.end(0)
    end.end(1)
    end.finish()
    lax.fori_loop(1, n, lambda i, c: (cross(own, inbox, i, me, as_, ar).start(), c)[1], 0)
    inbox[me] = own[me]

    def fill(i, carry):
        b = lax.rem(me + i, n)

        def add(a, sums):
            out = []
            for i in range(per_dev):
                out.append(sums[i] + jnp.where(second[a] == b * per_dev + i, own[a], 0.0))
            return tuple(out)

        sums = tuple(jnp.zeros(shape, F32) for _ in range(per_dev))
        sums = lax.fori_loop(0, n, add, sums, unroll=min(n, 8))
        for i_, v in enumerate(paired(sums)):
            outbox[b, i_] = v

        @pl.when(i > 0)
        def _():
            cross(outbox, sumbox, i, me, bs, br).start()

        return carry

    lax.fori_loop(1, n, fill, 0)
    fill(jnp.int32(0), 0)
    sumbox[me] = outbox[me]
    for yy in range(2):

        @pl.when(jnp.logical_or(jnp.logical_not(pg.inner), yy != y))
        def _(yy=yy):
            remote(ein.at[yy], ein.at[yy], es.at[0], er.at[yy], {"ka": z * 2 + 1 - y}).wait_recv()

    def inner_level(zz, carry):
        @pl.when(zz != z)
        def _():
            remote(
                emir.at[zz], emir.at[zz], fs, fr.at[zz], {"ka": z * 2 + 1 - y}
            ).wait_recv()

        return carry

    lax.fori_loop(1, nz - 1, inner_level, 0)
    def arrived(box, src, ss, rs):
        def one(i, carry):
            cross(src, box, i, lax.rem(me + n - i, n), ss, rs).wait_recv()
            return carry

        lax.fori_loop(1, n, one, 0)

    arrived(inbox, own, as_, ar)
    sub = quarter // 2

    def picked(ref, at, r):
        even = ref[at + (pl.ds(0, sub, stride=2),)]
        odd = ref[at + (pl.ds(1, sub, stride=2),)]
        zero = jnp.concatenate([even[:, :nt], odd[:, :nt]], axis=1)
        one = jnp.concatenate([even[:, nt:], odd[:, nt:]], axis=1)
        return jnp.where(r == 0, zero, one)

    for j in range(rows):
        at, et_ = at_ref[0, j], at_ref[1, j]
        b = et_ // CAPQ
        direct = picked(inbox, (at // CAPQ,), at % CAPQ)
        term = picked(ein, (b % 2, b // 2), et_ % CAPQ)
        lines[g, pl.ds(j * sub, sub)] = 2.0 * term - direct
    base = rows * sub
    x, c = g // 2, g % 2
    mate, far = x * 2 + 1 - c, (1 - x) * 2 + c
    parts = (pl.ds(0, base), pl.ds(base, doubles * quarter))

    def spread(i, m, whose, to):
        block = lines.at[whose, parts[m]]
        return remote(block, block, gs.at[i * 2 + m], gr.at[i * 2 + m], {"ga": to})

    spread(0, 0, g, far).start()
    spread(1, 0, g, mate).start()
    arrived(sumbox, outbox, bs, br)
    for i in range(doubles):
        total = lax.fori_loop(
            1, n, lambda o, t, i=i: t + sumbox[o, i], sumbox[0, i]
        )
        term = lax.fori_loop(
            2, nz - 1, lambda zz, t, i=i: t + emir[zz, i], emir[1, i]
        )
        lines[g, pl.ds(base + i * quarter, quarter)] = 2.0 * term - total
    spread(0, 1, g, far).start()
    spread(1, 1, g, mate).start()
    for m in range(2):
        spread(0, m, far, far).wait_recv()
        spread(2, m, far, mate).start()
    for src, ss in ((own, as_), (outbox, bs)):
        rest = src.at[pl.ds(0, n - 1)]
        remote(rest, rest, ss, ss, {"ka": z * 2 + 1 - y}).wait_send()
    @pl.when(pg.inner)
    def _():
        others(sent)
        rest = ebox.at[pl.ds(0, nz - 1)]
        remote(rest, rest, fs, fs, {"ka": z * 2 + 1 - y}).wait_send()

    for m in range(2):
        spread(1, m, mate, mate).wait_recv()
        spread(2, m, (1 - x) * 2 + 1 - c, mate).wait_recv()
        spread(0, m, g, far).wait_send()
        spread(1, m, g, mate).wait_send()
        spread(2, m, far, mate).wait_send()


def layout(lines, blocks_ref, mirr_ref, turned, flat):
    n_ga = lines.shape[0]
    rows, per_dev = blocks_ref.shape[0], mirr_ref.shape[0]
    nt = turned.shape[1]
    quarter, sub, doubles = nt // n_ga, nt // n_ga // 2, per_dev // 2
    base = rows * sub
    lanes = 2 * nt
    for q in range(n_ga):
        for t in range(sub):
            blocks_ref[:, (q * sub + t) * lanes : (q * sub + t + 1) * lanes] = lines[
                q, pl.ds(t, rows, stride=sub)
            ]
    for i in range(doubles):
        whole = jnp.concatenate(
            [lines[q, pl.ds(base + i * quarter, quarter)] for q in range(n_ga)], axis=0
        )
        turned[...] = whole.T
        even = turned[pl.ds(0, nt, stride=2)]
        odd = turned[pl.ds(1, nt, stride=2)]
        both = jnp.concatenate([even, odd], axis=1)
        flat[pl.ds(i * nt // 2, nt // 2)] = both[: nt // 2]
        flat[pl.ds((i + doubles) * nt // 2, nt // 2)] = both[nt // 2 :]
    for t in range(nt // 2):
        mirr_ref[:, t * lanes : (t + 1) * lanes] = flat[pl.ds(t, per_dev, stride=nt // 2)]


def per_device(x_dens, y_dens, p_dens, coulomb, screened, pairs, q_slot):
    n = lax.axis_size("ka")
    n_ga = lax.axis_size("ga")
    per_dev, nt, g = x_dens.shape
    q_slots = screened.shape[0]
    rows = pairs.shape[0]
    slots = n * CAPQ
    nz = n // 2
    shape = jax.ShapeDtypeStruct
    wide = F32 if slots * nt <= 2048 else BF16
    quarter = nt // n_ga
    each = (quarter, CAPQ * nt)
    line = (n,) + each
    dma = lambda m: pltpu.SemaphoreType.DMA((m,))
    one = pltpu.SemaphoreType.DMA
    row_len = -(-5 * slots // 128) * 128
    k_all = n * per_dev
    lines = pl.pallas_call(
        functools.partial(kernel, n),
        out_shape=shape((n_ga, rows * quarter // 2 + per_dev // 2 * quarter, CAPQ * nt), F32),
        in_specs=[SM, SM, VM, VM, VM, VM, HB],
        out_specs=VM,
        scratch_shapes=[
            pltpu.SMEM((n, row_len), I32),
            pltpu.SMEM((2, rows), I32),
            pltpu.VMEM((1, row_len), I32),
            pltpu.VMEM((g, q_slots, screened.shape[2]), BF16),
            pltpu.VMEM((q_slots, g, screened.shape[2]), BF16),
            pltpu.VMEM((nz * per_dev, nt, g), BF16),
            pltpu.VMEM((nz * CAPQ, nt, g), BF16),
            pltpu.VMEM((nz * CAPQ, nt, g), BF16),
            pltpu.VMEM((k_all, nt, g), BF16),
            pltpu.VMEM((k_all, nt, g), BF16),
            pltpu.VMEM((n_ga, slots, nt, g), wide),
            pltpu.VMEM((slots, nt, g), BF16),
            pltpu.VMEM((2, slots, nt, g), wide),
            pltpu.VMEM((slots, nt, g), BF16),
            pltpu.VMEM((slots, nt, g), BF16),
            pltpu.VMEM((n_ga,) + line, F32),
            pltpu.VMEM(line, F32),
            pltpu.VMEM((2,) + line, F32),
            pltpu.VMEM(line, F32),
            pltpu.VMEM(line, F32),
            pltpu.VMEM(line, I32),
            pltpu.VMEM((n, per_dev // 2) + each, F32),
            pltpu.VMEM((n, per_dev // 2) + each, F32),
            pltpu.VMEM(line, F32),
            pltpu.VMEM((4 * per_dev, 2 * nt, g), BF16),
            pltpu.VMEM((n_ga, 4 * nz) + each, F32),
            pltpu.VMEM((nz, 4) + each, F32),
            pltpu.VMEM((2, 4 * nz) + each, F32),
            pltpu.VMEM((4 * nz,) + each, F32),
            pltpu.VMEM((4 * nz,) + each, F32),
            pltpu.VMEM((nz, per_dev // 2) + each, F32),
            pltpu.VMEM((2, nz) + each, F32),
            pltpu.VMEM((nz, per_dev // 2) + each, F32),
            one, one,
            dma(n), dma(n),
            dma(2 * nz), dma(nz * per_dev),
            dma(nz), dma(nz),
            dma(3 * n), dma(k_all),
            dma(2 * nz + 2), dma(nz * per_dev + 2),
            one, dma(2 * nz), one, dma(nz),
            one, dma(4), one, dma(2),
            one, dma(2 * nz), one, dma(nz),
            dma(4), dma(2), one, dma(nz),
            one, dma(n), one, dma(n),
            dma(6), dma(6),
        ],
        compiler_params=pltpu.CompilerParams(
            collective_id=0, has_side_effects=True, vmem_limit_bytes=LIMIT
        ),
        name="window",
    )(pairs.T, q_slot, x_dens, y_dens, p_dens, coulomb, screened.transpose(1, 0, 2))
    blocks, mirrored = pl.pallas_call(
        layout,
        out_shape=[shape((rows, nt * nt), F32), shape((per_dev, nt * nt), F32)],
        in_specs=[VM],
        out_specs=[VM, VM],
        scratch_shapes=[
            pltpu.VMEM((2 * nt, nt), F32),
            pltpu.VMEM((per_dev * nt // 2, 2 * nt), F32),
        ],
        name="layout",
    )(lines)
    return (blocks, mirrored)


def solution(mesh):
    in_specs = (
        P("ka", None, "ga"),
        P("ka", None, "ga"),
        P("ka", None, "ga"),
        P("ga"),
        P("ka", "ga", None),
        P("ka", None),
        P(),
    )
    out_specs = (P("ka", None), P("ka", None))
    return jax.shard_map(
        per_device, mesh=mesh, in_specs=in_specs, out_specs=out_specs, check_vma=False
    )
```

```python
import functools
import jax
import jax.numpy as jnp
from jax import lax
from jax.experimental import pallas as pl
from jax.experimental.pallas import tpu as pltpu
from jax.sharding import PartitionSpec as P

CAPQ = 2
F32 = jnp.float32
BF16 = jnp.bfloat16
I32 = jnp.int32
VM = pl.BlockSpec(memory_space=pltpu.VMEM)
SM = pl.BlockSpec(memory_space=pltpu.SMEM)
HB = pl.BlockSpec(memory_space=pl.ANY)
LIMIT = 66000000
DIMS = (((1,), (1,)), ((), ()))


def start(c):
    c.start()


def sent(c):
    c.wait_send()


def remote(src, dst, ss, rs, to):
    return pltpu.make_async_remote_copy(
        src_ref=src,
        dst_ref=dst,
        send_sem=ss,
        recv_sem=rs,
        device_id=to,
        device_id_type=pl.DeviceIdType.MESH,
    )


def greet(n, meanwhile):
    barrier = pltpu.get_barrier_semaphore()
    me = lax.axis_index("ka")
    g = lax.axis_index("ga")
    z, y = me // 2, me % 2
    nz = n // 2

    def hello(to):
        pl.semaphore_signal(barrier, inc=1, device_id=to, device_id_type=pl.DeviceIdType.MESH)

    @pl.when(z > 0)
    def _():
        hello({"ka": me - 2})

    @pl.when(z < nz - 1)
    def _():
        hello({"ka": me + 2})

    hello({"ka": z * 2 + 1 - y})
    hello({"ga": g // 2 * 2 + 1 - g % 2})
    hello({"ga": (1 - g // 2) * 2 + g % 2})
    meanwhile()
    pl.semaphore_wait(barrier, 5 - jnp.where(z > 0, 0, 1) - jnp.where(z < nz - 1, 0, 1))


class Gather:
    def __init__(self, n, src, out, send, recv, cut):
        self.n, self.nz = n, n // 2
        self.me = lax.axis_index("ka")
        self.z, self.y = self.me // 2, self.me % 2
        self.src, self.out, self.send, self.recv = src, out, send, recv
        self.size = src.shape[0]
        self.cut = cut

    def copy(self, zz, yy, k, way, own=False):
        at = (zz * 2 + yy) * self.size + k
        block = self.out.at[at]
        if way == 2:
            target = self.z * 2 + 1 - self.y
        else:
            target = (self.z + (1 if way == 0 else -1)) * 2 + self.y
        return remote(
            self.src.at[k] if own else block,
            block,
            self.send.at[way * self.n + zz * 2 + yy],
            self.recv.at[at],
            {"ka": target},
        )

    def all_sent(self, zz, yy, way, count):
        block = self.out.at[pl.ds((zz * 2 + yy) * self.size, count)]
        done = self.send.at[way * self.n + zz * 2 + yy]
        remote(block, block, done, done, {"ka": self.z * 2 + 1 - self.y}).wait_send()

    def chained(self, zz, yy, count, ways=(0, 1)):
        for way in ways:
            free = self.z < self.nz - 1 if way == 0 else self.z > 0

            @pl.when(free)
            def _(way=way):
                self.all_sent(zz, yy, way, count)

    def chain(self, zz, yy, k, act, ways=(0, 1), own=False):
        for way in ways:
            free = self.z < self.nz - 1 if way == 0 else self.z > 0

            @pl.when(free)
            def _(way=way):
                act(self.copy(zz, yy, k, way, own))

    def early(self):
        return range(self.cut, self.size)

    def across_early(self):
        for k in self.early():
            self.copy(self.z, self.y, k, 2, True).start()

    def across_late(self):
        for k in range(self.cut):
            self.copy(self.z, self.y, k, 2, True).start()
        self.out[pl.ds(self.me * self.size, self.size)] = self.src[...]

    def first(self):
        for k in range(self.size):
            self.chain(self.z, self.y, k, start, own=True)

    def second(self):
        for k in self.early():
            self.copy(self.z, 1 - self.y, k, 2).wait_recv()
            self.chain(self.z, 1 - self.y, k, start)

    def sides(self, h, act):
        for way in (0, 1):
            zz = self.z - h if way == 0 else self.z + h
            there = zz >= 0 if way == 0 else zz < self.nz

            @pl.when(there)
            def _(zz=zz, way=way):
                act(zz, way)

    def hop(self, h, low=0, high=None):
        def one(k, yy, zz, way):
            self.copy(zz, yy, k, 2).wait_recv()
            self.chain(zz, yy, k, start, (way,))

        for k in range(self.size)[low:high]:

            def own(zz, way, k=k):
                one(k, self.y, zz, way)
                if k < self.cut:
                    self.copy(zz, self.y, k, 2).start()

            self.sides(h, own)
        for k in self.early() if high is None else ():
            self.sides(h, lambda zz, way, k=k: one(k, 1 - self.y, zz, way))

    def finish(self):
        few = len(self.early())
        self.chained(self.z, self.y, self.size)
        self.all_sent(self.z, self.y, 2, self.size)
        self.chained(self.z, 1 - self.y, few)
        for k in range(self.cut):
            self.copy(self.z, 1 - self.y, k, 2).wait_recv()

        def tail(h, carry):
            def side(zz, way):
                self.chained(zz, self.y, self.size, (way,))
                self.chained(zz, 1 - self.y, few, (way,))
                self.all_sent(zz, self.y, 2, self.cut)
                for k in range(self.cut):
                    self.copy(zz, 1 - self.y, k, 2).wait_recv()

            self.sides(h, side)
            return carry

        lax.fori_loop(1, self.nz, tail, 0)


class Rows(Gather):
    def all_sent(self, zz, yy, way, count):
        block = self.out.at[zz * 2 + yy]
        done = self.send.at[way * self.n + zz * 2 + yy]
        remote(block, block, done, done, {"ka": self.z * 2 + 1 - self.y}).wait_send()

    def begin(self):
        self.chain(self.z, self.y, 0, start, own=True)
        self.copy(self.z, self.y, 0, 2, True).start()

    def other(self, zz):
        self.copy(zz, 1 - self.y, 0, 2).wait_recv()

    def finish(self):
        self.chained(self.z, self.y, 1)
        self.all_sent(self.z, self.y, 2, 1)

        def tail(h, carry):
            def side(zz, way):
                self.chained(zz, self.y, 1, (way,))
                self.all_sent(zz, self.y, 2, 1)

            self.sides(h, side)
            return carry

        lax.fori_loop(1, self.nz, tail, 0)


class Hub(Gather):
    def __init__(self, n, src, out, send, recv):
        super().__init__(n, src, out, send, recv, src.shape[0])
        self.inner = jnp.logical_and(self.z >= 1, self.z <= self.nz - 2)
        self.edged = jnp.logical_or(self.z == 1, self.z == self.nz - 2)
        self.edge = jnp.where(self.z == 1, 0, self.nz - 1)

    def copy(self, zz, yy, k, way, own=False):
        base = (zz * 2 + yy) * self.size
        target = (self.z + (1 if way == 0 else -1)) * 2 + self.y
        return remote(
            self.src.at[k] if own else self.out.at[base + k],
            self.out.at[base + k],
            self.send.at[way * self.nz + zz],
            self.recv.at[zz * self.size + k],
            {"ka": target},
        )

    def cross(self, zz, yy, i):
        block = self.out.at[pl.ds((zz * 2 + yy) * self.size, self.size)]
        return remote(
            self.src if i == 0 and yy is self.y else block,
            block,
            self.send.at[2 * self.nz + i],
            self.recv.at[self.nz * self.size + i],
            {"ka": self.z * 2 + 1 - self.y},
        )

    def all_sent(self, zz, yy, way, count):
        block = self.out.at[pl.ds((zz * 2 + yy) * self.size, count)]
        done = self.send.at[way * self.nz + zz]
        remote(block, block, done, done, {"ka": self.z * 2 + 1 - self.y}).wait_send()

    def chained(self, zz, yy, count, ways=(0, 1)):
        for way in ways:
            free = self.z <= self.nz - 3 if way == 0 else self.z >= 2

            @pl.when(free)
            def _(way=way):
                self.all_sent(zz, yy, way, count)

    def chain(self, zz, yy, k, act, ways=(0, 1), own=False):
        for way in ways:
            free = self.z <= self.nz - 3 if way == 0 else self.z >= 2

            @pl.when(free)
            def _(way=way):
                act(self.copy(zz, yy, k, way, own))

    def first(self):
        for k in range(self.size):
            self.chain(self.z, self.y, k, start, own=True)
        self.out[pl.ds(self.me * self.size, self.size)] = self.src[...]

    def across(self):
        self.cross(self.z, self.y, 0).start()

    def hop(self, h):
        def own(zz, way):
            end = jnp.logical_and(self.edged, zz == self.edge)
            for k in range(self.size):

                @pl.when(jnp.logical_not(end))
                def _(k=k):
                    self.copy(zz, self.y, k, way).wait_recv()

                self.chain(zz, self.y, k, start, (way,))

        self.sides(h, own)

    def crossed(self):
        self.cross(self.z, 1 - self.y, 0).wait_recv()

        @pl.when(self.edged)
        def _():
            self.cross(self.edge, 1 - self.y, 1).wait_recv()

    def across_edge(self):
        @pl.when(self.edged)
        def _():
            self.cross(self.edge, self.y, 1).start()

    def edge_in(self):
        @pl.when(self.edged)
        def _():
            for k in range(self.size):
                self.copy(self.edge, self.y, k, 2).wait_recv()

    def finish(self):
        self.chained(self.z, self.y, self.size)

        @pl.when(self.inner)
        def _():
            self.cross(self.z, self.y, 0).wait_send()

            @pl.when(self.edged)
            def _():
                self.cross(self.edge, self.y, 1).wait_send()

            def tail(h, carry):
                self.sides(h, lambda zz, way: self.chained(zz, self.y, self.size, (way,)))
                return carry

            lax.fori_loop(1, self.nz, tail, 0)


class Pick:
    def __init__(self, n, src, col, out, got, tab, send, recv, ps, pr):
        self.n, self.nz = n, n // 2
        self.me = lax.axis_index("ka")
        self.z, self.y = self.me // 2, self.me % 2
        self.src, self.col, self.out, self.got, self.tab = src, col, out, got, tab
        self.send, self.recv, self.ps, self.pr = send, recv, ps, pr
        self.size = src.shape[0]

    def copy(self, zz, k, way, own=False):
        at = zz * self.size + k
        target = (self.z + (1 if way == 0 else -1)) * 2 + self.y
        return remote(
            self.src.at[k] if own else self.col.at[at],
            self.col.at[at],
            self.send.at[way * self.nz + zz],
            self.recv.at[at],
            {"ka": target},
        )

    def chain(self, zz, k, act, ways=(0, 1), own=False):
        for way in ways:
            free = self.z < self.nz - 1 if way == 0 else self.z > 0

            @pl.when(free)
            def _(way=way):
                act(self.copy(zz, k, way, own))

    def sides(self, h, act):
        for way in (0, 1):
            zz = self.z - h if way == 0 else self.z + h
            there = zz >= 0 if way == 0 else zz < self.nz

            @pl.when(there)
            def _(zz=zz, way=way):
                act(zz, way)

    def first(self):
        for k in range(self.size):
            self.chain(self.z, k, start, own=True)
        self.col[pl.ds(self.z * self.size, self.size)] = self.src[...]

    def hop(self, h):
        for k in range(self.size):

            def one(zz, way, k=k):
                self.copy(zz, k, way).wait_recv()
                self.chain(zz, k, start, (way,))

            self.sides(h, one)

    def chosen(self, zz, owner, r):
        which = self.tab[zz * 2 + self.y, owner * CAPQ + r]
        v = self.col[zz * self.size]
        for k in range(1, self.size):
            v = jnp.where(which == k, self.col[zz * self.size + k], v)
        return v

    def across(self, zz):
        rows = pl.ds(zz * CAPQ, CAPQ)
        return remote(
            self.out.at[rows],
            self.got.at[rows],
            self.ps.at[zz],
            self.pr.at[zz],
            {"ka": self.z * 2 + 1 - self.y},
        )

    def pass_on(self, zz):
        for r in range(CAPQ):
            self.out[zz * CAPQ + r] = self.chosen(zz, self.z * 2 + 1 - self.y, r)
        self.across(zz).start()

    def chained(self, zz, ways=(0, 1)):
        block = self.col.at[pl.ds(zz * self.size, self.size)]
        for way in ways:
            free = self.z < self.nz - 1 if way == 0 else self.z > 0
            done = self.send.at[way * self.nz + zz]

            @pl.when(free)
            def _(done=done):
                remote(block, block, done, done, {"ka": self.z * 2 + 1 - self.y}).wait_send()

    def finish(self):
        self.chained(self.z)
        self.across(self.z).wait_send()

        def tail(h, carry):
            def side(zz, way):
                self.chained(zz, (way,))
                self.across(zz).wait_send()

            self.sides(h, side)
            return carry

        lax.fori_loop(1, self.nz, tail, 0)


class Reduce:
    def __init__(self, part, out, recv1, tsend, recv2, s1, r1, s2, r2, per):
        self.g = lax.axis_index("ga")
        self.x, self.c = self.g // 2, self.g % 2
        self.part, self.out = part, out
        self.recv1, self.tsend, self.recv2 = recv1, tsend, recv2
        self.s1, self.r1, self.s2, self.r2, self.per = s1, r1, s2, r2, per

    def rows(self, i):
        return pl.ds(i * self.per, self.per)

    def one(self, t, i):
        xx = self.x if t else 1 - self.x
        return remote(
            self.part.at[xx * 2 + 1 - self.c, self.rows(i)],
            self.recv1.at[xx, self.rows(i)],
            self.s1,
            self.r1.at[i * 2 + t],
            {"ga": self.x * 2 + 1 - self.c},
        )

    def two(self, i):
        return remote(
            self.tsend.at[self.rows(i)],
            self.recv2.at[self.rows(i)],
            self.s2,
            self.r2.at[i],
            {"ga": (1 - self.x) * 2 + self.c},
        )

    def sum_one(self, xx, i):
        v = self.part[xx * 2 + self.c, self.rows(i)].astype(F32)
        return v + self.recv1[xx, self.rows(i)].astype(F32)

    def begin(self, i):
        self.one(0, i).start()
        self.one(1, i).start()

    def middle(self, i):
        self.one(0, i).wait_recv()
        self.tsend[self.rows(i)] = self.sum_one(1 - self.x, i).astype(self.tsend.dtype)
        self.two(i).start()

    def end(self, i):
        self.one(1, i).wait_recv()
        v = self.sum_one(self.x, i)
        self.two(i).wait_recv()
        v = (v + self.recv2[self.rows(i)].astype(F32)).astype(self.out.dtype)
        if len(self.out.shape) == len(self.tsend.shape):
            self.out[self.rows(i)] = v
        else:
            self.out[i] = v

    def finish(self):
        to = {"ga": self.x * 2 + 1 - self.c}
        both = self.part.at[pl.ds(0, 2)]
        remote(both, both, self.s1, self.s1, to).wait_send()
        remote(self.tsend, self.tsend, self.s2, self.s2, to).wait_send()


def make_row(n, q_slots, per_dev, pairs_ref, qs_ref, row_ref, at_ref):
    rows = pairs_ref.shape[1]
    slots = n * CAPQ
    lane = lax.broadcasted_iota(I32, row_ref.shape, 1)
    section = lane // slots
    spot = lane % slots
    row = jnp.where(jnp.logical_or(section == 2, section == 4), -1, 0)
    holders = ([], [])
    for j in range(rows):
        slot = qs_ref[pairs_ref[2, j]]
        owner = slot // q_slots
        first, second = pairs_ref[0, j] % per_dev, pairs_ref[1, j]
        at = []
        for i, o in enumerate((owner, second // per_dev)):
            rank = jnp.int32(0)
            for other in holders[i]:
                rank = rank + jnp.where(other == o, 1, 0)
            holders[i].append(o)
            at.append(o * CAPQ + rank)
            at_ref[i, j] = at[i]
        value = jnp.where(section == 1, slot - owner * q_slots, second)
        value = jnp.where(jnp.logical_or(section == 0, section == 3), first, value)
        hit = spot == jnp.where(section < 3, at[0], at[1])
        row = jnp.where(hit, value, row)
    row_ref[...] = row


def kernel(n, pairs_ref, qs_ref, x_ref, y_ref, p_ref, v_ref, w_hbm, lines,
           tab, at_ref, row_ref, wt, w_ref, x_col, x_out, x_got, y_all, p_all, part, half,
           recv1, tsend, recv2, part2, own, q1, qt, q2, second, outbox, sumbox, inbox,
           split, part3, eown, e1, et, e2, ebox, ein, emir,
           ws, ls, ts, tr, xs, xr, xps, xpr, ys, yr, ps, pr, s1, r1, s2, r2, t1, u1, t2, u2,
           v1, w1, v2, w2, es, er, fs, fr, as_, ar, bs, br, gs, gr):
    per_dev, nt, width = x_ref.shape
    rows = pairs_ref.shape[1]
    q_slots = w_ref.shape[0]
    nz = n // 2
    slots = n * CAPQ
    n_ga = part.shape[0]
    me = lax.axis_index("ka")
    g = lax.axis_index("ga")
    z, y = me // 2, me % 2
    fetch = pltpu.make_async_copy(w_hbm, wt, ws)
    fetch.start()
    greet(n, lambda: make_row(n, q_slots, per_dev, pairs_ref, qs_ref, row_ref, at_ref))
    xg = Pick(n, x_ref, x_col, x_out, x_got, tab, xs, xr, xps, xpr)
    yg = Gather(n, y_ref, y_all, ys, yr, per_dev - 1)
    pg = Hub(n, p_ref, p_all, ps, pr)
    outer = jnp.logical_not(pg.inner)
    keep = pltpu.make_async_copy(row_ref.at[0], tab.at[me], ls)

    rg = Rows(n, row_ref, tab, ts, tr, 1)
    rg.begin()
    xg.first()
    keep.start()
    keep.wait()
    xg.pass_on(z)

    yg.across_early()

    @pl.when(outer)
    def _():
        pg.first()
        yg.first()
        yg.across_late()

    @pl.when(pg.inner)
    def _():
        pg.across()

    fetch.wait()
    turn = 16
    whole = width // turn * turn

    def relay(i, carry):
        at = pl.ds(pl.multiple_of(i * turn, turn), turn)
        w_ref[:, at] = jnp.swapaxes(wt[at], 0, 1)
        return carry

    lax.fori_loop(0, width // turn, relay, 0)
    if whole < width:
        w_ref[:, whole:] = jnp.swapaxes(wt[whole:], 0, 1)
    red = Reduce(part, half, recv1, tsend, recv2, s1, r1, s2, r2, 2 * CAPQ)

    def multiply(v, a, r):
        w = tab[a, slots + me * CAPQ + r]
        v = jnp.dot(v, w_ref[w], preferred_element_type=F32)
        for i in range(n_ga):
            part[i, a * CAPQ + r] = v[:, i * width : (i + 1) * width].astype(part.dtype)

    def piece(zz):
        for r in range(CAPQ):
            multiply(xg.chosen(zz, me, r), zz * 2 + y, r)
        rg.other(zz)
        xg.across(zz).wait_recv()
        for r in range(CAPQ):
            multiply(x_got[zz * CAPQ + r], zz * 2 + 1 - y, r)
        red.begin(zz)

    quarter = nt // n_ga
    weight = v_ref[...].reshape(1, width)
    sets = jnp.where(pg.edged, 4, 2)
    ered = Reduce(part3, eown, e1, et, e2, v1, w1, v2, w2, 4)

    def of(q):
        return jnp.where(q // 2 == 0, z, pg.edge) * 2 + q % 2

    def joined(both, out, at):
        v = jnp.concatenate(both, axis=1)
        for i in range(n_ga):
            out[i, at] = v[i * quarter : (i + 1) * quarter]

    def weigh(q, carry):
        for k in range(per_dev):
            weighted = p_all[of(q) * per_dev + k].astype(F32) * weight
            high = weighted.astype(BF16)
            split[q * per_dev + k, :nt] = high
            split[q * per_dev + k, nt:] = (weighted - high.astype(F32)).astype(BF16)
        return carry

    def exchange(zz):
        base = (zz * 2 + y) * per_dev

        def one(q, carry):
            a = of(q)
            both = []
            for r in range(CAPQ):
                at = 3 * slots + (zz * 2 + y) * CAPQ + r
                which = tab[a, at + slots] - base
                other = p_all[base]
                for k in range(1, per_dev):
                    other = jnp.where(which == k, p_all[base + k], other)
                v = lax.dot_general(
                    split[q * per_dev + tab[a, at]], other, DIMS, preferred_element_type=F32
                )
                both.append(v[:nt] + v[nt:])
            joined(both, part3, zz * 4 + q)
            return carry

        lax.fori_loop(0, sets, one, 0)
        ered.begin(zz)

    rg.hop(1)
    xg.hop(1)

    @pl.when(pg.inner)
    def _():
        pg.first()

    xg.sides(1, lambda zz, way: xg.pass_on(zz))
    piece(z)

    def stage(h, carry):
        @pl.when(h < nz)
        def _():
            rg.hop(h)
            xg.hop(h)

        @pl.when(h == 2)
        def _():
            @pl.when(pg.inner)
            def _():
                yg.first()

            yg.second()

        @pl.when(h < nz)
        def _():
            xg.sides(h, lambda zz, way: xg.pass_on(zz))

        @pl.when(h == 2)
        def _():
            @pl.when(pg.inner)
            def _():
                pg.edge_in()
                pg.across_edge()
                yg.across_late()

            red.middle(z)

        @pl.when(h > 2)
        def _():
            xg.sides(h - 2, lambda zz, way: red.middle(zz))

        xg.sides(h - 1, lambda zz, way: piece(zz))

        @pl.when(jnp.logical_and(h >= 3, h < nz))
        def _():
            yg.hop(h - 2)

        return carry

    lax.fori_loop(2, nz + 1, stage, 0)

    @pl.when(pg.inner)
    def _():
        pg.hop(1)
        pg.crossed()
        lax.fori_loop(0, sets, weigh, 0)
        exchange(z)

    xg.sides(nz - 1, lambda zz, way: red.middle(zz))
    half_way = per_dev // 2
    yg.hop(nz - 2, 0, half_way)

    @pl.when(pg.inner)
    def _():
        pg.sides(1, lambda zz, way: exchange(zz))

    yg.hop(nz - 2, half_way)

    @pl.when(pg.inner)
    def _():
        ered.middle(z)
        pg.sides(1, lambda zz, way: ered.middle(zz))

    @pl.when(pg.inner)
    def _():
        def level(h, carry):
            pg.hop(h)
            pg.sides(h, lambda zz, way: exchange(zz))
            return carry

        lax.fori_loop(2, nz, level, 0)

    pg.finish()
    yg.hop(nz - 1)

    @pl.when(pg.inner)
    def _():
        def level(h, carry):
            pg.sides(h, lambda zz, way: ered.middle(zz))
            return carry

        lax.fori_loop(2, nz, level, 0)

    xg.finish()
    lax.fori_loop(0, nz, lambda i, c: (red.end(i), c)[1], 0)
    yg.finish()
    rg.finish()
    red.finish()

    def source(a, carry):
        both = []
        for r in range(CAPQ):
            k2 = jnp.maximum(tab[a, 2 * slots + me * CAPQ + r], 0)
            both.append(
                lax.dot_general(half[a * CAPQ + r], y_all[k2], DIMS, preferred_element_type=F32)
            )
        joined(both, part2, a)
        return carry

    end = Reduce(part2, own, q1, qt, q2, t1, u1, t2, u2, n // 2)
    for i in range(2):
        lax.fori_loop(i * n // 2, (i + 1) * n // 2, source, 0, unroll=2)
        end.begin(i)
    shape = own.shape[1:]
    left = lax.broadcasted_iota(I32, shape, 1) < nt
    doubles = per_dev // 2

    def paired(sums):
        sums = [v[:, :nt] + v[:, nt:] for v in sums]
        return [
            jnp.concatenate([sums[i], sums[i + doubles]], axis=1) for i in range(doubles)
        ]

    def seconds(a, carry):
        at = 2 * slots + me * CAPQ
        second[a] = jnp.where(left, tab[a, at], tab[a, at + 1])
        return carry

    lax.fori_loop(0, n, seconds, 0)

    def to_first(q):
        return remote(
            eown.at[:, q], ein.at[y], es.at[q], er.at[y], {"ka": of(q)}
        )

    def to_second(zz):
        return remote(ebox.at[zz], emir.at[z], fs, fr.at[z], {"ka": zz * 2 + y})

    def others(act):
        def one(q, carry):
            @pl.when(q != y)
            def _():
                act(to_first(q))

            return carry

        lax.fori_loop(0, sets, one, 0)

    def levels(act):
        def one(zz, carry):
            @pl.when(zz != z)
            def _():
                act(to_second(zz))

            return carry

        lax.fori_loop(0, nz, one, 0)

    end.middle(0)
    end.middle(1)

    @pl.when(pg.inner)
    def _():
        lax.fori_loop(0, nz, lambda i, c: (ered.end(i), c)[1], 0)
        ered.finish()
        others(start)
        ein[y] = eown[:, y]

        def level(zz, carry):
            def add(q, sums):
                at = 4 * slots + (zz * 2 + y) * CAPQ
                k2 = jnp.where(left, tab[of(q), at], tab[of(q), at + 1])
                v = eown[zz, q]
                base = (zz * 2 + y) * per_dev
                return tuple(
                    t + jnp.where(k2 == base + i, v, 0.0) for i, t in enumerate(sums)
                )

            sums = lax.fori_loop(
                0, sets, add, tuple(jnp.zeros(shape, F32) for _ in range(per_dev))
            )
            for i, v in enumerate(paired(sums)):
                ebox[zz, i] = v
            return carry

        lax.fori_loop(0, nz, level, 0)
        levels(start)
        emir[z] = ebox[z]

    def cross(src, box, i, whose, ss, rs):
        to = lax.rem(me + i, n)
        return remote(src.at[to], box.at[whose], ss, rs, {"ka": to})

    end.end(0)
    end.end(1)
    end.finish()
    lax.fori_loop(1, n, lambda i, c: (cross(own, inbox, i, me, as_, ar).start(), c)[1], 0)
    inbox[me] = own[me]

    def fill(i, carry):
        b = lax.rem(me + i, n)

        def add(a, sums):
            out = []
            for i in range(per_dev):
                out.append(sums[i] + jnp.where(second[a] == b * per_dev + i, own[a], 0.0))
            return tuple(out)

        sums = tuple(jnp.zeros(shape, F32) for _ in range(per_dev))
        sums = lax.fori_loop(0, n, add, sums, unroll=min(n, 8))
        for i_, v in enumerate(paired(sums)):
            outbox[b, i_] = v

        @pl.when(i > 0)
        def _():
            cross(outbox, sumbox, i, me, bs, br).start()

        return carry

    lax.fori_loop(1, n, fill, 0)
    fill(jnp.int32(0), 0)
    sumbox[me] = outbox[me]
    for yy in range(2):

        @pl.when(jnp.logical_or(jnp.logical_not(pg.inner), yy != y))
        def _(yy=yy):
            remote(ein.at[yy], ein.at[yy], es.at[0], er.at[yy], {"ka": z * 2 + 1 - y}).wait_recv()

    def inner_level(zz, carry):
        @pl.when(zz != z)
        def _():
            remote(
                emir.at[zz], emir.at[zz], fs, fr.at[zz], {"ka": z * 2 + 1 - y}
            ).wait_recv()

        return carry

    lax.fori_loop(1, nz - 1, inner_level, 0)
    def arrived(box, rs):
        rest = box.at[pl.ds(0, n - 1)]
        remote(rest, rest, rs, rs, {"ka": z * 2 + 1 - y}).wait_recv()

    arrived(inbox, ar)
    sub = quarter // 2

    def picked(ref, at, r):
        even = ref[at + (pl.ds(0, sub, stride=2),)]
        odd = ref[at + (pl.ds(1, sub, stride=2),)]
        zero = jnp.concatenate([even[:, :nt], odd[:, :nt]], axis=1)
        one = jnp.concatenate([even[:, nt:], odd[:, nt:]], axis=1)
        return jnp.where(r == 0, zero, one)

    for j in range(rows):
        at, et_ = at_ref[0, j], at_ref[1, j]
        b = et_ // CAPQ
        direct = picked(inbox, (at // CAPQ,), at % CAPQ)
        term = picked(ein, (b % 2, b // 2), et_ % CAPQ)
        lines[g, pl.ds(j * sub, sub)] = 2.0 * term - direct
    base = rows * sub
    x, c = g // 2, g % 2
    mate, far = x * 2 + 1 - c, (1 - x) * 2 + c
    parts = (pl.ds(0, base), pl.ds(base, doubles * quarter))

    def spread(i, m, whose, to):
        block = lines.at[whose, parts[m]]
        return remote(block, block, gs.at[i * 2 + m], gr.at[i * 2 + m], {"ga": to})

    spread(0, 0, g, far).start()
    spread(1, 0, g, mate).start()
    arrived(sumbox, br)
    for i in range(doubles):
        total = lax.fori_loop(
            1, n, lambda o, t, i=i: t + sumbox[o, i], sumbox[0, i]
        )
        term = lax.fori_loop(
            2, nz - 1, lambda zz, t, i=i: t + emir[zz, i], emir[1, i]
        )
        lines[g, pl.ds(base + i * quarter, quarter)] = 2.0 * term - total
    spread(0, 1, g, far).start()
    spread(1, 1, g, mate).start()
    for m in range(2):
        spread(0, m, far, far).wait_recv()
        spread(2, m, far, mate).start()
    for src, ss in ((own, as_), (outbox, bs)):
        rest = src.at[pl.ds(0, n - 1)]
        remote(rest, rest, ss, ss, {"ka": z * 2 + 1 - y}).wait_send()
    @pl.when(pg.inner)
    def _():
        others(sent)
        rest = ebox.at[pl.ds(0, nz - 1)]
        remote(rest, rest, fs, fs, {"ka": z * 2 + 1 - y}).wait_send()

    for m in range(2):
        spread(1, m, mate, mate).wait_recv()
        spread(2, m, (1 - x) * 2 + 1 - c, mate).wait_recv()
        spread(0, m, g, far).wait_send()
        spread(1, m, g, mate).wait_send()
        spread(2, m, far, mate).wait_send()


def layout(lines, blocks_ref, mirr_ref, turned, flat):
    n_ga = lines.shape[0]
    rows, per_dev = blocks_ref.shape[0], mirr_ref.shape[0]
    nt = turned.shape[1]
    quarter, sub, doubles = nt // n_ga, nt // n_ga // 2, per_dev // 2
    base = rows * sub
    lanes = 2 * nt
    for q in range(n_ga):
        for t in range(sub):
            blocks_ref[:, (q * sub + t) * lanes : (q * sub + t + 1) * lanes] = lines[
                q, pl.ds(t, rows, stride=sub)
            ]
    for i in range(doubles):
        whole = jnp.concatenate(
            [lines[q, pl.ds(base + i * quarter, quarter)] for q in range(n_ga)], axis=0
        )
        turned[...] = whole.T
        even = turned[pl.ds(0, nt, stride=2)]
        odd = turned[pl.ds(1, nt, stride=2)]
        both = jnp.concatenate([even, odd], axis=1)
        flat[pl.ds(i * nt // 2, nt // 2)] = both[: nt // 2]
        flat[pl.ds((i + doubles) * nt // 2, nt // 2)] = both[nt // 2 :]
    for t in range(nt // 2):
        mirr_ref[:, t * lanes : (t + 1) * lanes] = flat[pl.ds(t, per_dev, stride=nt // 2)]


def per_device(x_dens, y_dens, p_dens, coulomb, screened, pairs, q_slot):
    n = lax.axis_size("ka")
    n_ga = lax.axis_size("ga")
    per_dev, nt, g = x_dens.shape
    q_slots = screened.shape[0]
    rows = pairs.shape[0]
    slots = n * CAPQ
    nz = n // 2
    shape = jax.ShapeDtypeStruct
    wide = F32 if slots * nt <= 2048 else BF16
    quarter = nt // n_ga
    each = (quarter, CAPQ * nt)
    line = (n,) + each
    dma = lambda m: pltpu.SemaphoreType.DMA((m,))
    one = pltpu.SemaphoreType.DMA
    row_len = -(-5 * slots // 128) * 128
    k_all = n * per_dev
    lines = pl.pallas_call(
        functools.partial(kernel, n),
        out_shape=shape((n_ga, rows * quarter // 2 + per_dev // 2 * quarter, CAPQ * nt), F32),
        in_specs=[SM, SM, VM, VM, VM, VM, HB],
        out_specs=VM,
        scratch_shapes=[
            pltpu.SMEM((n, row_len), I32),
            pltpu.SMEM((2, rows), I32),
            pltpu.VMEM((1, row_len), I32),
            pltpu.VMEM((g, q_slots, screened.shape[2]), BF16),
            pltpu.VMEM((q_slots, g, screened.shape[2]), BF16),
            pltpu.VMEM((nz * per_dev, nt, g), BF16),
            pltpu.VMEM((nz * CAPQ, nt, g), BF16),
            pltpu.VMEM((nz * CAPQ, nt, g), BF16),
            pltpu.VMEM((k_all, nt, g), BF16),
            pltpu.VMEM((k_all, nt, g), BF16),
            pltpu.VMEM((n_ga, slots, nt, g), wide),
            pltpu.VMEM((slots, nt, g), BF16),
            pltpu.VMEM((2, slots, nt, g), wide),
            pltpu.VMEM((slots, nt, g), BF16),
            pltpu.VMEM((slots, nt, g), BF16),
            pltpu.VMEM((n_ga,) + line, F32),
            pltpu.VMEM(line, F32),
            pltpu.VMEM((2,) + line, F32),
            pltpu.VMEM(line, F32),
            pltpu.VMEM(line, F32),
            pltpu.VMEM(line, I32),
            pltpu.VMEM((n, per_dev // 2) + each, F32),
            pltpu.VMEM((n, per_dev // 2) + each, F32),
            pltpu.VMEM(line, F32),
            pltpu.VMEM((4 * per_dev, 2 * nt, g), BF16),
            pltpu.VMEM((n_ga, 4 * nz) + each, F32),
            pltpu.VMEM((nz, 4) + each, F32),
            pltpu.VMEM((2, 4 * nz) + each, F32),
            pltpu.VMEM((4 * nz,) + each, F32),
            pltpu.VMEM((4 * nz,) + each, F32),
            pltpu.VMEM((nz, per_dev // 2) + each, F32),
            pltpu.VMEM((2, nz) + each, F32),
            pltpu.VMEM((nz, per_dev // 2) + each, F32),
            one, one,
            dma(3 * n), dma(n),
            dma(2 * nz), dma(nz * per_dev),
            dma(nz), dma(nz),
            dma(3 * n), dma(k_all),
            dma(2 * nz + 2), dma(nz * per_dev + 2),
            one, dma(2 * nz), one, dma(nz),
            one, dma(4), one, dma(2),
            one, dma(2 * nz), one, dma(nz),
            dma(4), dma(2), one, dma(nz),
            one, one, one, one,
            dma(6), dma(6),
        ],
        compiler_params=pltpu.CompilerParams(
            collective_id=0, has_side_effects=True, vmem_limit_bytes=LIMIT
        ),
        name="window",
    )(pairs.T, q_slot, x_dens, y_dens, p_dens, coulomb, screened.transpose(1, 0, 2))
    blocks, mirrored = pl.pallas_call(
        layout,
        out_shape=[shape((rows, nt * nt), F32), shape((per_dev, nt * nt), F32)],
        in_specs=[VM],
        out_specs=[VM, VM],
        scratch_shapes=[
            pltpu.VMEM((2 * nt, nt), F32),
            pltpu.VMEM((per_dev * nt // 2, 2 * nt), F32),
        ],
        name="layout",
    )(lines)
    return (blocks, mirrored)


def solution(mesh):
    in_specs = (
        P("ka", None, "ga"),
        P("ka", None, "ga"),
        P("ka", None, "ga"),
        P("ga"),
        P("ka", "ga", None),
        P("ka", None),
        P(),
    )
    out_specs = (P("ka", None), P("ka", None))
    return jax.shard_map(
        per_device, mesh=mesh, in_specs=in_specs, out_specs=out_specs, check_vma=False
    )
```

```python
import functools
import jax
import jax.numpy as jnp
from jax import lax
from jax.experimental import pallas as pl
from jax.experimental.pallas import tpu as pltpu
from jax.sharding import PartitionSpec as P

CAPQ = 2
F32 = jnp.float32
BF16 = jnp.bfloat16
I32 = jnp.int32
VM = pl.BlockSpec(memory_space=pltpu.VMEM)
SM = pl.BlockSpec(memory_space=pltpu.SMEM)
HB = pl.BlockSpec(memory_space=pl.ANY)
LIMIT = 66000000
DIMS = (((1,), (1,)), ((), ()))


def start(c):
    c.start()


def sent(c):
    c.wait_send()


def remote(src, dst, ss, rs, to):
    return pltpu.make_async_remote_copy(
        src_ref=src,
        dst_ref=dst,
        send_sem=ss,
        recv_sem=rs,
        device_id=to,
        device_id_type=pl.DeviceIdType.MESH,
    )


def greet(n, meanwhile):
    barrier = pltpu.get_barrier_semaphore()
    me = lax.axis_index("ka")
    g = lax.axis_index("ga")
    z, y = me // 2, me % 2
    nz = n // 2

    def hello(to):
        pl.semaphore_signal(barrier, inc=1, device_id=to, device_id_type=pl.DeviceIdType.MESH)

    @pl.when(z > 0)
    def _():
        hello({"ka": me - 2})

    @pl.when(z < nz - 1)
    def _():
        hello({"ka": me + 2})

    hello({"ka": z * 2 + 1 - y})
    hello({"ga": g // 2 * 2 + 1 - g % 2})
    hello({"ga": (1 - g // 2) * 2 + g % 2})
    meanwhile()
    pl.semaphore_wait(barrier, 5 - jnp.where(z > 0, 0, 1) - jnp.where(z < nz - 1, 0, 1))


class Gather:
    def __init__(self, n, src, out, send, recv, cut):
        self.n, self.nz = n, n // 2
        self.me = lax.axis_index("ka")
        self.z, self.y = self.me // 2, self.me % 2
        self.src, self.out, self.send, self.recv = src, out, send, recv
        self.size = src.shape[0]
        self.cut = cut

    def landed(self, zz, same, k):
        few = self.size - self.cut
        if same:
            return self.recv.at[zz * self.size + k]
        if k >= self.cut:
            return self.recv.at[self.nz * self.size + zz * few + k - self.cut]
        return self.recv.at[self.nz * (self.size + few) + zz]

    def copy(self, zz, yy, k, way, own=False):
        at = (zz * 2 + yy) * self.size + k
        block = self.out.at[at]
        if way == 2:
            target = self.z * 2 + 1 - self.y
        else:
            target = (self.z + (1 if way == 0 else -1)) * 2 + self.y
        return remote(
            self.src.at[k] if own else block,
            block,
            self.send.at[way * self.nz + zz],
            self.landed(zz, (yy is self.y) != (way == 2), k),
            {"ka": target},
        )

    def take(self, zz, yy, k):
        block = self.out.at[(zz * 2 + yy) * self.size + k]
        done = self.landed(zz, yy is self.y, k)
        remote(block, block, done, done, {"ka": self.z * 2 + 1 - self.y}).wait_recv()

    def some(self, count):
        return self.out.at[pl.ds(0, count)]

    def take_late(self, zz):
        block, done = self.some(self.cut), self.landed(zz, False, 0)
        remote(block, block, done, done, {"ka": self.z * 2 + 1 - self.y}).wait_recv()

    def all_sent(self, zz, way, count):
        block, done = self.some(count), self.send.at[way * self.nz + zz]
        remote(block, block, done, done, {"ka": self.z * 2 + 1 - self.y}).wait_send()

    def chained(self, zz, ways=(0, 1)):
        for way in ways:
            free = self.z < self.nz - 1 if way == 0 else self.z > 0

            @pl.when(free)
            def _(way=way):
                self.all_sent(zz, way, 2 * self.size - self.cut)

    def chain(self, zz, yy, k, act, ways=(0, 1), own=False):
        for way in ways:
            free = self.z < self.nz - 1 if way == 0 else self.z > 0

            @pl.when(free)
            def _(way=way):
                act(self.copy(zz, yy, k, way, own))

    def early(self):
        return range(self.cut, self.size)

    def across_early(self):
        for k in self.early():
            self.copy(self.z, self.y, k, 2, True).start()

    def across_late(self):
        for k in range(self.cut):
            self.copy(self.z, self.y, k, 2, True).start()
        self.out[pl.ds(self.me * self.size, self.size)] = self.src[...]

    def first(self):
        for k in range(self.size):
            self.chain(self.z, self.y, k, start, own=True)

    def second(self):
        for k in self.early():
            self.take(self.z, 1 - self.y, k)
            self.chain(self.z, 1 - self.y, k, start)

    def sides(self, h, act):
        for way in (0, 1):
            zz = self.z - h if way == 0 else self.z + h
            there = zz >= 0 if way == 0 else zz < self.nz

            @pl.when(there)
            def _(zz=zz, way=way):
                act(zz, way)

    def hop(self, h, low=0, high=None):
        def one(k, yy, zz, way):
            self.take(zz, yy, k)
            self.chain(zz, yy, k, start, (way,))

        for k in range(self.size)[low:high]:

            def own(zz, way, k=k):
                one(k, self.y, zz, way)
                if k < self.cut:
                    self.copy(zz, self.y, k, 2).start()

            self.sides(h, own)
        for k in self.early() if high is None else ():
            self.sides(h, lambda zz, way, k=k: one(k, 1 - self.y, zz, way))

    def finish(self):
        self.chained(self.z)
        self.all_sent(self.z, 2, self.size)
        self.take_late(self.z)

        def tail(h, carry):
            def side(zz, way):
                self.chained(zz, (way,))
                self.all_sent(zz, 2, self.cut)
                self.take_late(zz)

            self.sides(h, side)
            return carry

        lax.fori_loop(1, self.nz, tail, 0)


class Rows(Gather):
    def some(self, count):
        return self.out.at[0]

    def begin(self):
        self.chain(self.z, self.y, 0, start, own=True)
        self.copy(self.z, self.y, 0, 2, True).start()

    def finish(self):
        self.chained(self.z)
        self.all_sent(self.z, 2, 1)

        def tail(h, carry):
            def side(zz, way):
                self.chained(zz, (way,))
                self.all_sent(zz, 2, 1)

            self.sides(h, side)
            return carry

        lax.fori_loop(1, self.nz, tail, 0)


class Hub(Gather):
    def __init__(self, n, src, out, send, recv):
        super().__init__(n, src, out, send, recv, src.shape[0])
        self.inner = jnp.logical_and(self.z >= 1, self.z <= self.nz - 2)
        self.edged = jnp.logical_or(self.z == 1, self.z == self.nz - 2)
        self.edge = jnp.where(self.z == 1, 0, self.nz - 1)

    def copy(self, zz, yy, k, way, own=False):
        base = (zz * 2 + yy) * self.size
        target = (self.z + (1 if way == 0 else -1)) * 2 + self.y
        return remote(
            self.src.at[k] if own else self.out.at[base + k],
            self.out.at[base + k],
            self.send.at[way * self.nz + zz],
            self.recv.at[zz * self.size + k],
            {"ka": target},
        )

    def block(self, zz, yy):
        return self.out.at[pl.ds((zz * 2 + yy) * self.size, self.size)]

    def cross(self, i):
        return remote(
            self.src,
            self.block(self.z, self.y),
            self.send.at[2 * self.nz + i],
            self.recv.at[self.nz * self.size + i],
            {"ka": self.z * 2 + 1 - self.y},
        )

    def crossed(self, zz, i):
        block, done = self.block(zz, 1 - self.y), self.recv.at[self.nz * self.size + i]
        remote(block, block, done, done, {"ka": self.z * 2 + 1 - self.y}).wait_recv()

    def inward(self):
        block = self.block(self.z, 1 - self.y)
        return remote(
            block,
            block,
            self.send.at[2 * self.nz + 2],
            self.recv.at[self.nz * self.size + 1],
            {"ka": jnp.where(self.z == 0, 1, self.nz - 2) * 2 + self.y},
        )

    def pass_inward(self):
        self.crossed(self.z, 1)
        self.inward().start()

    def chained(self, zz, ways=(0, 1)):
        for way in ways:
            free = self.z <= self.nz - 3 if way == 0 else self.z >= 2

            @pl.when(free)
            def _(way=way):
                self.all_sent(zz, way, self.size)

    def chain(self, zz, yy, k, act, ways=(0, 1), own=False):
        for way in ways:
            free = self.z <= self.nz - 3 if way == 0 else self.z >= 2

            @pl.when(free)
            def _(way=way):
                act(self.copy(zz, yy, k, way, own))

    def first(self):
        for k in range(self.size):
            self.chain(self.z, self.y, k, start, own=True)
        self.out[pl.ds(self.me * self.size, self.size)] = self.src[...]

    def hop(self, h):
        def own(zz, way):
            end = jnp.logical_and(self.edged, zz == self.edge)
            for k in range(self.size):

                @pl.when(jnp.logical_not(end))
                def _(k=k):
                    self.copy(zz, self.y, k, way).wait_recv()

                self.chain(zz, self.y, k, start, (way,))

        self.sides(h, own)

    def edge_in(self):
        @pl.when(self.edged)
        def _():
            for k in range(self.size):
                self.copy(self.edge, self.y, k, 2).wait_recv()

    def finish(self):
        self.chained(self.z)

        @pl.when(jnp.logical_not(self.inner))
        def _():
            self.cross(1).wait_send()
            self.inward().wait_send()

        @pl.when(self.inner)
        def _():
            self.cross(0).wait_send()

            def tail(h, carry):
                self.sides(h, lambda zz, way: self.chained(zz, (way,)))
                return carry

            lax.fori_loop(1, self.nz, tail, 0)


class Pick:
    def __init__(self, n, src, col, out, got, tab, send, recv, ps, pr):
        self.n, self.nz = n, n // 2
        self.me = lax.axis_index("ka")
        self.z, self.y = self.me // 2, self.me % 2
        self.src, self.col, self.out, self.got, self.tab = src, col, out, got, tab
        self.send, self.recv, self.ps, self.pr = send, recv, ps, pr
        self.size = src.shape[0]

    def copy(self, zz, k, way, own=False):
        at = zz * self.size + k
        target = (self.z + (1 if way == 0 else -1)) * 2 + self.y
        return remote(
            self.src.at[k] if own else self.col.at[at],
            self.col.at[at],
            self.send.at[way * self.nz + zz],
            self.recv.at[at],
            {"ka": target},
        )

    def chain(self, zz, k, act, ways=(0, 1), own=False):
        for way in ways:
            free = self.z < self.nz - 1 if way == 0 else self.z > 0

            @pl.when(free)
            def _(way=way):
                act(self.copy(zz, k, way, own))

    def sides(self, h, act):
        for way in (0, 1):
            zz = self.z - h if way == 0 else self.z + h
            there = zz >= 0 if way == 0 else zz < self.nz

            @pl.when(there)
            def _(zz=zz, way=way):
                act(zz, way)

    def first(self):
        for k in range(self.size):
            self.chain(self.z, k, start, own=True)
        self.col[pl.ds(self.z * self.size, self.size)] = self.src[...]

    def hop(self, h):
        for k in range(self.size):

            def one(zz, way, k=k):
                self.copy(zz, k, way).wait_recv()
                self.chain(zz, k, start, (way,))

            self.sides(h, one)

    def chosen(self, zz, owner, r):
        which = self.tab[zz * 2 + self.y, owner * CAPQ + r]
        v = self.col[zz * self.size]
        for k in range(1, self.size):
            v = jnp.where(which == k, self.col[zz * self.size + k], v)
        return v

    def across(self, zz):
        rows = pl.ds(zz * CAPQ, CAPQ)
        return remote(
            self.out.at[rows],
            self.got.at[rows],
            self.ps.at[zz],
            self.pr.at[zz],
            {"ka": self.z * 2 + 1 - self.y},
        )

    def pass_on(self, zz):
        for r in range(CAPQ):
            self.out[zz * CAPQ + r] = self.chosen(zz, self.z * 2 + 1 - self.y, r)
        self.across(zz).start()

    def chained(self, zz, ways=(0, 1)):
        block = self.col.at[pl.ds(zz * self.size, self.size)]
        for way in ways:
            free = self.z < self.nz - 1 if way == 0 else self.z > 0
            done = self.send.at[way * self.nz + zz]

            @pl.when(free)
            def _(done=done):
                remote(block, block, done, done, {"ka": self.z * 2 + 1 - self.y}).wait_send()

    def finish(self):
        self.chained(self.z)
        self.across(self.z).wait_send()

        def tail(h, carry):
            def side(zz, way):
                self.chained(zz, (way,))
                self.across(zz).wait_send()

            self.sides(h, side)
            return carry

        lax.fori_loop(1, self.nz, tail, 0)


class Reduce:
    def __init__(self, part, out, recv1, tsend, recv2, s1, r1, s2, r2, per, lump):
        self.g = lax.axis_index("ga")
        self.x, self.c = self.g // 2, self.g % 2
        self.part, self.out = part, out
        self.recv1, self.tsend, self.recv2 = recv1, tsend, recv2
        self.s1, self.r1, self.s2, self.r2, self.per = s1, r1, s2, r2, per
        self.lump, self.pieces = lump, part.shape[1] // per

    def rows(self, i):
        return pl.ds(i * self.per, self.per)

    def one(self, t, i):
        xx = self.x if t else 1 - self.x
        return remote(
            self.part.at[xx * 2 + 1 - self.c, self.rows(i)],
            self.recv1.at[xx, self.rows(i)],
            self.s1,
            self.r1.at[self.pieces + (0 if self.lump else i) if t else i],
            {"ga": self.x * 2 + 1 - self.c},
        )

    def two(self, i):
        return remote(
            self.tsend.at[self.rows(i)],
            self.recv2.at[self.rows(i)],
            self.s2,
            self.r2.at[0 if self.lump else i],
            {"ga": (1 - self.x) * 2 + self.c},
        )

    def sum_one(self, xx, i):
        v = self.part[xx * 2 + self.c, self.rows(i)].astype(F32)
        return v + self.recv1[xx, self.rows(i)].astype(F32)

    def begin(self, i):
        self.one(0, i).start()
        self.one(1, i).start()

    def middle(self, i):
        self.one(0, i).wait_recv()
        self.tsend[self.rows(i)] = self.sum_one(1 - self.x, i).astype(self.tsend.dtype)
        self.two(i).start()

    def arrive(self):
        to = {"ga": self.x * 2 + 1 - self.c}
        for block, done in ((self.recv1.at[self.x], self.r1.at[self.pieces]), (self.recv2, self.r2.at[0])):
            remote(block, block, done, done, to).wait_recv()

    def end(self, i):
        if not self.lump:
            self.one(1, i).wait_recv()
            self.two(i).wait_recv()
        v = self.sum_one(self.x, i)
        v = (v + self.recv2[self.rows(i)].astype(F32)).astype(self.out.dtype)
        if len(self.out.shape) == len(self.tsend.shape):
            self.out[self.rows(i)] = v
        else:
            self.out[i] = v

    def finish(self):
        to = {"ga": self.x * 2 + 1 - self.c}
        both = self.part.at[pl.ds(0, 2)]
        remote(both, both, self.s1, self.s1, to).wait_send()
        remote(self.tsend, self.tsend, self.s2, self.s2, to).wait_send()


def make_row(n, q_slots, per_dev, pairs_ref, qs_ref, row_ref, at_ref):
    rows = pairs_ref.shape[1]
    slots = n * CAPQ
    lane = lax.broadcasted_iota(I32, row_ref.shape, 1)
    section = lane // slots
    spot = lane % slots
    row = jnp.where(jnp.logical_or(section == 2, section == 4), -1, 0)
    holders = ([], [])
    for j in range(rows):
        slot = qs_ref[pairs_ref[2, j]]
        owner = slot // q_slots
        first, second = pairs_ref[0, j] % per_dev, pairs_ref[1, j]
        at = []
        for i, o in enumerate((owner, second // per_dev)):
            rank = jnp.int32(0)
            for other in holders[i]:
                rank = rank + jnp.where(other == o, 1, 0)
            holders[i].append(o)
            at.append(o * CAPQ + rank)
            at_ref[i, j] = at[i]
        value = jnp.where(section == 1, slot - owner * q_slots, second)
        value = jnp.where(jnp.logical_or(section == 0, section == 3), first, value)
        hit = spot == jnp.where(section < 3, at[0], at[1])
        row = jnp.where(hit, value, row)
    row_ref[...] = row


def kernel(n, pairs_ref, qs_ref, x_ref, y_ref, p_ref, v_ref, w_hbm, lines,
           tab, at_ref, row_ref, wt, w_ref, x_col, x_out, x_got, y_all, p_all, part, half,
           recv1, tsend, recv2, part2, own, q1, qt, q2, second, outbox, sumbox, inbox,
           split, part3, eown, e1, et, e2, ebox, ein, emir,
           ws, ls, ts, tr, xs, xr, xps, xpr, ys, yr, ps, pr, s1, r1, s2, r2, t1, u1, t2, u2,
           v1, w1, v2, w2, es, er, fs, fr, as_, ar, bs, br, gs, gr):
    per_dev, nt, width = x_ref.shape
    rows = pairs_ref.shape[1]
    q_slots = w_ref.shape[0]
    nz = n // 2
    slots = n * CAPQ
    n_ga = part.shape[0]
    me = lax.axis_index("ka")
    g = lax.axis_index("ga")
    z, y = me // 2, me % 2
    fetch = pltpu.make_async_copy(w_hbm, wt, ws)
    fetch.start()
    greet(n, lambda: make_row(n, q_slots, per_dev, pairs_ref, qs_ref, row_ref, at_ref))
    xg = Pick(n, x_ref, x_col, x_out, x_got, tab, xs, xr, xps, xpr)
    yg = Gather(n, y_ref, y_all, ys, yr, per_dev - 1)
    pg = Hub(n, p_ref, p_all, ps, pr)
    outer = jnp.logical_not(pg.inner)
    keep = pltpu.make_async_copy(row_ref.at[0], tab.at[me], ls)

    rg = Rows(n, row_ref, tab, ts, tr, 1)
    rg.begin()
    xg.first()
    keep.start()
    keep.wait()
    xg.pass_on(z)

    yg.across_early()

    @pl.when(outer)
    def _():
        pg.first()
        pg.cross(1).start()
        yg.first()

    @pl.when(pg.inner)
    def _():
        pg.cross(0).start()

    fetch.wait()
    turn = 16
    whole = width // turn * turn

    def relay(i, carry):
        at = pl.ds(pl.multiple_of(i * turn, turn), turn)
        w_ref[:, at] = jnp.swapaxes(wt[at], 0, 1)
        return carry

    lax.fori_loop(0, width // turn, relay, 0)
    if whole < width:
        w_ref[:, whole:] = jnp.swapaxes(wt[whole:], 0, 1)
    red = Reduce(part, half, recv1, tsend, recv2, s1, r1, s2, r2, 2 * CAPQ, True)

    def multiply(v, a, r):
        w = tab[a, slots + me * CAPQ + r]
        v = jnp.dot(v, w_ref[w], preferred_element_type=F32)
        for i in range(n_ga):
            part[i, a * CAPQ + r] = v[:, i * width : (i + 1) * width].astype(part.dtype)

    def piece(zz):
        for r in range(CAPQ):
            multiply(xg.chosen(zz, me, r), zz * 2 + y, r)
        rg.take_late(zz)
        xg.across(zz).wait_recv()
        for r in range(CAPQ):
            multiply(x_got[zz * CAPQ + r], zz * 2 + 1 - y, r)
        red.begin(zz)

    quarter = nt // n_ga
    weight = v_ref[...].reshape(1, width)
    sets = jnp.where(pg.edged, 4, 2)
    ered = Reduce(part3, eown, e1, et, e2, v1, w1, v2, w2, 4, True)

    def of(q):
        return jnp.where(q // 2 == 0, z, pg.edge) * 2 + q % 2

    def joined(both, out, at):
        v = jnp.concatenate(both, axis=1)
        for i in range(n_ga):
            out[i, at] = v[i * quarter : (i + 1) * quarter]

    def weigh(q, carry):
        for k in range(per_dev):
            weighted = p_all[of(q) * per_dev + k].astype(F32) * weight
            high = weighted.astype(BF16)
            split[q * per_dev + k, :nt] = high
            split[q * per_dev + k, nt:] = (weighted - high.astype(F32)).astype(BF16)
        return carry

    def exchange(zz):
        base = (zz * 2 + y) * per_dev

        def one(q, carry):
            a = of(q)
            both = []
            for r in range(CAPQ):
                at = 3 * slots + (zz * 2 + y) * CAPQ + r
                which = tab[a, at + slots] - base
                other = p_all[base]
                for k in range(1, per_dev):
                    other = jnp.where(which == k, p_all[base + k], other)
                v = lax.dot_general(
                    split[q * per_dev + tab[a, at]], other, DIMS, preferred_element_type=F32
                )
                both.append(v[:nt] + v[nt:])
            joined(both, part3, zz * 4 + q)
            return carry

        lax.fori_loop(0, sets, one, 0)
        ered.begin(zz)

    rg.hop(1)
    xg.hop(1)

    @pl.when(pg.inner)
    def _():
        pg.first()

    xg.sides(1, lambda zz, way: xg.pass_on(zz))
    piece(z)

    def stage(h, carry):
        @pl.when(h < nz)
        def _():
            rg.hop(h)
            xg.hop(h)

        @pl.when(h == 2)
        def _():
            @pl.when(pg.inner)
            def _():
                yg.first()

            yg.second()

        @pl.when(h < nz)
        def _():
            xg.sides(h, lambda zz, way: xg.pass_on(zz))

        @pl.when(h == 2)
        def _():
            @pl.when(pg.inner)
            def _():
                pg.edge_in()

            @pl.when(outer)
            def _():
                pg.pass_inward()

            yg.across_late()

            red.middle(z)

        @pl.when(h > 2)
        def _():
            xg.sides(h - 2, lambda zz, way: red.middle(zz))

        xg.sides(h - 1, lambda zz, way: piece(zz))

        @pl.when(jnp.logical_and(h >= 3, h < nz))
        def _():
            yg.hop(h - 2)

        return carry

    lax.fori_loop(2, nz + 1, stage, 0)

    @pl.when(pg.inner)
    def _():
        pg.hop(1)
        pg.crossed(z, 0)

        @pl.when(pg.edged)
        def _():
            pg.crossed(pg.edge, 1)

        lax.fori_loop(0, sets, weigh, 0)
        exchange(z)

    xg.sides(nz - 1, lambda zz, way: red.middle(zz))
    half_way = per_dev // 2
    yg.hop(nz - 2, 0, half_way)

    @pl.when(pg.inner)
    def _():
        pg.sides(1, lambda zz, way: exchange(zz))

    yg.hop(nz - 2, half_way)

    @pl.when(pg.inner)
    def _():
        ered.middle(z)
        pg.sides(1, lambda zz, way: ered.middle(zz))

    @pl.when(pg.inner)
    def _():
        def level(h, carry):
            pg.hop(h)
            pg.sides(h, lambda zz, way: exchange(zz))
            return carry

        lax.fori_loop(2, nz, level, 0)

    pg.finish()
    yg.hop(nz - 1)

    @pl.when(pg.inner)
    def _():
        def level(h, carry):
            pg.sides(h, lambda zz, way: ered.middle(zz))
            return carry

        lax.fori_loop(2, nz, level, 0)

    xg.finish()
    red.arrive()
    lax.fori_loop(0, nz, lambda i, c: (red.end(i), c)[1], 0)
    yg.finish()
    rg.finish()
    red.finish()

    def source(a, carry):
        both = []
        for r in range(CAPQ):
            k2 = jnp.maximum(tab[a, 2 * slots + me * CAPQ + r], 0)
            both.append(
                lax.dot_general(half[a * CAPQ + r], y_all[k2], DIMS, preferred_element_type=F32)
            )
        joined(both, part2, a)
        return carry

    end = Reduce(part2, own, q1, qt, q2, t1, u1, t2, u2, n // 4, False)
    for i in range(4):
        lax.fori_loop(i * n // 4, (i + 1) * n // 4, source, 0, unroll=2)
        end.begin(i)
    shape = own.shape[1:]
    left = lax.broadcasted_iota(I32, shape, 1) < nt
    doubles = per_dev // 2

    def paired(sums):
        sums = [v[:, :nt] + v[:, nt:] for v in sums]
        return [
            jnp.concatenate([sums[i], sums[i + doubles]], axis=1) for i in range(doubles)
        ]

    def seconds(a, carry):
        at = 2 * slots + me * CAPQ
        second[a] = jnp.where(left, tab[a, at], tab[a, at + 1])
        return carry

    lax.fori_loop(0, n, seconds, 0)

    def to_first(q):
        return remote(
            eown.at[:, q], ein.at[y], es.at[q], er.at[y], {"ka": of(q)}
        )

    def to_second(zz):
        return remote(ebox.at[zz], emir.at[z], fs, fr.at[z], {"ka": zz * 2 + y})

    def others(act):
        def one(q, carry):
            @pl.when(q != y)
            def _():
                act(to_first(q))

            return carry

        lax.fori_loop(0, sets, one, 0)

    def levels(act):
        def one(zz, carry):
            @pl.when(zz != z)
            def _():
                act(to_second(zz))

            return carry

        lax.fori_loop(0, nz, one, 0)

    for i in range(4):
        end.middle(i)

    @pl.when(pg.inner)
    def _():
        ered.arrive()
        lax.fori_loop(0, nz, lambda i, c: (ered.end(i), c)[1], 0)
        ered.finish()
        others(start)
        ein[y] = eown[:, y]

        def level(zz, carry):
            def add(q, sums):
                at = 4 * slots + (zz * 2 + y) * CAPQ
                k2 = jnp.where(left, tab[of(q), at], tab[of(q), at + 1])
                v = eown[zz, q]
                base = (zz * 2 + y) * per_dev
                return tuple(
                    t + jnp.where(k2 == base + i, v, 0.0) for i, t in enumerate(sums)
                )

            sums = lax.fori_loop(
                0, sets, add, tuple(jnp.zeros(shape, F32) for _ in range(per_dev))
            )
            for i, v in enumerate(paired(sums)):
                ebox[zz, i] = v
            return carry

        lax.fori_loop(0, nz, level, 0)
        levels(start)
        emir[z] = ebox[z]

    def cross(src, box, i, whose, ss, rs):
        return remote(src.at[i], box.at[whose], ss, rs, {"ka": i})

    def far_first(i):
        return jnp.where(z < nz // 2, n - 1 - i, i)

    for i in range(4):
        end.end(i)
    end.finish()

    def give(i, carry):
        b = far_first(i)

        @pl.when(b != me)
        def _():
            cross(own, inbox, b, me, as_, ar).start()

        return carry

    lax.fori_loop(0, n, give, 0)
    inbox[me] = own[me]

    def fill(i, carry):
        b = far_first(i)

        def add(a, sums):
            out = []
            for i in range(per_dev):
                out.append(sums[i] + jnp.where(second[a] == b * per_dev + i, own[a], 0.0))
            return tuple(out)

        sums = tuple(jnp.zeros(shape, F32) for _ in range(per_dev))
        sums = lax.fori_loop(0, n, add, sums, unroll=min(n, 8))
        for i_, v in enumerate(paired(sums)):
            outbox[b, i_] = v

        @pl.when(b != me)
        def _():
            cross(outbox, sumbox, b, me, bs, br).start()

        return carry

    lax.fori_loop(0, n, fill, 0)
    sumbox[me] = outbox[me]
    for yy in range(2):

        @pl.when(jnp.logical_or(jnp.logical_not(pg.inner), yy != y))
        def _(yy=yy):
            remote(ein.at[yy], ein.at[yy], es.at[0], er.at[yy], {"ka": z * 2 + 1 - y}).wait_recv()

    def inner_level(zz, carry):
        @pl.when(zz != z)
        def _():
            remote(
                emir.at[zz], emir.at[zz], fs, fr.at[zz], {"ka": z * 2 + 1 - y}
            ).wait_recv()

        return carry

    lax.fori_loop(1, nz - 1, inner_level, 0)
    def arrived(box, rs):
        rest = box.at[pl.ds(0, n - 1)]
        remote(rest, rest, rs, rs, {"ka": z * 2 + 1 - y}).wait_recv()

    arrived(inbox, ar)
    sub = quarter // 2

    def picked(ref, at, r):
        even = ref[at + (pl.ds(0, sub, stride=2),)]
        odd = ref[at + (pl.ds(1, sub, stride=2),)]
        zero = jnp.concatenate([even[:, :nt], odd[:, :nt]], axis=1)
        one = jnp.concatenate([even[:, nt:], odd[:, nt:]], axis=1)
        return jnp.where(r == 0, zero, one)

    for j in range(rows):
        at, et_ = at_ref[0, j], at_ref[1, j]
        b = et_ // CAPQ
        direct = picked(inbox, (at // CAPQ,), at % CAPQ)
        term = picked(ein, (b % 2, b // 2), et_ % CAPQ)
        lines[g, pl.ds(j * sub, sub)] = 2.0 * term - direct
    base = rows * sub
    x, c = g // 2, g % 2
    mate, far = x * 2 + 1 - c, (1 - x) * 2 + c
    parts = (pl.ds(0, base), pl.ds(base, doubles * quarter))

    def spread(i, m, whose, to):
        block = lines.at[whose, parts[m]]
        return remote(block, block, gs, gr.at[m if i == 0 else 2], {"ga": to})

    spread(0, 0, g, far).start()
    spread(1, 0, g, mate).start()
    arrived(sumbox, br)
    for i in range(doubles):
        total = lax.fori_loop(
            1, n, lambda o, t, i=i: t + sumbox[o, i], sumbox[0, i]
        )
        term = lax.fori_loop(
            2, nz - 1, lambda zz, t, i=i: t + emir[zz, i], emir[1, i]
        )
        lines[g, pl.ds(base + i * quarter, quarter)] = 2.0 * term - total
    spread(0, 1, g, far).start()
    spread(1, 1, g, mate).start()
    for m in range(2):
        spread(0, m, far, far).wait_recv()
        spread(2, m, far, mate).start()
    for src, ss in ((own, as_), (outbox, bs)):
        rest = src.at[pl.ds(0, n - 1)]
        remote(rest, rest, ss, ss, {"ka": z * 2 + 1 - y}).wait_send()
    @pl.when(pg.inner)
    def _():
        others(sent)
        rest = ebox.at[pl.ds(0, nz - 1)]
        remote(rest, rest, fs, fs, {"ka": z * 2 + 1 - y}).wait_send()

    for count, ss, rs in ((3, gs, None), (2, None, gr.at[2])):
        block = lines.at[pl.ds(0, count)]
        if rs is None:
            remote(block, block, ss, ss, {"ga": mate}).wait_send()
        else:
            remote(block, block, rs, rs, {"ga": mate}).wait_recv()


def layout(lines, blocks_ref, mirr_ref, turned, flat):
    n_ga = lines.shape[0]
    rows, per_dev = blocks_ref.shape[0], mirr_ref.shape[0]
    nt = turned.shape[1]
    quarter, sub, doubles = nt // n_ga, nt // n_ga // 2, per_dev // 2
    base = rows * sub
    lanes = 2 * nt
    for q in range(n_ga):
        for t in range(sub):
            blocks_ref[:, (q * sub + t) * lanes : (q * sub + t + 1) * lanes] = lines[
                q, pl.ds(t, rows, stride=sub)
            ]
    for i in range(doubles):
        whole = jnp.concatenate(
            [lines[q, pl.ds(base + i * quarter, quarter)] for q in range(n_ga)], axis=0
        )
        turned[...] = whole.T
        even = turned[pl.ds(0, nt, stride=2)]
        odd = turned[pl.ds(1, nt, stride=2)]
        both = jnp.concatenate([even, odd], axis=1)
        flat[pl.ds(i * nt // 2, nt // 2)] = both[: nt // 2]
        flat[pl.ds((i + doubles) * nt // 2, nt // 2)] = both[nt // 2 :]
    for t in range(nt // 2):
        mirr_ref[:, t * lanes : (t + 1) * lanes] = flat[pl.ds(t, per_dev, stride=nt // 2)]


def per_device(x_dens, y_dens, p_dens, coulomb, screened, pairs, q_slot):
    n = lax.axis_size("ka")
    n_ga = lax.axis_size("ga")
    per_dev, nt, g = x_dens.shape
    q_slots = screened.shape[0]
    rows = pairs.shape[0]
    slots = n * CAPQ
    nz = n // 2
    shape = jax.ShapeDtypeStruct
    wide = F32 if slots * nt <= 2048 else BF16
    quarter = nt // n_ga
    each = (quarter, CAPQ * nt)
    line = (n,) + each
    dma = lambda m: pltpu.SemaphoreType.DMA((m,))
    one = pltpu.SemaphoreType.DMA
    row_len = -(-5 * slots // 128) * 128
    k_all = n * per_dev
    lines = pl.pallas_call(
        functools.partial(kernel, n),
        out_shape=shape((n_ga, rows * quarter // 2 + per_dev // 2 * quarter, CAPQ * nt), F32),
        in_specs=[SM, SM, VM, VM, VM, VM, HB],
        out_specs=VM,
        scratch_shapes=[
            pltpu.SMEM((n, row_len), I32),
            pltpu.SMEM((2, rows), I32),
            pltpu.VMEM((1, row_len), I32),
            pltpu.VMEM((g, q_slots, screened.shape[2]), BF16),
            pltpu.VMEM((q_slots, g, screened.shape[2]), BF16),
            pltpu.VMEM((nz * per_dev, nt, g), BF16),
            pltpu.VMEM((nz * CAPQ, nt, g), BF16),
            pltpu.VMEM((nz * CAPQ, nt, g), BF16),
            pltpu.VMEM((k_all, nt, g), BF16),
            pltpu.VMEM((k_all, nt, g), BF16),
            pltpu.VMEM((n_ga, slots, nt, g), wide),
            pltpu.VMEM((slots, nt, g), BF16),
            pltpu.VMEM((2, slots, nt, g), wide),
            pltpu.VMEM((slots, nt, g), BF16),
            pltpu.VMEM((slots, nt, g), BF16),
            pltpu.VMEM((n_ga,) + line, F32),
            pltpu.VMEM(line, F32),
            pltpu.VMEM((2,) + line, F32),
            pltpu.VMEM(line, F32),
            pltpu.VMEM(line, F32),
            pltpu.VMEM(line, I32),
            pltpu.VMEM((n, per_dev // 2) + each, F32),
            pltpu.VMEM((n, per_dev // 2) + each, F32),
            pltpu.VMEM(line, F32),
            pltpu.VMEM((4 * per_dev, 2 * nt, g), BF16),
            pltpu.VMEM((n_ga, 4 * nz) + each, F32),
            pltpu.VMEM((nz, 4) + each, F32),
            pltpu.VMEM((2, 4 * nz) + each, F32),
            pltpu.VMEM((4 * nz,) + each, F32),
            pltpu.VMEM((4 * nz,) + each, F32),
            pltpu.VMEM((nz, per_dev // 2) + each, F32),
            pltpu.VMEM((2, nz) + each, F32),
            pltpu.VMEM((nz, per_dev // 2) + each, F32),
            one, one,
            dma(3 * nz), dma(2 * nz),
            dma(2 * nz), dma(nz * per_dev),
            dma(nz), dma(nz),
            dma(3 * nz), dma(nz * (per_dev + 2)),
            dma(2 * nz + 3), dma(nz * per_dev + 2),
            one, dma(nz + 1), one, dma(1),
            one, dma(8), one, dma(4),
            one, dma(nz + 1), one, dma(1),
            dma(4), dma(2), one, dma(nz),
            one, one, one, one,
            one, dma(3),
        ],
        compiler_params=pltpu.CompilerParams(
            collective_id=0, has_side_effects=True, vmem_limit_bytes=LIMIT
        ),
        name="window",
    )(pairs.T, q_slot, x_dens, y_dens, p_dens, coulomb, screened.transpose(1, 0, 2))
    blocks, mirrored = pl.pallas_call(
        layout,
        out_shape=[shape((rows, nt * nt), F32), shape((per_dev, nt * nt), F32)],
        in_specs=[VM],
        out_specs=[VM, VM],
        scratch_shapes=[
            pltpu.VMEM((2 * nt, nt), F32),
            pltpu.VMEM((per_dev * nt // 2, 2 * nt), F32),
        ],
        name="layout",
    )(lines)
    return (blocks, mirrored)


def solution(mesh):
    in_specs = (
        P("ka", None, "ga"),
        P("ka", None, "ga"),
        P("ka", None, "ga"),
        P("ga"),
        P("ka", "ga", None),
        P("ka", None),
        P(),
    )
    out_specs = (P("ka", None), P("ka", None))
    return jax.shard_map(
        per_device, mesh=mesh, in_specs=in_specs, out_specs=out_specs, check_vma=False
    )
```

```python
import functools
import jax
import jax.numpy as jnp
from jax import lax
from jax.experimental import pallas as pl
from jax.experimental.pallas import tpu as pltpu
from jax.sharding import PartitionSpec as P

CAPQ = 2
F32 = jnp.float32
BF16 = jnp.bfloat16
I32 = jnp.int32
VM = pl.BlockSpec(memory_space=pltpu.VMEM)
SM = pl.BlockSpec(memory_space=pltpu.SMEM)
HB = pl.BlockSpec(memory_space=pl.ANY)
LIMIT = 66000000
DIMS = (((1,), (1,)), ((), ()))


def start(c):
    c.start()


def sent(c):
    c.wait_send()


def remote(src, dst, ss, rs, to):
    return pltpu.make_async_remote_copy(
        src_ref=src,
        dst_ref=dst,
        send_sem=ss,
        recv_sem=rs,
        device_id=to,
        device_id_type=pl.DeviceIdType.MESH,
    )


def greet(n, meanwhile):
    barrier = pltpu.get_barrier_semaphore()
    me = lax.axis_index("ka")
    g = lax.axis_index("ga")
    z, y = me // 2, me % 2
    nz = n // 2

    def hello(to):
        pl.semaphore_signal(barrier, inc=1, device_id=to, device_id_type=pl.DeviceIdType.MESH)

    @pl.when(z > 0)
    def _():
        hello({"ka": me - 2})

    @pl.when(z < nz - 1)
    def _():
        hello({"ka": me + 2})

    hello({"ka": z * 2 + 1 - y})
    hello({"ga": g // 2 * 2 + 1 - g % 2})
    hello({"ga": (1 - g // 2) * 2 + g % 2})
    meanwhile()
    pl.semaphore_wait(barrier, 5 - jnp.where(z > 0, 0, 1) - jnp.where(z < nz - 1, 0, 1))


class Gather:
    def __init__(self, n, src, out, send, recv, cut):
        self.n, self.nz = n, n // 2
        self.me = lax.axis_index("ka")
        self.z, self.y = self.me // 2, self.me % 2
        self.src, self.out, self.send, self.recv = src, out, send, recv
        self.size = src.shape[0]
        self.cut = cut

    def landed(self, zz, same, k):
        few = self.size - self.cut
        if same:
            return self.recv.at[zz * self.size + k]
        if k >= self.cut:
            return self.recv.at[self.nz * self.size + zz * few + k - self.cut]
        return self.recv.at[self.nz * (self.size + few) + zz]

    def copy(self, zz, yy, k, way, own=False):
        at = (zz * 2 + yy) * self.size + k
        block = self.out.at[at]
        if way == 2:
            target = self.z * 2 + 1 - self.y
        else:
            target = (self.z + (1 if way == 0 else -1)) * 2 + self.y
        return remote(
            self.src.at[k] if own else block,
            block,
            self.send.at[way * self.nz + zz],
            self.landed(zz, (yy is self.y) != (way == 2), k),
            {"ka": target},
        )

    def take(self, zz, yy, k):
        block = self.out.at[(zz * 2 + yy) * self.size + k]
        done = self.landed(zz, yy is self.y, k)
        remote(block, block, done, done, {"ka": self.z * 2 + 1 - self.y}).wait_recv()

    def some(self, count):
        return self.out.at[pl.ds(0, count)]

    def take_late(self, zz):
        block, done = self.some(self.cut), self.landed(zz, False, 0)
        remote(block, block, done, done, {"ka": self.z * 2 + 1 - self.y}).wait_recv()

    def all_sent(self, zz, way, count):
        block, done = self.some(count), self.send.at[way * self.nz + zz]
        remote(block, block, done, done, {"ka": self.z * 2 + 1 - self.y}).wait_send()

    def chained(self, zz, ways=(0, 1)):
        for way in ways:
            free = self.z < self.nz - 1 if way == 0 else self.z > 0

            @pl.when(free)
            def _(way=way):
                self.all_sent(zz, way, 2 * self.size - self.cut)

    def chain(self, zz, yy, k, act, ways=(0, 1), own=False):
        for way in ways:
            free = self.z < self.nz - 1 if way == 0 else self.z > 0

            @pl.when(free)
            def _(way=way):
                act(self.copy(zz, yy, k, way, own))

    def early(self):
        return range(self.cut, self.size)

    def across_early(self):
        for k in self.early():
            self.copy(self.z, self.y, k, 2, True).start()

    def across_late(self):
        for k in range(self.cut):
            self.copy(self.z, self.y, k, 2, True).start()

    def first(self):
        for k in range(self.size):
            self.chain(self.z, self.y, k, start, own=True)

    def second(self):
        for k in self.early():
            self.take(self.z, 1 - self.y, k)
            self.chain(self.z, 1 - self.y, k, start)

    def sides(self, h, act):
        for way in (0, 1):
            zz = self.z - h if way == 0 else self.z + h
            there = zz >= 0 if way == 0 else zz < self.nz

            @pl.when(there)
            def _(zz=zz, way=way):
                act(zz, way)

    def hop(self, h, low=0, high=None):
        def one(k, yy, zz, way):
            self.take(zz, yy, k)
            self.chain(zz, yy, k, start, (way,))

        for k in range(self.size)[low:high]:

            def own(zz, way, k=k):
                one(k, self.y, zz, way)
                if k < self.cut:
                    self.copy(zz, self.y, k, 2).start()

            self.sides(h, own)
        for k in self.early() if high is None else ():
            self.sides(h, lambda zz, way, k=k: one(k, 1 - self.y, zz, way))

    def finish(self):
        self.chained(self.z)
        self.all_sent(self.z, 2, self.size)
        self.take_late(self.z)

        def tail(h, carry):
            def side(zz, way):
                self.chained(zz, (way,))
                self.all_sent(zz, 2, self.cut)
                self.take_late(zz)

            self.sides(h, side)
            return carry

        lax.fori_loop(1, self.nz, tail, 0)


class Rows(Gather):
    def some(self, count):
        return self.out.at[0]

    def begin(self):
        self.chain(self.z, self.y, 0, start, own=True)
        self.copy(self.z, self.y, 0, 2, True).start()

    def finish(self):
        self.chained(self.z)
        self.all_sent(self.z, 2, 1)

        def tail(h, carry):
            def side(zz, way):
                self.chained(zz, (way,))
                self.all_sent(zz, 2, 1)

            self.sides(h, side)
            return carry

        lax.fori_loop(1, self.nz, tail, 0)


class Hub(Gather):
    def __init__(self, n, src, out, send, recv):
        super().__init__(n, src, out, send, recv, src.shape[0])
        self.inner = jnp.logical_and(self.z >= 1, self.z <= self.nz - 2)
        self.edged = jnp.logical_or(self.z == 1, self.z == self.nz - 2)
        self.edge = jnp.where(self.z == 1, 0, self.nz - 1)

    def copy(self, zz, yy, k, way, own=False):
        base = (zz * 2 + yy) * self.size
        target = (self.z + (1 if way == 0 else -1)) * 2 + self.y
        return remote(
            self.src.at[k] if own else self.out.at[base + k],
            self.out.at[base + k],
            self.send.at[way * self.nz + zz],
            self.recv.at[zz * self.size + k],
            {"ka": target},
        )

    def block(self, zz, yy):
        return self.out.at[pl.ds((zz * 2 + yy) * self.size, self.size)]

    def cross(self, i):
        return remote(
            self.src,
            self.block(self.z, self.y),
            self.send.at[2 * self.nz + i],
            self.recv.at[self.nz * self.size + i],
            {"ka": self.z * 2 + 1 - self.y},
        )

    def crossed(self, zz, i):
        block, done = self.block(zz, 1 - self.y), self.recv.at[self.nz * self.size + i]
        remote(block, block, done, done, {"ka": self.z * 2 + 1 - self.y}).wait_recv()

    def inward(self):
        block = self.block(self.z, 1 - self.y)
        return remote(
            block,
            block,
            self.send.at[2 * self.nz + 2],
            self.recv.at[self.nz * self.size + 1],
            {"ka": jnp.where(self.z == 0, 1, self.nz - 2) * 2 + self.y},
        )

    def pass_inward(self):
        self.crossed(self.z, 1)
        self.inward().start()

    def chained(self, zz, ways=(0, 1)):
        for way in ways:
            free = self.z <= self.nz - 3 if way == 0 else self.z >= 2

            @pl.when(free)
            def _(way=way):
                self.all_sent(zz, way, self.size)

    def chain(self, zz, yy, k, act, ways=(0, 1), own=False):
        for way in ways:
            free = self.z <= self.nz - 3 if way == 0 else self.z >= 2

            @pl.when(free)
            def _(way=way):
                act(self.copy(zz, yy, k, way, own))

    def first(self):
        for k in range(self.size):
            self.chain(self.z, self.y, k, start, own=True)

    def hop(self, h):
        def own(zz, way):
            end = jnp.logical_and(self.edged, zz == self.edge)
            for k in range(self.size):

                @pl.when(jnp.logical_not(end))
                def _(k=k):
                    self.copy(zz, self.y, k, way).wait_recv()

                self.chain(zz, self.y, k, start, (way,))

        self.sides(h, own)

    def edge_in(self):
        @pl.when(self.edged)
        def _():
            for k in range(self.size):
                self.copy(self.edge, self.y, k, 2).wait_recv()

    def finish(self):
        self.chained(self.z)

        @pl.when(jnp.logical_not(self.inner))
        def _():
            self.cross(1).wait_send()
            self.inward().wait_send()

        @pl.when(self.inner)
        def _():
            self.cross(0).wait_send()

            def tail(h, carry):
                self.sides(h, lambda zz, way: self.chained(zz, (way,)))
                return carry

            lax.fori_loop(1, self.nz, tail, 0)


class Pick:
    def __init__(self, n, src, col, out, got, tab, send, recv, ps, pr):
        self.n, self.nz = n, n // 2
        self.me = lax.axis_index("ka")
        self.z, self.y = self.me // 2, self.me % 2
        self.src, self.col, self.out, self.got, self.tab = src, col, out, got, tab
        self.send, self.recv, self.ps, self.pr = send, recv, ps, pr
        self.size = src.shape[0]

    def copy(self, zz, k, way, own=False):
        at = zz * self.size + k
        target = (self.z + (1 if way == 0 else -1)) * 2 + self.y
        return remote(
            self.src.at[k] if own else self.col.at[at],
            self.col.at[at],
            self.send.at[way * self.nz + zz],
            self.recv.at[at],
            {"ka": target},
        )

    def chain(self, zz, k, act, ways=(0, 1), own=False):
        for way in ways:
            free = self.z < self.nz - 1 if way == 0 else self.z > 0

            @pl.when(free)
            def _(way=way):
                act(self.copy(zz, k, way, own))

    def sides(self, h, act):
        for way in (0, 1):
            zz = self.z - h if way == 0 else self.z + h
            there = zz >= 0 if way == 0 else zz < self.nz

            @pl.when(there)
            def _(zz=zz, way=way):
                act(zz, way)

    def first(self):
        for k in range(self.size):
            self.chain(self.z, k, start, own=True)

    def hop(self, h):
        for k in range(self.size):

            def one(zz, way, k=k):
                self.copy(zz, k, way).wait_recv()
                self.chain(zz, k, start, (way,))

            self.sides(h, one)

    def chosen(self, zz, owner, r):
        which = self.tab[zz * 2 + self.y, owner * CAPQ + r]
        v = self.col[zz * self.size]
        for k in range(1, self.size):
            v = jnp.where(which == k, self.col[zz * self.size + k], v)
        return v

    def across(self, zz):
        rows = pl.ds(zz * CAPQ, CAPQ)
        return remote(
            self.out.at[rows],
            self.got.at[rows],
            self.ps.at[zz],
            self.pr.at[zz],
            {"ka": self.z * 2 + 1 - self.y},
        )

    def pass_on(self, zz):
        for r in range(CAPQ):
            self.out[zz * CAPQ + r] = self.chosen(zz, self.z * 2 + 1 - self.y, r)
        self.across(zz).start()

    def chained(self, zz, ways=(0, 1)):
        block = self.col.at[pl.ds(zz * self.size, self.size)]
        for way in ways:
            free = self.z < self.nz - 1 if way == 0 else self.z > 0
            done = self.send.at[way * self.nz + zz]

            @pl.when(free)
            def _(done=done):
                remote(block, block, done, done, {"ka": self.z * 2 + 1 - self.y}).wait_send()

    def finish(self):
        self.chained(self.z)
        self.across(self.z).wait_send()

        def tail(h, carry):
            def side(zz, way):
                self.chained(zz, (way,))
                self.across(zz).wait_send()

            self.sides(h, side)
            return carry

        lax.fori_loop(1, self.nz, tail, 0)


class Reduce:
    def __init__(self, part, out, recv1, tsend, recv2, s1, r1, s2, r2, per, lump):
        self.g = lax.axis_index("ga")
        self.x, self.c = self.g // 2, self.g % 2
        self.part, self.out = part, out
        self.recv1, self.tsend, self.recv2 = recv1, tsend, recv2
        self.s1, self.r1, self.s2, self.r2, self.per = s1, r1, s2, r2, per
        self.lump, self.pieces = lump, part.shape[1] // per

    def rows(self, i):
        return pl.ds(i * self.per, self.per)

    def one(self, t, i):
        xx = self.x if t else 1 - self.x
        return remote(
            self.part.at[xx * 2 + 1 - self.c, self.rows(i)],
            self.recv1.at[xx, self.rows(i)],
            self.s1,
            self.r1.at[self.pieces + (0 if self.lump else i) if t else i],
            {"ga": self.x * 2 + 1 - self.c},
        )

    def two(self, i):
        return remote(
            self.tsend.at[self.rows(i)],
            self.recv2.at[self.rows(i)],
            self.s2,
            self.r2.at[0 if self.lump else i],
            {"ga": (1 - self.x) * 2 + self.c},
        )

    def sum_one(self, xx, i):
        v = self.part[xx * 2 + self.c, self.rows(i)].astype(F32)
        return v + self.recv1[xx, self.rows(i)].astype(F32)

    def begin(self, i):
        self.one(0, i).start()
        self.one(1, i).start()

    def middle(self, i):
        self.one(0, i).wait_recv()
        self.tsend[self.rows(i)] = self.sum_one(1 - self.x, i).astype(self.tsend.dtype)
        self.two(i).start()

    def arrive(self):
        to = {"ga": self.x * 2 + 1 - self.c}
        for block, done in ((self.recv1.at[self.x], self.r1.at[self.pieces]), (self.recv2, self.r2.at[0])):
            remote(block, block, done, done, to).wait_recv()

    def end(self, i):
        if not self.lump:
            self.one(1, i).wait_recv()
            self.two(i).wait_recv()
        v = self.sum_one(self.x, i)
        v = (v + self.recv2[self.rows(i)].astype(F32)).astype(self.out.dtype)
        if len(self.out.shape) == len(self.tsend.shape):
            self.out[self.rows(i)] = v
        else:
            self.out[i] = v

    def finish(self):
        to = {"ga": self.x * 2 + 1 - self.c}
        both = self.part.at[pl.ds(0, 2)]
        remote(both, both, self.s1, self.s1, to).wait_send()
        remote(self.tsend, self.tsend, self.s2, self.s2, to).wait_send()


def make_row(n, q_slots, per_dev, pairs_ref, qs_ref, row_ref, at_ref):
    rows = pairs_ref.shape[1]
    slots = n * CAPQ
    lane = lax.broadcasted_iota(I32, row_ref.shape, 1)
    section = lane // slots
    spot = lane % slots
    row = jnp.where(jnp.logical_or(section == 2, section == 4), -1, 0)
    holders = ([], [])
    for j in range(rows):
        slot = qs_ref[pairs_ref[2, j]]
        owner = slot // q_slots
        first, second = pairs_ref[0, j] % per_dev, pairs_ref[1, j]
        at = []
        for i, o in enumerate((owner, second // per_dev)):
            rank = jnp.int32(0)
            for other in holders[i]:
                rank = rank + jnp.where(other == o, 1, 0)
            holders[i].append(o)
            at.append(o * CAPQ + rank)
            at_ref[i, j] = at[i]
        value = jnp.where(section == 1, slot - owner * q_slots, second)
        value = jnp.where(jnp.logical_or(section == 0, section == 3), first, value)
        hit = spot == jnp.where(section < 3, at[0], at[1])
        row = jnp.where(hit, value, row)
    row_ref[...] = row


def kernel(n, pairs_ref, qs_ref, x_ref, y_ref, p_ref, v_ref, w_hbm, lines,
           tab, at_ref, row_ref, wt, w_ref, x_col, x_out, x_got, y_all, p_all, part, half,
           recv1, tsend, recv2, part2, own, q1, qt, q2, second, outbox, sumbox, inbox,
           split, part3, eown, e1, et, e2, ebox, ein, emir,
           ws, ls, ks, ts, tr, xs, xr, xps, xpr, ys, yr, ps, pr, s1, r1, s2, r2, t1, u1, t2, u2,
           v1, w1, v2, w2, es, er, fs, fr, as_, ar, bs, br, gs, gr):
    per_dev, nt, width = x_ref.shape
    rows = pairs_ref.shape[1]
    q_slots = w_ref.shape[0]
    nz = n // 2
    slots = n * CAPQ
    n_ga = part.shape[0]
    me = lax.axis_index("ka")
    g = lax.axis_index("ga")
    z, y = me // 2, me % 2
    fetch = pltpu.make_async_copy(w_hbm, wt, ws)
    fetch.start()
    mine = pl.ds(me * per_dev, per_dev)
    keeps = [
        pltpu.make_async_copy(x_ref, x_col.at[pl.ds(z * per_dev, per_dev)], ks.at[0]),
        pltpu.make_async_copy(p_ref, p_all.at[mine], ks.at[1]),
        pltpu.make_async_copy(y_ref, y_all.at[mine], ks.at[2]),
    ]
    for c in keeps:
        c.start()
    greet(n, lambda: make_row(n, q_slots, per_dev, pairs_ref, qs_ref, row_ref, at_ref))
    xg = Pick(n, x_ref, x_col, x_out, x_got, tab, xs, xr, xps, xpr)
    yg = Gather(n, y_ref, y_all, ys, yr, per_dev - 1)
    pg = Hub(n, p_ref, p_all, ps, pr)
    outer = jnp.logical_not(pg.inner)
    keep = pltpu.make_async_copy(row_ref.at[0], tab.at[me], ls)

    rg = Rows(n, row_ref, tab, ts, tr, 1)
    rg.begin()
    xg.first()
    keep.start()
    keep.wait()
    for c in keeps:
        c.wait()
    xg.pass_on(z)

    yg.across_early()

    @pl.when(outer)
    def _():
        pg.first()
        pg.cross(1).start()
        yg.first()

    @pl.when(pg.inner)
    def _():
        pg.cross(0).start()

    fetch.wait()
    turn = 16
    whole = width // turn * turn

    def relay(i, carry):
        at = pl.ds(pl.multiple_of(i * turn, turn), turn)
        w_ref[:, at] = jnp.swapaxes(wt[at], 0, 1)
        return carry

    lax.fori_loop(0, width // turn, relay, 0)
    if whole < width:
        w_ref[:, whole:] = jnp.swapaxes(wt[whole:], 0, 1)
    red = Reduce(part, half, recv1, tsend, recv2, s1, r1, s2, r2, 2 * CAPQ, True)

    def multiply(v, a, r):
        w = tab[a, slots + me * CAPQ + r]
        v = jnp.dot(v, w_ref[w], preferred_element_type=F32)
        for i in range(n_ga):
            part[i, a * CAPQ + r] = v[:, i * width : (i + 1) * width].astype(part.dtype)

    def piece(zz):
        for r in range(CAPQ):
            multiply(xg.chosen(zz, me, r), zz * 2 + y, r)
        rg.take_late(zz)
        xg.across(zz).wait_recv()
        for r in range(CAPQ):
            multiply(x_got[zz * CAPQ + r], zz * 2 + 1 - y, r)
        red.begin(zz)

    quarter = nt // n_ga
    weight = v_ref[...].reshape(1, width)
    sets = jnp.where(pg.edged, 4, 2)
    ered = Reduce(part3, eown, e1, et, e2, v1, w1, v2, w2, 4, False)

    def of(q):
        return jnp.where(q // 2 == 0, z, pg.edge) * 2 + q % 2

    def joined(both, out, at):
        v = jnp.concatenate(both, axis=1)
        for i in range(n_ga):
            out[i, at] = v[i * quarter : (i + 1) * quarter]

    def weigh(q, carry):
        for k in range(per_dev):
            weighted = p_all[of(q) * per_dev + k].astype(F32) * weight
            high = weighted.astype(BF16)
            split[q * per_dev + k, :nt] = high
            split[q * per_dev + k, nt:] = (weighted - high.astype(F32)).astype(BF16)
        return carry

    def exchange(zz):
        base = (zz * 2 + y) * per_dev

        def one(q, carry):
            a = of(q)
            both = []
            for r in range(CAPQ):
                at = 3 * slots + (zz * 2 + y) * CAPQ + r
                which = tab[a, at + slots] - base
                other = p_all[base]
                for k in range(1, per_dev):
                    other = jnp.where(which == k, p_all[base + k], other)
                v = lax.dot_general(
                    split[q * per_dev + tab[a, at]], other, DIMS, preferred_element_type=F32
                )
                both.append(v[:nt] + v[nt:])
            joined(both, part3, zz * 4 + q)
            return carry

        lax.fori_loop(0, sets, one, 0)
        ered.begin(zz)

    shape = own.shape[1:]
    left = lax.broadcasted_iota(I32, shape, 1) < nt
    doubles = per_dev // 2

    def paired(sums):
        sums = [v[:, :nt] + v[:, nt:] for v in sums]
        return [
            jnp.concatenate([sums[i], sums[i + doubles]], axis=1) for i in range(doubles)
        ]

    def to_first(q, zz):
        return remote(eown.at[zz, q], ein.at[y, zz], es, er.at[y], {"ka": of(q)})

    def to_second(zz):
        return remote(ebox.at[zz], emir.at[z], fs, fr.at[z], {"ka": zz * 2 + y})

    def deliver(zz):
        ered.end(zz)

        def give(q, carry):
            @pl.when(q != y)
            def _():
                to_first(q, zz).start()

            return carry

        lax.fori_loop(0, sets, give, 0)
        ein[y, zz] = eown[zz, y]

        def add(q, sums):
            at = 4 * slots + (zz * 2 + y) * CAPQ
            k2 = jnp.where(left, tab[of(q), at], tab[of(q), at + 1])
            v = eown[zz, q]
            base = (zz * 2 + y) * per_dev
            return tuple(t + jnp.where(k2 == base + i, v, 0.0) for i, t in enumerate(sums))

        sums = lax.fori_loop(0, sets, add, tuple(jnp.zeros(shape, F32) for _ in range(per_dev)))
        for i, v in enumerate(paired(sums)):
            ebox[zz, i] = v

        @pl.when(zz != z)
        def _():
            to_second(zz).start()

        @pl.when(zz == z)
        def _():
            emir[z] = ebox[z]

    rg.hop(1)
    xg.hop(1)

    @pl.when(pg.inner)
    def _():
        pg.first()

    xg.sides(1, lambda zz, way: xg.pass_on(zz))
    piece(z)

    def stage(h, carry):
        @pl.when(h < nz)
        def _():
            rg.hop(h)
            xg.hop(h)

        @pl.when(h == 2)
        def _():
            @pl.when(pg.inner)
            def _():
                yg.first()

            yg.second()

        @pl.when(h < nz)
        def _():
            xg.sides(h, lambda zz, way: xg.pass_on(zz))

        @pl.when(h == 2)
        def _():
            @pl.when(pg.inner)
            def _():
                pg.edge_in()

            @pl.when(outer)
            def _():
                pg.pass_inward()

            yg.across_late()

            red.middle(z)

        @pl.when(h > 2)
        def _():
            xg.sides(h - 2, lambda zz, way: red.middle(zz))

        xg.sides(h - 1, lambda zz, way: piece(zz))

        @pl.when(jnp.logical_and(h >= 3, h < nz))
        def _():
            yg.hop(h - 2)

        return carry

    lax.fori_loop(2, nz + 1, stage, 0)

    @pl.when(pg.inner)
    def _():
        pg.hop(1)
        pg.crossed(z, 0)

        @pl.when(pg.edged)
        def _():
            pg.crossed(pg.edge, 1)

        lax.fori_loop(0, sets, weigh, 0)
        exchange(z)

    xg.sides(nz - 1, lambda zz, way: red.middle(zz))
    half_way = per_dev // 2
    yg.hop(nz - 2, 0, half_way)

    @pl.when(pg.inner)
    def _():
        pg.sides(1, lambda zz, way: exchange(zz))

    yg.hop(nz - 2, half_way)

    @pl.when(pg.inner)
    def _():
        ered.middle(z)
        pg.sides(1, lambda zz, way: ered.middle(zz))

    @pl.when(pg.inner)
    def _():
        def level(h, carry):
            pg.hop(h)
            pg.sides(h, lambda zz, way: exchange(zz))
            return carry

        lax.fori_loop(2, nz, level, 0)

    pg.finish()
    yg.hop(nz - 1)

    red.arrive()
    lax.fori_loop(0, nz, lambda i, c: (red.end(i), c)[1], 0)
    yg.finish()

    def source(a, carry):
        both = []
        for r in range(CAPQ):
            k2 = jnp.maximum(tab[a, 2 * slots + me * CAPQ + r], 0)
            both.append(
                lax.dot_general(half[a * CAPQ + r], y_all[k2], DIMS, preferred_element_type=F32)
            )
        joined(both, part2, a)
        return carry

    end = Reduce(part2, own, q1, qt, q2, t1, u1, t2, u2, n // 4, False)
    for i in range(4):
        lax.fori_loop(i * n // 4, (i + 1) * n // 4, source, 0, unroll=2)
        end.begin(i)
    def seconds(a, carry):
        at = 2 * slots + me * CAPQ
        second[a] = jnp.where(left, tab[a, at], tab[a, at + 1])
        return carry

    lax.fori_loop(0, n, seconds, 0)

    @pl.when(pg.inner)
    def _():
        def level(h, carry):
            pg.sides(h, lambda zz, way: ered.middle(zz))
            return carry

        lax.fori_loop(2, nz, level, 0)

    for i in range(4):
        end.middle(i)

    @pl.when(pg.inner)
    def _():
        deliver(z)

        def level(h, carry):
            pg.sides(h, lambda zz, way: deliver(zz))
            return carry

        lax.fori_loop(1, nz, level, 0)


    def cross(src, box, i, whose, ss, rs):
        return remote(src.at[i], box.at[whose], ss, rs, {"ka": i})

    def far_first(i):
        return jnp.where(z < nz // 2, n - 1 - i, i)

    for i in range(4):
        end.end(i)

    def give(i, carry):
        b = far_first(i)

        @pl.when(b != me)
        def _():
            cross(own, inbox, b, me, as_, ar).start()

        return carry

    lax.fori_loop(0, n, give, 0)
    inbox[me] = own[me]


    def fill(i, carry):
        b = far_first(i)

        def add(a, sums):
            out = []
            for i in range(per_dev):
                out.append(sums[i] + jnp.where(second[a] == b * per_dev + i, own[a], 0.0))
            return tuple(out)

        sums = tuple(jnp.zeros(shape, F32) for _ in range(per_dev))
        sums = lax.fori_loop(0, n, add, sums, unroll=min(n, 8))
        for i_, v in enumerate(paired(sums)):
            outbox[b, i_] = v

        @pl.when(b != me)
        def _():
            cross(outbox, sumbox, b, me, bs, br).start()

        return carry

    lax.fori_loop(0, n, fill, 0)
    sumbox[me] = outbox[me]
    for yy in range(2):

        @pl.when(jnp.logical_or(jnp.logical_not(pg.inner), yy != y))
        def _(yy=yy):
            remote(ein.at[yy], ein.at[yy], es, er.at[yy], {"ka": z * 2 + 1 - y}).wait_recv()

    def inner_level(zz, carry):
        @pl.when(zz != z)
        def _():
            remote(
                emir.at[zz], emir.at[zz], fs, fr.at[zz], {"ka": z * 2 + 1 - y}
            ).wait_recv()

        return carry

    lax.fori_loop(1, nz - 1, inner_level, 0)
    def arrived(box, rs):
        rest = box.at[pl.ds(0, n - 1)]
        remote(rest, rest, rs, rs, {"ka": z * 2 + 1 - y}).wait_recv()

    arrived(inbox, ar)
    sub = quarter // 2

    def picked(ref, at, r):
        even = ref[at + (pl.ds(0, sub, stride=2),)]
        odd = ref[at + (pl.ds(1, sub, stride=2),)]
        zero = jnp.concatenate([even[:, :nt], odd[:, :nt]], axis=1)
        one = jnp.concatenate([even[:, nt:], odd[:, nt:]], axis=1)
        return jnp.where(r == 0, zero, one)

    for j in range(rows):
        at, et_ = at_ref[0, j], at_ref[1, j]
        b = et_ // CAPQ
        direct = picked(inbox, (at // CAPQ,), at % CAPQ)
        term = picked(ein, (b % 2, b // 2), et_ % CAPQ)
        lines[g, pl.ds(j * sub, sub)] = 2.0 * term - direct
    base = rows * sub
    x, c = g // 2, g % 2
    mate, far = x * 2 + 1 - c, (1 - x) * 2 + c
    parts = (pl.ds(0, base), pl.ds(base, doubles * quarter))

    def spread(i, m, whose, to):
        block = lines.at[whose, parts[m]]
        return remote(block, block, gs, gr.at[m if i == 0 else 2], {"ga": to})

    spread(0, 0, g, far).start()
    spread(1, 0, g, mate).start()
    xg.finish()
    rg.finish()
    red.finish()
    end.finish()
    arrived(sumbox, br)
    for i in range(doubles):
        total = lax.fori_loop(
            1, n, lambda o, t, i=i: t + sumbox[o, i], sumbox[0, i]
        )
        term = lax.fori_loop(
            2, nz - 1, lambda zz, t, i=i: t + emir[zz, i], emir[1, i]
        )
        lines[g, pl.ds(base + i * quarter, quarter)] = 2.0 * term - total
    spread(0, 1, g, far).start()
    spread(1, 1, g, mate).start()
    for m in range(2):
        spread(0, m, far, far).wait_recv()
        spread(2, m, far, mate).start()
    for src, ss in ((own, as_), (outbox, bs)):
        rest = src.at[pl.ds(0, n - 1)]
        remote(rest, rest, ss, ss, {"ka": z * 2 + 1 - y}).wait_send()
    @pl.when(pg.inner)
    def _():
        ered.finish()
        for edged, count in ((True, 3), (False, 1)):

            @pl.when(pg.edged if edged else jnp.logical_not(pg.edged))
            def _(count=count):
                sent_lines = eown.at[:, pl.ds(0, count)]
                remote(sent_lines, sent_lines, es, es, {"ka": z * 2 + 1 - y}).wait_send()

        rest = ebox.at[pl.ds(0, nz - 1)]
        remote(rest, rest, fs, fs, {"ka": z * 2 + 1 - y}).wait_send()

    for count, ss, rs in ((3, gs, None), (2, None, gr.at[2])):
        block = lines.at[pl.ds(0, count)]
        if rs is None:
            remote(block, block, ss, ss, {"ga": mate}).wait_send()
        else:
            remote(block, block, rs, rs, {"ga": mate}).wait_recv()


def layout(lines, blocks_ref, mirr_ref, turned, flat):
    n_ga = lines.shape[0]
    rows, per_dev = blocks_ref.shape[0], mirr_ref.shape[0]
    nt = turned.shape[1]
    quarter, sub, doubles = nt // n_ga, nt // n_ga // 2, per_dev // 2
    base = rows * sub
    lanes = 2 * nt
    for q in range(n_ga):
        for t in range(sub):
            blocks_ref[:, (q * sub + t) * lanes : (q * sub + t + 1) * lanes] = lines[
                q, pl.ds(t, rows, stride=sub)
            ]
    for i in range(doubles):
        whole = jnp.concatenate(
            [lines[q, pl.ds(base + i * quarter, quarter)] for q in range(n_ga)], axis=0
        )
        turned[...] = whole.T
        even = turned[pl.ds(0, nt, stride=2)]
        odd = turned[pl.ds(1, nt, stride=2)]
        both = jnp.concatenate([even, odd], axis=1)
        flat[pl.ds(i * nt // 2, nt // 2)] = both[: nt // 2]
        flat[pl.ds((i + doubles) * nt // 2, nt // 2)] = both[nt // 2 :]
    for t in range(nt // 2):
        mirr_ref[:, t * lanes : (t + 1) * lanes] = flat[pl.ds(t, per_dev, stride=nt // 2)]


def per_device(x_dens, y_dens, p_dens, coulomb, screened, pairs, q_slot):
    n = lax.axis_size("ka")
    n_ga = lax.axis_size("ga")
    per_dev, nt, g = x_dens.shape
    q_slots = screened.shape[0]
    rows = pairs.shape[0]
    slots = n * CAPQ
    nz = n // 2
    shape = jax.ShapeDtypeStruct
    wide = F32 if slots * nt <= 2048 else BF16
    quarter = nt // n_ga
    each = (quarter, CAPQ * nt)
    line = (n,) + each
    dma = lambda m: pltpu.SemaphoreType.DMA((m,))
    one = pltpu.SemaphoreType.DMA
    row_len = -(-5 * slots // 128) * 128
    k_all = n * per_dev
    lines = pl.pallas_call(
        functools.partial(kernel, n),
        out_shape=shape((n_ga, rows * quarter // 2 + per_dev // 2 * quarter, CAPQ * nt), F32),
        in_specs=[SM, SM, HB, HB, HB, VM, HB],
        out_specs=VM,
        scratch_shapes=[
            pltpu.SMEM((n, row_len), I32),
            pltpu.SMEM((2, rows), I32),
            pltpu.VMEM((1, row_len), I32),
            pltpu.VMEM((g, q_slots, screened.shape[2]), BF16),
            pltpu.VMEM((q_slots, g, screened.shape[2]), BF16),
            pltpu.VMEM((nz * per_dev, nt, g), BF16),
            pltpu.VMEM((nz * CAPQ, nt, g), BF16),
            pltpu.VMEM((nz * CAPQ, nt, g), BF16),
            pltpu.VMEM((k_all, nt, g), BF16),
            pltpu.VMEM((k_all, nt, g), BF16),
            pltpu.VMEM((n_ga, slots, nt, g), wide),
            pltpu.VMEM((slots, nt, g), BF16),
            pltpu.VMEM((2, slots, nt, g), wide),
            pltpu.VMEM((slots, nt, g), BF16),
            pltpu.VMEM((slots, nt, g), BF16),
            pltpu.VMEM((n_ga,) + line, F32),
            pltpu.VMEM(line, F32),
            pltpu.VMEM((2,) + line, F32),
            pltpu.VMEM(line, F32),
            pltpu.VMEM(line, F32),
            pltpu.VMEM(line, I32),
            pltpu.VMEM((n, per_dev // 2) + each, F32),
            pltpu.VMEM((n, per_dev // 2) + each, F32),
            pltpu.VMEM(line, F32),
            pltpu.VMEM((4 * per_dev, 2 * nt, g), BF16),
            pltpu.VMEM((n_ga, 4 * nz) + each, F32),
            pltpu.VMEM((nz, 4) + each, F32),
            pltpu.VMEM((2, 4 * nz) + each, F32),
            pltpu.VMEM((4 * nz,) + each, F32),
            pltpu.VMEM((4 * nz,) + each, F32),
            pltpu.VMEM((nz, per_dev // 2) + each, F32),
            pltpu.VMEM((2, nz) + each, F32),
            pltpu.VMEM((nz, per_dev // 2) + each, F32),
            one, one, dma(3),
            dma(3 * nz), dma(2 * nz),
            dma(2 * nz), dma(nz * per_dev),
            dma(nz), dma(nz),
            dma(3 * nz), dma(nz * (per_dev + 2)),
            dma(2 * nz + 3), dma(nz * per_dev + 2),
            one, dma(nz + 1), one, dma(1),
            one, dma(8), one, dma(4),
            one, dma(2 * nz), one, dma(nz),
            one, dma(2), one, dma(nz),
            one, one, one, one,
            one, dma(3),
        ],
        compiler_params=pltpu.CompilerParams(
            collective_id=0, has_side_effects=True, vmem_limit_bytes=LIMIT
        ),
        name="window",
    )(pairs.T, q_slot, x_dens, y_dens, p_dens, coulomb, screened.transpose(1, 0, 2))
    blocks, mirrored = pl.pallas_call(
        layout,
        out_shape=[shape((rows, nt * nt), F32), shape((per_dev, nt * nt), F32)],
        in_specs=[VM],
        out_specs=[VM, VM],
        scratch_shapes=[
            pltpu.VMEM((2 * nt, nt), F32),
            pltpu.VMEM((per_dev * nt // 2, 2 * nt), F32),
        ],
        name="layout",
    )(lines)
    return (blocks, mirrored)


def solution(mesh):
    in_specs = (
        P("ka", None, "ga"),
        P("ka", None, "ga"),
        P("ka", None, "ga"),
        P("ga"),
        P("ka", "ga", None),
        P("ka", None),
        P(),
    )
    out_specs = (P("ka", None), P("ka", None))
    return jax.shard_map(
        per_device, mesh=mesh, in_specs=in_specs, out_specs=out_specs, check_vma=False
    )
```

```python
import functools
import jax
import jax.numpy as jnp
from jax import lax
from jax.experimental import pallas as pl
from jax.experimental.pallas import tpu as pltpu
from jax.sharding import PartitionSpec as P

CAPQ = 2
F32 = jnp.float32
BF16 = jnp.bfloat16
I32 = jnp.int32
VM = pl.BlockSpec(memory_space=pltpu.VMEM)
SM = pl.BlockSpec(memory_space=pltpu.SMEM)
HB = pl.BlockSpec(memory_space=pl.ANY)
LIMIT = 66000000
DIMS = (((1,), (1,)), ((), ()))


def start(c):
    c.start()


def sent(c):
    c.wait_send()


def remote(src, dst, ss, rs, to):
    return pltpu.make_async_remote_copy(
        src_ref=src,
        dst_ref=dst,
        send_sem=ss,
        recv_sem=rs,
        device_id=to,
        device_id_type=pl.DeviceIdType.MESH,
    )


def greet(n, meanwhile):
    barrier = pltpu.get_barrier_semaphore()
    me = lax.axis_index("ka")
    g = lax.axis_index("ga")
    z, y = me // 2, me % 2
    nz = n // 2

    def hello(to):
        pl.semaphore_signal(barrier, inc=1, device_id=to, device_id_type=pl.DeviceIdType.MESH)

    @pl.when(z > 0)
    def _():
        hello({"ka": me - 2})

    @pl.when(z < nz - 1)
    def _():
        hello({"ka": me + 2})

    hello({"ka": z * 2 + 1 - y})
    hello({"ga": g // 2 * 2 + 1 - g % 2})
    hello({"ga": (1 - g // 2) * 2 + g % 2})
    meanwhile()
    pl.semaphore_wait(barrier, 5 - jnp.where(z > 0, 0, 1) - jnp.where(z < nz - 1, 0, 1))


class Gather:
    def __init__(self, n, src, out, send, recv, cut):
        self.n, self.nz = n, n // 2
        self.me = lax.axis_index("ka")
        self.z, self.y = self.me // 2, self.me % 2
        self.src, self.out, self.send, self.recv = src, out, send, recv
        self.size = src.shape[0]
        self.cut = cut

    def landed(self, zz, same, k):
        few = self.size - self.cut
        if same:
            return self.recv.at[zz * self.size + k]
        if k >= self.cut:
            return self.recv.at[self.nz * self.size + zz * few + k - self.cut]
        return self.recv.at[self.nz * (self.size + few) + zz]

    def copy(self, zz, yy, k, way, own=False):
        at = (zz * 2 + yy) * self.size + k
        block = self.out.at[at]
        if way == 2:
            target = self.z * 2 + 1 - self.y
        else:
            target = (self.z + (1 if way == 0 else -1)) * 2 + self.y
        return remote(
            self.src.at[k] if own else block,
            block,
            self.send.at[way * self.nz + zz],
            self.landed(zz, (yy is self.y) != (way == 2), k),
            {"ka": target},
        )

    def take(self, zz, yy, k):
        block = self.out.at[(zz * 2 + yy) * self.size + k]
        done = self.landed(zz, yy is self.y, k)
        remote(block, block, done, done, {"ka": self.z * 2 + 1 - self.y}).wait_recv()

    def some(self, count):
        return self.out.at[pl.ds(0, count)]

    def take_late(self, zz):
        block, done = self.some(self.cut), self.landed(zz, False, 0)
        remote(block, block, done, done, {"ka": self.z * 2 + 1 - self.y}).wait_recv()

    def all_sent(self, zz, way, count):
        block, done = self.some(count), self.send.at[way * self.nz + zz]
        remote(block, block, done, done, {"ka": self.z * 2 + 1 - self.y}).wait_send()

    def chained(self, zz, ways=(0, 1)):
        for way in ways:
            free = self.z < self.nz - 1 if way == 0 else self.z > 0

            @pl.when(free)
            def _(way=way):
                self.all_sent(zz, way, 2 * self.size - self.cut)

    def chain(self, zz, yy, k, act, ways=(0, 1), own=False):
        for way in ways:
            free = self.z < self.nz - 1 if way == 0 else self.z > 0

            @pl.when(free)
            def _(way=way):
                act(self.copy(zz, yy, k, way, own))

    def early(self):
        return range(self.cut, self.size)

    def across_early(self):
        for k in self.early():
            self.copy(self.z, self.y, k, 2, True).start()

    def across_late(self):
        for k in range(self.cut):
            self.copy(self.z, self.y, k, 2, True).start()

    def first(self):
        for k in range(self.size):
            self.chain(self.z, self.y, k, start, own=True)

    def second(self):
        for k in self.early():
            self.take(self.z, 1 - self.y, k)
            self.chain(self.z, 1 - self.y, k, start)

    def sides(self, h, act):
        for way in (0, 1):
            zz = self.z - h if way == 0 else self.z + h
            there = zz >= 0 if way == 0 else zz < self.nz

            @pl.when(there)
            def _(zz=zz, way=way):
                act(zz, way)

    def hop(self, h, low=0, high=None):
        def one(k, yy, zz, way):
            self.take(zz, yy, k)
            self.chain(zz, yy, k, start, (way,))

        for k in range(self.size)[low:high]:

            def own(zz, way, k=k):
                one(k, self.y, zz, way)
                if k < self.cut:
                    self.copy(zz, self.y, k, 2).start()

            self.sides(h, own)
        for k in self.early() if high is None else ():
            self.sides(h, lambda zz, way, k=k: one(k, 1 - self.y, zz, way))

    def finish(self):
        self.chained(self.z)
        self.all_sent(self.z, 2, self.size)
        self.take_late(self.z)

        def tail(h, carry):
            def side(zz, way):
                self.chained(zz, (way,))
                self.all_sent(zz, 2, self.cut)
                self.take_late(zz)

            self.sides(h, side)
            return carry

        lax.fori_loop(1, self.nz, tail, 0)


class Rows(Gather):
    def some(self, count):
        return self.out.at[0]

    def begin(self):
        self.chain(self.z, self.y, 0, start, own=True)
        self.copy(self.z, self.y, 0, 2, True).start()

    def finish(self):
        self.chained(self.z)
        self.all_sent(self.z, 2, 1)

        def tail(h, carry):
            def side(zz, way):
                self.chained(zz, (way,))
                self.all_sent(zz, 2, 1)

            self.sides(h, side)
            return carry

        lax.fori_loop(1, self.nz, tail, 0)


class Hub(Gather):
    def __init__(self, n, src, out, send, recv):
        super().__init__(n, src, out, send, recv, src.shape[0])
        self.inner = jnp.logical_and(self.z >= 1, self.z <= self.nz - 2)
        self.edged = jnp.logical_or(self.z == 1, self.z == self.nz - 2)
        self.edge = jnp.where(self.z == 1, 0, self.nz - 1)

    def copy(self, zz, yy, k, way, own=False):
        base = (zz * 2 + yy) * self.size
        target = (self.z + (1 if way == 0 else -1)) * 2 + self.y
        return remote(
            self.src.at[k] if own else self.out.at[base + k],
            self.out.at[base + k],
            self.send.at[way * self.nz + zz],
            self.recv.at[zz * self.size + k],
            {"ka": target},
        )

    def block(self, zz, yy):
        return self.out.at[pl.ds((zz * 2 + yy) * self.size, self.size)]

    def cross(self, i):
        return remote(
            self.src,
            self.block(self.z, self.y),
            self.send.at[2 * self.nz + i],
            self.recv.at[self.nz * self.size + i],
            {"ka": self.z * 2 + 1 - self.y},
        )

    def crossed(self, zz, i):
        block, done = self.block(zz, 1 - self.y), self.recv.at[self.nz * self.size + i]
        remote(block, block, done, done, {"ka": self.z * 2 + 1 - self.y}).wait_recv()

    def inward(self):
        block = self.block(self.z, 1 - self.y)
        return remote(
            block,
            block,
            self.send.at[2 * self.nz + 2],
            self.recv.at[self.nz * self.size + 1],
            {"ka": jnp.where(self.z == 0, 1, self.nz - 2) * 2 + self.y},
        )

    def pass_inward(self):
        self.crossed(self.z, 1)
        self.inward().start()

    def chained(self, zz, ways=(0, 1)):
        for way in ways:
            free = self.z <= self.nz - 3 if way == 0 else self.z >= 2

            @pl.when(free)
            def _(way=way):
                self.all_sent(zz, way, self.size)

    def chain(self, zz, yy, k, act, ways=(0, 1), own=False):
        for way in ways:
            free = self.z <= self.nz - 3 if way == 0 else self.z >= 2

            @pl.when(free)
            def _(way=way):
                act(self.copy(zz, yy, k, way, own))

    def first(self):
        for k in range(self.size):
            self.chain(self.z, self.y, k, start, own=True)

    def hop(self, h):
        def own(zz, way):
            end = jnp.logical_and(self.edged, zz == self.edge)
            for k in range(self.size):

                @pl.when(jnp.logical_not(end))
                def _(k=k):
                    self.copy(zz, self.y, k, way).wait_recv()

                self.chain(zz, self.y, k, start, (way,))

        self.sides(h, own)

    def edge_in(self):
        @pl.when(self.edged)
        def _():
            for k in range(self.size):
                self.copy(self.edge, self.y, k, 2).wait_recv()

    def finish(self):
        self.chained(self.z)

        @pl.when(jnp.logical_not(self.inner))
        def _():
            self.cross(1).wait_send()
            self.inward().wait_send()

        @pl.when(self.inner)
        def _():
            self.cross(0).wait_send()

            def tail(h, carry):
                self.sides(h, lambda zz, way: self.chained(zz, (way,)))
                return carry

            lax.fori_loop(1, self.nz, tail, 0)


class Pick:
    def __init__(self, n, src, col, out, got, tab, send, recv, ps, pr):
        self.n, self.nz = n, n // 2
        self.me = lax.axis_index("ka")
        self.z, self.y = self.me // 2, self.me % 2
        self.src, self.col, self.out, self.got, self.tab = src, col, out, got, tab
        self.send, self.recv, self.ps, self.pr = send, recv, ps, pr
        self.size = src.shape[0]

    def copy(self, zz, k, way, own=False):
        at = zz * self.size + k
        target = (self.z + (1 if way == 0 else -1)) * 2 + self.y
        return remote(
            self.src.at[k] if own else self.col.at[at],
            self.col.at[at],
            self.send.at[way * self.nz + zz],
            self.recv.at[at],
            {"ka": target},
        )

    def chain(self, zz, k, act, ways=(0, 1), own=False):
        for way in ways:
            free = self.z < self.nz - 1 if way == 0 else self.z > 0

            @pl.when(free)
            def _(way=way):
                act(self.copy(zz, k, way, own))

    def sides(self, h, act):
        for way in (0, 1):
            zz = self.z - h if way == 0 else self.z + h
            there = zz >= 0 if way == 0 else zz < self.nz

            @pl.when(there)
            def _(zz=zz, way=way):
                act(zz, way)

    def first(self):
        for k in range(self.size):
            self.chain(self.z, k, start, own=True)

    def hop(self, h):
        for k in range(self.size):

            def one(zz, way, k=k):
                self.copy(zz, k, way).wait_recv()
                self.chain(zz, k, start, (way,))

            self.sides(h, one)

    def chosen(self, zz, owner, r):
        which = self.tab[zz * 2 + self.y, owner * CAPQ + r]
        v = self.col[zz * self.size]
        for k in range(1, self.size):
            v = jnp.where(which == k, self.col[zz * self.size + k], v)
        return v

    def across(self, zz):
        rows = pl.ds(zz * CAPQ, CAPQ)
        return remote(
            self.out.at[rows],
            self.got.at[rows],
            self.ps.at[zz],
            self.pr.at[zz],
            {"ka": self.z * 2 + 1 - self.y},
        )

    def pass_on(self, zz):
        for r in range(CAPQ):
            self.out[zz * CAPQ + r] = self.chosen(zz, self.z * 2 + 1 - self.y, r)
        self.across(zz).start()

    def chained(self, zz, ways=(0, 1)):
        block = self.col.at[pl.ds(zz * self.size, self.size)]
        for way in ways:
            free = self.z < self.nz - 1 if way == 0 else self.z > 0
            done = self.send.at[way * self.nz + zz]

            @pl.when(free)
            def _(done=done):
                remote(block, block, done, done, {"ka": self.z * 2 + 1 - self.y}).wait_send()

    def finish(self):
        self.chained(self.z)
        self.across(self.z).wait_send()

        def tail(h, carry):
            def side(zz, way):
                self.chained(zz, (way,))
                self.across(zz).wait_send()

            self.sides(h, side)
            return carry

        lax.fori_loop(1, self.nz, tail, 0)


class Reduce:
    def __init__(self, part, out, recv1, tsend, recv2, s1, r1, s2, r2, per, lump):
        self.g = lax.axis_index("ga")
        self.x, self.c = self.g // 2, self.g % 2
        self.part, self.out = part, out
        self.recv1, self.tsend, self.recv2 = recv1, tsend, recv2
        self.s1, self.r1, self.s2, self.r2, self.per = s1, r1, s2, r2, per
        self.lump, self.pieces = lump, part.shape[1] // per

    def rows(self, i):
        return pl.ds(i * self.per, self.per)

    def one(self, t, i):
        xx = self.x if t else 1 - self.x
        return remote(
            self.part.at[xx * 2 + 1 - self.c, self.rows(i)],
            self.recv1.at[xx, self.rows(i)],
            self.s1,
            self.r1.at[self.pieces + (0 if self.lump else i) if t else i],
            {"ga": self.x * 2 + 1 - self.c},
        )

    def two(self, i):
        return remote(
            self.tsend.at[self.rows(i)],
            self.recv2.at[self.rows(i)],
            self.s2,
            self.r2.at[0 if self.lump else i],
            {"ga": (1 - self.x) * 2 + self.c},
        )

    def sum_one(self, xx, i):
        v = self.part[xx * 2 + self.c, self.rows(i)].astype(F32)
        return v + self.recv1[xx, self.rows(i)].astype(F32)

    def begin(self, i):
        self.one(0, i).start()
        self.one(1, i).start()

    def middle(self, i):
        self.one(0, i).wait_recv()
        self.tsend[self.rows(i)] = self.sum_one(1 - self.x, i).astype(self.tsend.dtype)
        self.two(i).start()

    def arrive(self):
        to = {"ga": self.x * 2 + 1 - self.c}
        for block, done in ((self.recv1.at[self.x], self.r1.at[self.pieces]), (self.recv2, self.r2.at[0])):
            remote(block, block, done, done, to).wait_recv()

    def end(self, i):
        if not self.lump:
            self.one(1, i).wait_recv()
            self.two(i).wait_recv()
        v = self.sum_one(self.x, i)
        v = (v + self.recv2[self.rows(i)].astype(F32)).astype(self.out.dtype)
        if len(self.out.shape) == len(self.tsend.shape):
            self.out[self.rows(i)] = v
        else:
            self.out[i] = v

    def finish(self):
        to = {"ga": self.x * 2 + 1 - self.c}
        both = self.part.at[pl.ds(0, 2)]
        remote(both, both, self.s1, self.s1, to).wait_send()
        remote(self.tsend, self.tsend, self.s2, self.s2, to).wait_send()


def make_row(n, q_slots, per_dev, pairs_ref, qs_ref, row_ref, at_ref):
    rows = pairs_ref.shape[1]
    slots = n * CAPQ
    lane = lax.broadcasted_iota(I32, row_ref.shape, 1)
    section = lane // slots
    spot = lane % slots
    row = jnp.where(jnp.logical_or(section == 2, section == 4), -1, 0)
    holders = ([], [])
    for j in range(rows):
        slot = qs_ref[pairs_ref[2, j]]
        owner = slot // q_slots
        first, second = pairs_ref[0, j] % per_dev, pairs_ref[1, j]
        at = []
        for i, o in enumerate((owner, second // per_dev)):
            rank = jnp.int32(0)
            for other in holders[i]:
                rank = rank + jnp.where(other == o, 1, 0)
            holders[i].append(o)
            at.append(o * CAPQ + rank)
            at_ref[i, j] = at[i]
        value = jnp.where(section == 1, slot - owner * q_slots, second)
        value = jnp.where(jnp.logical_or(section == 0, section == 3), first, value)
        hit = spot == jnp.where(section < 3, at[0], at[1])
        row = jnp.where(hit, value, row)
    row_ref[...] = row


def kernel(n, pairs_hbm, qs_hbm, x_ref, y_ref, p_ref, v_hbm, w_hbm, lines,
           pairs_ref, qs_ref, v_ref, tab, at_ref, row_ref, wt, w_ref, x_col, x_out, x_got, y_all, p_all, part, half,
           recv1, tsend, recv2, part2, own, q1, qt, q2, second, outbox, sumbox, inbox,
           split, part3, eown, e1, et, e2, ebox, ein, emir,
           ws, ls, ks, ts, tr, xs, xr, xps, xpr, ys, yr, ps, pr, s1, r1, s2, r2, t1, u1, t2, u2,
           v1, w1, v2, w2, es, er, fs, fr, as_, ar, bs, br, gs, gr):
    per_dev, nt, width = x_ref.shape
    rows = pairs_ref.shape[1]
    q_slots = w_ref.shape[0]
    nz = n // 2
    slots = n * CAPQ
    n_ga = part.shape[0]
    me = lax.axis_index("ka")
    g = lax.axis_index("ga")
    z, y = me // 2, me % 2
    fetch = pltpu.make_async_copy(w_hbm, wt, ws)
    lists = [
        pltpu.make_async_copy(pairs_hbm, pairs_ref, ks.at[3]),
        pltpu.make_async_copy(qs_hbm, qs_ref, ks.at[4]),
    ]
    for c in lists:
        c.start()
    weights = pltpu.make_async_copy(v_hbm, v_ref, ks.at[5])
    weights.start()
    fetch.start()
    mine = pl.ds(me * per_dev, per_dev)
    keeps = [
        pltpu.make_async_copy(x_ref, x_col.at[pl.ds(z * per_dev, per_dev)], ks.at[0]),
        pltpu.make_async_copy(p_ref, p_all.at[mine], ks.at[1]),
        pltpu.make_async_copy(y_ref, y_all.at[mine], ks.at[2]),
    ]
    for c in keeps:
        c.start()

    def table():
        for c in lists:
            c.wait()
        make_row(n, q_slots, per_dev, pairs_ref, qs_ref, row_ref, at_ref)

    greet(n, table)
    xg = Pick(n, x_ref, x_col, x_out, x_got, tab, xs, xr, xps, xpr)
    yg = Gather(n, y_ref, y_all, ys, yr, per_dev - 1)
    pg = Hub(n, p_ref, p_all, ps, pr)
    outer = jnp.logical_not(pg.inner)
    keep = pltpu.make_async_copy(row_ref.at[0], tab.at[me], ls)

    rg = Rows(n, row_ref, tab, ts, tr, 1)
    rg.begin()
    xg.first()
    keep.start()
    keep.wait()
    for c in keeps:
        c.wait()
    xg.pass_on(z)

    yg.across_early()

    @pl.when(outer)
    def _():
        pg.first()
        pg.cross(1).start()
        yg.first()

    @pl.when(pg.inner)
    def _():
        pg.cross(0).start()

    fetch.wait()
    turn = 16
    whole = width // turn * turn

    def relay(i, carry):
        at = pl.ds(pl.multiple_of(i * turn, turn), turn)
        w_ref[:, at] = jnp.swapaxes(wt[at], 0, 1)
        return carry

    lax.fori_loop(0, width // turn, relay, 0)
    if whole < width:
        w_ref[:, whole:] = jnp.swapaxes(wt[whole:], 0, 1)
    red = Reduce(part, half, recv1, tsend, recv2, s1, r1, s2, r2, 2 * CAPQ, True)

    def multiply(v, a, r):
        w = tab[a, slots + me * CAPQ + r]
        v = jnp.dot(v, w_ref[w], preferred_element_type=F32)
        for i in range(n_ga):
            part[i, a * CAPQ + r] = v[:, i * width : (i + 1) * width].astype(part.dtype)

    def piece(zz):
        for r in range(CAPQ):
            multiply(xg.chosen(zz, me, r), zz * 2 + y, r)
        rg.take_late(zz)
        xg.across(zz).wait_recv()
        for r in range(CAPQ):
            multiply(x_got[zz * CAPQ + r], zz * 2 + 1 - y, r)
        red.begin(zz)

    quarter = nt // n_ga
    weights.wait()
    weight = v_ref[...].reshape(1, width)
    sets = jnp.where(pg.edged, 4, 2)
    ered = Reduce(part3, eown, e1, et, e2, v1, w1, v2, w2, 4, False)

    def of(q):
        return jnp.where(q // 2 == 0, z, pg.edge) * 2 + q % 2

    def joined(both, out, at):
        v = jnp.concatenate(both, axis=1)
        for i in range(n_ga):
            out[i, at] = v[i * quarter : (i + 1) * quarter]

    def weigh(q, carry):
        for k in range(per_dev):
            weighted = p_all[of(q) * per_dev + k].astype(F32) * weight
            high = weighted.astype(BF16)
            split[q * per_dev + k, :nt] = high
            split[q * per_dev + k, nt:] = (weighted - high.astype(F32)).astype(BF16)
        return carry

    def exchange(zz):
        base = (zz * 2 + y) * per_dev

        def one(q, carry):
            a = of(q)
            both = []
            for r in range(CAPQ):
                at = 3 * slots + (zz * 2 + y) * CAPQ + r
                which = tab[a, at + slots] - base
                other = p_all[base]
                for k in range(1, per_dev):
                    other = jnp.where(which == k, p_all[base + k], other)
                v = lax.dot_general(
                    split[q * per_dev + tab[a, at]], other, DIMS, preferred_element_type=F32
                )
                both.append(v[:nt] + v[nt:])
            joined(both, part3, zz * 4 + q)
            return carry

        lax.fori_loop(0, sets, one, 0)
        ered.begin(zz)

    shape = own.shape[1:]
    left = lax.broadcasted_iota(I32, shape, 1) < nt
    doubles = per_dev // 2

    def paired(sums):
        sums = [v[:, :nt] + v[:, nt:] for v in sums]
        return [
            jnp.concatenate([sums[i], sums[i + doubles]], axis=1) for i in range(doubles)
        ]

    def to_first(q, zz):
        return remote(eown.at[zz, q], ein.at[y, zz], es, er.at[y], {"ka": of(q)})

    def to_second(zz):
        return remote(ebox.at[zz], emir.at[z], fs, fr.at[z], {"ka": zz * 2 + y})

    def deliver(zz):
        ered.end(zz)

        def give(q, carry):
            @pl.when(q != y)
            def _():
                to_first(q, zz).start()

            return carry

        lax.fori_loop(0, sets, give, 0)
        ein[y, zz] = eown[zz, y]

        def add(q, sums):
            at = 4 * slots + (zz * 2 + y) * CAPQ
            k2 = jnp.where(left, tab[of(q), at], tab[of(q), at + 1])
            v = eown[zz, q]
            base = (zz * 2 + y) * per_dev
            return tuple(t + jnp.where(k2 == base + i, v, 0.0) for i, t in enumerate(sums))

        sums = lax.fori_loop(0, sets, add, tuple(jnp.zeros(shape, F32) for _ in range(per_dev)))
        for i, v in enumerate(paired(sums)):
            ebox[zz, i] = v

        @pl.when(zz != z)
        def _():
            to_second(zz).start()

        @pl.when(zz == z)
        def _():
            emir[z] = ebox[z]

    rg.hop(1)
    xg.hop(1)

    @pl.when(pg.inner)
    def _():
        pg.first()

    xg.sides(1, lambda zz, way: xg.pass_on(zz))
    piece(z)

    def stage(h, carry):
        @pl.when(h < nz)
        def _():
            rg.hop(h)
            xg.hop(h)

        @pl.when(h == 2)
        def _():
            @pl.when(pg.inner)
            def _():
                yg.first()

            yg.second()

        @pl.when(h < nz)
        def _():
            xg.sides(h, lambda zz, way: xg.pass_on(zz))

        @pl.when(h == 2)
        def _():
            @pl.when(pg.inner)
            def _():
                pg.edge_in()

            @pl.when(outer)
            def _():
                pg.pass_inward()

            yg.across_late()

            red.middle(z)

        @pl.when(h > 2)
        def _():
            xg.sides(h - 2, lambda zz, way: red.middle(zz))

        xg.sides(h - 1, lambda zz, way: piece(zz))

        @pl.when(jnp.logical_and(h >= 3, h < nz))
        def _():
            yg.hop(h - 2)

        return carry

    lax.fori_loop(2, nz + 1, stage, 0)

    @pl.when(pg.inner)
    def _():
        pg.hop(1)
        pg.crossed(z, 0)

        @pl.when(pg.edged)
        def _():
            pg.crossed(pg.edge, 1)

        lax.fori_loop(0, sets, weigh, 0)
        exchange(z)

    xg.sides(nz - 1, lambda zz, way: red.middle(zz))
    half_way = per_dev // 2
    yg.hop(nz - 2, 0, half_way)

    @pl.when(pg.inner)
    def _():
        pg.sides(1, lambda zz, way: exchange(zz))

    yg.hop(nz - 2, half_way)

    @pl.when(pg.inner)
    def _():
        ered.middle(z)
        pg.sides(1, lambda zz, way: ered.middle(zz))

    @pl.when(pg.inner)
    def _():
        def level(h, carry):
            pg.hop(h)
            pg.sides(h, lambda zz, way: exchange(zz))
            return carry

        lax.fori_loop(2, nz, level, 0)

    pg.finish()
    yg.hop(nz - 1)

    red.arrive()
    lax.fori_loop(0, nz, lambda i, c: (red.end(i), c)[1], 0)
    yg.finish()

    def source(a, carry):
        both = []
        for r in range(CAPQ):
            k2 = jnp.maximum(tab[a, 2 * slots + me * CAPQ + r], 0)
            both.append(
                lax.dot_general(half[a * CAPQ + r], y_all[k2], DIMS, preferred_element_type=F32)
            )
        joined(both, part2, a)
        return carry

    end = Reduce(part2, own, q1, qt, q2, t1, u1, t2, u2, n // 4, False)
    for i in range(4):
        lax.fori_loop(i * n // 4, (i + 1) * n // 4, source, 0, unroll=2)
        end.begin(i)
    def seconds(a, carry):
        at = 2 * slots + me * CAPQ
        second[a] = jnp.where(left, tab[a, at], tab[a, at + 1])
        return carry

    lax.fori_loop(0, n, seconds, 0)

    @pl.when(pg.inner)
    def _():
        def level(h, carry):
            pg.sides(h, lambda zz, way: ered.middle(zz))
            return carry

        lax.fori_loop(2, nz, level, 0)

    for i in range(4):
        end.middle(i)

    @pl.when(pg.inner)
    def _():
        deliver(z)

        def level(h, carry):
            pg.sides(h, lambda zz, way: deliver(zz))
            return carry

        lax.fori_loop(1, nz, level, 0)


    def cross(src, box, i, whose, ss, rs):
        return remote(src.at[i], box.at[whose], ss, rs, {"ka": i})

    def far_first(i):
        return jnp.where(z < nz // 2, n - 1 - i, i)

    for i in range(4):
        end.end(i)

    def give(i, carry):
        b = far_first(i)

        @pl.when(b != me)
        def _():
            cross(own, inbox, b, me, as_, ar).start()

        return carry

    lax.fori_loop(0, n, give, 0)
    inbox[me] = own[me]


    def fill(i, carry):
        b = far_first(i)

        def add(a, sums):
            out = []
            for i in range(per_dev):
                out.append(sums[i] + jnp.where(second[a] == b * per_dev + i, own[a], 0.0))
            return tuple(out)

        sums = tuple(jnp.zeros(shape, F32) for _ in range(per_dev))
        sums = lax.fori_loop(0, n, add, sums, unroll=min(n, 8))
        for i_, v in enumerate(paired(sums)):
            outbox[b, i_] = v

        @pl.when(b != me)
        def _():
            cross(outbox, sumbox, b, me, bs, br).start()

        return carry

    lax.fori_loop(0, n, fill, 0)
    sumbox[me] = outbox[me]
    for yy in range(2):

        @pl.when(jnp.logical_or(jnp.logical_not(pg.inner), yy != y))
        def _(yy=yy):
            remote(ein.at[yy], ein.at[yy], es, er.at[yy], {"ka": z * 2 + 1 - y}).wait_recv()

    def inner_level(zz, carry):
        @pl.when(zz != z)
        def _():
            remote(
                emir.at[zz], emir.at[zz], fs, fr.at[zz], {"ka": z * 2 + 1 - y}
            ).wait_recv()

        return carry

    lax.fori_loop(1, nz - 1, inner_level, 0)
    def arrived(box, rs):
        rest = box.at[pl.ds(0, n - 1)]
        remote(rest, rest, rs, rs, {"ka": z * 2 + 1 - y}).wait_recv()

    arrived(inbox, ar)
    sub = quarter // 2

    def picked(ref, at, r):
        even = ref[at + (pl.ds(0, sub, stride=2),)]
        odd = ref[at + (pl.ds(1, sub, stride=2),)]
        zero = jnp.concatenate([even[:, :nt], odd[:, :nt]], axis=1)
        one = jnp.concatenate([even[:, nt:], odd[:, nt:]], axis=1)
        return jnp.where(r == 0, zero, one)

    for j in range(rows):
        at, et_ = at_ref[0, j], at_ref[1, j]
        b = et_ // CAPQ
        direct = picked(inbox, (at // CAPQ,), at % CAPQ)
        term = picked(ein, (b % 2, b // 2), et_ % CAPQ)
        lines[g, pl.ds(j * sub, sub)] = 2.0 * term - direct
    base = rows * sub
    x, c = g // 2, g % 2
    mate, far = x * 2 + 1 - c, (1 - x) * 2 + c
    parts = (pl.ds(0, base), pl.ds(base, doubles * quarter))

    def spread(i, m, whose, to):
        block = lines.at[whose, parts[m]]
        return remote(block, block, gs, gr.at[m if i == 0 else 2], {"ga": to})

    spread(0, 0, g, far).start()
    spread(1, 0, g, mate).start()
    xg.finish()
    rg.finish()
    red.finish()
    end.finish()
    arrived(sumbox, br)
    for i in range(doubles):
        total = lax.fori_loop(
            1, n, lambda o, t, i=i: t + sumbox[o, i], sumbox[0, i]
        )
        term = lax.fori_loop(
            2, nz - 1, lambda zz, t, i=i: t + emir[zz, i], emir[1, i]
        )
        lines[g, pl.ds(base + i * quarter, quarter)] = 2.0 * term - total
    diag = (1 - x) * 2 + 1 - c
    spread(0, 1, g, far).start()
    spread(2, 1, g, diag).start()
    spread(1, 1, g, mate).start()
    spread(0, 0, far, far).wait_recv()
    spread(2, 0, far, mate).start()
    spread(0, 1, far, far).wait_recv()
    for src, ss in ((own, as_), (outbox, bs)):
        rest = src.at[pl.ds(0, n - 1)]
        remote(rest, rest, ss, ss, {"ka": z * 2 + 1 - y}).wait_send()
    @pl.when(pg.inner)
    def _():
        ered.finish()
        for edged, count in ((True, 3), (False, 1)):

            @pl.when(pg.edged if edged else jnp.logical_not(pg.edged))
            def _(count=count):
                sent_lines = eown.at[:, pl.ds(0, count)]
                remote(sent_lines, sent_lines, es, es, {"ka": z * 2 + 1 - y}).wait_send()

        rest = ebox.at[pl.ds(0, nz - 1)]
        remote(rest, rest, fs, fs, {"ka": z * 2 + 1 - y}).wait_send()

    for count, ss, rs in ((3, gs, None), (2, None, gr.at[2])):
        block = lines.at[pl.ds(0, count)]
        if rs is None:
            remote(block, block, ss, ss, {"ga": mate}).wait_send()
        else:
            remote(block, block, rs, rs, {"ga": mate}).wait_recv()


def layout(lines, blocks_ref, mirr_ref, turned, flat):
    n_ga = lines.shape[0]
    rows, per_dev = blocks_ref.shape[0], mirr_ref.shape[0]
    nt = turned.shape[1]
    quarter, sub, doubles = nt // n_ga, nt // n_ga // 2, per_dev // 2
    base = rows * sub
    lanes = 2 * nt
    for q in range(n_ga):
        for t in range(sub):
            blocks_ref[:, (q * sub + t) * lanes : (q * sub + t + 1) * lanes] = lines[
                q, pl.ds(t, rows, stride=sub)
            ]
    for i in range(doubles):
        whole = jnp.concatenate(
            [lines[q, pl.ds(base + i * quarter, quarter)] for q in range(n_ga)], axis=0
        )
        turned[...] = whole.T
        even = turned[pl.ds(0, nt, stride=2)]
        odd = turned[pl.ds(1, nt, stride=2)]
        both = jnp.concatenate([even, odd], axis=1)
        flat[pl.ds(i * nt // 2, nt // 2)] = both[: nt // 2]
        flat[pl.ds((i + doubles) * nt // 2, nt // 2)] = both[nt // 2 :]
    for t in range(nt // 2):
        mirr_ref[:, t * lanes : (t + 1) * lanes] = flat[pl.ds(t, per_dev, stride=nt // 2)]


def per_device(x_dens, y_dens, p_dens, coulomb, screened, pairs, q_slot):
    n = lax.axis_size("ka")
    n_ga = lax.axis_size("ga")
    per_dev, nt, g = x_dens.shape
    q_slots = screened.shape[0]
    rows = pairs.shape[0]
    slots = n * CAPQ
    nz = n // 2
    shape = jax.ShapeDtypeStruct
    wide = F32 if slots * nt <= 2048 else BF16
    quarter = nt // n_ga
    each = (quarter, CAPQ * nt)
    line = (n,) + each
    dma = lambda m: pltpu.SemaphoreType.DMA((m,))
    one = pltpu.SemaphoreType.DMA
    row_len = -(-5 * slots // 128) * 128
    k_all = n * per_dev
    lines = pl.pallas_call(
        functools.partial(kernel, n),
        out_shape=shape((n_ga, rows * quarter // 2 + per_dev // 2 * quarter, CAPQ * nt), F32),
        in_specs=[HB] * 7,
        out_specs=VM,
        scratch_shapes=[
            pltpu.SMEM((pairs.shape[1], rows), I32),
            pltpu.SMEM(q_slot.shape, I32),
            pltpu.VMEM((g,), F32),
            pltpu.SMEM((n, row_len), I32),
            pltpu.SMEM((2, rows), I32),
            pltpu.VMEM((1, row_len), I32),
            pltpu.VMEM((g, q_slots, screened.shape[2]), BF16),
            pltpu.VMEM((q_slots, g, screened.shape[2]), BF16),
            pltpu.VMEM((nz * per_dev, nt, g), BF16),
            pltpu.VMEM((nz * CAPQ, nt, g), BF16),
            pltpu.VMEM((nz * CAPQ, nt, g), BF16),
            pltpu.VMEM((k_all, nt, g), BF16),
            pltpu.VMEM((k_all, nt, g), BF16),
            pltpu.VMEM((n_ga, slots, nt, g), wide),
            pltpu.VMEM((slots, nt, g), BF16),
            pltpu.VMEM((2, slots, nt, g), wide),
            pltpu.VMEM((slots, nt, g), BF16),
            pltpu.VMEM((slots, nt, g), BF16),
            pltpu.VMEM((n_ga,) + line, F32),
            pltpu.VMEM(line, F32),
            pltpu.VMEM((2,) + line, F32),
            pltpu.VMEM(line, F32),
            pltpu.VMEM(line, F32),
            pltpu.VMEM(line, I32),
            pltpu.VMEM((n, per_dev // 2) + each, F32),
            pltpu.VMEM((n, per_dev // 2) + each, F32),
            pltpu.VMEM(line, F32),
            pltpu.VMEM((4 * per_dev, 2 * nt, g), BF16),
            pltpu.VMEM((n_ga, 4 * nz) + each, F32),
            pltpu.VMEM((nz, 4) + each, F32),
            pltpu.VMEM((2, 4 * nz) + each, F32),
            pltpu.VMEM((4 * nz,) + each, F32),
            pltpu.VMEM((4 * nz,) + each, F32),
            pltpu.VMEM((nz, per_dev // 2) + each, F32),
            pltpu.VMEM((2, nz) + each, F32),
            pltpu.VMEM((nz, per_dev // 2) + each, F32),
            one, one, dma(6),
            dma(3 * nz), dma(2 * nz),
            dma(2 * nz), dma(nz * per_dev),
            dma(nz), dma(nz),
            dma(3 * nz), dma(nz * (per_dev + 2)),
            dma(2 * nz + 3), dma(nz * per_dev + 2),
            one, dma(nz + 1), one, dma(1),
            one, dma(8), one, dma(4),
            one, dma(2 * nz), one, dma(nz),
            one, dma(2), one, dma(nz),
            one, one, one, one,
            one, dma(3),
        ],
        compiler_params=pltpu.CompilerParams(
            collective_id=0, has_side_effects=True, vmem_limit_bytes=LIMIT
        ),
        name="window",
    )(pairs.T, q_slot, x_dens, y_dens, p_dens, coulomb, screened.transpose(1, 0, 2))
    blocks, mirrored = pl.pallas_call(
        layout,
        out_shape=[shape((rows, nt * nt), F32), shape((per_dev, nt * nt), F32)],
        in_specs=[VM],
        out_specs=[VM, VM],
        scratch_shapes=[
            pltpu.VMEM((2 * nt, nt), F32),
            pltpu.VMEM((per_dev * nt // 2, 2 * nt), F32),
        ],
        name="layout",
    )(lines)
    return (blocks, mirrored)


def solution(mesh):
    in_specs = (
        P("ka", None, "ga"),
        P("ka", None, "ga"),
        P("ka", None, "ga"),
        P("ga"),
        P("ka", "ga", None),
        P("ka", None),
        P(),
    )
    out_specs = (P("ka", None), P("ka", None))
    return jax.shard_map(
        per_device, mesh=mesh, in_specs=in_specs, out_specs=out_specs, check_vma=False
    )
```

```python
import functools
import jax
import jax.numpy as jnp
from jax import lax
from jax.experimental import pallas as pl
from jax.experimental.pallas import tpu as pltpu
from jax.sharding import PartitionSpec as P

CAPQ = 2
F32 = jnp.float32
BF16 = jnp.bfloat16
I32 = jnp.int32
VM = pl.BlockSpec(memory_space=pltpu.VMEM)
SM = pl.BlockSpec(memory_space=pltpu.SMEM)
HB = pl.BlockSpec(memory_space=pl.ANY)
LIMIT = 66000000
DIMS = (((1,), (1,)), ((), ()))


def start(c):
    c.start()


def sent(c):
    c.wait_send()


def remote(src, dst, ss, rs, to):
    return pltpu.make_async_remote_copy(
        src_ref=src,
        dst_ref=dst,
        send_sem=ss,
        recv_sem=rs,
        device_id=to,
        device_id_type=pl.DeviceIdType.MESH,
    )


def greet(n, meanwhile):
    barrier = pltpu.get_barrier_semaphore()
    me = lax.axis_index("ka")
    g = lax.axis_index("ga")
    z, y = me // 2, me % 2
    nz = n // 2

    def hello(to):
        pl.semaphore_signal(barrier, inc=1, device_id=to, device_id_type=pl.DeviceIdType.MESH)

    @pl.when(z > 0)
    def _():
        hello({"ka": me - 2})

    @pl.when(z < nz - 1)
    def _():
        hello({"ka": me + 2})

    hello({"ka": z * 2 + 1 - y})
    hello({"ga": g // 2 * 2 + 1 - g % 2})
    hello({"ga": (1 - g // 2) * 2 + g % 2})
    meanwhile()
    pl.semaphore_wait(barrier, 5 - jnp.where(z > 0, 0, 1) - jnp.where(z < nz - 1, 0, 1))


class Gather:
    def __init__(self, n, src, out, send, recv, cut):
        self.n, self.nz = n, n // 2
        self.me = lax.axis_index("ka")
        self.z, self.y = self.me // 2, self.me % 2
        self.src, self.out, self.send, self.recv = src, out, send, recv
        self.size = src.shape[0]
        self.cut = cut

    def landed(self, zz, same, k):
        few = self.size - self.cut
        if same:
            return self.recv.at[zz * self.size + k]
        if k >= self.cut:
            return self.recv.at[self.nz * self.size + zz * few + k - self.cut]
        return self.recv.at[self.nz * (self.size + few) + zz]

    def copy(self, zz, yy, k, way, own=False):
        at = (zz * 2 + yy) * self.size + k
        block = self.out.at[at]
        if way == 2:
            target = self.z * 2 + 1 - self.y
        else:
            target = (self.z + (1 if way == 0 else -1)) * 2 + self.y
        return remote(
            self.src.at[k] if own else block,
            block,
            self.send.at[way * self.nz + zz],
            self.landed(zz, (yy is self.y) != (way == 2), k),
            {"ka": target},
        )

    def take(self, zz, yy, k):
        block = self.out.at[(zz * 2 + yy) * self.size + k]
        done = self.landed(zz, yy is self.y, k)
        remote(block, block, done, done, {"ka": self.z * 2 + 1 - self.y}).wait_recv()

    def some(self, count):
        return self.out.at[pl.ds(0, count)]

    def take_late(self, zz):
        block, done = self.some(self.cut), self.landed(zz, False, 0)
        remote(block, block, done, done, {"ka": self.z * 2 + 1 - self.y}).wait_recv()

    def all_sent(self, zz, way, count):
        block, done = self.some(count), self.send.at[way * self.nz + zz]
        remote(block, block, done, done, {"ka": self.z * 2 + 1 - self.y}).wait_send()

    def chained(self, zz, ways=(0, 1)):
        for way in ways:
            free = self.z < self.nz - 1 if way == 0 else self.z > 0

            @pl.when(free)
            def _(way=way):
                self.all_sent(zz, way, 2 * self.size - self.cut)

    def chain(self, zz, yy, k, act, ways=(0, 1), own=False):
        for way in ways:
            free = self.z < self.nz - 1 if way == 0 else self.z > 0

            @pl.when(free)
            def _(way=way):
                act(self.copy(zz, yy, k, way, own))

    def early(self):
        return range(self.cut, self.size)

    def across_early(self):
        for k in self.early():
            self.copy(self.z, self.y, k, 2, True).start()

    def across_late(self):
        for k in range(self.cut):
            self.copy(self.z, self.y, k, 2, True).start()

    def first(self):
        for k in range(self.size):
            self.chain(self.z, self.y, k, start, own=True)

    def second(self):
        for k in self.early():
            self.take(self.z, 1 - self.y, k)
            self.chain(self.z, 1 - self.y, k, start)

    def sides(self, h, act):
        for way in (0, 1):
            zz = self.z - h if way == 0 else self.z + h
            there = zz >= 0 if way == 0 else zz < self.nz

            @pl.when(there)
            def _(zz=zz, way=way):
                act(zz, way)

    def hop(self, h, low=0, high=None):
        def one(k, yy, zz, way):
            self.take(zz, yy, k)
            self.chain(zz, yy, k, start, (way,))

        for k in range(self.size)[low:high]:

            def own(zz, way, k=k):
                one(k, self.y, zz, way)
                if k < self.cut:
                    self.copy(zz, self.y, k, 2).start()

            self.sides(h, own)
        for k in self.early() if high is None else ():
            self.sides(h, lambda zz, way, k=k: one(k, 1 - self.y, zz, way))

    def finish(self):
        self.chained(self.z)
        self.all_sent(self.z, 2, self.size)
        self.take_late(self.z)

        def tail(h, carry):
            def side(zz, way):
                self.chained(zz, (way,))
                self.all_sent(zz, 2, self.cut)
                self.take_late(zz)

            self.sides(h, side)
            return carry

        lax.fori_loop(1, self.nz, tail, 0)


class Rows(Gather):
    def some(self, count):
        return self.out.at[0]

    def begin(self):
        self.chain(self.z, self.y, 0, start, own=True)
        self.copy(self.z, self.y, 0, 2, True).start()

    def finish(self):
        self.chained(self.z)
        self.all_sent(self.z, 2, 1)

        def tail(h, carry):
            def side(zz, way):
                self.chained(zz, (way,))
                self.all_sent(zz, 2, 1)

            self.sides(h, side)
            return carry

        lax.fori_loop(1, self.nz, tail, 0)


class Hub(Gather):
    def __init__(self, n, src, out, send, recv):
        super().__init__(n, src, out, send, recv, src.shape[0])
        self.inner = jnp.logical_and(self.z >= 1, self.z <= self.nz - 2)
        self.edged = jnp.logical_or(self.z == 1, self.z == self.nz - 2)
        self.edge = jnp.where(self.z == 1, 0, self.nz - 1)

    def copy(self, zz, yy, k, way, own=False):
        base = (zz * 2 + yy) * self.size
        target = (self.z + (1 if way == 0 else -1)) * 2 + self.y
        return remote(
            self.src.at[k] if own else self.out.at[base + k],
            self.out.at[base + k],
            self.send.at[way * self.nz + zz],
            self.recv.at[zz * self.size + k],
            {"ka": target},
        )

    def block(self, zz, yy):
        return self.out.at[pl.ds((zz * 2 + yy) * self.size, self.size)]

    def cross(self, i):
        return remote(
            self.src,
            self.block(self.z, self.y),
            self.send.at[2 * self.nz + i],
            self.recv.at[self.nz * self.size + i],
            {"ka": self.z * 2 + 1 - self.y},
        )

    def crossed(self, zz, i):
        block, done = self.block(zz, 1 - self.y), self.recv.at[self.nz * self.size + i]
        remote(block, block, done, done, {"ka": self.z * 2 + 1 - self.y}).wait_recv()

    def inward(self):
        block = self.block(self.z, 1 - self.y)
        return remote(
            block,
            block,
            self.send.at[2 * self.nz + 2],
            self.recv.at[self.nz * self.size + 1],
            {"ka": jnp.where(self.z == 0, 1, self.nz - 2) * 2 + self.y},
        )

    def pass_inward(self):
        self.crossed(self.z, 1)
        self.inward().start()

    def chained(self, zz, ways=(0, 1)):
        for way in ways:
            free = self.z <= self.nz - 3 if way == 0 else self.z >= 2

            @pl.when(free)
            def _(way=way):
                self.all_sent(zz, way, self.size)

    def chain(self, zz, yy, k, act, ways=(0, 1), own=False):
        for way in ways:
            free = self.z <= self.nz - 3 if way == 0 else self.z >= 2

            @pl.when(free)
            def _(way=way):
                act(self.copy(zz, yy, k, way, own))

    def first(self):
        for k in range(self.size):
            self.chain(self.z, self.y, k, start, own=True)

    def hop(self, h):
        def own(zz, way):
            end = jnp.logical_and(self.edged, zz == self.edge)
            for k in range(self.size):

                @pl.when(jnp.logical_not(end))
                def _(k=k):
                    self.copy(zz, self.y, k, way).wait_recv()

                self.chain(zz, self.y, k, start, (way,))

        self.sides(h, own)

    def edge_in(self):
        @pl.when(self.edged)
        def _():
            for k in range(self.size):
                self.copy(self.edge, self.y, k, 2).wait_recv()

    def finish(self):
        self.chained(self.z)

        @pl.when(jnp.logical_not(self.inner))
        def _():
            self.cross(1).wait_send()
            self.inward().wait_send()

        @pl.when(self.inner)
        def _():
            self.cross(0).wait_send()

            def tail(h, carry):
                self.sides(h, lambda zz, way: self.chained(zz, (way,)))
                return carry

            lax.fori_loop(1, self.nz, tail, 0)


class Pick:
    def __init__(self, n, src, col, out, got, tab, send, recv, ps, pr):
        self.n, self.nz = n, n // 2
        self.me = lax.axis_index("ka")
        self.z, self.y = self.me // 2, self.me % 2
        self.src, self.col, self.out, self.got, self.tab = src, col, out, got, tab
        self.send, self.recv, self.ps, self.pr = send, recv, ps, pr
        self.size = src.shape[0]

    def copy(self, zz, k, way, own=False):
        at = zz * self.size + k
        target = (self.z + (1 if way == 0 else -1)) * 2 + self.y
        return remote(
            self.src.at[k] if own else self.col.at[at],
            self.col.at[at],
            self.send.at[way * self.nz + zz],
            self.recv.at[at],
            {"ka": target},
        )

    def chain(self, zz, k, act, ways=(0, 1), own=False):
        for way in ways:
            free = self.z < self.nz - 1 if way == 0 else self.z > 0

            @pl.when(free)
            def _(way=way):
                act(self.copy(zz, k, way, own))

    def sides(self, h, act):
        for way in (0, 1):
            zz = self.z - h if way == 0 else self.z + h
            there = zz >= 0 if way == 0 else zz < self.nz

            @pl.when(there)
            def _(zz=zz, way=way):
                act(zz, way)

    def first(self):
        for k in range(self.size):
            self.chain(self.z, k, start, own=True)

    def hop(self, h):
        for k in range(self.size):

            def one(zz, way, k=k):
                self.copy(zz, k, way).wait_recv()
                self.chain(zz, k, start, (way,))

            self.sides(h, one)

    def chosen(self, zz, owner, r):
        which = self.tab[zz * 2 + self.y, owner * CAPQ + r]
        v = self.col[zz * self.size]
        for k in range(1, self.size):
            v = jnp.where(which == k, self.col[zz * self.size + k], v)
        return v

    def across(self, zz):
        rows = pl.ds(zz * CAPQ, CAPQ)
        return remote(
            self.out.at[rows],
            self.got.at[rows],
            self.ps.at[zz],
            self.pr.at[zz],
            {"ka": self.z * 2 + 1 - self.y},
        )

    def pass_on(self, zz):
        for r in range(CAPQ):
            self.out[zz * CAPQ + r] = self.chosen(zz, self.z * 2 + 1 - self.y, r)
        self.across(zz).start()

    def chained(self, zz, ways=(0, 1)):
        block = self.col.at[pl.ds(zz * self.size, self.size)]
        for way in ways:
            free = self.z < self.nz - 1 if way == 0 else self.z > 0
            done = self.send.at[way * self.nz + zz]

            @pl.when(free)
            def _(done=done):
                remote(block, block, done, done, {"ka": self.z * 2 + 1 - self.y}).wait_send()

    def finish(self):
        self.chained(self.z)
        self.across(self.z).wait_send()

        def tail(h, carry):
            def side(zz, way):
                self.chained(zz, (way,))
                self.across(zz).wait_send()

            self.sides(h, side)
            return carry

        lax.fori_loop(1, self.nz, tail, 0)


class Reduce:
    def __init__(self, part, out, recv1, tsend, recv2, s1, r1, s2, r2, per, lump):
        self.g = lax.axis_index("ga")
        self.x, self.c = self.g // 2, self.g % 2
        self.part, self.out = part, out
        self.recv1, self.tsend, self.recv2 = recv1, tsend, recv2
        self.s1, self.r1, self.s2, self.r2, self.per = s1, r1, s2, r2, per
        self.lump, self.pieces = lump, part.shape[1] // per

    def rows(self, i):
        return pl.ds(i * self.per, self.per)

    def one(self, t, i):
        xx = self.x if t else 1 - self.x
        return remote(
            self.part.at[xx * 2 + 1 - self.c, self.rows(i)],
            self.recv1.at[xx, self.rows(i)],
            self.s1,
            self.r1.at[self.pieces + (0 if self.lump else i) if t else i],
            {"ga": self.x * 2 + 1 - self.c},
        )

    def two(self, i):
        return remote(
            self.tsend.at[self.rows(i)],
            self.recv2.at[self.rows(i)],
            self.s2,
            self.r2.at[0 if self.lump else i],
            {"ga": (1 - self.x) * 2 + self.c},
        )

    def sum_one(self, xx, i):
        v = self.part[xx * 2 + self.c, self.rows(i)].astype(F32)
        return v + self.recv1[xx, self.rows(i)].astype(F32)

    def begin(self, i):
        self.one(0, i).start()
        self.one(1, i).start()

    def middle(self, i):
        self.one(0, i).wait_recv()
        self.tsend[self.rows(i)] = self.sum_one(1 - self.x, i).astype(self.tsend.dtype)
        self.two(i).start()

    def arrive(self):
        to = {"ga": self.x * 2 + 1 - self.c}
        for block, done in ((self.recv1.at[self.x], self.r1.at[self.pieces]), (self.recv2, self.r2.at[0])):
            remote(block, block, done, done, to).wait_recv()

    def end(self, i):
        if not self.lump:
            self.one(1, i).wait_recv()
            self.two(i).wait_recv()
        v = self.sum_one(self.x, i)
        v = (v + self.recv2[self.rows(i)].astype(F32)).astype(self.out.dtype)
        if len(self.out.shape) == len(self.tsend.shape):
            self.out[self.rows(i)] = v
        else:
            self.out[i] = v

    def finish(self):
        to = {"ga": self.x * 2 + 1 - self.c}
        both = self.part.at[pl.ds(0, 2)]
        remote(both, both, self.s1, self.s1, to).wait_send()
        remote(self.tsend, self.tsend, self.s2, self.s2, to).wait_send()


def make_row(n, q_slots, per_dev, pairs_ref, qs_ref, row_ref, at_ref):
    rows = pairs_ref.shape[1]
    slots = n * CAPQ
    lane = lax.broadcasted_iota(I32, row_ref.shape, 1)
    section = lane // slots
    spot = lane % slots
    row = jnp.where(jnp.logical_or(section == 2, section == 4), -1, 0)
    holders = ([], [])
    for j in range(rows):
        slot = qs_ref[pairs_ref[2, j]]
        owner = slot // q_slots
        first, second = pairs_ref[0, j] % per_dev, pairs_ref[1, j]
        at = []
        for i, o in enumerate((owner, second // per_dev)):
            rank = jnp.int32(0)
            for other in holders[i]:
                rank = rank + jnp.where(other == o, 1, 0)
            holders[i].append(o)
            at.append(o * CAPQ + rank)
            at_ref[i, j] = at[i]
        value = jnp.where(section == 1, slot - owner * q_slots, second)
        value = jnp.where(jnp.logical_or(section == 0, section == 3), first, value)
        hit = spot == jnp.where(section < 3, at[0], at[1])
        row = jnp.where(hit, value, row)
    row_ref[...] = row


def kernel(n, pairs_hbm, qs_hbm, x_ref, y_ref, p_ref, v_hbm, w_hbm, lines,
           pairs_ref, qs_ref, v_ref, tab, at_ref, row_ref, wt, w_ref, x_col, x_out, x_got, y_all, p_all, part, half,
           recv1, tsend, recv2, part2, own, q1, qt, q2, second, outbox, sumbox, inbox,
           split, part3, eown, e1, et, e2, ebox, ein, emir,
           ws, ls, ks, ts, tr, xs, xr, xps, xpr, ys, yr, ps, pr, s1, r1, s2, r2, t1, u1, t2, u2,
           v1, w1, v2, w2, es, er, fs, fr, as_, ar, bs, br, gs, gr):
    per_dev, nt, width = x_ref.shape
    rows = pairs_ref.shape[1]
    q_slots = w_ref.shape[0]
    nz = n // 2
    slots = n * CAPQ
    n_ga = part.shape[0]
    me = lax.axis_index("ka")
    g = lax.axis_index("ga")
    z, y = me // 2, me % 2
    fetch = pltpu.make_async_copy(w_hbm, wt, ws)
    lists = [
        pltpu.make_async_copy(pairs_hbm, pairs_ref, ks.at[3]),
        pltpu.make_async_copy(qs_hbm, qs_ref, ks.at[4]),
    ]
    for c in lists:
        c.start()
    weights = pltpu.make_async_copy(v_hbm, v_ref, ks.at[5])
    weights.start()
    fetch.start()
    mine = pl.ds(me * per_dev, per_dev)
    keeps = [
        pltpu.make_async_copy(x_ref, x_col.at[pl.ds(z * per_dev, per_dev)], ks.at[0]),
        pltpu.make_async_copy(p_ref, p_all.at[mine], ks.at[1]),
        pltpu.make_async_copy(y_ref, y_all.at[mine], ks.at[2]),
    ]
    for c in keeps:
        c.start()

    def table():
        for c in lists:
            c.wait()
        make_row(n, q_slots, per_dev, pairs_ref, qs_ref, row_ref, at_ref)

    greet(n, table)
    xg = Pick(n, x_ref, x_col, x_out, x_got, tab, xs, xr, xps, xpr)
    yg = Gather(n, y_ref, y_all, ys, yr, per_dev - 1)
    pg = Hub(n, p_ref, p_all, ps, pr)
    outer = jnp.logical_not(pg.inner)
    keep = pltpu.make_async_copy(row_ref.at[0], tab.at[me], ls)

    rg = Rows(n, row_ref, tab, ts, tr, 1)
    rg.begin()
    xg.first()
    keep.start()
    keep.wait()
    for c in keeps:
        c.wait()
    xg.pass_on(z)

    yg.across_early()

    @pl.when(outer)
    def _():
        pg.first()
        pg.cross(1).start()
        yg.first()

    @pl.when(pg.inner)
    def _():
        pg.cross(0).start()

    fetch.wait()
    turn = 16
    whole = width // turn * turn

    def relay(i, carry):
        at = pl.ds(pl.multiple_of(i * turn, turn), turn)
        w_ref[:, at] = jnp.swapaxes(wt[at], 0, 1)
        return carry

    lax.fori_loop(0, width // turn, relay, 0)
    if whole < width:
        w_ref[:, whole:] = jnp.swapaxes(wt[whole:], 0, 1)
    red = Reduce(part, half, recv1, tsend, recv2, s1, r1, s2, r2, 2 * CAPQ, True)

    def multiply(v, a, r):
        w = tab[a, slots + me * CAPQ + r]
        v = jnp.dot(v, w_ref[w], preferred_element_type=F32)
        for i in range(n_ga):
            part[i, a * CAPQ + r] = v[:, i * width : (i + 1) * width].astype(part.dtype)

    def piece(zz):
        for r in range(CAPQ):
            multiply(xg.chosen(zz, me, r), zz * 2 + y, r)
        rg.take_late(zz)
        xg.across(zz).wait_recv()
        for r in range(CAPQ):
            multiply(x_got[zz * CAPQ + r], zz * 2 + 1 - y, r)
        red.begin(zz)

    quarter = nt // n_ga
    weights.wait()
    weight = v_ref[...].reshape(1, width)
    sets = jnp.where(pg.edged, 4, 2)
    ered = Reduce(part3, eown, e1, et, e2, v1, w1, v2, w2, 4, False)

    def of(q):
        return jnp.where(q // 2 == 0, z, pg.edge) * 2 + q % 2

    def joined(both, out, at):
        v = jnp.concatenate(both, axis=1)
        for i in range(n_ga):
            out[i, at] = v[i * quarter : (i + 1) * quarter]

    def weigh(q, carry):
        for k in range(per_dev):
            weighted = p_all[of(q) * per_dev + k].astype(F32) * weight
            high = weighted.astype(BF16)
            split[q * per_dev + k, :nt] = high
            split[q * per_dev + k, nt:] = (weighted - high.astype(F32)).astype(BF16)
        return carry

    def exchange(zz):
        base = (zz * 2 + y) * per_dev

        def one(q, carry):
            a = of(q)
            both = []
            for r in range(CAPQ):
                at = 3 * slots + (zz * 2 + y) * CAPQ + r
                which = tab[a, at + slots] - base
                other = p_all[base]
                for k in range(1, per_dev):
                    other = jnp.where(which == k, p_all[base + k], other)
                v = lax.dot_general(
                    split[q * per_dev + tab[a, at]], other, DIMS, preferred_element_type=F32
                )
                both.append(v[:nt] + v[nt:])
            joined(both, part3, zz * 4 + q)
            return carry

        lax.fori_loop(0, sets, one, 0)
        ered.begin(zz)

    shape = own.shape[1:]
    left = lax.broadcasted_iota(I32, shape, 1) < nt
    doubles = per_dev // 2

    def paired(sums):
        sums = [v[:, :nt] + v[:, nt:] for v in sums]
        return [
            jnp.concatenate([sums[i], sums[i + doubles]], axis=1) for i in range(doubles)
        ]

    def to_first(q, zz):
        return remote(eown.at[zz, q], ein.at[y, zz], es, er.at[y], {"ka": of(q)})

    def to_second(zz):
        return remote(ebox.at[zz], emir.at[z], fs, fr.at[z], {"ka": zz * 2 + y})

    def deliver(zz):
        ered.end(zz)

        def give(q, carry):
            @pl.when(q != y)
            def _():
                to_first(q, zz).start()

            return carry

        lax.fori_loop(0, sets, give, 0)
        ein[y, zz] = eown[zz, y]

        def add(q, sums):
            at = 4 * slots + (zz * 2 + y) * CAPQ
            k2 = jnp.where(left, tab[of(q), at], tab[of(q), at + 1])
            v = eown[zz, q]
            base = (zz * 2 + y) * per_dev
            return tuple(t + jnp.where(k2 == base + i, v, 0.0) for i, t in enumerate(sums))

        sums = lax.fori_loop(0, sets, add, tuple(jnp.zeros(shape, F32) for _ in range(per_dev)))
        for i, v in enumerate(paired(sums)):
            ebox[zz, i] = v

        @pl.when(zz != z)
        def _():
            to_second(zz).start()

        @pl.when(zz == z)
        def _():
            emir[z] = ebox[z]

    rg.hop(1)
    xg.hop(1)

    @pl.when(pg.inner)
    def _():
        pg.first()

    xg.sides(1, lambda zz, way: xg.pass_on(zz))
    piece(z)

    def stage(h, carry):
        @pl.when(h < nz)
        def _():
            rg.hop(h)
            xg.hop(h)

        @pl.when(h == 2)
        def _():
            @pl.when(pg.inner)
            def _():
                yg.first()

            yg.second()

        @pl.when(h < nz)
        def _():
            xg.sides(h, lambda zz, way: xg.pass_on(zz))

        @pl.when(h == 2)
        def _():
            @pl.when(pg.inner)
            def _():
                pg.edge_in()

            @pl.when(outer)
            def _():
                pg.pass_inward()

            yg.across_late()

            red.middle(z)

        @pl.when(h > 2)
        def _():
            xg.sides(h - 2, lambda zz, way: red.middle(zz))

        xg.sides(h - 1, lambda zz, way: piece(zz))

        @pl.when(jnp.logical_and(h >= 3, h < nz))
        def _():
            yg.hop(h - 2)

        return carry

    lax.fori_loop(2, nz + 1, stage, 0)

    @pl.when(pg.inner)
    def _():
        pg.hop(1)
        pg.crossed(z, 0)

        @pl.when(pg.edged)
        def _():
            pg.crossed(pg.edge, 1)

        lax.fori_loop(0, sets, weigh, 0)
        exchange(z)

    xg.sides(nz - 1, lambda zz, way: red.middle(zz))
    half_way = per_dev // 2
    yg.hop(nz - 2, 0, half_way)

    @pl.when(pg.inner)
    def _():
        pg.sides(1, lambda zz, way: exchange(zz))

    yg.hop(nz - 2, half_way)

    @pl.when(pg.inner)
    def _():
        ered.middle(z)
        pg.sides(1, lambda zz, way: ered.middle(zz))

    @pl.when(pg.inner)
    def _():
        def level(h, carry):
            pg.hop(h)
            pg.sides(h, lambda zz, way: exchange(zz))
            return carry

        lax.fori_loop(2, nz, level, 0)

    pg.finish()
    yg.hop(nz - 1)

    red.arrive()
    lax.fori_loop(0, nz, lambda i, c: (red.end(i), c)[1], 0)
    yg.finish()

    def source(a, carry):
        both = []
        for r in range(CAPQ):
            k2 = jnp.maximum(tab[a, 2 * slots + me * CAPQ + r], 0)
            both.append(
                lax.dot_general(half[a * CAPQ + r], y_all[k2], DIMS, preferred_element_type=F32)
            )
        joined(both, part2, a)
        return carry

    end = Reduce(part2, own, q1, qt, q2, t1, u1, t2, u2, n // 4, False)
    for i in range(4):
        lax.fori_loop(i * n // 4, (i + 1) * n // 4, source, 0, unroll=2)
        end.begin(i)
    def seconds(a, carry):
        at = 2 * slots + me * CAPQ
        second[a] = jnp.where(left, tab[a, at], tab[a, at + 1])
        return carry

    lax.fori_loop(0, n, seconds, 0)

    @pl.when(pg.inner)
    def _():
        def level(h, carry):
            pg.sides(h, lambda zz, way: ered.middle(zz))
            return carry

        lax.fori_loop(2, nz, level, 0)

    for i in range(4):
        end.middle(i)

    @pl.when(pg.inner)
    def _():
        deliver(z)

        def level(h, carry):
            pg.sides(h, lambda zz, way: deliver(zz))
            return carry

        lax.fori_loop(1, nz, level, 0)


    def cross(src, box, i, whose, ss, rs):
        return remote(src.at[i], box.at[whose], ss, rs, {"ka": i})

    def far_first(i):
        return jnp.where(z < nz // 2, n - 1 - i, i)

    for i in range(4):
        end.end(i)

    def give(i, carry):
        b = far_first(i)

        @pl.when(b != me)
        def _():
            cross(own, inbox, b, me, as_, ar).start()

        return carry

    lax.fori_loop(0, n, give, 0)
    inbox[me] = own[me]


    def fill(i, carry):
        b = far_first(i)

        def add(a, sums):
            out = []
            for i in range(per_dev):
                out.append(sums[i] + jnp.where(second[a] == b * per_dev + i, own[a], 0.0))
            return tuple(out)

        sums = tuple(jnp.zeros(shape, F32) for _ in range(per_dev))
        sums = lax.fori_loop(0, n, add, sums, unroll=min(n, 8))
        for i_, v in enumerate(paired(sums)):
            outbox[b, i_] = v

        @pl.when(b != me)
        def _():
            cross(outbox, sumbox, b, me, bs, br).start()

        return carry

    lax.fori_loop(0, n, fill, 0)
    sumbox[me] = outbox[me]
    for yy in range(2):

        @pl.when(jnp.logical_or(jnp.logical_not(pg.inner), yy != y))
        def _(yy=yy):
            remote(ein.at[yy], ein.at[yy], es, er.at[yy], {"ka": z * 2 + 1 - y}).wait_recv()

    def inner_level(zz, carry):
        @pl.when(zz != z)
        def _():
            remote(
                emir.at[zz], emir.at[zz], fs, fr.at[zz], {"ka": z * 2 + 1 - y}
            ).wait_recv()

        return carry

    lax.fori_loop(1, nz - 1, inner_level, 0)
    def arrived(box, rs):
        rest = box.at[pl.ds(0, n - 1)]
        remote(rest, rest, rs, rs, {"ka": z * 2 + 1 - y}).wait_recv()

    arrived(inbox, ar)
    sub = quarter // 2

    def picked(ref, at, r):
        even = ref[at + (pl.ds(0, sub, stride=2),)]
        odd = ref[at + (pl.ds(1, sub, stride=2),)]
        zero = jnp.concatenate([even[:, :nt], odd[:, :nt]], axis=1)
        one = jnp.concatenate([even[:, nt:], odd[:, nt:]], axis=1)
        return jnp.where(r == 0, zero, one)

    for j in range(rows):
        at, et_ = at_ref[0, j], at_ref[1, j]
        b = et_ // CAPQ
        direct = picked(inbox, (at // CAPQ,), at % CAPQ)
        term = picked(ein, (b % 2, b // 2), et_ % CAPQ)
        lines[g, pl.ds(j * sub, sub)] = 2.0 * term - direct
    base = rows * sub
    x, c = g // 2, g % 2
    mate, far = x * 2 + 1 - c, (1 - x) * 2 + c
    parts = (pl.ds(0, base // 2), pl.ds(base, doubles * quarter), pl.ds(base // 2, base // 2))

    def spread(i, m, whose, to):
        block = lines.at[whose, parts[m]]
        return remote(block, block, gs, gr.at[m if i == 0 else 3], {"ga": to})

    diag = (1 - x) * 2 + 1 - c
    spread(0, 0, g, far).start()
    spread(0, 2, g, far).start()
    spread(2, 2, g, diag).start()
    spread(1, 0, g, mate).start()
    spread(1, 2, g, mate).start()
    xg.finish()
    rg.finish()
    red.finish()
    end.finish()
    arrived(sumbox, br)
    for i in range(doubles):
        total = lax.fori_loop(
            1, n, lambda o, t, i=i: t + sumbox[o, i], sumbox[0, i]
        )
        term = lax.fori_loop(
            2, nz - 1, lambda zz, t, i=i: t + emir[zz, i], emir[1, i]
        )
        lines[g, pl.ds(base + i * quarter, quarter)] = 2.0 * term - total
    spread(0, 1, g, far).start()
    spread(2, 1, g, diag).start()
    spread(1, 1, g, mate).start()
    spread(0, 0, far, far).wait_recv()
    spread(2, 0, far, mate).start()
    spread(0, 2, far, far).wait_recv()
    spread(0, 1, far, far).wait_recv()
    for src, ss in ((own, as_), (outbox, bs)):
        rest = src.at[pl.ds(0, n - 1)]
        remote(rest, rest, ss, ss, {"ka": z * 2 + 1 - y}).wait_send()
    @pl.when(pg.inner)
    def _():
        ered.finish()
        for edged, count in ((True, 3), (False, 1)):

            @pl.when(pg.edged if edged else jnp.logical_not(pg.edged))
            def _(count=count):
                sent_lines = eown.at[:, pl.ds(0, count)]
                remote(sent_lines, sent_lines, es, es, {"ka": z * 2 + 1 - y}).wait_send()

        rest = ebox.at[pl.ds(0, nz - 1)]
        remote(rest, rest, fs, fs, {"ka": z * 2 + 1 - y}).wait_send()

    for count, ss, rs in ((3, gs, None), (2, None, gr.at[3])):
        block = lines.at[pl.ds(0, count)]
        if rs is None:
            remote(block, block, ss, ss, {"ga": mate}).wait_send()
        else:
            remote(block, block, rs, rs, {"ga": mate}).wait_recv()


def layout(lines, blocks_ref, mirr_ref, turned, flat):
    n_ga = lines.shape[0]
    rows, per_dev = blocks_ref.shape[0], mirr_ref.shape[0]
    nt = turned.shape[1]
    quarter, sub, doubles = nt // n_ga, nt // n_ga // 2, per_dev // 2
    base = rows * sub
    lanes = 2 * nt
    for q in range(n_ga):
        for t in range(sub):
            blocks_ref[:, (q * sub + t) * lanes : (q * sub + t + 1) * lanes] = lines[
                q, pl.ds(t, rows, stride=sub)
            ]
    for i in range(doubles):
        whole = jnp.concatenate(
            [lines[q, pl.ds(base + i * quarter, quarter)] for q in range(n_ga)], axis=0
        )
        turned[...] = whole.T
        even = turned[pl.ds(0, nt, stride=2)]
        odd = turned[pl.ds(1, nt, stride=2)]
        both = jnp.concatenate([even, odd], axis=1)
        flat[pl.ds(i * nt // 2, nt // 2)] = both[: nt // 2]
        flat[pl.ds((i + doubles) * nt // 2, nt // 2)] = both[nt // 2 :]
    for t in range(nt // 2):
        mirr_ref[:, t * lanes : (t + 1) * lanes] = flat[pl.ds(t, per_dev, stride=nt // 2)]


def per_device(x_dens, y_dens, p_dens, coulomb, screened, pairs, q_slot):
    n = lax.axis_size("ka")
    n_ga = lax.axis_size("ga")
    per_dev, nt, g = x_dens.shape
    q_slots = screened.shape[0]
    rows = pairs.shape[0]
    slots = n * CAPQ
    nz = n // 2
    shape = jax.ShapeDtypeStruct
    wide = F32 if slots * nt <= 2048 else BF16
    quarter = nt // n_ga
    each = (quarter, CAPQ * nt)
    line = (n,) + each
    dma = lambda m: pltpu.SemaphoreType.DMA((m,))
    one = pltpu.SemaphoreType.DMA
    row_len = -(-5 * slots // 128) * 128
    k_all = n * per_dev
    lines = pl.pallas_call(
        functools.partial(kernel, n),
        out_shape=shape((n_ga, rows * quarter // 2 + per_dev // 2 * quarter, CAPQ * nt), F32),
        in_specs=[HB] * 7,
        out_specs=VM,
        scratch_shapes=[
            pltpu.SMEM((pairs.shape[1], rows), I32),
            pltpu.SMEM(q_slot.shape, I32),
            pltpu.VMEM((g,), F32),
            pltpu.SMEM((n, row_len), I32),
            pltpu.SMEM((2, rows), I32),
            pltpu.VMEM((1, row_len), I32),
            pltpu.VMEM((g, q_slots, screened.shape[2]), BF16),
            pltpu.VMEM((q_slots, g, screened.shape[2]), BF16),
            pltpu.VMEM((nz * per_dev, nt, g), BF16),
            pltpu.VMEM((nz * CAPQ, nt, g), BF16),
            pltpu.VMEM((nz * CAPQ, nt, g), BF16),
            pltpu.VMEM((k_all, nt, g), BF16),
            pltpu.VMEM((k_all, nt, g), BF16),
            pltpu.VMEM((n_ga, slots, nt, g), wide),
            pltpu.VMEM((slots, nt, g), BF16),
            pltpu.VMEM((2, slots, nt, g), wide),
            pltpu.VMEM((slots, nt, g), BF16),
            pltpu.VMEM((slots, nt, g), BF16),
            pltpu.VMEM((n_ga,) + line, F32),
            pltpu.VMEM(line, F32),
            pltpu.VMEM((2,) + line, F32),
            pltpu.VMEM(line, F32),
            pltpu.VMEM(line, F32),
            pltpu.VMEM(line, I32),
            pltpu.VMEM((n, per_dev // 2) + each, F32),
            pltpu.VMEM((n, per_dev // 2) + each, F32),
            pltpu.VMEM(line, F32),
            pltpu.VMEM((4 * per_dev, 2 * nt, g), BF16),
            pltpu.VMEM((n_ga, 4 * nz) + each, F32),
            pltpu.VMEM((nz, 4) + each, F32),
            pltpu.VMEM((2, 4 * nz) + each, F32),
            pltpu.VMEM((4 * nz,) + each, F32),
            pltpu.VMEM((4 * nz,) + each, F32),
            pltpu.VMEM((nz, per_dev // 2) + each, F32),
            pltpu.VMEM((2, nz) + each, F32),
            pltpu.VMEM((nz, per_dev // 2) + each, F32),
            one, one, dma(6),
            dma(3 * nz), dma(2 * nz),
            dma(2 * nz), dma(nz * per_dev),
            dma(nz), dma(nz),
            dma(3 * nz), dma(nz * (per_dev + 2)),
            dma(2 * nz + 3), dma(nz * per_dev + 2),
            one, dma(nz + 1), one, dma(1),
            one, dma(8), one, dma(4),
            one, dma(2 * nz), one, dma(nz),
            one, dma(2), one, dma(nz),
            one, one, one, one,
            one, dma(4),
        ],
        compiler_params=pltpu.CompilerParams(
            collective_id=0, has_side_effects=True, vmem_limit_bytes=LIMIT
        ),
        name="window",
    )(pairs.T, q_slot, x_dens, y_dens, p_dens, coulomb, screened.transpose(1, 0, 2))
    blocks, mirrored = pl.pallas_call(
        layout,
        out_shape=[shape((rows, nt * nt), F32), shape((per_dev, nt * nt), F32)],
        in_specs=[VM],
        out_specs=[VM, VM],
        scratch_shapes=[
            pltpu.VMEM((2 * nt, nt), F32),
            pltpu.VMEM((per_dev * nt // 2, 2 * nt), F32),
        ],
        name="layout",
    )(lines)
    return (blocks, mirrored)


def solution(mesh):
    in_specs = (
        P("ka", None, "ga"),
        P("ka", None, "ga"),
        P("ka", None, "ga"),
        P("ga"),
        P("ka", "ga", None),
        P("ka", None),
        P(),
    )
    out_specs = (P("ka", None), P("ka", None))
    return jax.shard_map(
        per_device, mesh=mesh, in_specs=in_specs, out_specs=out_specs, check_vma=False
    )
```

```python
import functools
import jax
import jax.numpy as jnp
from jax import lax
from jax.experimental import pallas as pl
from jax.experimental.pallas import tpu as pltpu
from jax.sharding import PartitionSpec as P

CAPQ = 2
F32 = jnp.float32
BF16 = jnp.bfloat16
I32 = jnp.int32
VM = pl.BlockSpec(memory_space=pltpu.VMEM)
SM = pl.BlockSpec(memory_space=pltpu.SMEM)
HB = pl.BlockSpec(memory_space=pl.ANY)
LIMIT = 66000000
DIMS = (((1,), (1,)), ((), ()))


def start(c):
    c.start()


def sent(c):
    c.wait_send()


def remote(src, dst, ss, rs, to):
    return pltpu.make_async_remote_copy(
        src_ref=src,
        dst_ref=dst,
        send_sem=ss,
        recv_sem=rs,
        device_id=to,
        device_id_type=pl.DeviceIdType.MESH,
    )


def greet(n, meanwhile):
    barrier = pltpu.get_barrier_semaphore()
    me = lax.axis_index("ka")
    g = lax.axis_index("ga")
    z, y = me // 2, me % 2
    nz = n // 2

    def hello(to):
        pl.semaphore_signal(barrier, inc=1, device_id=to, device_id_type=pl.DeviceIdType.MESH)

    @pl.when(z > 0)
    def _():
        hello({"ka": me - 2})

    @pl.when(z < nz - 1)
    def _():
        hello({"ka": me + 2})

    hello({"ka": z * 2 + 1 - y})
    hello({"ga": g // 2 * 2 + 1 - g % 2})
    hello({"ga": (1 - g // 2) * 2 + g % 2})
    meanwhile()
    pl.semaphore_wait(barrier, 5 - jnp.where(z > 0, 0, 1) - jnp.where(z < nz - 1, 0, 1))


class Gather:
    def __init__(self, n, src, out, send, recv, cut):
        self.n, self.nz = n, n // 2
        self.me = lax.axis_index("ka")
        self.z, self.y = self.me // 2, self.me % 2
        self.src, self.out, self.send, self.recv = src, out, send, recv
        self.size = src.shape[0]
        self.cut = cut

    def landed(self, zz, same, k):
        few = self.size - self.cut
        if same:
            return self.recv.at[zz * self.size + k]
        if k >= self.cut:
            return self.recv.at[self.nz * self.size + zz * few + k - self.cut]
        return self.recv.at[self.nz * (self.size + few) + zz]

    def copy(self, zz, yy, k, way, own=False):
        at = (zz * 2 + yy) * self.size + k
        block = self.out.at[at]
        if way == 2:
            target = self.z * 2 + 1 - self.y
        else:
            target = (self.z + (1 if way == 0 else -1)) * 2 + self.y
        return remote(
            self.src.at[k] if own else block,
            block,
            self.send.at[way * self.nz + zz],
            self.landed(zz, (yy is self.y) != (way == 2), k),
            {"ka": target},
        )

    def take(self, zz, yy, k):
        block = self.out.at[(zz * 2 + yy) * self.size + k]
        done = self.landed(zz, yy is self.y, k)
        remote(block, block, done, done, {"ka": self.z * 2 + 1 - self.y}).wait_recv()

    def some(self, count):
        return self.out.at[pl.ds(0, count)]

    def take_late(self, zz):
        block, done = self.some(self.cut), self.landed(zz, False, 0)
        remote(block, block, done, done, {"ka": self.z * 2 + 1 - self.y}).wait_recv()

    def all_sent(self, zz, way, count):
        block, done = self.some(count), self.send.at[way * self.nz + zz]
        remote(block, block, done, done, {"ka": self.z * 2 + 1 - self.y}).wait_send()

    def chained(self, zz, ways=(0, 1)):
        for way in ways:
            free = self.z < self.nz - 1 if way == 0 else self.z > 0

            @pl.when(free)
            def _(way=way):
                self.all_sent(zz, way, 2 * self.size - self.cut)

    def chain(self, zz, yy, k, act, ways=(0, 1), own=False):
        for way in ways:
            free = self.z < self.nz - 1 if way == 0 else self.z > 0

            @pl.when(free)
            def _(way=way):
                act(self.copy(zz, yy, k, way, own))

    def early(self):
        return range(self.cut, self.size)

    def across_early(self):
        for k in self.early():
            self.copy(self.z, self.y, k, 2, True).start()

    def across_late(self):
        for k in range(self.cut):
            self.copy(self.z, self.y, k, 2, True).start()

    def first(self):
        for k in range(self.size):
            self.chain(self.z, self.y, k, start, own=True)

    def second(self):
        for k in self.early():
            self.take(self.z, 1 - self.y, k)
            self.chain(self.z, 1 - self.y, k, start)

    def sides(self, h, act):
        for way in (0, 1):
            zz = self.z - h if way == 0 else self.z + h
            there = zz >= 0 if way == 0 else zz < self.nz

            @pl.when(there)
            def _(zz=zz, way=way):
                act(zz, way)

    def hop(self, h, low=0, high=None):
        def one(k, yy, zz, way):
            self.take(zz, yy, k)
            self.chain(zz, yy, k, start, (way,))

        for k in range(self.size)[low:high]:

            def own(zz, way, k=k):
                one(k, self.y, zz, way)
                if k < self.cut:
                    self.copy(zz, self.y, k, 2).start()

            self.sides(h, own)
        for k in self.early() if high is None else ():
            self.sides(h, lambda zz, way, k=k: one(k, 1 - self.y, zz, way))

    def finish(self):
        self.chained(self.z)
        self.all_sent(self.z, 2, self.size)
        self.take_late(self.z)

        def tail(h, carry):
            def side(zz, way):
                self.chained(zz, (way,))
                self.all_sent(zz, 2, self.cut)
                self.take_late(zz)

            self.sides(h, side)
            return carry

        lax.fori_loop(1, self.nz, tail, 0)


class Rows(Gather):
    def some(self, count):
        return self.out.at[0]

    def begin(self):
        self.chain(self.z, self.y, 0, start, own=True)
        self.copy(self.z, self.y, 0, 2, True).start()

    def finish(self):
        self.chained(self.z)
        self.all_sent(self.z, 2, 1)

        def tail(h, carry):
            def side(zz, way):
                self.chained(zz, (way,))
                self.all_sent(zz, 2, 1)

            self.sides(h, side)
            return carry

        lax.fori_loop(1, self.nz, tail, 0)


class Hub(Gather):
    def __init__(self, n, src, out, send, recv):
        super().__init__(n, src, out, send, recv, src.shape[0])
        self.inner = jnp.logical_and(self.z >= 1, self.z <= self.nz - 2)
        self.edged = jnp.logical_or(self.z == 1, self.z == self.nz - 2)
        self.edge = jnp.where(self.z == 1, 0, self.nz - 1)

    def copy(self, zz, yy, k, way, own=False):
        base = (zz * 2 + yy) * self.size
        target = (self.z + (1 if way == 0 else -1)) * 2 + self.y
        return remote(
            self.src.at[k] if own else self.out.at[base + k],
            self.out.at[base + k],
            self.send.at[way * self.nz + zz],
            self.recv.at[zz * self.size + k],
            {"ka": target},
        )

    def block(self, zz, yy):
        return self.out.at[pl.ds((zz * 2 + yy) * self.size, self.size)]

    def cross(self, i):
        return remote(
            self.src,
            self.block(self.z, self.y),
            self.send.at[2 * self.nz + i],
            self.recv.at[self.nz * self.size + i],
            {"ka": self.z * 2 + 1 - self.y},
        )

    def crossed(self, zz, i):
        block, done = self.block(zz, 1 - self.y), self.recv.at[self.nz * self.size + i]
        remote(block, block, done, done, {"ka": self.z * 2 + 1 - self.y}).wait_recv()

    def inward(self):
        block = self.block(self.z, 1 - self.y)
        return remote(
            block,
            block,
            self.send.at[2 * self.nz + 2],
            self.recv.at[self.nz * self.size + 1],
            {"ka": jnp.where(self.z == 0, 1, self.nz - 2) * 2 + self.y},
        )

    def pass_inward(self):
        self.crossed(self.z, 1)
        self.inward().start()

    def chained(self, zz, ways=(0, 1)):
        for way in ways:
            free = self.z <= self.nz - 3 if way == 0 else self.z >= 2

            @pl.when(free)
            def _(way=way):
                self.all_sent(zz, way, self.size)

    def chain(self, zz, yy, k, act, ways=(0, 1), own=False):
        for way in ways:
            free = self.z <= self.nz - 3 if way == 0 else self.z >= 2

            @pl.when(free)
            def _(way=way):
                act(self.copy(zz, yy, k, way, own))

    def first(self):
        for k in range(self.size):
            self.chain(self.z, self.y, k, start, own=True)

    def hop(self, h):
        def own(zz, way):
            end = jnp.logical_and(self.edged, zz == self.edge)
            for k in range(self.size):

                @pl.when(jnp.logical_not(end))
                def _(k=k):
                    self.copy(zz, self.y, k, way).wait_recv()

                self.chain(zz, self.y, k, start, (way,))

        self.sides(h, own)

    def edge_in(self):
        @pl.when(self.edged)
        def _():
            for k in range(self.size):
                self.copy(self.edge, self.y, k, 2).wait_recv()

    def finish(self):
        self.chained(self.z)

        @pl.when(jnp.logical_not(self.inner))
        def _():
            self.cross(1).wait_send()
            self.inward().wait_send()

        @pl.when(self.inner)
        def _():
            self.cross(0).wait_send()

            def tail(h, carry):
                self.sides(h, lambda zz, way: self.chained(zz, (way,)))
                return carry

            lax.fori_loop(1, self.nz, tail, 0)


class Pick:
    def __init__(self, n, src, col, out, got, tab, send, recv, ps, pr):
        self.n, self.nz = n, n // 2
        self.me = lax.axis_index("ka")
        self.z, self.y = self.me // 2, self.me % 2
        self.src, self.col, self.out, self.got, self.tab = src, col, out, got, tab
        self.send, self.recv, self.ps, self.pr = send, recv, ps, pr
        self.size = src.shape[0]

    def copy(self, zz, k, way, own=False):
        at = zz * self.size + k
        target = (self.z + (1 if way == 0 else -1)) * 2 + self.y
        return remote(
            self.src.at[k] if own else self.col.at[at],
            self.col.at[at],
            self.send.at[way * self.nz + zz],
            self.recv.at[at],
            {"ka": target},
        )

    def chain(self, zz, k, act, ways=(0, 1), own=False):
        for way in ways:
            free = self.z < self.nz - 1 if way == 0 else self.z > 0

            @pl.when(free)
            def _(way=way):
                act(self.copy(zz, k, way, own))

    def sides(self, h, act):
        for way in (0, 1):
            zz = self.z - h if way == 0 else self.z + h
            there = zz >= 0 if way == 0 else zz < self.nz

            @pl.when(there)
            def _(zz=zz, way=way):
                act(zz, way)

    def first(self):
        for k in range(self.size):
            self.chain(self.z, k, start, own=True)

    def hop(self, h):
        for k in range(self.size):

            def one(zz, way, k=k):
                self.copy(zz, k, way).wait_recv()
                self.chain(zz, k, start, (way,))

            self.sides(h, one)

    def chosen(self, zz, owner, r):
        which = self.tab[zz * 2 + self.y, owner * CAPQ + r]
        v = self.col[zz * self.size]
        for k in range(1, self.size):
            v = jnp.where(which == k, self.col[zz * self.size + k], v)
        return v

    def across(self, zz):
        rows = pl.ds(zz * CAPQ, CAPQ)
        return remote(
            self.out.at[rows],
            self.got.at[rows],
            self.ps.at[zz],
            self.pr.at[zz],
            {"ka": self.z * 2 + 1 - self.y},
        )

    def pass_on(self, zz):
        for r in range(CAPQ):
            self.out[zz * CAPQ + r] = self.chosen(zz, self.z * 2 + 1 - self.y, r)
        self.across(zz).start()

    def chained(self, zz, ways=(0, 1)):
        block = self.col.at[pl.ds(zz * self.size, self.size)]
        for way in ways:
            free = self.z < self.nz - 1 if way == 0 else self.z > 0
            done = self.send.at[way * self.nz + zz]

            @pl.when(free)
            def _(done=done):
                remote(block, block, done, done, {"ka": self.z * 2 + 1 - self.y}).wait_send()

    def finish(self):
        self.chained(self.z)
        self.across(self.z).wait_send()

        def tail(h, carry):
            def side(zz, way):
                self.chained(zz, (way,))
                self.across(zz).wait_send()

            self.sides(h, side)
            return carry

        lax.fori_loop(1, self.nz, tail, 0)


class Reduce:
    def __init__(self, part, out, recv1, tsend, recv2, s1, r1, s2, r2, per, lump):
        self.g = lax.axis_index("ga")
        self.x, self.c = self.g // 2, self.g % 2
        self.part, self.out = part, out
        self.recv1, self.tsend, self.recv2 = recv1, tsend, recv2
        self.s1, self.r1, self.s2, self.r2, self.per = s1, r1, s2, r2, per
        self.lump, self.pieces = lump, part.shape[1] // per

    def rows(self, i):
        return pl.ds(i * self.per, self.per)

    def one(self, t, i):
        xx = self.x if t else 1 - self.x
        return remote(
            self.part.at[xx * 2 + 1 - self.c, self.rows(i)],
            self.recv1.at[xx, self.rows(i)],
            self.s1,
            self.r1.at[self.pieces + (0 if self.lump else i) if t else i],
            {"ga": self.x * 2 + 1 - self.c},
        )

    def two(self, i):
        return remote(
            self.tsend.at[self.rows(i)],
            self.recv2.at[self.rows(i)],
            self.s2,
            self.r2.at[0 if self.lump else i],
            {"ga": (1 - self.x) * 2 + self.c},
        )

    def sum_one(self, xx, i):
        v = self.part[xx * 2 + self.c, self.rows(i)].astype(F32)
        return v + self.recv1[xx, self.rows(i)].astype(F32)

    def begin(self, i):
        self.one(0, i).start()
        self.one(1, i).start()

    def middle(self, i):
        self.one(0, i).wait_recv()
        self.tsend[self.rows(i)] = self.sum_one(1 - self.x, i).astype(self.tsend.dtype)
        self.two(i).start()

    def arrive(self):
        to = {"ga": self.x * 2 + 1 - self.c}
        for block, done in ((self.recv1.at[self.x], self.r1.at[self.pieces]), (self.recv2, self.r2.at[0])):
            remote(block, block, done, done, to).wait_recv()

    def end(self, i):
        if not self.lump:
            self.one(1, i).wait_recv()
            self.two(i).wait_recv()
        v = self.sum_one(self.x, i)
        v = (v + self.recv2[self.rows(i)].astype(F32)).astype(self.out.dtype)
        if len(self.out.shape) == len(self.tsend.shape):
            self.out[self.rows(i)] = v
        else:
            self.out[i] = v

    def finish(self):
        to = {"ga": self.x * 2 + 1 - self.c}
        both = self.part.at[pl.ds(0, 2)]
        remote(both, both, self.s1, self.s1, to).wait_send()
        remote(self.tsend, self.tsend, self.s2, self.s2, to).wait_send()


def make_row(n, q_slots, per_dev, pairs_ref, qs_ref, row_ref, at_ref):
    rows = pairs_ref.shape[1]
    slots = n * CAPQ
    lane = lax.broadcasted_iota(I32, row_ref.shape, 1)
    section = lane // slots
    spot = lane % slots
    row = jnp.where(jnp.logical_or(section == 2, section == 4), -1, 0)
    holders = ([], [])
    for j in range(rows):
        slot = qs_ref[pairs_ref[2, j]]
        owner = slot // q_slots
        first, second = pairs_ref[0, j] % per_dev, pairs_ref[1, j]
        at = []
        for i, o in enumerate((owner, second // per_dev)):
            rank = jnp.int32(0)
            for other in holders[i]:
                rank = rank + jnp.where(other == o, 1, 0)
            holders[i].append(o)
            at.append(o * CAPQ + rank)
            at_ref[i, j] = at[i]
        value = jnp.where(section == 1, slot - owner * q_slots, second)
        value = jnp.where(jnp.logical_or(section == 0, section == 3), first, value)
        hit = spot == jnp.where(section < 3, at[0], at[1])
        row = jnp.where(hit, value, row)
    row_ref[...] = row


def kernel(n, pairs_hbm, qs_hbm, x_ref, y_ref, p_ref, v_hbm, w_hbm, lines,
           pairs_ref, qs_ref, v_ref, tab, at_ref, row_ref, wt, w_ref, x_col, x_out, x_got, y_all, p_all, part, half,
           recv1, tsend, recv2, part2, own, q1, qt, q2, second, outbox, sumbox, inbox,
           split, part3, eown, e1, et, e2, ebox, ein, emir,
           ws, ls, ks, ts, tr, xs, xr, xps, xpr, ys, yr, ps, pr, s1, r1, s2, r2, t1, u1, t2, u2,
           v1, w1, v2, w2, es, er, fs, fr, as_, ar, bs, br, gs, gr):
    per_dev, nt, width = x_ref.shape
    rows = pairs_ref.shape[1]
    q_slots = w_ref.shape[0]
    nz = n // 2
    slots = n * CAPQ
    n_ga = part.shape[0]
    me = lax.axis_index("ka")
    g = lax.axis_index("ga")
    z, y = me // 2, me % 2
    fetch = pltpu.make_async_copy(w_hbm, wt, ws)
    lists = [
        pltpu.make_async_copy(pairs_hbm, pairs_ref, ks.at[3]),
        pltpu.make_async_copy(qs_hbm, qs_ref, ks.at[4]),
    ]
    for c in lists:
        c.start()
    weights = pltpu.make_async_copy(v_hbm, v_ref, ks.at[5])
    weights.start()
    fetch.start()
    mine = pl.ds(me * per_dev, per_dev)
    keeps = [
        pltpu.make_async_copy(x_ref, x_col.at[pl.ds(z * per_dev, per_dev)], ks.at[0]),
        pltpu.make_async_copy(p_ref, p_all.at[mine], ks.at[1]),
        pltpu.make_async_copy(y_ref, y_all.at[mine], ks.at[2]),
    ]
    for c in keeps:
        c.start()

    keep = pltpu.make_async_copy(row_ref.at[0], tab.at[me], ls)

    def table():
        for c in lists:
            c.wait()
        make_row(n, q_slots, per_dev, pairs_ref, qs_ref, row_ref, at_ref)
        keep.start()

    greet(n, table)
    xg = Pick(n, x_ref, x_col, x_out, x_got, tab, xs, xr, xps, xpr)
    yg = Gather(n, y_ref, y_all, ys, yr, per_dev - 1)
    pg = Hub(n, p_ref, p_all, ps, pr)
    outer = jnp.logical_not(pg.inner)

    rg = Rows(n, row_ref, tab, ts, tr, 1)
    rg.begin()
    xg.first()
    keep.wait()
    for c in keeps:
        c.wait()
    xg.pass_on(z)

    yg.across_early()

    @pl.when(outer)
    def _():
        pg.first()
        pg.cross(1).start()
        yg.first()

    @pl.when(pg.inner)
    def _():
        pg.cross(0).start()

    fetch.wait()
    turn = 16
    whole = width // turn * turn

    def relay(i, carry):
        at = pl.ds(pl.multiple_of(i * turn, turn), turn)
        w_ref[:, at] = jnp.swapaxes(wt[at], 0, 1)
        return carry

    lax.fori_loop(0, width // turn, relay, 0)
    if whole < width:
        w_ref[:, whole:] = jnp.swapaxes(wt[whole:], 0, 1)
    red = Reduce(part, half, recv1, tsend, recv2, s1, r1, s2, r2, 2 * CAPQ, True)

    def multiply(v, a, r):
        w = tab[a, slots + me * CAPQ + r]
        v = jnp.dot(v, w_ref[w], preferred_element_type=F32)
        for i in range(n_ga):
            part[i, a * CAPQ + r] = v[:, i * width : (i + 1) * width].astype(part.dtype)

    def piece(zz):
        for r in range(CAPQ):
            multiply(xg.chosen(zz, me, r), zz * 2 + y, r)
        rg.take_late(zz)
        xg.across(zz).wait_recv()
        for r in range(CAPQ):
            multiply(x_got[zz * CAPQ + r], zz * 2 + 1 - y, r)
        red.begin(zz)

    quarter = nt // n_ga
    weights.wait()
    weight = v_ref[...].reshape(1, width)
    sets = jnp.where(pg.edged, 4, 2)
    ered = Reduce(part3, eown, e1, et, e2, v1, w1, v2, w2, 4, False)

    def of(q):
        return jnp.where(q // 2 == 0, z, pg.edge) * 2 + q % 2

    def joined(both, out, at):
        v = jnp.concatenate(both, axis=1)
        for i in range(n_ga):
            out[i, at] = v[i * quarter : (i + 1) * quarter]

    def weigh(q, carry):
        for k in range(per_dev):
            weighted = p_all[of(q) * per_dev + k].astype(F32) * weight
            high = weighted.astype(BF16)
            split[q * per_dev + k, :nt] = high
            split[q * per_dev + k, nt:] = (weighted - high.astype(F32)).astype(BF16)
        return carry

    def exchange(zz):
        base = (zz * 2 + y) * per_dev

        def one(q, carry):
            a = of(q)
            both = []
            for r in range(CAPQ):
                at = 3 * slots + (zz * 2 + y) * CAPQ + r
                which = tab[a, at + slots] - base
                other = p_all[base]
                for k in range(1, per_dev):
                    other = jnp.where(which == k, p_all[base + k], other)
                v = lax.dot_general(
                    split[q * per_dev + tab[a, at]], other, DIMS, preferred_element_type=F32
                )
                both.append(v[:nt] + v[nt:])
            joined(both, part3, zz * 4 + q)
            return carry

        lax.fori_loop(0, sets, one, 0)
        ered.begin(zz)

    shape = own.shape[1:]
    left = lax.broadcasted_iota(I32, shape, 1) < nt
    doubles = per_dev // 2

    def paired(sums):
        sums = [v[:, :nt] + v[:, nt:] for v in sums]
        return [
            jnp.concatenate([sums[i], sums[i + doubles]], axis=1) for i in range(doubles)
        ]

    def to_first(q, zz):
        return remote(eown.at[zz, q], ein.at[y, zz], es, er.at[y], {"ka": of(q)})

    def to_second(zz):
        return remote(ebox.at[zz], emir.at[z], fs, fr.at[z], {"ka": zz * 2 + y})

    def deliver(zz):
        ered.end(zz)

        def give(q, carry):
            @pl.when(q != y)
            def _():
                to_first(q, zz).start()

            return carry

        lax.fori_loop(0, sets, give, 0)
        ein[y, zz] = eown[zz, y]

        def add(q, sums):
            at = 4 * slots + (zz * 2 + y) * CAPQ
            k2 = jnp.where(left, tab[of(q), at], tab[of(q), at + 1])
            v = eown[zz, q]
            base = (zz * 2 + y) * per_dev
            return tuple(t + jnp.where(k2 == base + i, v, 0.0) for i, t in enumerate(sums))

        sums = lax.fori_loop(0, sets, add, tuple(jnp.zeros(shape, F32) for _ in range(per_dev)))
        for i, v in enumerate(paired(sums)):
            ebox[zz, i] = v

        @pl.when(zz != z)
        def _():
            to_second(zz).start()

        @pl.when(zz == z)
        def _():
            emir[z] = ebox[z]

    rg.hop(1)
    xg.hop(1)

    @pl.when(pg.inner)
    def _():
        pg.first()

    xg.sides(1, lambda zz, way: xg.pass_on(zz))
    piece(z)

    def stage(h, carry):
        @pl.when(h < nz)
        def _():
            rg.hop(h)
            xg.hop(h)

        @pl.when(h == 2)
        def _():
            @pl.when(pg.inner)
            def _():
                yg.first()

            yg.second()

        @pl.when(h < nz)
        def _():
            xg.sides(h, lambda zz, way: xg.pass_on(zz))

        @pl.when(h == 2)
        def _():
            @pl.when(pg.inner)
            def _():
                pg.edge_in()

            @pl.when(outer)
            def _():
                pg.pass_inward()

            yg.across_late()

            red.middle(z)

        @pl.when(h > 2)
        def _():
            xg.sides(h - 2, lambda zz, way: red.middle(zz))

        xg.sides(h - 1, lambda zz, way: piece(zz))

        @pl.when(jnp.logical_and(h >= 3, h < nz))
        def _():
            yg.hop(h - 2)

        return carry

    lax.fori_loop(2, nz + 1, stage, 0)

    @pl.when(pg.inner)
    def _():
        pg.hop(1)
        pg.crossed(z, 0)

        @pl.when(pg.edged)
        def _():
            pg.crossed(pg.edge, 1)

        lax.fori_loop(0, sets, weigh, 0)
        exchange(z)

    xg.sides(nz - 1, lambda zz, way: red.middle(zz))
    half_way = per_dev // 2
    yg.hop(nz - 2, 0, half_way)

    @pl.when(pg.inner)
    def _():
        pg.sides(1, lambda zz, way: exchange(zz))

    yg.hop(nz - 2, half_way)

    @pl.when(pg.inner)
    def _():
        ered.middle(z)
        pg.sides(1, lambda zz, way: ered.middle(zz))

    @pl.when(pg.inner)
    def _():
        def level(h, carry):
            pg.hop(h)
            pg.sides(h, lambda zz, way: exchange(zz))
            return carry

        lax.fori_loop(2, nz, level, 0)

    pg.finish()
    yg.hop(nz - 1)

    red.arrive()
    lax.fori_loop(0, nz, lambda i, c: (red.end(i), c)[1], 0)
    yg.finish()

    def source(a, carry):
        both = []
        for r in range(CAPQ):
            k2 = jnp.maximum(tab[a, 2 * slots + me * CAPQ + r], 0)
            both.append(
                lax.dot_general(half[a * CAPQ + r], y_all[k2], DIMS, preferred_element_type=F32)
            )
        joined(both, part2, a)
        return carry

    end = Reduce(part2, own, q1, qt, q2, t1, u1, t2, u2, n // 4, False)
    for i in range(4):
        lax.fori_loop(i * n // 4, (i + 1) * n // 4, source, 0, unroll=2)
        end.begin(i)
    def seconds(a, carry):
        at = 2 * slots + me * CAPQ
        second[a] = jnp.where(left, tab[a, at], tab[a, at + 1])
        return carry

    lax.fori_loop(0, n, seconds, 0)

    @pl.when(pg.inner)
    def _():
        def level(h, carry):
            pg.sides(h, lambda zz, way: ered.middle(zz))
            return carry

        lax.fori_loop(2, nz, level, 0)

    for i in range(4):
        end.middle(i)

    @pl.when(pg.inner)
    def _():
        deliver(z)

        def level(h, carry):
            pg.sides(h, lambda zz, way: deliver(zz))
            return carry

        lax.fori_loop(1, nz, level, 0)


    def cross(src, box, i, whose, ss, rs):
        return remote(src.at[i], box.at[whose], ss, rs, {"ka": i})

    def far_first(i):
        return jnp.where(z < nz // 2, n - 1 - i, i)

    for i in range(4):
        end.end(i)

    def give(i, carry):
        b = far_first(i)

        @pl.when(b != me)
        def _():
            cross(own, inbox, b, me, as_, ar).start()

        return carry

    lax.fori_loop(0, n, give, 0)
    inbox[me] = own[me]


    def fill(i, carry):
        b = far_first(i)

        def add(a, sums):
            out = []
            for i in range(per_dev):
                out.append(sums[i] + jnp.where(second[a] == b * per_dev + i, own[a], 0.0))
            return tuple(out)

        sums = tuple(jnp.zeros(shape, F32) for _ in range(per_dev))
        sums = lax.fori_loop(0, n, add, sums, unroll=min(n, 8))
        for i_, v in enumerate(paired(sums)):
            outbox[b, i_] = v

        @pl.when(b != me)
        def _():
            cross(outbox, sumbox, b, me, bs, br).start()

        return carry

    lax.fori_loop(0, n, fill, 0)
    sumbox[me] = outbox[me]
    for yy in range(2):

        @pl.when(jnp.logical_or(jnp.logical_not(pg.inner), yy != y))
        def _(yy=yy):
            remote(ein.at[yy], ein.at[yy], es, er.at[yy], {"ka": z * 2 + 1 - y}).wait_recv()

    def inner_level(zz, carry):
        @pl.when(zz != z)
        def _():
            remote(
                emir.at[zz], emir.at[zz], fs, fr.at[zz], {"ka": z * 2 + 1 - y}
            ).wait_recv()

        return carry

    lax.fori_loop(1, nz - 1, inner_level, 0)
    def arrived(box, rs):
        rest = box.at[pl.ds(0, n - 1)]
        remote(rest, rest, rs, rs, {"ka": z * 2 + 1 - y}).wait_recv()

    arrived(inbox, ar)
    sub = quarter // 2

    def picked(ref, at, r):
        even = ref[at + (pl.ds(0, sub, stride=2),)]
        odd = ref[at + (pl.ds(1, sub, stride=2),)]
        zero = jnp.concatenate([even[:, :nt], odd[:, :nt]], axis=1)
        one = jnp.concatenate([even[:, nt:], odd[:, nt:]], axis=1)
        return jnp.where(r == 0, zero, one)

    for j in range(rows):
        at, et_ = at_ref[0, j], at_ref[1, j]
        b = et_ // CAPQ
        direct = picked(inbox, (at // CAPQ,), at % CAPQ)
        term = picked(ein, (b % 2, b // 2), et_ % CAPQ)
        lines[g, pl.ds(j * sub, sub)] = 2.0 * term - direct
    base = rows * sub
    x, c = g // 2, g % 2
    mate, far = x * 2 + 1 - c, (1 - x) * 2 + c
    parts = (pl.ds(0, base // 2), pl.ds(base, doubles * quarter), pl.ds(base // 2, base // 2))

    def spread(i, m, whose, to):
        block = lines.at[whose, parts[m]]
        return remote(block, block, gs, gr.at[m if i == 0 else 3], {"ga": to})

    diag = (1 - x) * 2 + 1 - c
    spread(0, 0, g, far).start()
    spread(0, 2, g, far).start()
    spread(2, 2, g, diag).start()
    spread(1, 0, g, mate).start()
    spread(1, 2, g, mate).start()
    xg.finish()
    rg.finish()
    red.finish()
    end.finish()
    arrived(sumbox, br)
    for i in range(doubles):
        total = lax.fori_loop(
            1, n, lambda o, t, i=i: t + sumbox[o, i], sumbox[0, i]
        )
        term = lax.fori_loop(
            2, nz - 1, lambda zz, t, i=i: t + emir[zz, i], emir[1, i]
        )
        lines[g, pl.ds(base + i * quarter, quarter)] = 2.0 * term - total
    spread(0, 1, g, far).start()
    spread(2, 1, g, diag).start()
    spread(1, 1, g, mate).start()
    spread(0, 0, far, far).wait_recv()
    spread(2, 0, far, mate).start()
    spread(0, 2, far, far).wait_recv()
    spread(0, 1, far, far).wait_recv()
    for src, ss in ((own, as_), (outbox, bs)):
        rest = src.at[pl.ds(0, n - 1)]
        remote(rest, rest, ss, ss, {"ka": z * 2 + 1 - y}).wait_send()
    @pl.when(pg.inner)
    def _():
        ered.finish()
        for edged, count in ((True, 3), (False, 1)):

            @pl.when(pg.edged if edged else jnp.logical_not(pg.edged))
            def _(count=count):
                sent_lines = eown.at[:, pl.ds(0, count)]
                remote(sent_lines, sent_lines, es, es, {"ka": z * 2 + 1 - y}).wait_send()

        rest = ebox.at[pl.ds(0, nz - 1)]
        remote(rest, rest, fs, fs, {"ka": z * 2 + 1 - y}).wait_send()

    for count, ss, rs in ((3, gs, None), (2, None, gr.at[3])):
        block = lines.at[pl.ds(0, count)]
        if rs is None:
            remote(block, block, ss, ss, {"ga": mate}).wait_send()
        else:
            remote(block, block, rs, rs, {"ga": mate}).wait_recv()


def layout(lines, blocks_ref, mirr_ref, turned, flat):
    n_ga = lines.shape[0]
    rows, per_dev = blocks_ref.shape[0], mirr_ref.shape[0]
    nt = turned.shape[1]
    quarter, sub, doubles = nt // n_ga, nt // n_ga // 2, per_dev // 2
    base = rows * sub
    lanes = 2 * nt
    for q in range(n_ga):
        for t in range(sub):
            blocks_ref[:, (q * sub + t) * lanes : (q * sub + t + 1) * lanes] = lines[
                q, pl.ds(t, rows, stride=sub)
            ]
    for i in range(doubles):
        whole = jnp.concatenate(
            [lines[q, pl.ds(base + i * quarter, quarter)] for q in range(n_ga)], axis=0
        )
        turned[...] = whole.T
        even = turned[pl.ds(0, nt, stride=2)]
        odd = turned[pl.ds(1, nt, stride=2)]
        both = jnp.concatenate([even, odd], axis=1)
        flat[pl.ds(i * nt // 2, nt // 2)] = both[: nt // 2]
        flat[pl.ds((i + doubles) * nt // 2, nt // 2)] = both[nt // 2 :]
    for t in range(nt // 2):
        mirr_ref[:, t * lanes : (t + 1) * lanes] = flat[pl.ds(t, per_dev, stride=nt // 2)]


def per_device(x_dens, y_dens, p_dens, coulomb, screened, pairs, q_slot):
    n = lax.axis_size("ka")
    n_ga = lax.axis_size("ga")
    per_dev, nt, g = x_dens.shape
    q_slots = screened.shape[0]
    rows = pairs.shape[0]
    slots = n * CAPQ
    nz = n // 2
    shape = jax.ShapeDtypeStruct
    wide = F32 if slots * nt <= 2048 else BF16
    quarter = nt // n_ga
    each = (quarter, CAPQ * nt)
    line = (n,) + each
    dma = lambda m: pltpu.SemaphoreType.DMA((m,))
    one = pltpu.SemaphoreType.DMA
    row_len = -(-5 * slots // 128) * 128
    k_all = n * per_dev
    lines = pl.pallas_call(
        functools.partial(kernel, n),
        out_shape=shape((n_ga, rows * quarter // 2 + per_dev // 2 * quarter, CAPQ * nt), F32),
        in_specs=[HB] * 7,
        out_specs=VM,
        scratch_shapes=[
            pltpu.SMEM((pairs.shape[1], rows), I32),
            pltpu.SMEM(q_slot.shape, I32),
            pltpu.VMEM((g,), F32),
            pltpu.SMEM((n, row_len), I32),
            pltpu.SMEM((2, rows), I32),
            pltpu.VMEM((1, row_len), I32),
            pltpu.VMEM((g, q_slots, screened.shape[2]), BF16),
            pltpu.VMEM((q_slots, g, screened.shape[2]), BF16),
            pltpu.VMEM((nz * per_dev, nt, g), BF16),
            pltpu.VMEM((nz * CAPQ, nt, g), BF16),
            pltpu.VMEM((nz * CAPQ, nt, g), BF16),
            pltpu.VMEM((k_all, nt, g), BF16),
            pltpu.VMEM((k_all, nt, g), BF16),
            pltpu.VMEM((n_ga, slots, nt, g), wide),
            pltpu.VMEM((slots, nt, g), BF16),
            pltpu.VMEM((2, slots, nt, g), wide),
            pltpu.VMEM((slots, nt, g), BF16),
            pltpu.VMEM((slots, nt, g), BF16),
            pltpu.VMEM((n_ga,) + line, F32),
            pltpu.VMEM(line, F32),
            pltpu.VMEM((2,) + line, F32),
            pltpu.VMEM(line, F32),
            pltpu.VMEM(line, F32),
            pltpu.VMEM(line, I32),
            pltpu.VMEM((n, per_dev // 2) + each, F32),
            pltpu.VMEM((n, per_dev // 2) + each, F32),
            pltpu.VMEM(line, F32),
            pltpu.VMEM((4 * per_dev, 2 * nt, g), BF16),
            pltpu.VMEM((n_ga, 4 * nz) + each, F32),
            pltpu.VMEM((nz, 4) + each, F32),
            pltpu.VMEM((2, 4 * nz) + each, F32),
            pltpu.VMEM((4 * nz,) + each, F32),
            pltpu.VMEM((4 * nz,) + each, F32),
            pltpu.VMEM((nz, per_dev // 2) + each, F32),
            pltpu.VMEM((2, nz) + each, F32),
            pltpu.VMEM((nz, per_dev // 2) + each, F32),
            one, one, dma(6),
            dma(3 * nz), dma(2 * nz),
            dma(2 * nz), dma(nz * per_dev),
            dma(nz), dma(nz),
            dma(3 * nz), dma(nz * (per_dev + 2)),
            dma(2 * nz + 3), dma(nz * per_dev + 2),
            one, dma(nz + 1), one, dma(1),
            one, dma(8), one, dma(4),
            one, dma(2 * nz), one, dma(nz),
            one, dma(2), one, dma(nz),
            one, one, one, one,
            one, dma(4),
        ],
        compiler_params=pltpu.CompilerParams(
            collective_id=0, has_side_effects=True, vmem_limit_bytes=LIMIT
        ),
        name="window",
    )(pairs.T, q_slot, x_dens, y_dens, p_dens, coulomb, screened.transpose(1, 0, 2))
    blocks, mirrored = pl.pallas_call(
        layout,
        out_shape=[shape((rows, nt * nt), F32), shape((per_dev, nt * nt), F32)],
        in_specs=[VM],
        out_specs=[VM, VM],
        scratch_shapes=[
            pltpu.VMEM((2 * nt, nt), F32),
            pltpu.VMEM((per_dev * nt // 2, 2 * nt), F32),
        ],
        name="layout",
    )(lines)
    return (blocks, mirrored)


def solution(mesh):
    in_specs = (
        P("ka", None, "ga"),
        P("ka", None, "ga"),
        P("ka", None, "ga"),
        P("ga"),
        P("ka", "ga", None),
        P("ka", None),
        P(),
    )
    out_specs = (P("ka", None), P("ka", None))
    return jax.shard_map(
        per_device, mesh=mesh, in_specs=in_specs, out_specs=out_specs, check_vma=False
    )
```
